128 devices in a mesh: dom: 128 (over y, z, x, core).
Axes of the slice: x: 4, y: 4, z: 4, core: 2. Of those that a mesh axis runs over, the one named last changes fastest.
Arguments:
- right_side: float32 [131072, 3], P('dom'), may hold values from -10 to 10
- fine_diagonal: float32 [131072, 3], P('dom'), may hold values from 2 to 4
- fine_columns: int32 [131072, 27], P('dom'), may hold values from 0 to 131071, as said below
- fine_blocks: float32 [131072, 27, 3, 3], P('dom'), may hold values from -0.625 to 0.625
- aggregate_of_node: int32 [131072], P('dom'), may hold values from 0 to 31, as said below
- coarse_row_of_aggregate: int32 [4096], P('dom'), may hold values from 0 to 4095, as said below
- coarse_diagonal: float32 [4096, 3], P('dom'), may hold values from 2 to 4
- coarse_columns: int32 [4096, 27], P('dom'), may hold values from 0 to 4095
- coarse_blocks: float32 [4096, 27, 3, 3], P('dom'), may hold values from -0.625 to 0.625
Outputs:
- solution: float32 [131072, 3], P('dom')
- correction: float32 [4096, 3], P('dom')
The draws below stay inside these ranges and needn't reach their ends.
Inputs may be any that keep to these rules, and one draw needn't show every extreme that they name: Every entry of fine_columns differs from its row number by at most 256, and some entry by exactly 256. `aggregate_of_node`: on each device every aggregate number 0 to 31 is used by at least one of its nodes. coarse_row_of_aggregate is a permutation of 0 to 4095; among the 32 aggregates of one device (an aligned block of entries) at most 8 get rows of any one owner, and exactly 8 for some owner.
All inputs are finite; a program needn't handle non-finite values.
Results may differ from the reference program's by a relative error of at most 0.0003.
Values sent between devices are 32-bit elements.
No kernel may reach another device: no remote copies, remote signals or barrier semaphores. Data moves between devices by JAX's collectives and lax.ppermute only.
A program may use at most 64 MiB of HBM per device.

```python
import jax
import jax.numpy as jnp
from jax import lax

NODE_DEV = 1024
CAP = 8
WIN = 256
NNZ = 27
CNNZ = 27
SWEEPS = 2
CSWEEPS = 6
AGG_DEV = 32
NODES = 131072
AGGS = 4096


def draw_fine_columns(key, part):
    row_ids = jnp.arange(NODES, dtype=jnp.int32)[:, None]
    offset = jax.random.randint(jax.random.fold_in(key, 13), (NODES, NNZ), -WIN, WIN + 1)
    columns = jnp.clip(row_ids + offset, 0, NODES - 1)
    return columns.at[0, 0].set(WIN).astype(jnp.int32)


def draw_aggregate_of_node(key, part):
    devices = NODES // NODE_DEV
    key_raw, key_mix = jax.random.split(jax.random.fold_in(key, 11))
    labels_raw = jax.random.randint(key_raw, (devices, NODE_DEV), 0, AGG_DEV)
    labels_raw = labels_raw.at[:, :AGG_DEV].set(jnp.arange(AGG_DEV, dtype=jnp.int32)[None, :])
    mixers = jax.random.split(key_mix, devices)
    shuffles = jax.vmap(lambda one_key: jax.random.permutation(one_key, NODE_DEV))(mixers)
    return jnp.take_along_axis(labels_raw, shuffles, axis=1).reshape(-1).astype(jnp.int32)


def draw_coarse_row_of_aggregate(key, part):
    devices = AGGS // AGG_DEV
    groups = AGG_DEV // CAP
    key_group, key_slot, key_label = jax.random.split(jax.random.fold_in(key, 17), 3)
    scores = jax.random.permutation(key_group, devices).astype(jnp.int32)
    scores = scores.at[devices // 2].set(-3).at[1].set(-2).at[devices - 1].set(-1)
    offsets = jnp.argsort(scores, stable=True)[:groups].astype(jnp.int32)
    sources = jnp.arange(devices, dtype=jnp.int32)[:, None]
    label_mix = jax.vmap(lambda one_key: jax.random.permutation(one_key, AGG_DEV))(jax.random.split(key_label, devices)).astype(jnp.int32)
    group_ids = label_mix // CAP
    owners = (sources + offsets[group_ids]) % devices
    within = group_ids * CAP + label_mix % CAP
    slot_mix = jax.vmap(lambda one_key: jax.random.permutation(one_key, AGG_DEV))(jax.random.split(key_slot, devices)).astype(jnp.int32)
    slots = slot_mix[owners, within]
    return (owners * AGG_DEV + slots).reshape(-1).astype(jnp.int32)


def with_ends(drawn, own_key, low, high):
    spot = [jax.random.randint(jax.random.fold_in(own_key, axis), (), 0, length) for axis, length in enumerate(drawn.shape)]
    main_axis = drawn.shape.index(max(drawn.shape))
    neighbour = spot[:main_axis] + [(spot[main_axis] + 1) % drawn.shape[main_axis]] + spot[main_axis + 1:]
    return drawn.at[tuple(spot)].set(low).at[tuple(neighbour)].set(high)


def level_of(own_key, extent, cuts, low, high):
    loudness, own = 1.0, jax.random.fold_in(own_key, 6)
    for dim, blocks in cuts:
        draws = jnp.exp(jax.random.uniform(jax.random.fold_in(own, dim), (blocks,), jnp.float32, low / len(cuts), high / len(cuts)))
        loudness = loudness * jnp.repeat(draws, extent[dim] // blocks).reshape([-1 if axis == dim else 1 for axis in range(len(extent))])
    return loudness


def bell_draw(key, shape, scale, reach, cuts=(), kind=jnp.bfloat16):
    gain = level_of(key, shape, cuts, -0.22, 0.18) if cuts else 1.0
    values = jax.random.normal(key, shape, jnp.float32) * scale * gain
    return jnp.minimum(jnp.maximum(values, -reach), reach).astype(kind)


def setup_inputs(seed: int = 0) -> dict:
    seeds = jax.random.split(jax.random.key(seed), 10)
    return {
        "right_side": bell_draw(seeds[0], (NODES, 3), 2.0, 10.0, ((0, 128),), jnp.float32),
        "fine_diagonal": jnp.clip(2.0 + 2.0 * jax.random.uniform(seeds[1], (NODES, 3), jnp.float32) ** level_of(seeds[1], (NODES, 3), ((0, 128),), -0.2, 0.2), 2.0, 4.0),
        "fine_columns": draw_fine_columns(jax.random.fold_in(seeds[9], 71), 0),
        "fine_blocks": bell_draw(seeds[3], (NODES, NNZ, 3, 3), (3 * NNZ) ** -0.5, 0.625, ((0, 128),), jnp.float32),
        "aggregate_of_node": draw_aggregate_of_node(jax.random.fold_in(seeds[9], 71), 0),
        "coarse_row_of_aggregate": draw_coarse_row_of_aggregate(jax.random.fold_in(seeds[9], 71), 0),
        "coarse_diagonal": jnp.clip(2.0 + 2.0 * jax.random.uniform(seeds[6], (AGGS, 3), jnp.float32) ** level_of(seeds[6], (AGGS, 3), ((0, 128),), -0.2, 0.2), 2.0, 4.0),
        "coarse_columns": with_ends(jax.random.randint(seeds[7], (AGGS, CNNZ), 0, AGGS), jax.random.fold_in(seeds[7], 1), 0, AGGS - 1).astype(jnp.int32),
        "coarse_blocks": bell_draw(seeds[8], (AGGS, CNNZ, 3, 3), (3 * CNNZ) ** -0.5, 0.625, ((0, 128),), jnp.float32),
    }


damping = 0.7


def apply_level(field, diagonal, columns, blocks):
    nearby = field[columns]
    pulled = jnp.einsum("rkij,rkj->ri", blocks, nearby, precision=lax.Precision.HIGHEST)
    return diagonal * field - pulled


def reference(right_side, fine_diagonal, fine_columns, fine_blocks, aggregate_of_node, coarse_row_of_aggregate, coarse_diagonal, coarse_columns, coarse_blocks):
    solution = jnp.zeros_like(right_side)
    for sweep in range(SWEEPS):
        solution = solution + damping * (right_side - apply_level(solution, fine_diagonal, fine_columns, fine_blocks)) / fine_diagonal
    residual = right_side - apply_level(solution, fine_diagonal, fine_columns, fine_blocks)
    node_ids = jnp.arange(NODES, dtype=jnp.int32)
    labels = (node_ids // NODE_DEV) * AGG_DEV + aggregate_of_node
    coarse_rows = coarse_row_of_aggregate[labels]
    coarse_rhs = jax.ops.segment_sum(residual, coarse_rows, num_segments=AGGS)
    correction = jnp.zeros_like(coarse_rhs)
    for sweep in range(CSWEEPS):
        correction = correction + damping * (coarse_rhs - apply_level(correction, coarse_diagonal, coarse_columns, coarse_blocks)) / coarse_diagonal
    solution = solution + correction[coarse_rows]
    for sweep in range(SWEEPS):
        solution = solution + damping * (right_side - apply_level(solution, fine_diagonal, fine_columns, fine_blocks)) / fine_diagonal
    return solution, correction
```

```python
import jax
import jax.numpy as jnp
from jax import lax
from jax.experimental import pallas as pl
from jax.experimental.pallas import tpu as pltpu
from jax.sharding import Mesh
from jax.sharding import PartitionSpec as P

DOM = ("dom_0", "dom_1", "dom_2", "dom_3")
SWEEPS = 2
CSWEEPS = 6
damping = 0.7
highest = lax.Precision.HIGHEST

ROWS = 1024
LANES = 128
SLOTS = 27
FULL = 24
HALO = 256
WIDE = 512
BLOCKS = ROWS // LANES
P_COL = 9 * FULL
P_BTAIL = P_COL + FULL
P_CTAIL = P_BTAIL + 27
P_RHS = P_CTAIL + 3
P_DIA = P_RHS + 6
P_ROW = P_DIA + 6
P_ALL = 288
f32 = jnp.float32
i32 = jnp.int32


def lanes(start, size=LANES):
    if isinstance(start, int):
        return slice(start, start + size)
    return pl.ds(pl.multiple_of(start, LANES), size)


def picked(row, where):
    return jnp.take_along_axis(
        jnp.broadcast_to(row, where.shape), where, axis=1, mode="promise_in_bounds"
    )


def pack_kernel(rhs, dia, col, blk, agg, owner_row, up, down, node_row):
    table = owner_row[...]
    found = picked(table, agg[...]).astype(f32)
    node_row[...] = found
    for out, near, wide in ((up, ROWS - HALO, ROWS - WIDE), (down, 0, 0)):
        for i in range(3):
            for j in range(3):
                g = 3 * i + j
                out[g * FULL : (g + 1) * FULL, :] = blk[i, j, 0:FULL, lanes(near, HALO)]
                out[P_BTAIL + 3 * g : P_BTAIL + 3 * g + 3, :] = blk[
                    i, j, FULL:SLOTS, lanes(near, HALO)
                ]
        out[P_COL : P_COL + FULL, :] = col[0:FULL, lanes(near, HALO)].astype(f32)
        out[P_CTAIL : P_CTAIL + 3, :] = col[FULL:SLOTS, lanes(near, HALO)].astype(f32)
        for h in range(2):
            out[P_RHS + 3 * h : P_RHS + 3 * h + 3, :] = rhs[:, lanes(wide + HALO * h, HALO)]
            out[P_DIA + 3 * h : P_DIA + 3 * h + 3, :] = dia[:, lanes(wide + HALO * h, HALO)]
            for q in range(2):
                s = wide // LANES + 2 * h + q
                out[P_ROW + h : P_ROW + h + 1, lanes(LANES * q)] = found[s : s + 1, :]
        out[P_ROW + 2 : P_ALL, :] = jnp.zeros((P_ALL - P_ROW - 2, HALO), f32)


def pulled_block(columns, blocks, table, first_chunk):
    total = [None, None, None]
    for part in range(4):
        where = columns(part)
        chunk = lax.shift_right_arithmetic(where, 7)
        lane = lax.bitwise_and(where, 127)
        near = [jnp.zeros(where.shape, f32) for _ in range(3)]
        for c in range(5):
            here = chunk == c
            for j in range(3):
                row = table[j : j + 1, lanes(first_chunk * LANES + c * LANES)]
                near[j] = jnp.where(here, picked(row, lane), near[j])
        for i in range(3):
            s = blocks(i, 0, part) * near[0]
            s = s + blocks(i, 1, part) * near[1]
            s = s + blocks(i, 2, part) * near[2]
            if part < 3:
                total[i] = s if total[i] is None else total[i] + s
            else:
                total[i] = jnp.sum(total[i], axis=0, keepdims=True) + jnp.sum(
                    s, axis=0, keepdims=True
                )
    return total


def local_getters(col, blk, start, b):
    def columns(part):
        lo, hi = 8 * part, min(8 * part + 8, SLOTS)
        return col[lo:hi, lanes(b * LANES)] - start

    def blocks(i, j, part):
        lo, hi = 8 * part, min(8 * part + 8, SLOTS)
        return blk[i, j, lo:hi, lanes(b * LANES)]

    return columns, blocks


def halo_getters(halo, start, b):
    def columns(part):
        if part < 3:
            got = halo[P_COL + 8 * part : P_COL + 8 * part + 8, lanes(b * LANES)]
        else:
            got = halo[P_CTAIL : P_CTAIL + 3, lanes(b * LANES)]
        return got.astype(i32) - start

    def blocks(i, j, part):
        g = 3 * i + j
        if part < 3:
            return halo[g * FULL + 8 * part : g * FULL + 8 * part + 8, lanes(b * LANES)]
        return halo[P_BTAIL + 3 * g : P_BTAIL + 3 * g + 3, lanes(b * LANES)]

    return columns, blocks


def wide_vector(out, local, before, after, row):
    out[:, lanes(WIDE, ROWS)] = local[...]
    for h in range(2):
        out[:, lanes(HALO * h, HALO)] = before[row + 3 * h : row + 3 * h + 3, :]
        out[:, lanes(WIDE + ROWS + HALO * h, HALO)] = after[row + 3 * h : row + 3 * h + 3, :]


def smoothed(table, pulled, rhs, dia, at):
    pull = jnp.concatenate(pulled, axis=0)
    s = table[:, lanes(at)]
    b = rhs[:, lanes(at)]
    d = dia[:, lanes(at)]
    return s + damping * (b - (d * s - pull)) / d


def sweep_halo(out, table, rhs, dia, halo, base, first):
    for b in range(2):
        at = first + LANES * b
        start = base + (at - WIDE) - 2 * LANES
        cols, blks = halo_getters(halo, start, b)
        pull = pulled_block(cols, blks, table, at // LANES - 2)
        out[:, lanes(at)] = smoothed(table, pull, rhs, dia, at)


def own_block(table, col, blk, base, b):
    start = base + b * LANES - 2 * LANES
    cols, blks = local_getters(col, blk, start, b)
    return pulled_block(cols, blks, table, b + WIDE // LANES - 2)


def pre_kernel(base_ref, rhs, dia, col, blk, agg, owner_row, before, after,
               send, first_iter, keep_rhs, keep_dia, up2, down2, one, two, res):
    base = base_ref[0]
    wide_vector(keep_rhs, rhs, before, after, P_RHS)
    wide_vector(keep_dia, dia, before, after, P_DIA)
    raw = keep_dia[...]
    keep_dia[...] = jnp.where(raw == 0.0, 1.0, raw)
    one[...] = damping * keep_rhs[...] / keep_dia[...]
    two[...] = jnp.zeros(two.shape, f32)
    sweep_halo(two, one, keep_rhs, keep_dia, before, base, WIDE - HALO)
    sweep_halo(two, one, keep_rhs, keep_dia, after, base, WIDE + ROWS)

    def second(b, carry):
        at = WIDE + b * LANES
        pull = own_block(one, col, blk, base, b)
        two[:, lanes(at)] = smoothed(one, pull, keep_rhs, keep_dia, at)
        return carry

    lax.fori_loop(0, BLOCKS, second, 0)

    def third(b, carry):
        at = WIDE + b * LANES
        pull = jnp.concatenate(own_block(two, col, blk, base, b), axis=0)
        s, d = two[:, lanes(at)], keep_dia[:, lanes(at)]
        res[0:3, lanes(b * LANES)] = keep_rhs[:, lanes(at)] - (d * s - pull)
        return carry

    res[...] = jnp.zeros(res.shape, f32)
    lax.fori_loop(0, BLOCKS, third, 0)
    first_iter[...] = two[...]
    up2[...] = two[:, lanes(WIDE + ROWS - WIDE, HALO)]
    down2[...] = two[:, lanes(WIDE + HALO, HALO)]
    label = lax.broadcasted_iota(i32, (32, LANES), 0)
    sums = None
    for b in range(BLOCKS):
        member = (label == jnp.broadcast_to(agg[b : b + 1, :], (32, LANES))).astype(f32)
        part = lax.dot_general(
            res[:, lanes(b * LANES)], member, (((1,), (1,)), ((), ())),
            precision=highest, preferred_element_type=f32,
        )
        sums = part if sums is None else sums + part
    row = jnp.concatenate(
        [sums[0:1], sums[1:2], sums[2:3], owner_row[0:1, 0:32].astype(f32)], axis=1
    )
    send[...] = jnp.broadcast_to(row, (LANES, LANES))


def spread(parts):
    group = lax.shift_right_logical(lax.broadcasted_iota(i32, (1, LANES), 1), 5)
    return jnp.where(group == 0, parts[0], jnp.where(group == 1, parts[1], parts[2]))


def coarse_setup_kernel(me_ref, sums, dia, col, blk, send, keep_rhs, keep_dia, where, weights):
    me = me_ref[0]
    got = sums[...]
    group = lax.shift_right_logical(lax.broadcasted_iota(i32, (LANES, LANES), 1), 5)
    rows = jnp.where(group == 3, got, 0.0)
    rows = rows + pltpu.roll(rows, 64, axis=1)
    rows = rows + pltpu.roll(rows, 32, axis=1)
    rows = rows.astype(i32) - me * 32
    lines = []
    for r in range(32):
        lines.append(jnp.sum(jnp.where(rows == r, got, 0.0), axis=0, keepdims=True))
    lines = jnp.concatenate(lines, axis=0)
    pick = lax.broadcasted_iota(i32, (8, LANES), 0) == lax.shift_right_logical(
        lax.broadcasted_iota(i32, (8, LANES), 1), 5
    )
    mine = lax.dot_general(
        pick.astype(f32), lines, (((1,), (1,)), ((), ())),
        precision=highest, preferred_element_type=f32,
    )
    pad = jnp.zeros((1, 32), f32)
    rhs = jnp.concatenate([mine[0:1], mine[1:2], mine[2:3], pad], axis=1)
    d = jnp.concatenate([dia[0:1, :], dia[1:2, :], dia[2:3, :], pad + 1.0], axis=1)
    keep_rhs[...] = rhs
    keep_dia[...] = d
    send[...] = jnp.broadcast_to(damping * rhs / d, (LANES, LANES))

    def folded(a):
        z = jnp.concatenate([a, jnp.zeros((32, 5), f32)], axis=1)
        z = jnp.transpose(z)
        return jnp.concatenate([z[8 * k : 8 * k + 8, :] for k in range(4)], axis=1)

    where[...] = folded(col[...].astype(f32)).astype(i32)
    for i in range(3):
        for j in range(3):
            weights[3 * i + j] = folded(blk[i, j])


def coarse_lookup(table, column, shape):
    chunk = lax.bitwise_and(column, 31)
    lane = lax.shift_right_logical(column, 5)
    near = [jnp.zeros(shape, f32) for _ in range(3)]
    for c in range(32):
        here = chunk == c
        for j in range(3):
            row = table[32 * j + c : 32 * j + c + 1, :]
            near[j] = jnp.where(here, picked(row, lane), near[j])
    return near


def coarse_kernel(got, own, rhs, dia, where, weights, send, mine, table):
    table[...] = jnp.transpose(got[...])
    near = coarse_lookup(table, where[...], (8, LANES))
    parts = []
    for i in range(3):
        s = weights[3 * i] * near[0] + weights[3 * i + 1] * near[1] + weights[3 * i + 2] * near[2]
        s = jnp.sum(s, axis=0, keepdims=True)
        s = s + pltpu.roll(s, 64, axis=1)
        parts.append(s + pltpu.roll(s, 32, axis=1))
    c, d = own[0:1, :], dia[...]
    new = c + damping * (rhs[...] - (d * c - spread(parts))) / d
    send[...] = jnp.broadcast_to(new, (LANES, LANES))
    mine[...] = jnp.concatenate([new[:, 32 * i : 32 * i + 32] for i in range(3)], axis=0)


def post_kernel(base_ref, got, first_iter, rhs, dia, col, blk, node_row, before, after,
                before2, after2, out, table, one, two):
    base = base_ref[0]
    table[...] = jnp.transpose(got[...])
    one[...] = first_iter[...]
    one[:, lanes(0, HALO)] = before2[...]
    one[:, lanes(WIDE + ROWS + HALO, HALO)] = after2[...]
    edge = [
        h[P_ROW + t : P_ROW + t + 1, lanes(LANES * q)]
        for h in (before, after) for t in range(2) for q in range(2)
    ]
    edge = jnp.concatenate(edge, axis=0)
    own = coarse_lookup(table, node_row[...].astype(i32), (8, LANES))
    far = coarse_lookup(table, edge.astype(i32), (8, LANES))
    for s in range(16):
        if s < 4:
            row = [f[s : s + 1, :] for f in far]
        elif s < 12:
            row = [f[s - 4 : s - 3, :] for f in own]
        else:
            row = [f[s - 8 : s - 7, :] for f in far]
        one[:, lanes(s * LANES)] = one[:, lanes(s * LANES)] + jnp.concatenate(row, axis=0)
    two[...] = jnp.zeros(two.shape, f32)
    sweep_halo(two, one, rhs, dia, before, base, WIDE - HALO)
    sweep_halo(two, one, rhs, dia, after, base, WIDE + ROWS)

    def first(b, carry):
        at = WIDE + b * LANES
        pull = own_block(one, col, blk, base, b)
        two[:, lanes(at)] = smoothed(one, pull, rhs, dia, at)
        return carry

    def second(b, carry):
        at = WIDE + b * LANES
        pull = own_block(two, col, blk, base, b)
        out[:, lanes(b * LANES)] = smoothed(two, pull, rhs, dia, at)
        return carry

    lax.fori_loop(0, BLOCKS, first, 0)
    lax.fori_loop(0, BLOCKS, second, 0)


def call(kernel, name, outs, args, scratch=(), scalar=False):
    vmem = pl.BlockSpec(memory_space=pltpu.VMEM)
    specs = [vmem] * len(args)
    if scalar:
        specs[0] = pl.BlockSpec(memory_space=pltpu.SMEM)
    return pl.pallas_call(
        kernel,
        name=name,
        in_specs=specs,
        out_specs=[vmem] * len(outs),
        out_shape=[jax.ShapeDtypeStruct(o, t) for o, t in outs],
        scratch_shapes=[pltpu.VMEM(s, f32) for s in scratch],
    )(*args)


def everywhere(row):
    return lax.all_to_all(row, DOM, 0, 0, tiled=True)


def shifts(up, down):
    count = lax.axis_size(DOM)
    forward = [(i, i + 1) for i in range(count - 1)]
    backward = [(i + 1, i) for i in range(count - 1)]
    return lax.ppermute(up, DOM, forward), lax.ppermute(down, DOM, backward)


def body(right_side, fine_diagonal, fine_columns, fine_blocks, aggregate_of_node,
         coarse_row_of_aggregate, coarse_diagonal, coarse_columns, coarse_blocks):
    rhs, dia = right_side.T, fine_diagonal.T
    col, blk = fine_columns.T, fine_blocks.transpose(2, 3, 1, 0)
    agg = aggregate_of_node.reshape(8, LANES)
    owner = jnp.pad(coarse_row_of_aggregate, (0, 96)).reshape(1, LANES)
    cdia, cblk = coarse_diagonal.T, coarse_blocks.transpose(2, 3, 0, 1)
    me = lax.axis_index(DOM).astype(i32).reshape(1)
    base = me * ROWS
    wide = WIDE + ROWS + WIDE

    up, down, node_row = call(
        pack_kernel, "pack",
        [((P_ALL, HALO), f32), ((P_ALL, HALO), f32), ((8, LANES), f32)],
        [rhs, dia, col, blk, agg, owner],
    )
    before, after = shifts(up, down)
    square = ((LANES, LANES), f32)
    send, first_iter, wrhs, wdia, up2, down2 = call(
        pre_kernel, "pre",
        [square, ((3, wide), f32), ((3, wide), f32), ((3, wide), f32),
         ((3, HALO), f32), ((3, HALO), f32)],
        [base, rhs, dia, col, blk, agg, owner, before, after],
        scratch=[(3, wide), (3, wide), (8, ROWS)], scalar=True,
    )
    before2, after2 = shifts(up2, down2)
    sums = everywhere(send)
    line = ((1, LANES), f32)
    send, crhs, cd, where, weights = call(
        coarse_setup_kernel, "coarse_setup",
        [square, line, line, ((8, LANES), i32), ((9, 8, LANES), f32)],
        [me, sums, cdia, coarse_columns, cblk], scalar=True,
    )
    for sweep in range(CSWEEPS - 1):
        got = everywhere(send)
        send, mine = call(
            coarse_kernel, "coarse", [square, ((3, 32), f32)],
            [got, send, crhs, cd, where, weights], scratch=[(LANES, LANES)],
        )
    got = everywhere(send)
    solution, = call(
        post_kernel, "post", [((3, ROWS), f32)],
        [base, got, first_iter, wrhs, wdia, col, blk, node_row, before, after, before2, after2],
        scratch=[(LANES, LANES), (3, wide), (3, wide)], scalar=True,
    )
    return solution.T, mine.T


def solution(mesh):
    torus = Mesh(mesh.devices.reshape(4, 4, 4, 2), DOM)
    return jax.shard_map(
        body,
        mesh=torus,
        in_specs=(
            P(DOM, None),
            P(DOM, None),
            P(DOM, None),
            P(DOM, None, None, None),
            P(DOM),
            P(DOM),
            P(DOM, None),
            P(DOM, None),
            P(DOM, None, None, None),
        ),
        out_specs=(P(DOM, None), P(DOM, None)),
        check_vma=False,
    )
```

```python
import jax
import jax.numpy as jnp
from jax import lax
from jax.experimental import pallas as pl
from jax.experimental.pallas import tpu as pltpu
from jax.sharding import Mesh
from jax.sharding import PartitionSpec as P

DOM = ("dom_0", "dom_1", "dom_2", "dom_3")
SWEEPS = 2
CSWEEPS = 6
damping = 0.7
highest = lax.Precision.HIGHEST

ROWS = 1024
LANES = 128
SLOTS = 27
FULL = 24
HALO = 256
WIDE = 512
BLOCKS = ROWS // LANES
P_COL = 9 * FULL
P_BTAIL = P_COL + FULL
P_CTAIL = P_BTAIL + 27
P_RHS = P_CTAIL + 3
P_DIA = P_RHS + 6
P_ROW = P_DIA + 6
P_ALL = 288
f32 = jnp.float32
i32 = jnp.int32


def lanes(start, size=LANES):
    if isinstance(start, int):
        return slice(start, start + size)
    return pl.ds(pl.multiple_of(start, LANES), size)


def picked(row, where):
    return jnp.take_along_axis(
        jnp.broadcast_to(row, where.shape), where, axis=1, mode="promise_in_bounds"
    )


def pack_kernel(rhs, dia, col, blk, agg, owner_row, up, down, node_row):
    table = jnp.concatenate([owner_row[...]] * 4, axis=1)
    found = picked(table, agg[...]).astype(f32)
    node_row[...] = found
    for out, near, wide in ((up, ROWS - HALO, ROWS - WIDE), (down, 0, 0)):
        for i in range(3):
            for j in range(3):
                g = 3 * i + j
                out[g * FULL : (g + 1) * FULL, :] = blk[i, j, 0:FULL, lanes(near, HALO)]
                out[P_BTAIL + 3 * g : P_BTAIL + 3 * g + 3, :] = blk[
                    i, j, FULL:SLOTS, lanes(near, HALO)
                ]
        out[P_COL : P_COL + FULL, :] = col[0:FULL, lanes(near, HALO)].astype(f32)
        out[P_CTAIL : P_CTAIL + 3, :] = col[FULL:SLOTS, lanes(near, HALO)].astype(f32)
        for h in range(2):
            out[P_RHS + 3 * h : P_RHS + 3 * h + 3, :] = rhs[:, lanes(wide + HALO * h, HALO)]
            out[P_DIA + 3 * h : P_DIA + 3 * h + 3, :] = dia[:, lanes(wide + HALO * h, HALO)]
            for q in range(2):
                s = wide // LANES + 2 * h + q
                out[P_ROW + h : P_ROW + h + 1, lanes(LANES * q)] = found[s : s + 1, :]
        out[P_ROW + 2 : P_ALL, :] = jnp.zeros((P_ALL - P_ROW - 2, HALO), f32)


def pulled_block(columns, blocks, table, first_chunk):
    total = [None, None, None]
    for part in range(4):
        where = columns(part)
        chunk = lax.shift_right_arithmetic(where, 7)
        lane = lax.bitwise_and(where, 127)
        near = [jnp.zeros(where.shape, f32) for _ in range(3)]
        for c in range(5):
            here = chunk == c
            for j in range(3):
                row = table[j : j + 1, lanes(first_chunk * LANES + c * LANES)]
                near[j] = jnp.where(here, picked(row, lane), near[j])
        for i in range(3):
            s = blocks(i, 0, part) * near[0]
            s = s + blocks(i, 1, part) * near[1]
            s = s + blocks(i, 2, part) * near[2]
            if part < 3:
                total[i] = s if total[i] is None else total[i] + s
            else:
                total[i] = jnp.sum(total[i], axis=0, keepdims=True) + jnp.sum(
                    s, axis=0, keepdims=True
                )
    return total


def local_getters(col, blk, start, b):
    def columns(part):
        lo, hi = 8 * part, min(8 * part + 8, SLOTS)
        return col[lo:hi, lanes(b * LANES)] - start

    def blocks(i, j, part):
        lo, hi = 8 * part, min(8 * part + 8, SLOTS)
        return blk[i, j, lo:hi, lanes(b * LANES)]

    return columns, blocks


def halo_getters(halo, start, b):
    def columns(part):
        if part < 3:
            got = halo[P_COL + 8 * part : P_COL + 8 * part + 8, lanes(b * LANES)]
        else:
            got = halo[P_CTAIL : P_CTAIL + 3, lanes(b * LANES)]
        return got.astype(i32) - start

    def blocks(i, j, part):
        g = 3 * i + j
        if part < 3:
            return halo[g * FULL + 8 * part : g * FULL + 8 * part + 8, lanes(b * LANES)]
        return halo[P_BTAIL + 3 * g : P_BTAIL + 3 * g + 3, lanes(b * LANES)]

    return columns, blocks


def wide_vector(out, local, before, after, row):
    out[:, lanes(WIDE, ROWS)] = local[...]
    for h in range(2):
        out[:, lanes(HALO * h, HALO)] = before[row + 3 * h : row + 3 * h + 3, :]
        out[:, lanes(WIDE + ROWS + HALO * h, HALO)] = after[row + 3 * h : row + 3 * h + 3, :]


def smoothed(table, pulled, rhs, dia, at):
    pull = jnp.concatenate(pulled, axis=0)
    s = table[:, lanes(at)]
    b = rhs[:, lanes(at)]
    d = dia[:, lanes(at)]
    return s + damping * (b - (d * s - pull)) / d


def sweep_halo(out, table, rhs, dia, halo, base, first):
    for b in range(2):
        at = first + LANES * b
        start = base + (at - WIDE) - 2 * LANES
        cols, blks = halo_getters(halo, start, b)
        pull = pulled_block(cols, blks, table, at // LANES - 2)
        out[:, lanes(at)] = smoothed(table, pull, rhs, dia, at)


def own_block(table, col, blk, base, b):
    start = base + b * LANES - 2 * LANES
    cols, blks = local_getters(col, blk, start, b)
    return pulled_block(cols, blks, table, b + WIDE // LANES - 2)


def pre_kernel(base_ref, rhs, dia, col, blk, agg, owner_row, before, after,
               send, first_iter, keep_rhs, keep_dia, up2, down2, one, two, res):
    base = base_ref[0]
    wide_vector(keep_rhs, rhs, before, after, P_RHS)
    wide_vector(keep_dia, dia, before, after, P_DIA)
    raw = keep_dia[...]
    keep_dia[...] = jnp.where(raw == 0.0, 1.0, raw)
    one[...] = damping * keep_rhs[...] / keep_dia[...]
    two[...] = jnp.zeros(two.shape, f32)
    sweep_halo(two, one, keep_rhs, keep_dia, before, base, WIDE - HALO)
    sweep_halo(two, one, keep_rhs, keep_dia, after, base, WIDE + ROWS)

    def second(b, carry):
        at = WIDE + b * LANES
        pull = own_block(one, col, blk, base, b)
        two[:, lanes(at)] = smoothed(one, pull, keep_rhs, keep_dia, at)
        return carry

    lax.fori_loop(0, BLOCKS, second, 0)

    def third(b, carry):
        at = WIDE + b * LANES
        pull = jnp.concatenate(own_block(two, col, blk, base, b), axis=0)
        s, d = two[:, lanes(at)], keep_dia[:, lanes(at)]
        res[0:3, lanes(b * LANES)] = keep_rhs[:, lanes(at)] - (d * s - pull)
        return carry

    res[...] = jnp.zeros(res.shape, f32)
    lax.fori_loop(0, BLOCKS, third, 0)
    first_iter[...] = two[...]
    up2[...] = two[:, lanes(WIDE + ROWS - WIDE, HALO)]
    down2[...] = two[:, lanes(WIDE + HALO, HALO)]
    label = lax.broadcasted_iota(i32, (32, LANES), 0)
    sums = None
    for b in range(BLOCKS):
        member = (label == jnp.broadcast_to(agg[b : b + 1, :], (32, LANES))).astype(f32)
        part = lax.dot_general(
            res[:, lanes(b * LANES)], member, (((1,), (1,)), ((), ())),
            precision=highest, preferred_element_type=f32,
        )
        sums = part if sums is None else sums + part
    row = jnp.concatenate(
        [sums[0:1], sums[1:2], sums[2:3], owner_row[...].astype(f32)], axis=1
    )
    send[...] = jnp.broadcast_to(row, (LANES, LANES))


def spread(parts):
    group = lax.shift_right_logical(lax.broadcasted_iota(i32, (1, LANES), 1), 5)
    return jnp.where(group == 0, parts[0], jnp.where(group == 1, parts[1], parts[2]))


def coarse_setup_kernel(me_ref, sums, dia, col, blk, send, own, keep_rhs, keep_dia, where, weights):
    me = me_ref[0]
    got = sums[...]
    group = lax.shift_right_logical(lax.broadcasted_iota(i32, (LANES, LANES), 1), 5)
    rows = jnp.where(group == 3, got, 0.0)
    rows = rows + pltpu.roll(rows, 64, axis=1)
    rows = rows + pltpu.roll(rows, 32, axis=1)
    rows = rows.astype(i32) - me * 32
    lines = []
    for r in range(32):
        lines.append(jnp.sum(jnp.where(rows == r, got, 0.0), axis=0, keepdims=True))
    lines = jnp.concatenate(lines, axis=0)
    pick = lax.broadcasted_iota(i32, (8, LANES), 0) == lax.shift_right_logical(
        lax.broadcasted_iota(i32, (8, LANES), 1), 5
    )
    mine = lax.dot_general(
        pick.astype(f32), lines, (((1,), (1,)), ((), ())),
        precision=highest, preferred_element_type=f32,
    )
    pad = jnp.zeros((1, 32), f32)
    rhs = jnp.concatenate([mine[0:1], mine[1:2], mine[2:3], pad], axis=1)
    d = jnp.concatenate([dia[0:1, :], dia[1:2, :], dia[2:3, :], pad + 1.0], axis=1)
    keep_rhs[...] = rhs
    keep_dia[...] = d
    own[...] = damping * rhs / d
    send[...] = jnp.broadcast_to(own[...], (LANES, LANES))

    def folded(a):
        z = jnp.concatenate([a, jnp.zeros((32, 5), f32)], axis=1)
        z = jnp.transpose(z)
        return jnp.concatenate([z[8 * k : 8 * k + 8, :] for k in range(4)], axis=1)

    where[...] = folded(col[...].astype(f32)).astype(i32)
    for i in range(3):
        for j in range(3):
            weights[3 * i + j] = folded(blk[i, j])


def coarse_lookup(table, column, shape):
    chunk = lax.bitwise_and(column, 31)
    lane = lax.shift_right_logical(column, 5)
    near = [jnp.zeros(shape, f32) for _ in range(3)]
    for c in range(32):
        here = chunk == c
        for j in range(3):
            row = table[32 * j + c : 32 * j + c + 1, :]
            near[j] = jnp.where(here, picked(row, lane), near[j])
    return near


def coarse_kernel(got, own, rhs, dia, where, weights, send, new_own, mine, table):
    table[...] = jnp.transpose(got[...])
    near = coarse_lookup(table, where[...], (8, LANES))
    parts = []
    for i in range(3):
        s = weights[3 * i] * near[0] + weights[3 * i + 1] * near[1] + weights[3 * i + 2] * near[2]
        s = jnp.sum(s, axis=0, keepdims=True)
        s = s + pltpu.roll(s, 64, axis=1)
        parts.append(s + pltpu.roll(s, 32, axis=1))
    c, d = own[...], dia[...]
    new = c + damping * (rhs[...] - (d * c - spread(parts))) / d
    new_own[...] = new
    send[...] = jnp.broadcast_to(new, (LANES, LANES))
    mine[...] = jnp.concatenate([new[:, 32 * i : 32 * i + 32] for i in range(3)], axis=0)


def post_kernel(base_ref, got, first_iter, rhs, dia, col, blk, node_row, before, after,
                before2, after2, out, table, one, two):
    base = base_ref[0]
    table[...] = jnp.transpose(got[...])
    one[...] = first_iter[...]
    one[:, lanes(0, HALO)] = before2[...]
    one[:, lanes(WIDE + ROWS + HALO, HALO)] = after2[...]
    edge = [
        h[P_ROW + t : P_ROW + t + 1, lanes(LANES * q)]
        for h in (before, after) for t in range(2) for q in range(2)
    ]
    edge = jnp.concatenate(edge, axis=0)
    own = coarse_lookup(table, node_row[...].astype(i32), (8, LANES))
    far = coarse_lookup(table, edge.astype(i32), (8, LANES))
    for s in range(16):
        if s < 4:
            row = [f[s : s + 1, :] for f in far]
        elif s < 12:
            row = [f[s - 4 : s - 3, :] for f in own]
        else:
            row = [f[s - 8 : s - 7, :] for f in far]
        one[:, lanes(s * LANES)] = one[:, lanes(s * LANES)] + jnp.concatenate(row, axis=0)
    two[...] = jnp.zeros(two.shape, f32)
    sweep_halo(two, one, rhs, dia, before, base, WIDE - HALO)
    sweep_halo(two, one, rhs, dia, after, base, WIDE + ROWS)

    def first(b, carry):
        at = WIDE + b * LANES
        pull = own_block(one, col, blk, base, b)
        two[:, lanes(at)] = smoothed(one, pull, rhs, dia, at)
        return carry

    def second(b, carry):
        at = WIDE + b * LANES
        pull = own_block(two, col, blk, base, b)
        out[:, lanes(b * LANES)] = smoothed(two, pull, rhs, dia, at)
        return carry

    lax.fori_loop(0, BLOCKS, first, 0)
    lax.fori_loop(0, BLOCKS, second, 0)


def call(kernel, name, outs, args, scratch=(), scalar=False):
    vmem = pl.BlockSpec(memory_space=pltpu.VMEM)
    specs = [vmem] * len(args)
    if scalar:
        specs[0] = pl.BlockSpec(memory_space=pltpu.SMEM)
    return pl.pallas_call(
        kernel,
        name=name,
        in_specs=specs,
        out_specs=[vmem] * len(outs),
        out_shape=[jax.ShapeDtypeStruct(o, t) for o, t in outs],
        scratch_shapes=[pltpu.VMEM(s, f32) for s in scratch],
        compiler_params=pltpu.CompilerParams(vmem_limit_bytes=12 * 2**20),
    )(*args)


def everywhere(row):
    return lax.all_to_all(row, DOM, 0, 0, tiled=True)


def shifts(up, down):
    count = lax.axis_size(DOM)
    forward = [(i, i + 1) for i in range(count - 1)]
    backward = [(i + 1, i) for i in range(count - 1)]
    return lax.ppermute(up, DOM, forward), lax.ppermute(down, DOM, backward)


def body(right_side, fine_diagonal, fine_columns, fine_blocks, aggregate_of_node,
         coarse_row_of_aggregate, coarse_diagonal, coarse_columns, coarse_blocks):
    rhs, dia = right_side.T, fine_diagonal.T
    col, blk = fine_columns.T, fine_blocks.transpose(2, 3, 1, 0)
    agg = aggregate_of_node.reshape(8, LANES)
    owner = coarse_row_of_aggregate.reshape(1, 32)
    cdia, cblk = coarse_diagonal.T, coarse_blocks.transpose(2, 3, 0, 1)
    me = lax.axis_index(DOM).astype(i32).reshape(1)
    base = me * ROWS
    wide = WIDE + ROWS + WIDE

    up, down, node_row = call(
        pack_kernel, "pack",
        [((P_ALL, HALO), f32), ((P_ALL, HALO), f32), ((8, LANES), f32)],
        [rhs, dia, col, blk, agg, owner],
    )
    before, after = shifts(up, down)
    square = ((LANES, LANES), f32)
    send, first_iter, wrhs, wdia, up2, down2 = call(
        pre_kernel, "pre",
        [square, ((3, wide), f32), ((3, wide), f32), ((3, wide), f32),
         ((3, HALO), f32), ((3, HALO), f32)],
        [base, rhs, dia, col, blk, agg, owner, before, after],
        scratch=[(3, wide), (3, wide), (8, ROWS)], scalar=True,
    )
    before2, after2 = shifts(up2, down2)
    sums = everywhere(send)
    line = ((1, LANES), f32)
    send, own, crhs, cd, where, weights = call(
        coarse_setup_kernel, "coarse_setup",
        [square, line, line, line, ((8, LANES), i32), ((9, 8, LANES), f32)],
        [me, sums, cdia, coarse_columns, cblk], scalar=True,
    )
    for sweep in range(CSWEEPS - 1):
        got = everywhere(send)
        send, own, mine = call(
            coarse_kernel, "coarse", [square, line, ((3, 32), f32)],
            [got, own, crhs, cd, where, weights], scratch=[(LANES, LANES)],
        )
    got = everywhere(send)
    solution, = call(
        post_kernel, "post", [((3, ROWS), f32)],
        [base, got, first_iter, wrhs, wdia, col, blk, node_row, before, after, before2, after2],
        scratch=[(LANES, LANES), (3, wide), (3, wide)], scalar=True,
    )
    return solution.T, mine.T


def solution(mesh):
    torus = Mesh(mesh.devices.reshape(4, 4, 4, 2), DOM)
    return jax.shard_map(
        body,
        mesh=torus,
        in_specs=(
            P(DOM, None),
            P(DOM, None),
            P(DOM, None),
            P(DOM, None, None, None),
            P(DOM),
            P(DOM),
            P(DOM, None),
            P(DOM, None),
            P(DOM, None, None, None),
        ),
        out_specs=(P(DOM, None), P(DOM, None)),
        check_vma=False,
    )
```

```python
import jax
import jax.numpy as jnp
from jax import lax
from jax.experimental import pallas as pl
from jax.experimental.pallas import tpu as pltpu
from jax.sharding import Mesh
from jax.sharding import PartitionSpec as P

DOM = ("dom_0", "dom_1", "dom_2", "dom_3", "dom_4", "dom_5")
OTHERS = ("dom_0", "dom_1", "dom_3")
PEERS = 16
UNROLL = 8
SWEEPS = 2
CSWEEPS = 6
damping = 0.7
highest = lax.Precision.HIGHEST

ROWS = 1024
LANES = 128
SLOTS = 27
FULL = 24
HALO = 256
WIDE = 512
BLOCKS = ROWS // LANES
P_COL = 9 * FULL
P_BTAIL = P_COL + FULL
P_CTAIL = P_BTAIL + 27
P_RHS = P_CTAIL + 3
P_DIA = P_RHS + 6
P_ROW = P_DIA + 6
P_ALL = 288
f32 = jnp.float32
i32 = jnp.int32


def lanes(start, size=LANES):
    if isinstance(start, int):
        return slice(start, start + size)
    return pl.ds(pl.multiple_of(start, LANES), size)


def picked(row, where):
    return jnp.take_along_axis(
        jnp.broadcast_to(row, where.shape), where, axis=1, mode="promise_in_bounds"
    )


def pack_kernel(rhs, dia, col, blk, agg, owner_row, up, down, node_row):
    table = jnp.concatenate([owner_row[...]] * 4, axis=1)
    found = picked(table, agg[...]).astype(f32)
    node_row[...] = found
    for out, near, wide in ((up, ROWS - HALO, ROWS - WIDE), (down, 0, 0)):
        for i in range(3):
            for j in range(3):
                g = 3 * i + j
                out[g * FULL : (g + 1) * FULL, :] = blk[i, j, 0:FULL, lanes(near, HALO)]
                out[P_BTAIL + 3 * g : P_BTAIL + 3 * g + 3, :] = blk[
                    i, j, FULL:SLOTS, lanes(near, HALO)
                ]
        out[P_COL : P_COL + FULL, :] = col[0:FULL, lanes(near, HALO)].astype(f32)
        out[P_CTAIL : P_CTAIL + 3, :] = col[FULL:SLOTS, lanes(near, HALO)].astype(f32)
        for h in range(2):
            out[P_RHS + 3 * h : P_RHS + 3 * h + 3, :] = rhs[:, lanes(wide + HALO * h, HALO)]
            out[P_DIA + 3 * h : P_DIA + 3 * h + 3, :] = dia[:, lanes(wide + HALO * h, HALO)]
            for q in range(2):
                s = wide // LANES + 2 * h + q
                out[P_ROW + h : P_ROW + h + 1, lanes(LANES * q)] = found[s : s + 1, :]
        out[P_ROW + 2 : P_ALL, :] = jnp.zeros((P_ALL - P_ROW - 2, HALO), f32)


def pulled_block(columns, blocks, table, first_chunk):
    total = [None, None, None]
    for part in range(4):
        where = columns(part)
        chunk = lax.shift_right_arithmetic(where, 7)
        lane = lax.bitwise_and(where, 127)
        near = [jnp.zeros(where.shape, f32) for _ in range(3)]
        for c in range(5):
            here = chunk == c
            for j in range(3):
                row = table[j : j + 1, lanes(first_chunk * LANES + c * LANES)]
                near[j] = jnp.where(here, picked(row, lane), near[j])
        for i in range(3):
            s = blocks(i, 0, part) * near[0]
            s = s + blocks(i, 1, part) * near[1]
            s = s + blocks(i, 2, part) * near[2]
            if part < 3:
                total[i] = s if total[i] is None else total[i] + s
            else:
                total[i] = jnp.sum(total[i], axis=0, keepdims=True) + jnp.sum(
                    s, axis=0, keepdims=True
                )
    return total


def local_getters(col, blk, start, b):
    def columns(part):
        lo, hi = 8 * part, min(8 * part + 8, SLOTS)
        return col[lo:hi, lanes(b * LANES)] - start

    def blocks(i, j, part):
        lo, hi = 8 * part, min(8 * part + 8, SLOTS)
        return blk[i, j, lo:hi, lanes(b * LANES)]

    return columns, blocks


def halo_getters(halo, start, b):
    def columns(part):
        if part < 3:
            got = halo[P_COL + 8 * part : P_COL + 8 * part + 8, lanes(b * LANES)]
        else:
            got = halo[P_CTAIL : P_CTAIL + 3, lanes(b * LANES)]
        return got.astype(i32) - start

    def blocks(i, j, part):
        g = 3 * i + j
        if part < 3:
            return halo[g * FULL + 8 * part : g * FULL + 8 * part + 8, lanes(b * LANES)]
        return halo[P_BTAIL + 3 * g : P_BTAIL + 3 * g + 3, lanes(b * LANES)]

    return columns, blocks


def wide_vector(out, local, before, after, row):
    out[:, lanes(WIDE, ROWS)] = local[...]
    for h in range(2):
        out[:, lanes(HALO * h, HALO)] = before[row + 3 * h : row + 3 * h + 3, :]
        out[:, lanes(WIDE + ROWS + HALO * h, HALO)] = after[row + 3 * h : row + 3 * h + 3, :]


def smoothed(table, pulled, rhs, dia, at):
    pull = jnp.concatenate(pulled, axis=0)
    s = table[:, lanes(at)]
    b = rhs[:, lanes(at)]
    d = dia[:, lanes(at)]
    return s + damping * (b - (d * s - pull)) / d


def sweep_halo(out, table, rhs, dia, halo, base, first):
    for b in range(2):
        at = first + LANES * b
        start = base + (at - WIDE) - 2 * LANES
        cols, blks = halo_getters(halo, start, b)
        pull = pulled_block(cols, blks, table, at // LANES - 2)
        out[:, lanes(at)] = smoothed(table, pull, rhs, dia, at)


def own_block(table, col, blk, base, b):
    start = base + b * LANES - 2 * LANES
    cols, blks = local_getters(col, blk, start, b)
    return pulled_block(cols, blks, table, b + WIDE // LANES - 2)


def pre_kernel(base_ref, rhs, dia, col, blk, agg, owner_row, cdia, before, after,
               send, first_iter, keep_rhs, keep_dia, up2, down2, one, two, res):
    base = base_ref[0]
    wide_vector(keep_rhs, rhs, before, after, P_RHS)
    wide_vector(keep_dia, dia, before, after, P_DIA)
    raw = keep_dia[...]
    keep_dia[...] = jnp.where(raw == 0.0, 1.0, raw)
    one[...] = damping * keep_rhs[...] / keep_dia[...]
    two[...] = jnp.zeros(two.shape, f32)
    sweep_halo(two, one, keep_rhs, keep_dia, before, base, WIDE - HALO)
    sweep_halo(two, one, keep_rhs, keep_dia, after, base, WIDE + ROWS)

    def second(b, carry):
        at = WIDE + b * LANES
        pull = own_block(one, col, blk, base, b)
        two[:, lanes(at)] = smoothed(one, pull, keep_rhs, keep_dia, at)
        return carry

    lax.fori_loop(0, BLOCKS, second, 0)

    def third(b, carry):
        at = WIDE + b * LANES
        pull = jnp.concatenate(own_block(two, col, blk, base, b), axis=0)
        s, d = two[:, lanes(at)], keep_dia[:, lanes(at)]
        res[0:3, lanes(b * LANES)] = keep_rhs[:, lanes(at)] - (d * s - pull)
        return carry

    res[...] = jnp.zeros(res.shape, f32)
    lax.fori_loop(0, BLOCKS, third, 0)
    first_iter[...] = two[...]
    up2[...] = two[:, lanes(WIDE + ROWS - WIDE, HALO)]
    down2[...] = two[:, lanes(WIDE + HALO, HALO)]
    label = lax.broadcasted_iota(i32, (32, LANES), 0)
    sums = None
    for b in range(BLOCKS):
        member = (label == jnp.broadcast_to(agg[b : b + 1, :], (32, LANES))).astype(f32)
        part = lax.dot_general(
            res[:, lanes(b * LANES)], member, (((1,), (1,)), ((), ())),
            precision=highest, preferred_element_type=f32,
        )
        sums = part if sums is None else sums + part
    row = jnp.concatenate(
        [sums[0:1], sums[1:2], sums[2:3], owner_row[...].astype(f32)], axis=1
    )
    send[:, 0, :] = jnp.broadcast_to(row, (LANES, LANES))
    row = jnp.concatenate(
        [cdia[0:1], cdia[1:2], cdia[2:3], jnp.ones((1, 32), f32)], axis=1
    )
    send[:, 1, :] = jnp.broadcast_to(row, (LANES, LANES))


def lane_of_device(p, me):
    p = lax.bitwise_xor(p, lax.bitwise_and(me, 11))

    def bit(at, to, mask=1):
        return lax.shift_left(lax.bitwise_and(lax.shift_right_logical(p, at), mask), to)

    return bit(3, 6) + bit(1, 5) + bit(0, 4) + bit(5, 2, 3) + bit(4, 1) + bit(2, 0)


def device_of_lane(q, me):
    def bit(at, to, mask=1):
        return lax.shift_left(lax.bitwise_and(lax.shift_right_logical(q, at), mask), to)

    p = bit(6, 3) + bit(5, 1) + bit(4, 0) + bit(2, 5, 3) + bit(1, 4) + bit(0, 2)
    return lax.bitwise_xor(p, lax.bitwise_and(me, 11))


def coarse_pack_kernel(col, blk, send):
    def folded(a):
        z = jnp.concatenate([a, jnp.zeros((32, 5), f32)], axis=1)
        z = jnp.transpose(z)
        return jnp.concatenate([z[8 * k : 8 * k + 8, :] for k in range(4)], axis=1)

    parts = [folded(blk[i, j]) for i in range(3) for j in range(3)]
    parts.append(folded(col[...].astype(f32)))
    for m in range(10):
        for d in range(PEERS):
            send[d, 8 * m : 8 * m + 8, :] = parts[m]


def spread(parts):
    group = lax.shift_right_logical(lax.broadcasted_iota(i32, parts[0].shape, 1), 5)
    return jnp.where(group == 0, parts[0], jnp.where(group == 1, parts[1], parts[2]))


def coarse_lookup(table, chunk, lane):
    near = [jnp.zeros(chunk.shape, f32) for _ in range(3)]
    for c in range(32):
        here = chunk == c
        for j in range(3):
            row = table[32 * j + c : 32 * j + c + 1, :]
            near[j] = jnp.where(here, picked(row, lane), near[j])
    return near


def coarse_step(table, where, data, own, rhs, dia, gather):
    def some(t, carry):
        for u in range(UNROLL):
            d = t * UNROLL + u
            w = where[d]
            near = coarse_lookup(table, lax.bitwise_and(w, 31), lax.shift_right_logical(w, 5))
            for i in range(3):
                a = data[d, lanes8(3 * i), :] * near[0]
                a = a + data[d, lanes8(3 * i + 1), :] * near[1]
                a = a + data[d, lanes8(3 * i + 2), :] * near[2]
                gather[i, pl.ds(d, 1), :] = jnp.sum(a, axis=0, keepdims=True)
        return carry

    lax.fori_loop(0, PEERS // UNROLL, some, 0)
    parts = []
    for i in range(3):
        s = gather[i]
        s = s + pltpu.roll(s, 64, axis=1)
        parts.append(s + pltpu.roll(s, 32, axis=1))
    return own + damping * (rhs - (dia * own - spread(parts))) / dia


def lanes8(m):
    return slice(8 * m, 8 * m + 8)


def coarse_first_kernel(me_ref, sums, data, far_up, far_down, new, rhs, dia, where,
                        table, gather, left, right):
    me = me_ref[0]
    got = jnp.transpose(sums[:, 0, :])
    rows = got[96:128].astype(i32)
    s = got[0:96]
    split = []
    for _ in range(3):
        t = s.astype(jnp.bfloat16).astype(f32)
        split.append(t)
        s = s - t
    chunk = lax.broadcasted_iota(i32, (32, LANES), 0)
    place = lax.broadcasted_iota(i32, (LANES, LANES), 0)
    low = lax.bitwise_and(rows, 31)
    lane = lane_of_device(lax.shift_right_logical(rows, 5), me)
    for a in range(32):
        here = chunk == jnp.broadcast_to(low[a : a + 1], (32, LANES))
        for t in range(3):
            for i in range(3):
                value = jnp.broadcast_to(split[t][32 * i + a : 32 * i + a + 1], (32, LANES))
                left[96 * t + 32 * i : 96 * t + 32 * i + 32, lanes(LANES * a)] = jnp.where(
                    here, value, 0.0
                ).astype(jnp.bfloat16)
        right[:, lanes(LANES * a)] = jnp.where(
            place == jnp.broadcast_to(lane[a : a + 1], (LANES, LANES)), 1.0, 0.0
        ).astype(jnp.bfloat16)
    both = lax.dot_general(
        left[...], right[...], (((1,), (1,)), ((), ())), preferred_element_type=f32
    )
    crhs = both[0:96] + both[96:192] + both[192:288]
    order = device_of_lane(lax.broadcasted_iota(i32, (96, LANES), 1), me)
    cdia = jnp.take_along_axis(
        jnp.transpose(sums[:, 1, :])[0:96], order, axis=1, mode="promise_in_bounds"
    )
    pad = jnp.zeros((32, LANES), f32)
    first = jnp.concatenate([damping * crhs / cdia, pad], axis=0)
    table[...] = first
    own = jnp.transpose(first)[0:PEERS]
    rhs[...] = jnp.transpose(jnp.concatenate([crhs, pad], axis=0))[0:PEERS]
    dia[...] = jnp.transpose(jnp.concatenate([cdia, pad + 1.0], axis=0))[0:PEERS]
    for d in range(PEERS):
        c = data[d, 72:80, :].astype(i32)
        at = lane_of_device(lax.shift_right_logical(c, 5), me)
        where[d] = lax.bitwise_and(c, 31) + lax.shift_left(at, 5)
    new[...] = coarse_step(table, where, data, own, rhs[...], dia[...], gather)


def gathered(table, pieces, mine):
    row = 0
    for piece in pieces:
        size = piece.shape[0]
        mine[row : row + size, :] = piece[...]
        row += size
    table[...] = jnp.transpose(mine[...])


def coarse_kernel(me_ref, p0, p1, p2, p3, rhs, dia, where, data, new, correction,
                  table, mine, gather):
    gathered(table, (p0, p1, p2, p3), mine)
    got = coarse_step(table, where, data, p0[...], rhs[...], dia[...], gather)
    new[...] = got
    mine[0:PEERS, :] = got
    me = me_ref[0]
    at = lane_of_device(me, me)
    row = mine[pl.ds(at, 1), :]
    correction[...] = jnp.concatenate([row[:, 32 * i : 32 * i + 32] for i in range(3)], axis=0)


def post_kernel(base_ref, p0, p1, p2, p3, first_iter, rhs, dia, col, blk, node_row, before, after,
                before2, after2, out, table, mine, one, two):
    base = base_ref[0]
    me = lax.shift_right_logical(base, 10)
    gathered(table, (p0, p1, p2, p3), mine)
    one[...] = first_iter[...]
    one[:, lanes(0, HALO)] = before2[...]
    one[:, lanes(WIDE + ROWS + HALO, HALO)] = after2[...]
    edge = [
        h[P_ROW + t : P_ROW + t + 1, lanes(LANES * q)]
        for h in (before, after) for t in range(2) for q in range(2)
    ]
    edge = jnp.concatenate(edge, axis=0)

    def found(rows):
        rows = rows.astype(i32)
        lane = lane_of_device(lax.shift_right_logical(rows, 5), me)
        return coarse_lookup(table, lax.bitwise_and(rows, 31), lane)

    own, far = found(node_row[...]), found(edge)
    for s in range(16):
        if s < 4:
            row = [f[s : s + 1, :] for f in far]
        elif s < 12:
            row = [f[s - 4 : s - 3, :] for f in own]
        else:
            row = [f[s - 8 : s - 7, :] for f in far]
        one[:, lanes(s * LANES)] = one[:, lanes(s * LANES)] + jnp.concatenate(row, axis=0)
    two[...] = jnp.zeros(two.shape, f32)
    sweep_halo(two, one, rhs, dia, before, base, WIDE - HALO)
    sweep_halo(two, one, rhs, dia, after, base, WIDE + ROWS)

    def first(b, carry):
        at = WIDE + b * LANES
        pull = own_block(one, col, blk, base, b)
        two[:, lanes(at)] = smoothed(one, pull, rhs, dia, at)
        return carry

    def second(b, carry):
        at = WIDE + b * LANES
        pull = own_block(two, col, blk, base, b)
        out[:, lanes(b * LANES)] = smoothed(two, pull, rhs, dia, at)
        return carry

    lax.fori_loop(0, BLOCKS, first, 0)
    lax.fori_loop(0, BLOCKS, second, 0)


def call(kernel, name, outs, args, scratch=(), scalar=False):
    vmem = pl.BlockSpec(memory_space=pltpu.VMEM)
    specs = [vmem] * len(args)
    if scalar:
        specs[0] = pl.BlockSpec(memory_space=pltpu.SMEM)
    return pl.pallas_call(
        kernel,
        name=name,
        in_specs=specs,
        out_specs=[vmem] * len(outs),
        out_shape=[jax.ShapeDtypeStruct(o, t) for o, t in outs],
        scratch_shapes=[
            pltpu.VMEM(*s) if isinstance(s[0], tuple) else pltpu.VMEM(s, f32) for s in scratch
        ],
        compiler_params=pltpu.CompilerParams(vmem_limit_bytes=12 * 2**20),
    )(*args)


def in_group(new):
    swap = [(0, 1), (1, 0)]
    p1 = lax.ppermute(new, "dom_5", swap)
    a = jnp.concatenate([new, p1], axis=0)
    p2 = lax.ppermute(a, "dom_4", swap)
    b = jnp.concatenate([a, p2], axis=0)
    p3 = lax.ppermute(b, "dom_2", swap)
    return new, p1, p2, p3


def shifts(up, down):
    count = lax.axis_size(DOM)
    forward = [(i, i + 1) for i in range(count - 1)]
    backward = [(i + 1, i) for i in range(count - 1)]
    return lax.ppermute(up, DOM, forward), lax.ppermute(down, DOM, backward)


def body(right_side, fine_diagonal, fine_columns, fine_blocks, aggregate_of_node,
         coarse_row_of_aggregate, coarse_diagonal, coarse_columns, coarse_blocks):
    rhs, dia = right_side.T, fine_diagonal.T
    col, blk = fine_columns.T, fine_blocks.transpose(2, 3, 1, 0)
    agg = aggregate_of_node.reshape(8, LANES)
    owner = coarse_row_of_aggregate.reshape(1, 32)
    cdia, cblk = coarse_diagonal.T, coarse_blocks.transpose(2, 3, 0, 1)
    me = lax.axis_index(DOM).astype(i32).reshape(1)
    base = me * ROWS
    wide = WIDE + ROWS + WIDE

    dsend, = call(
        coarse_pack_kernel, "coarse_pack", [((PEERS, 80, LANES), f32)], [coarse_columns, cblk]
    )
    data = lax.all_to_all(dsend, OTHERS, 0, 0, tiled=True)
    up, down, node_row = call(
        pack_kernel, "pack",
        [((P_ALL, HALO), f32), ((P_ALL, HALO), f32), ((8, LANES), f32)],
        [rhs, dia, col, blk, agg, owner],
    )
    before, after = shifts(up, down)
    send, first_iter, wrhs, wdia, up2, down2 = call(
        pre_kernel, "pre",
        [((LANES, 2, LANES), f32), ((3, wide), f32), ((3, wide), f32), ((3, wide), f32),
         ((3, HALO), f32), ((3, HALO), f32)],
        [base, rhs, dia, col, blk, agg, owner, cdia, before, after],
        scratch=[(3, wide), (3, wide), (8, ROWS)], scalar=True,
    )
    before2, after2 = shifts(up2, down2)
    sums = lax.all_to_all(send, DOM, 0, 0, tiled=True)
    peers = ((PEERS, LANES), f32)
    gather = (3, PEERS, LANES)
    square = (LANES, LANES)
    new, crhs, cd, where = call(
        coarse_first_kernel, "coarse_first",
        [peers, peers, peers, ((PEERS, 8, LANES), i32)],
        [me, sums, data, before2, after2],
        scratch=[square, gather, ((288, 4096), jnp.bfloat16), ((LANES, 4096), jnp.bfloat16)],
        scalar=True,
    )
    for sweep in range(CSWEEPS - 2):
        new, mine = call(
            coarse_kernel, "coarse", [peers, ((3, 32), f32)],
            [me, *in_group(new), crhs, cd, where, data],
            scratch=[square, square, gather], scalar=True,
        )
    solution, = call(
        post_kernel, "post", [((3, ROWS), f32)],
        [base, *in_group(new), first_iter, wrhs, wdia, col, blk, node_row,
         before, after, before2, after2],
        scratch=[square, square, (3, wide), (3, wide)], scalar=True,
    )
    return solution.T, mine.T


def solution(mesh):
    torus = Mesh(mesh.devices.reshape(4, 2, 2, 2, 2, 2), DOM)
    return jax.shard_map(
        body,
        mesh=torus,
        in_specs=(
            P(DOM, None),
            P(DOM, None),
            P(DOM, None),
            P(DOM, None, None, None),
            P(DOM),
            P(DOM),
            P(DOM, None),
            P(DOM, None),
            P(DOM, None, None, None),
        ),
        out_specs=(P(DOM, None), P(DOM, None)),
        check_vma=False,
    )
```

```python
import jax
import jax.numpy as jnp
from jax import lax
from jax.experimental import pallas as pl
from jax.experimental.pallas import tpu as pltpu
from jax.sharding import Mesh
from jax.sharding import PartitionSpec as P


DOM = ("dom_0", "dom_1", "dom_2", "dom_3", "dom_4", "dom_5")
OTHERS = ("dom_0", "dom_1", "dom_3")
PEERS = 16
UNROLL = 8
CSWEEPS = 6
damping = 0.7
highest = lax.Precision.HIGHEST

ROWS = 1024
LANES = 128
SLOTS = 27
FULL = 24
HALO = 256
WIDE = 512
BLOCKS = ROWS // LANES
P_COL = 9 * FULL
P_BTAIL = P_COL + FULL
P_CTAIL = P_BTAIL + 27
P_RHS = P_CTAIL + 3
P_DIA = P_RHS + 6
P_ROW = P_DIA + 6
P_ALL = 288
f32 = jnp.float32
i32 = jnp.int32


def lanes(start, size=LANES):
    if isinstance(start, int):
        return slice(start, start + size)
    return pl.ds(pl.multiple_of(start, LANES), size)


def picked(row, where):
    return jnp.take_along_axis(
        jnp.broadcast_to(row, where.shape), where, axis=1, mode="promise_in_bounds"
    )


def pack_kernel(rhs_in, dia_in, col_in, blk_in, agg_in, owner_in, up, down, node_row,
                rhs, dia, col, blk, agg, owner, sem):
    copies = [(rhs_in, rhs), (dia_in, dia), (agg_in, agg), (owner_in, owner)]
    for t, near in enumerate((ROWS - HALO, 0)):
        copies.append((col_in.at[:, lanes(near, HALO)], col.at[t]))
        copies.append((blk_in.at[:, :, :, lanes(near, HALO)], blk.at[t]))
    copies = [pltpu.make_async_copy(a, b, sem.at[n]) for n, (a, b) in enumerate(copies)]
    for c in copies:
        c.start()
    for c in copies:
        c.wait()
    table = jnp.concatenate([owner[...]] * 4, axis=1)
    found = picked(table, agg[...]).astype(f32)
    node_row[...] = found
    for t, (out, wide) in enumerate(((up, ROWS - WIDE), (down, 0))):
        for i in range(3):
            for j in range(3):
                g = 3 * i + j
                out[g * FULL : (g + 1) * FULL, :] = blk[t, i, j, 0:FULL, :]
                out[P_BTAIL + 3 * g : P_BTAIL + 3 * g + 3, :] = blk[t, i, j, FULL:SLOTS, :]
        out[P_COL : P_COL + FULL, :] = col[t, 0:FULL, :].astype(f32)
        out[P_CTAIL : P_CTAIL + 3, :] = col[t, FULL:SLOTS, :].astype(f32)
        for h in range(2):
            out[P_RHS + 3 * h : P_RHS + 3 * h + 3, :] = rhs[:, lanes(wide + HALO * h, HALO)]
            out[P_DIA + 3 * h : P_DIA + 3 * h + 3, :] = dia[:, lanes(wide + HALO * h, HALO)]
            for q in range(2):
                s = wide // LANES + 2 * h + q
                out[P_ROW + h : P_ROW + h + 1, lanes(LANES * q)] = found[s : s + 1, :]
        out[P_ROW + 2 : P_ALL, :] = jnp.zeros((P_ALL - P_ROW - 2, HALO), f32)


def pulled_block(columns, blocks, table, first_chunk):
    total = [None, None, None]
    for part in range(4):
        where = columns(part)
        chunk = lax.shift_right_arithmetic(where, 7)
        lane = lax.bitwise_and(where, 127)
        near = [jnp.zeros(where.shape, f32) for _ in range(3)]
        for c in range(5):
            here = chunk == c
            for j in range(3):
                row = table[j : j + 1, lanes(first_chunk * LANES + c * LANES)]
                near[j] = jnp.where(here, picked(row, lane), near[j])
        for i in range(3):
            s = blocks(i, 0, part) * near[0]
            s = s + blocks(i, 1, part) * near[1]
            s = s + blocks(i, 2, part) * near[2]
            if part < 3:
                total[i] = s if total[i] is None else total[i] + s
            else:
                total[i] = jnp.sum(total[i], axis=0, keepdims=True) + jnp.sum(
                    s, axis=0, keepdims=True
                )
    return total


def local_getters(col, blk, start, b):
    def columns(part):
        lo, hi = 8 * part, min(8 * part + 8, SLOTS)
        return col[lo:hi, lanes(b * LANES)] - start

    def blocks(i, j, part):
        lo, hi = 8 * part, min(8 * part + 8, SLOTS)
        return blk[i, j, lo:hi, lanes(b * LANES)]

    return columns, blocks


def halo_getters(halo, start, b):
    def columns(part):
        if part < 3:
            got = halo[P_COL + 8 * part : P_COL + 8 * part + 8, lanes(b * LANES)]
        else:
            got = halo[P_CTAIL : P_CTAIL + 3, lanes(b * LANES)]
        return got.astype(i32) - start

    def blocks(i, j, part):
        g = 3 * i + j
        if part < 3:
            return halo[g * FULL + 8 * part : g * FULL + 8 * part + 8, lanes(b * LANES)]
        return halo[P_BTAIL + 3 * g : P_BTAIL + 3 * g + 3, lanes(b * LANES)]

    return columns, blocks


def wide_vector(out, local, before, after, row):
    out[:, lanes(WIDE, ROWS)] = local[...]
    for h in range(2):
        out[:, lanes(HALO * h, HALO)] = before[row + 3 * h : row + 3 * h + 3, :]
        out[:, lanes(WIDE + ROWS + HALO * h, HALO)] = after[row + 3 * h : row + 3 * h + 3, :]


def smoothed(table, pulled, rhs, dia, at):
    pull = jnp.concatenate(pulled, axis=0)
    s = table[:, lanes(at)]
    b = rhs[:, lanes(at)]
    d = dia[:, lanes(at)]
    return s + damping * (b - (d * s - pull)) / d


def sweep_halo(out, table, rhs, dia, halo, base, first):
    for b in range(2):
        at = first + LANES * b
        start = base + (at - WIDE) - 2 * LANES
        cols, blks = halo_getters(halo, start, b)
        pull = pulled_block(cols, blks, table, at // LANES - 2)
        out[:, lanes(at)] = smoothed(table, pull, rhs, dia, at)


def own_block(table, col, blk, base, b):
    start = base + b * LANES - 2 * LANES
    cols, blks = local_getters(col, blk, start, b)
    return pulled_block(cols, blks, table, b + WIDE // LANES - 2)


def pre_kernel(base_ref, rhs, dia, col, blk, agg, owner_row, cdia, before, after,
               send, first_iter, keep_rhs, keep_dia, up2, down2, one, two, res):
    base = base_ref[0]
    wide_vector(keep_rhs, rhs, before, after, P_RHS)
    wide_vector(keep_dia, dia, before, after, P_DIA)
    raw = keep_dia[...]
    keep_dia[...] = jnp.where(raw == 0.0, 1.0, raw)
    one[...] = damping * keep_rhs[...] / keep_dia[...]
    two[...] = jnp.zeros(two.shape, f32)
    sweep_halo(two, one, keep_rhs, keep_dia, before, base, WIDE - HALO)
    sweep_halo(two, one, keep_rhs, keep_dia, after, base, WIDE + ROWS)

    def second(b, carry):
        at = WIDE + b * LANES
        pull = own_block(one, col, blk, base, b)
        two[:, lanes(at)] = smoothed(one, pull, keep_rhs, keep_dia, at)
        return carry

    lax.fori_loop(0, BLOCKS, second, 0)

    def third(b, carry):
        at = WIDE + b * LANES
        pull = jnp.concatenate(own_block(two, col, blk, base, b), axis=0)
        s, d = two[:, lanes(at)], keep_dia[:, lanes(at)]
        res[0:3, lanes(b * LANES)] = keep_rhs[:, lanes(at)] - (d * s - pull)
        return carry

    res[...] = jnp.zeros(res.shape, f32)
    lax.fori_loop(0, BLOCKS, third, 0)
    first_iter[...] = two[...]
    up2[...] = two[:, lanes(WIDE + ROWS - WIDE, HALO)]
    down2[...] = two[:, lanes(WIDE + HALO, HALO)]
    label = lax.broadcasted_iota(i32, (32, LANES), 0)
    sums = None
    for b in range(BLOCKS):
        member = (label == jnp.broadcast_to(agg[b : b + 1, :], (32, LANES))).astype(f32)
        part = lax.dot_general(
            res[:, lanes(b * LANES)], member, (((1,), (1,)), ((), ())),
            precision=highest, preferred_element_type=f32,
        )
        sums = part if sums is None else sums + part
    row = jnp.concatenate(
        [sums[0:1], sums[1:2], sums[2:3], owner_row[...].astype(f32)], axis=1
    )
    send[:, 0, :] = jnp.broadcast_to(row, (LANES, LANES))
    row = jnp.concatenate(
        [cdia[0:1], cdia[1:2], cdia[2:3], jnp.ones((1, 32), f32)], axis=1
    )
    send[:, 1, :] = jnp.broadcast_to(row, (LANES, LANES))


def lane_of_device(p, me):
    p = lax.bitwise_xor(p, lax.bitwise_and(me, 11))

    def bit(at, to, mask=1):
        return lax.shift_left(lax.bitwise_and(lax.shift_right_logical(p, at), mask), to)

    return bit(3, 6) + bit(1, 5) + bit(0, 4) + bit(5, 2, 3) + bit(4, 1) + bit(2, 0)


def device_of_lane(q, me):
    def bit(at, to, mask=1):
        return lax.shift_left(lax.bitwise_and(lax.shift_right_logical(q, at), mask), to)

    p = bit(6, 3) + bit(5, 1) + bit(4, 0) + bit(2, 5, 3) + bit(1, 4) + bit(0, 2)
    return lax.bitwise_xor(p, lax.bitwise_and(me, 11))


def coarse_pack_kernel(col, blk, send):
    def folded(a):
        z = jnp.concatenate([a, jnp.zeros((32, 5), f32)], axis=1)
        z = jnp.transpose(z)
        return jnp.concatenate([z[8 * k : 8 * k + 8, :] for k in range(4)], axis=1)

    parts = [folded(blk[i, j]) for i in range(3) for j in range(3)]
    parts.append(folded(col[...].astype(f32)))
    for m in range(10):
        for d in range(PEERS):
            send[d, 8 * m : 8 * m + 8, :] = parts[m]


def spread(parts):
    group = lax.shift_right_logical(lax.broadcasted_iota(i32, parts[0].shape, 1), 5)
    return jnp.where(group == 0, parts[0], jnp.where(group == 1, parts[1], parts[2]))


def coarse_lookup(table, chunk, lane):
    near = [jnp.zeros(chunk.shape, f32) for _ in range(3)]
    for c in range(32):
        here = chunk == c
        for j in range(3):
            row = table[32 * j + c : 32 * j + c + 1, :]
            near[j] = jnp.where(here, picked(row, lane), near[j])
    return near


def coarse_step(table, where, data, own, rhs, dia, gather):
    def some(t, carry):
        for u in range(UNROLL):
            d = t * UNROLL + u
            w = where[d]
            near = coarse_lookup(table, lax.bitwise_and(w, 31), lax.shift_right_logical(w, 5))
            for i in range(3):
                a = data[d, lanes8(3 * i), :] * near[0]
                a = a + data[d, lanes8(3 * i + 1), :] * near[1]
                a = a + data[d, lanes8(3 * i + 2), :] * near[2]
                gather[i, pl.ds(d, 1), :] = jnp.sum(a, axis=0, keepdims=True)
        return carry

    lax.fori_loop(0, PEERS // UNROLL, some, 0)
    parts = []
    for i in range(3):
        s = gather[i]
        s = s + pltpu.roll(s, 64, axis=1)
        parts.append(s + pltpu.roll(s, 32, axis=1))
    return own + damping * (rhs - (dia * own - spread(parts))) / dia


def lanes8(m):
    return slice(8 * m, 8 * m + 8)


def coarse_first_kernel(me_ref, sums, data, far_up, far_down, new, rhs, dia, where,
                        table, gather, left, right):
    me = me_ref[0]
    got = jnp.transpose(sums[:, 0, :])
    rows = got[96:128].astype(i32)
    s = got[0:96]
    split = []
    for _ in range(3):
        t = s.astype(jnp.bfloat16).astype(f32)
        split.append(t)
        s = s - t
    chunk = lax.broadcasted_iota(i32, (32, LANES), 0)
    place = lax.broadcasted_iota(i32, (LANES, LANES), 0)
    low = lax.bitwise_and(rows, 31)
    lane = lane_of_device(lax.shift_right_logical(rows, 5), me)
    for a in range(32):
        here = chunk == jnp.broadcast_to(low[a : a + 1], (32, LANES))
        for t in range(3):
            for i in range(3):
                value = jnp.broadcast_to(split[t][32 * i + a : 32 * i + a + 1], (32, LANES))
                left[96 * t + 32 * i : 96 * t + 32 * i + 32, lanes(LANES * a)] = jnp.where(
                    here, value, 0.0
                ).astype(jnp.bfloat16)
        right[:, lanes(LANES * a)] = jnp.where(
            place == jnp.broadcast_to(lane[a : a + 1], (LANES, LANES)), 1.0, 0.0
        ).astype(jnp.bfloat16)
    both = lax.dot_general(
        left[...], right[...], (((1,), (1,)), ((), ())), preferred_element_type=f32
    )
    crhs = both[0:96] + both[96:192] + both[192:288]
    order = device_of_lane(lax.broadcasted_iota(i32, (96, LANES), 1), me)
    cdia = jnp.take_along_axis(
        jnp.transpose(sums[:, 1, :])[0:96], order, axis=1, mode="promise_in_bounds"
    )
    pad = jnp.zeros((32, LANES), f32)
    first = jnp.concatenate([damping * crhs / cdia, pad], axis=0)
    table[...] = first
    own = jnp.transpose(first)[0:PEERS]
    rhs[...] = jnp.transpose(jnp.concatenate([crhs, pad], axis=0))[0:PEERS]
    dia[...] = jnp.transpose(jnp.concatenate([cdia, pad + 1.0], axis=0))[0:PEERS]
    for d in range(PEERS):
        c = data[d, 72:80, :].astype(i32)
        at = lane_of_device(lax.shift_right_logical(c, 5), me)
        where[d] = lax.bitwise_and(c, 31) + lax.shift_left(at, 5)
    new[...] = coarse_step(table, where, data, own, rhs[...], dia[...], gather)


def gathered(table, pieces, mine):
    row = 0
    for piece in pieces:
        size = piece.shape[0]
        mine[row : row + size, :] = piece[...]
        row += size
    table[...] = jnp.transpose(mine[...])


def coarse_kernel(me_ref, p0, p1, p2, p3, rhs, dia, where, data, new, correction,
                  table, mine, gather):
    gathered(table, (p0, p1, p2, p3), mine)
    got = coarse_step(table, where, data, p0[...], rhs[...], dia[...], gather)
    new[...] = got
    mine[0:PEERS, :] = got
    me = me_ref[0]
    at = lane_of_device(me, me)
    row = mine[pl.ds(at, 1), :]
    correction[...] = jnp.concatenate([row[:, 32 * i : 32 * i + 32] for i in range(3)], axis=0)


def post_kernel(base_ref, p0, p1, p2, p3, first_iter, rhs, dia, col, blk, node_row, before, after,
                before2, after2, out, table, mine, one, two):
    base = base_ref[0]
    me = lax.shift_right_logical(base, 10)
    gathered(table, (p0, p1, p2, p3), mine)
    one[...] = first_iter[...]
    one[:, lanes(0, HALO)] = before2[...]
    one[:, lanes(WIDE + ROWS + HALO, HALO)] = after2[...]
    edge = [
        h[P_ROW + t : P_ROW + t + 1, lanes(LANES * q)]
        for h in (before, after) for t in range(2) for q in range(2)
    ]
    edge = jnp.concatenate(edge, axis=0)

    def found(rows):
        rows = rows.astype(i32)
        lane = lane_of_device(lax.shift_right_logical(rows, 5), me)
        return coarse_lookup(table, lax.bitwise_and(rows, 31), lane)

    own, far = found(node_row[...]), found(edge)
    for s in range(16):
        if s < 4:
            row = [f[s : s + 1, :] for f in far]
        elif s < 12:
            row = [f[s - 4 : s - 3, :] for f in own]
        else:
            row = [f[s - 8 : s - 7, :] for f in far]
        one[:, lanes(s * LANES)] = one[:, lanes(s * LANES)] + jnp.concatenate(row, axis=0)
    two[...] = jnp.zeros(two.shape, f32)
    sweep_halo(two, one, rhs, dia, before, base, WIDE - HALO)
    sweep_halo(two, one, rhs, dia, after, base, WIDE + ROWS)

    def first(b, carry):
        at = WIDE + b * LANES
        pull = own_block(one, col, blk, base, b)
        two[:, lanes(at)] = smoothed(one, pull, rhs, dia, at)
        return carry

    def second(b, carry):
        at = WIDE + b * LANES
        pull = own_block(two, col, blk, base, b)
        out[:, lanes(b * LANES)] = smoothed(two, pull, rhs, dia, at)
        return carry

    lax.fori_loop(0, BLOCKS, first, 0)
    lax.fori_loop(0, BLOCKS, second, 0)


def call(kernel, outs, args, scratch=(), scalar=False):
    vmem = pl.BlockSpec(memory_space=pltpu.VMEM)
    specs = [vmem] * len(args)
    if scalar:
        specs[0] = pl.BlockSpec(memory_space=pltpu.SMEM)
    return pl.pallas_call(
        kernel,
        in_specs=specs,
        out_specs=[vmem] * len(outs),
        out_shape=[jax.ShapeDtypeStruct(o, t) for o, t in outs],
        scratch_shapes=[
            pltpu.VMEM(*s) if isinstance(s[0], tuple) else pltpu.VMEM(s, f32) for s in scratch
        ],
        compiler_params=pltpu.CompilerParams(vmem_limit_bytes=12 * 2**20),
    )(*args)


def in_group(new):
    swap = [(0, 1), (1, 0)]
    p1 = lax.ppermute(new, "dom_5", swap)
    a = jnp.concatenate([new, p1], axis=0)
    p2 = lax.ppermute(a, "dom_4", swap)
    b = jnp.concatenate([a, p2], axis=0)
    p3 = lax.ppermute(b, "dom_2", swap)
    return new, p1, p2, p3


def shifts(up, down):
    count = lax.axis_size(DOM)
    forward = [(i, i + 1) for i in range(count - 1)]
    backward = [(i + 1, i) for i in range(count - 1)]
    return lax.ppermute(up, DOM, forward), lax.ppermute(down, DOM, backward)


def cycle(right_side, fine_diagonal, fine_columns, fine_blocks, aggregate_of_node,
         coarse_row_of_aggregate, coarse_diagonal, coarse_columns, coarse_blocks):
    rhs, dia = right_side.T, fine_diagonal.T
    col, blk = fine_columns.T, fine_blocks.transpose(2, 3, 1, 0)
    agg = aggregate_of_node.reshape(8, LANES)
    owner = coarse_row_of_aggregate.reshape(1, 32)
    cdia, cblk = coarse_diagonal.T, coarse_blocks.transpose(2, 3, 0, 1)
    me = lax.axis_index(DOM).astype(i32).reshape(1)
    base = me * ROWS
    wide = WIDE + ROWS + WIDE

    dsend, = call(coarse_pack_kernel, [((PEERS, 80, LANES), f32)], [coarse_columns, cblk])
    data = lax.all_to_all(dsend, OTHERS, 0, 0, tiled=True)
    vmem, far = pl.BlockSpec(memory_space=pltpu.VMEM), pl.BlockSpec(memory_space=pltpu.HBM)
    up, down, node_row = pl.pallas_call(
        pack_kernel,
        name="pack",
        in_specs=[far] * 6,
        out_specs=[vmem] * 3,
        out_shape=[jax.ShapeDtypeStruct(o, f32) for o in ((P_ALL, HALO), (P_ALL, HALO), (8, LANES))],
        scratch_shapes=[
            pltpu.VMEM((3, ROWS), f32), pltpu.VMEM((3, ROWS), f32),
            pltpu.VMEM((2, SLOTS, HALO), i32), pltpu.VMEM((2, 3, 3, SLOTS, HALO), f32),
            pltpu.VMEM((8, LANES), i32), pltpu.VMEM((1, 32), i32), pltpu.SemaphoreType.DMA((8,)),
        ],
        compiler_params=pltpu.CompilerParams(vmem_limit_bytes=12 * 2**20),
    )(rhs, dia, col, blk, agg, owner)
    before, after = shifts(up, down)
    send, first_iter, wrhs, wdia, up2, down2 = call(
        pre_kernel,
        [((LANES, 2, LANES), f32), ((3, wide), f32), ((3, wide), f32), ((3, wide), f32),
         ((3, HALO), f32), ((3, HALO), f32)],
        [base, rhs, dia, col, blk, agg, owner, cdia, before, after],
        scratch=[(3, wide), (3, wide), (8, ROWS)], scalar=True,
    )
    before2, after2 = shifts(up2, down2)
    sums = lax.all_to_all(send, DOM, 0, 0, tiled=True)
    peers = ((PEERS, LANES), f32)
    gather = (3, PEERS, LANES)
    square = (LANES, LANES)
    new, crhs, cd, where = call(
        coarse_first_kernel,
        [peers, peers, peers, ((PEERS, 8, LANES), i32)],
        [me, sums, data, before2, after2],
        scratch=[square, gather, ((288, 4096), jnp.bfloat16), ((LANES, 4096), jnp.bfloat16)],
        scalar=True,
    )
    for _ in range(CSWEEPS - 2):
        new, mine = call(
            coarse_kernel, [peers, ((3, 32), f32)],
            [me, *in_group(new), crhs, cd, where, data],
            scratch=[square, square, gather], scalar=True,
        )
    solution, = call(
        post_kernel, [((3, ROWS), f32)],
        [base, *in_group(new), first_iter, wrhs, wdia, col, blk, node_row,
         before, after, before2, after2],
        scratch=[square, square, (3, wide), (3, wide)], scalar=True,
    )
    return solution.T, mine.T


def solution(mesh):
    torus = Mesh(mesh.devices.reshape(4, 2, 2, 2, 2, 2), DOM)
    return jax.shard_map(
        cycle,
        mesh=torus,
        in_specs=(
            P(DOM, None),
            P(DOM, None),
            P(DOM, None),
            P(DOM, None, None, None),
            P(DOM),
            P(DOM),
            P(DOM, None),
            P(DOM, None),
            P(DOM, None, None, None),
        ),
        out_specs=(P(DOM, None), P(DOM, None)),
        check_vma=False,
    )
```

```python
import jax
import jax.numpy as jnp
from jax import lax
from jax.experimental import pallas as pl
from jax.experimental.pallas import tpu as pltpu
from jax.sharding import Mesh
from jax.sharding import PartitionSpec as P


DOM = ("dom_0", "dom_1", "dom_2", "dom_3", "dom_4", "dom_5")
OTHERS = ("dom_0", "dom_1", "dom_2", "dom_3")
PEERS = 32
UNROLL = 8
CSWEEPS = 6
damping = 0.7
highest = lax.Precision.HIGHEST

ROWS = 1024
LANES = 128
SLOTS = 27
FULL = 24
HALO = 256
WIDE = 512
BLOCKS = ROWS // LANES
P_COL = 9 * FULL
P_BTAIL = P_COL + FULL
P_CTAIL = P_BTAIL + 27
P_RHS = P_CTAIL + 3
P_DIA = P_RHS + 6
P_ROW = P_DIA + 6
P_ALL = 288
f32 = jnp.float32
i32 = jnp.int32


def lanes(start, size=LANES):
    if isinstance(start, int):
        return slice(start, start + size)
    return pl.ds(pl.multiple_of(start, LANES), size)


def picked(row, where):
    return jnp.take_along_axis(
        jnp.broadcast_to(row, where.shape), where, axis=1, mode="promise_in_bounds"
    )


def pack_kernel(rhs_in, dia_in, col_in, blk_in, agg_in, owner_in, up, down, node_row,
                rhs, dia, col, blk, agg, owner, sem):
    copies = [(rhs_in, rhs), (dia_in, dia), (agg_in, agg), (owner_in, owner)]
    for t, near in enumerate((ROWS - HALO, 0)):
        copies.append((col_in.at[:, lanes(near, HALO)], col.at[t]))
        copies.append((blk_in.at[:, :, :, lanes(near, HALO)], blk.at[t]))
    copies = [pltpu.make_async_copy(a, b, sem.at[n]) for n, (a, b) in enumerate(copies)]
    for c in copies:
        c.start()
    for c in copies:
        c.wait()
    table = jnp.concatenate([owner[...]] * 4, axis=1)
    found = picked(table, agg[...]).astype(f32)
    node_row[...] = found
    for t, (out, wide) in enumerate(((up, ROWS - WIDE), (down, 0))):
        for i in range(3):
            for j in range(3):
                g = 3 * i + j
                out[g * FULL : (g + 1) * FULL, :] = blk[t, i, j, 0:FULL, :]
                out[P_BTAIL + 3 * g : P_BTAIL + 3 * g + 3, :] = blk[t, i, j, FULL:SLOTS, :]
        out[P_COL : P_COL + FULL, :] = col[t, 0:FULL, :].astype(f32)
        out[P_CTAIL : P_CTAIL + 3, :] = col[t, FULL:SLOTS, :].astype(f32)
        for h in range(2):
            out[P_RHS + 3 * h : P_RHS + 3 * h + 3, :] = rhs[:, lanes(wide + HALO * h, HALO)]
            out[P_DIA + 3 * h : P_DIA + 3 * h + 3, :] = dia[:, lanes(wide + HALO * h, HALO)]
            for q in range(2):
                s = wide // LANES + 2 * h + q
                out[P_ROW + h : P_ROW + h + 1, lanes(LANES * q)] = found[s : s + 1, :]
        out[P_ROW + 2 : P_ALL, :] = jnp.zeros((P_ALL - P_ROW - 2, HALO), f32)


def pulled_block(columns, blocks, table, first_chunk):
    total = [None, None, None]
    for part in range(4):
        where = columns(part)
        chunk = lax.shift_right_arithmetic(where, 7)
        lane = lax.bitwise_and(where, 127)
        near = [jnp.zeros(where.shape, f32) for _ in range(3)]
        for c in range(5):
            here = chunk == c
            for j in range(3):
                row = table[j : j + 1, lanes(first_chunk * LANES + c * LANES)]
                near[j] = jnp.where(here, picked(row, lane), near[j])
        for i in range(3):
            s = blocks(i, 0, part) * near[0]
            s = s + blocks(i, 1, part) * near[1]
            s = s + blocks(i, 2, part) * near[2]
            if part < 3:
                total[i] = s if total[i] is None else total[i] + s
            else:
                total[i] = jnp.sum(total[i], axis=0, keepdims=True) + jnp.sum(
                    s, axis=0, keepdims=True
                )
    return total


def local_getters(col, blk, start, b):
    def columns(part):
        lo, hi = 8 * part, min(8 * part + 8, SLOTS)
        return col[lo:hi, lanes(b * LANES)] - start

    def blocks(i, j, part):
        lo, hi = 8 * part, min(8 * part + 8, SLOTS)
        return blk[i, j, lo:hi, lanes(b * LANES)]

    return columns, blocks


def halo_getters(halo, start, b):
    def columns(part):
        if part < 3:
            got = halo[P_COL + 8 * part : P_COL + 8 * part + 8, lanes(b * LANES)]
        else:
            got = halo[P_CTAIL : P_CTAIL + 3, lanes(b * LANES)]
        return got.astype(i32) - start

    def blocks(i, j, part):
        g = 3 * i + j
        if part < 3:
            return halo[g * FULL + 8 * part : g * FULL + 8 * part + 8, lanes(b * LANES)]
        return halo[P_BTAIL + 3 * g : P_BTAIL + 3 * g + 3, lanes(b * LANES)]

    return columns, blocks


def wide_vector(out, local, before, after, row):
    out[:, lanes(WIDE, ROWS)] = local[...]
    for h in range(2):
        out[:, lanes(HALO * h, HALO)] = before[row + 3 * h : row + 3 * h + 3, :]
        out[:, lanes(WIDE + ROWS + HALO * h, HALO)] = after[row + 3 * h : row + 3 * h + 3, :]


def smoothed(table, pulled, rhs, dia, at):
    pull = jnp.concatenate(pulled, axis=0)
    s = table[:, lanes(at)]
    b = rhs[:, lanes(at)]
    d = dia[:, lanes(at)]
    return s + damping * (b - (d * s - pull)) / d


def sweep_halo(out, table, rhs, dia, halo, base, first):
    for b in range(2):
        at = first + LANES * b
        start = base + (at - WIDE) - 2 * LANES
        cols, blks = halo_getters(halo, start, b)
        pull = pulled_block(cols, blks, table, at // LANES - 2)
        out[:, lanes(at)] = smoothed(table, pull, rhs, dia, at)


def own_block(table, col, blk, base, b):
    start = base + b * LANES - 2 * LANES
    cols, blks = local_getters(col, blk, start, b)
    return pulled_block(cols, blks, table, b + WIDE // LANES - 2)


def pre_kernel(base_ref, rhs, dia, col, blk, agg, owner_row, cdia, before, after,
               send, first_iter, keep_rhs, keep_dia, up2, down2, one, two, res):
    base = base_ref[0]
    wide_vector(keep_rhs, rhs, before, after, P_RHS)
    wide_vector(keep_dia, dia, before, after, P_DIA)
    raw = keep_dia[...]
    keep_dia[...] = jnp.where(raw == 0.0, 1.0, raw)
    one[...] = damping * keep_rhs[...] / keep_dia[...]
    two[...] = jnp.zeros(two.shape, f32)
    sweep_halo(two, one, keep_rhs, keep_dia, before, base, WIDE - HALO)
    sweep_halo(two, one, keep_rhs, keep_dia, after, base, WIDE + ROWS)

    def second(b, carry):
        at = WIDE + b * LANES
        pull = own_block(one, col, blk, base, b)
        two[:, lanes(at)] = smoothed(one, pull, keep_rhs, keep_dia, at)
        return carry

    lax.fori_loop(0, BLOCKS, second, 0)

    def third(b, carry):
        at = WIDE + b * LANES
        pull = jnp.concatenate(own_block(two, col, blk, base, b), axis=0)
        s, d = two[:, lanes(at)], keep_dia[:, lanes(at)]
        res[0:3, lanes(b * LANES)] = keep_rhs[:, lanes(at)] - (d * s - pull)
        return carry

    res[...] = jnp.zeros(res.shape, f32)
    lax.fori_loop(0, BLOCKS, third, 0)
    first_iter[...] = two[...]
    up2[...] = two[:, lanes(WIDE + ROWS - WIDE, HALO)]
    down2[...] = two[:, lanes(WIDE + HALO, HALO)]
    label = lax.broadcasted_iota(i32, (32, LANES), 0)
    sums = None
    for b in range(BLOCKS):
        member = (label == jnp.broadcast_to(agg[b : b + 1, :], (32, LANES))).astype(f32)
        part = lax.dot_general(
            res[:, lanes(b * LANES)], member, (((1,), (1,)), ((), ())),
            precision=highest, preferred_element_type=f32,
        )
        sums = part if sums is None else sums + part
    row = jnp.concatenate(
        [sums[0:1], sums[1:2], sums[2:3], owner_row[...].astype(f32)], axis=1
    )
    send[:, 0, :] = jnp.broadcast_to(row, (LANES, LANES))
    row = jnp.concatenate(
        [cdia[0:1], cdia[1:2], cdia[2:3], jnp.ones((1, 32), f32)], axis=1
    )
    send[:, 1, :] = jnp.broadcast_to(row, (LANES, LANES))


def lane_of_device(p, me):
    p = lax.bitwise_xor(p, lax.bitwise_and(me, 3))
    return lax.shift_left(lax.bitwise_and(p, 3), 5) + lax.shift_right_logical(p, 2)


def device_of_lane(q, me):
    p = lax.shift_left(lax.bitwise_and(q, 31), 2) + lax.shift_right_logical(q, 5)
    return lax.bitwise_xor(p, lax.bitwise_and(me, 3))


def coarse_pack_kernel(col, blk, send):
    def folded(a):
        z = jnp.concatenate([a, jnp.zeros((32, 5), f32)], axis=1)
        z = jnp.transpose(z)
        return jnp.concatenate([z[8 * k : 8 * k + 8, :] for k in range(4)], axis=1)

    parts = [folded(blk[i, j]) for i in range(3) for j in range(3)]
    parts.append(folded(col[...].astype(f32)))
    for m in range(10):
        for d in range(PEERS):
            send[d, 8 * m : 8 * m + 8, :] = parts[m]


def spread(parts):
    group = lax.shift_right_logical(lax.broadcasted_iota(i32, parts[0].shape, 1), 5)
    return jnp.where(group == 0, parts[0], jnp.where(group == 1, parts[1], parts[2]))


def coarse_lookup(table, chunk, lane):
    near = [jnp.zeros(chunk.shape, f32) for _ in range(3)]
    for c in range(32):
        here = chunk == c
        for j in range(3):
            row = table[32 * j + c : 32 * j + c + 1, :]
            near[j] = jnp.where(here, picked(row, lane), near[j])
    return near


def coarse_step(table, where, data, own, rhs, dia, gather):
    def some(t, carry):
        for u in range(UNROLL):
            d = t * UNROLL + u
            w = where[d]
            near = coarse_lookup(table, lax.bitwise_and(w, 31), lax.shift_right_logical(w, 5))
            for i in range(3):
                a = data[d, lanes8(3 * i), :] * near[0]
                a = a + data[d, lanes8(3 * i + 1), :] * near[1]
                a = a + data[d, lanes8(3 * i + 2), :] * near[2]
                gather[i, pl.ds(d, 1), :] = jnp.sum(a, axis=0, keepdims=True)
        return carry

    lax.fori_loop(0, PEERS // UNROLL, some, 0)
    parts = []
    for i in range(3):
        s = gather[i]
        s = s + pltpu.roll(s, 64, axis=1)
        parts.append(s + pltpu.roll(s, 32, axis=1))
    return own + damping * (rhs - (dia * own - spread(parts))) / dia


def lanes8(m):
    return slice(8 * m, 8 * m + 8)


def coarse_first_kernel(me_ref, sums, data, far_up, far_down, new, rhs, dia, where,
                        table, gather, left, right):
    me = me_ref[0]
    got = jnp.transpose(sums[:, 0, :])
    rows = got[96:128].astype(i32)
    s = got[0:96]
    split = []
    for _ in range(3):
        t = s.astype(jnp.bfloat16).astype(f32)
        split.append(t)
        s = s - t
    chunk = lax.broadcasted_iota(i32, (32, LANES), 0)
    place = lax.broadcasted_iota(i32, (LANES, LANES), 0)
    low = lax.bitwise_and(rows, 31)
    lane = lane_of_device(lax.shift_right_logical(rows, 5), me)
    for a in range(32):
        here = chunk == jnp.broadcast_to(low[a : a + 1], (32, LANES))
        for t in range(3):
            for i in range(3):
                value = jnp.broadcast_to(split[t][32 * i + a : 32 * i + a + 1], (32, LANES))
                left[96 * t + 32 * i : 96 * t + 32 * i + 32, lanes(LANES * a)] = jnp.where(
                    here, value, 0.0
                ).astype(jnp.bfloat16)
        right[:, lanes(LANES * a)] = jnp.where(
            place == jnp.broadcast_to(lane[a : a + 1], (LANES, LANES)), 1.0, 0.0
        ).astype(jnp.bfloat16)
    both = lax.dot_general(
        left[...], right[...], (((1,), (1,)), ((), ())), preferred_element_type=f32
    )
    crhs = both[0:96] + both[96:192] + both[192:288]
    order = device_of_lane(lax.broadcasted_iota(i32, (96, LANES), 1), me)
    cdia = jnp.take_along_axis(
        jnp.transpose(sums[:, 1, :])[0:96], order, axis=1, mode="promise_in_bounds"
    )
    pad = jnp.zeros((32, LANES), f32)
    first = jnp.concatenate([damping * crhs / cdia, pad], axis=0)
    table[...] = first
    own = jnp.transpose(first)[0:PEERS]
    rhs[...] = jnp.transpose(jnp.concatenate([crhs, pad], axis=0))[0:PEERS]
    dia[...] = jnp.transpose(jnp.concatenate([cdia, pad + 1.0], axis=0))[0:PEERS]
    for d in range(PEERS):
        c = data[d, 72:80, :].astype(i32)
        at = lane_of_device(lax.shift_right_logical(c, 5), me)
        where[d] = lax.bitwise_and(c, 31) + lax.shift_left(at, 5)
    new[...] = coarse_step(table, where, data, own, rhs[...], dia[...], gather)


def gathered(table, pieces, mine):
    row = 0
    for piece in pieces:
        size = piece.shape[0]
        mine[row : row + size, :] = piece[...]
        row += size
    table[...] = jnp.transpose(mine[...])


def coarse_kernel(me_ref, p0, p1, p2, rhs, dia, where, data, new, correction,
                  table, mine, gather):
    gathered(table, (p0, p1, p2), mine)
    got = coarse_step(table, where, data, p0[...], rhs[...], dia[...], gather)
    new[...] = got
    mine[0:PEERS, :] = got
    me = me_ref[0]
    at = lane_of_device(me, me)
    row = mine[pl.ds(at, 1), :]
    correction[...] = jnp.concatenate([row[:, 32 * i : 32 * i + 32] for i in range(3)], axis=0)


def post_kernel(base_ref, p0, p1, p2, first_iter, rhs, dia, col, blk, node_row, before, after,
                before2, after2, out, table, mine, one, two):
    base = base_ref[0]
    me = lax.shift_right_logical(base, 10)
    gathered(table, (p0, p1, p2), mine)
    one[...] = first_iter[...]
    one[:, lanes(0, HALO)] = before2[...]
    one[:, lanes(WIDE + ROWS + HALO, HALO)] = after2[...]
    edge = [
        h[P_ROW + t : P_ROW + t + 1, lanes(LANES * q)]
        for h in (before, after) for t in range(2) for q in range(2)
    ]
    edge = jnp.concatenate(edge, axis=0)

    def found(rows):
        rows = rows.astype(i32)
        lane = lane_of_device(lax.shift_right_logical(rows, 5), me)
        return coarse_lookup(table, lax.bitwise_and(rows, 31), lane)

    own, far = found(node_row[...]), found(edge)
    for s in range(16):
        if s < 4:
            row = [f[s : s + 1, :] for f in far]
        elif s < 12:
            row = [f[s - 4 : s - 3, :] for f in own]
        else:
            row = [f[s - 8 : s - 7, :] for f in far]
        one[:, lanes(s * LANES)] = one[:, lanes(s * LANES)] + jnp.concatenate(row, axis=0)
    two[...] = jnp.zeros(two.shape, f32)
    sweep_halo(two, one, rhs, dia, before, base, WIDE - HALO)
    sweep_halo(two, one, rhs, dia, after, base, WIDE + ROWS)

    def first(b, carry):
        at = WIDE + b * LANES
        pull = own_block(one, col, blk, base, b)
        two[:, lanes(at)] = smoothed(one, pull, rhs, dia, at)
        return carry

    def second(b, carry):
        at = WIDE + b * LANES
        pull = own_block(two, col, blk, base, b)
        out[:, lanes(b * LANES)] = smoothed(two, pull, rhs, dia, at)
        return carry

    lax.fori_loop(0, BLOCKS, first, 0)
    lax.fori_loop(0, BLOCKS, second, 0)


def call(kernel, outs, args, scratch=(), scalar=False):
    vmem = pl.BlockSpec(memory_space=pltpu.VMEM)
    specs = [vmem] * len(args)
    if scalar:
        specs[0] = pl.BlockSpec(memory_space=pltpu.SMEM)
    return pl.pallas_call(
        kernel,
        in_specs=specs,
        out_specs=[vmem] * len(outs),
        out_shape=[jax.ShapeDtypeStruct(o, t) for o, t in outs],
        scratch_shapes=[
            pltpu.VMEM(*s) if isinstance(s[0], tuple) else pltpu.VMEM(s, f32) for s in scratch
        ],
        compiler_params=pltpu.CompilerParams(vmem_limit_bytes=12 * 2**20),
    )(*args)


def in_group(new):
    swap = [(0, 1), (1, 0)]
    p1 = lax.ppermute(new, "dom_5", swap)
    a = jnp.concatenate([new, p1], axis=0)
    p2 = lax.ppermute(a, "dom_4", swap)
    return new, p1, p2


def shifts(up, down):
    count = lax.axis_size(DOM)
    forward = [(i, i + 1) for i in range(count - 1)]
    backward = [(i + 1, i) for i in range(count - 1)]
    return lax.ppermute(up, DOM, forward), lax.ppermute(down, DOM, backward)


def cycle(right_side, fine_diagonal, fine_columns, fine_blocks, aggregate_of_node,
         coarse_row_of_aggregate, coarse_diagonal, coarse_columns, coarse_blocks):
    rhs, dia = right_side.T, fine_diagonal.T
    col, blk = fine_columns.T, fine_blocks.transpose(2, 3, 1, 0)
    agg = aggregate_of_node.reshape(8, LANES)
    owner = coarse_row_of_aggregate.reshape(1, 32)
    cdia, cblk = coarse_diagonal.T, coarse_blocks.transpose(2, 3, 0, 1)
    me = lax.axis_index(DOM).astype(i32).reshape(1)
    base = me * ROWS
    wide = WIDE + ROWS + WIDE

    dsend, = call(coarse_pack_kernel, [((PEERS, 80, LANES), f32)], [coarse_columns, cblk])
    data = lax.all_to_all(dsend, OTHERS, 0, 0, tiled=True)
    vmem, far = pl.BlockSpec(memory_space=pltpu.VMEM), pl.BlockSpec(memory_space=pltpu.HBM)
    up, down, node_row = pl.pallas_call(
        pack_kernel,
        name="pack",
        in_specs=[far] * 6,
        out_specs=[vmem] * 3,
        out_shape=[jax.ShapeDtypeStruct(o, f32) for o in ((P_ALL, HALO), (P_ALL, HALO), (8, LANES))],
        scratch_shapes=[
            pltpu.VMEM((3, ROWS), f32), pltpu.VMEM((3, ROWS), f32),
            pltpu.VMEM((2, SLOTS, HALO), i32), pltpu.VMEM((2, 3, 3, SLOTS, HALO), f32),
            pltpu.VMEM((8, LANES), i32), pltpu.VMEM((1, 32), i32), pltpu.SemaphoreType.DMA((8,)),
        ],
        compiler_params=pltpu.CompilerParams(vmem_limit_bytes=12 * 2**20),
    )(rhs, dia, col, blk, agg, owner)
    before, after = shifts(up, down)
    send, first_iter, wrhs, wdia, up2, down2 = call(
        pre_kernel,
        [((LANES, 2, LANES), f32), ((3, wide), f32), ((3, wide), f32), ((3, wide), f32),
         ((3, HALO), f32), ((3, HALO), f32)],
        [base, rhs, dia, col, blk, agg, owner, cdia, before, after],
        scratch=[(3, wide), (3, wide), (8, ROWS)], scalar=True,
    )
    before2, after2 = shifts(up2, down2)
    sums = lax.all_to_all(send, DOM, 0, 0, tiled=True)
    peers = ((PEERS, LANES), f32)
    gather = (3, PEERS, LANES)
    square = (LANES, LANES)
    new, crhs, cd, where = call(
        coarse_first_kernel,
        [peers, peers, peers, ((PEERS, 8, LANES), i32)],
        [me, sums, data, before2, after2],
        scratch=[square, gather, ((288, 4096), jnp.bfloat16), ((LANES, 4096), jnp.bfloat16)],
        scalar=True,
    )
    for _ in range(CSWEEPS - 2):
        new, mine = call(
            coarse_kernel, [peers, ((3, 32), f32)],
            [me, *in_group(new), crhs, cd, where, data],
            scratch=[square, square, gather], scalar=True,
        )
    solution, = call(
        post_kernel, [((3, ROWS), f32)],
        [base, *in_group(new), first_iter, wrhs, wdia, col, blk, node_row,
         before, after, before2, after2],
        scratch=[square, square, (3, wide), (3, wide)], scalar=True,
    )
    return solution.T, mine.T


def solution(mesh):
    torus = Mesh(mesh.devices.reshape(4, 2, 2, 2, 2, 2), DOM)
    return jax.shard_map(
        cycle,
        mesh=torus,
        in_specs=(
            P(DOM, None),
            P(DOM, None),
            P(DOM, None),
            P(DOM, None, None, None),
            P(DOM),
            P(DOM),
            P(DOM, None),
            P(DOM, None),
            P(DOM, None, None, None),
        ),
        out_specs=(P(DOM, None), P(DOM, None)),
        check_vma=False,
    )
```

```python
import jax
import jax.numpy as jnp
from jax import lax
from jax.experimental import pallas as pl
from jax.experimental.pallas import tpu as pltpu
from jax.sharding import Mesh
from jax.sharding import PartitionSpec as P


DOM = ("dom_0", "dom_1", "dom_2", "dom_3", "dom_4", "dom_5")
OTHERS = ("dom_0", "dom_1", "dom_2", "dom_3")
PEERS = 32
UNROLL = 2
CSWEEPS = 6
damping = 0.7
highest = lax.Precision.HIGHEST

ROWS = 1024
LANES = 128
SLOTS = 27
FULL = 24
HALO = 256
WIDE = 512
BLOCKS = ROWS // LANES
P_COL = 9 * FULL
P_BTAIL = P_COL + FULL
P_CTAIL = P_BTAIL + 27
P_RHS = P_CTAIL + 3
P_DIA = P_RHS + 6
P_ROW = P_DIA + 6
P_ALL = 288
f32 = jnp.float32
i32 = jnp.int32


def lanes(start, size=LANES):
    if isinstance(start, int):
        return slice(start, start + size)
    return pl.ds(pl.multiple_of(start, LANES), size)


def picked(row, where):
    return jnp.take_along_axis(
        jnp.broadcast_to(row, where.shape), where, axis=1, mode="promise_in_bounds"
    )


def pack_kernel(rhs_in, dia_in, col_in, blk_in, agg_in, owner_in, up, down, node_row,
                rhs, dia, col, blk, agg, owner, sem):
    copies = [(rhs_in, rhs), (dia_in, dia), (agg_in, agg), (owner_in, owner)]
    for t, near in enumerate((ROWS - HALO, 0)):
        copies.append((col_in.at[:, lanes(near, HALO)], col.at[t]))
        copies.append((blk_in.at[:, :, :, lanes(near, HALO)], blk.at[t]))
    copies = [pltpu.make_async_copy(a, b, sem.at[n]) for n, (a, b) in enumerate(copies)]
    for c in copies:
        c.start()
    for c in copies:
        c.wait()
    table = jnp.concatenate([owner[...]] * 4, axis=1)
    found = picked(table, agg[...]).astype(f32)
    node_row[...] = found
    for t, (out, wide) in enumerate(((up, ROWS - WIDE), (down, 0))):
        for i in range(3):
            for j in range(3):
                g = 3 * i + j
                out[g * FULL : (g + 1) * FULL, :] = blk[t, i, j, 0:FULL, :]
                out[P_BTAIL + 3 * g : P_BTAIL + 3 * g + 3, :] = blk[t, i, j, FULL:SLOTS, :]
        out[P_COL : P_COL + FULL, :] = col[t, 0:FULL, :].astype(f32)
        out[P_CTAIL : P_CTAIL + 3, :] = col[t, FULL:SLOTS, :].astype(f32)
        for h in range(2):
            out[P_RHS + 3 * h : P_RHS + 3 * h + 3, :] = rhs[:, lanes(wide + HALO * h, HALO)]
            out[P_DIA + 3 * h : P_DIA + 3 * h + 3, :] = dia[:, lanes(wide + HALO * h, HALO)]
            for q in range(2):
                s = wide // LANES + 2 * h + q
                out[P_ROW + h : P_ROW + h + 1, lanes(LANES * q)] = found[s : s + 1, :]
        out[P_ROW + 2 : P_ALL, :] = jnp.zeros((P_ALL - P_ROW - 2, HALO), f32)


def pulled_block(columns, blocks, table, first_chunk):
    total = [None, None, None]
    for part in range(4):
        where = columns(part)
        chunk = lax.shift_right_arithmetic(where, 7)
        lane = lax.bitwise_and(where, 127)
        near = [jnp.zeros(where.shape, f32) for _ in range(3)]
        for c in range(5):
            here = chunk == c
            for j in range(3):
                row = table[j : j + 1, lanes(first_chunk * LANES + c * LANES)]
                near[j] = jnp.where(here, picked(row, lane), near[j])
        for i in range(3):
            s = blocks(i, 0, part) * near[0]
            s = s + blocks(i, 1, part) * near[1]
            s = s + blocks(i, 2, part) * near[2]
            if part < 3:
                total[i] = s if total[i] is None else total[i] + s
            else:
                total[i] = jnp.sum(total[i], axis=0, keepdims=True) + jnp.sum(
                    s, axis=0, keepdims=True
                )
    return total


def local_getters(col, blk, start, b):
    def columns(part):
        lo, hi = 8 * part, min(8 * part + 8, SLOTS)
        return col[lo:hi, lanes(b * LANES)] - start

    def blocks(i, j, part):
        lo, hi = 8 * part, min(8 * part + 8, SLOTS)
        return blk[i, j, lo:hi, lanes(b * LANES)]

    return columns, blocks


def halo_getters(halo, start, b):
    def columns(part):
        if part < 3:
            got = halo[P_COL + 8 * part : P_COL + 8 * part + 8, lanes(b * LANES)]
        else:
            got = halo[P_CTAIL : P_CTAIL + 3, lanes(b * LANES)]
        return got.astype(i32) - start

    def blocks(i, j, part):
        g = 3 * i + j
        if part < 3:
            return halo[g * FULL + 8 * part : g * FULL + 8 * part + 8, lanes(b * LANES)]
        return halo[P_BTAIL + 3 * g : P_BTAIL + 3 * g + 3, lanes(b * LANES)]

    return columns, blocks


def wide_vector(out, local, before, after, row):
    out[:, lanes(WIDE, ROWS)] = local[...]
    for h in range(2):
        out[:, lanes(HALO * h, HALO)] = before[row + 3 * h : row + 3 * h + 3, :]
        out[:, lanes(WIDE + ROWS + HALO * h, HALO)] = after[row + 3 * h : row + 3 * h + 3, :]


def smoothed(table, pulled, rhs, dia, at):
    pull = jnp.concatenate(pulled, axis=0)
    s = table[:, lanes(at)]
    b = rhs[:, lanes(at)]
    d = dia[:, lanes(at)]
    return s + damping * (b - (d * s - pull)) / d


def sweep_halo(out, table, rhs, dia, halo, base, first):
    for b in range(2):
        at = first + LANES * b
        start = base + (at - WIDE) - 2 * LANES
        cols, blks = halo_getters(halo, start, b)
        pull = pulled_block(cols, blks, table, at // LANES - 2)
        out[:, lanes(at)] = smoothed(table, pull, rhs, dia, at)


def each_block(step):
    def some(t, carry):
        for u in range(UNROLL):
            step(t * UNROLL + u)
        return carry

    lax.fori_loop(0, BLOCKS // UNROLL, some, 0)


def own_block(table, col, blk, base, b):
    start = base + b * LANES - 2 * LANES
    cols, blks = local_getters(col, blk, start, b)
    return pulled_block(cols, blks, table, b + WIDE // LANES - 2)


def pre_kernel(base_ref, rhs, dia, col, blk, agg, owner_row, cdia, before, after,
               send, first_iter, keep_rhs, keep_dia, up2, down2, one, two, res):
    base = base_ref[0]
    wide_vector(keep_rhs, rhs, before, after, P_RHS)
    wide_vector(keep_dia, dia, before, after, P_DIA)
    raw = keep_dia[...]
    keep_dia[...] = jnp.where(raw == 0.0, 1.0, raw)
    one[...] = damping * keep_rhs[...] / keep_dia[...]
    two[...] = jnp.zeros(two.shape, f32)
    sweep_halo(two, one, keep_rhs, keep_dia, before, base, WIDE - HALO)
    sweep_halo(two, one, keep_rhs, keep_dia, after, base, WIDE + ROWS)

    def second(b):
        at = WIDE + b * LANES
        pull = own_block(one, col, blk, base, b)
        two[:, lanes(at)] = smoothed(one, pull, keep_rhs, keep_dia, at)

    each_block(second)

    def third(b):
        at = WIDE + b * LANES
        pull = jnp.concatenate(own_block(two, col, blk, base, b), axis=0)
        s, d = two[:, lanes(at)], keep_dia[:, lanes(at)]
        res[0:3, lanes(b * LANES)] = keep_rhs[:, lanes(at)] - (d * s - pull)

    res[...] = jnp.zeros(res.shape, f32)
    each_block(third)
    first_iter[...] = two[...]
    up2[...] = two[:, lanes(WIDE + ROWS - WIDE, HALO)]
    down2[...] = two[:, lanes(WIDE + HALO, HALO)]
    label = lax.broadcasted_iota(i32, (32, LANES), 0)
    sums = None
    for b in range(BLOCKS):
        member = (label == jnp.broadcast_to(agg[b : b + 1, :], (32, LANES))).astype(f32)
        part = lax.dot_general(
            res[:, lanes(b * LANES)], member, (((1,), (1,)), ((), ())),
            precision=highest, preferred_element_type=f32,
        )
        sums = part if sums is None else sums + part
    row = jnp.concatenate(
        [sums[0:1], sums[1:2], sums[2:3], owner_row[...].astype(f32)], axis=1
    )
    send[:, 0, :] = jnp.broadcast_to(row, (LANES, LANES))
    row = jnp.concatenate(
        [cdia[0:1], cdia[1:2], cdia[2:3], jnp.ones((1, 32), f32)], axis=1
    )
    send[:, 1, :] = jnp.broadcast_to(row, (LANES, LANES))


def lane_of_device(p, me):
    p = lax.bitwise_xor(p, lax.bitwise_and(me, 3))
    return lax.shift_left(lax.bitwise_and(p, 3), 5) + lax.shift_right_logical(p, 2)


def device_of_lane(q, me):
    p = lax.shift_left(lax.bitwise_and(q, 31), 2) + lax.shift_right_logical(q, 5)
    return lax.bitwise_xor(p, lax.bitwise_and(me, 3))


def coarse_pack_kernel(col, blk, send):
    def turned(a):
        z = jnp.transpose(jnp.concatenate([a, jnp.zeros((32, 5), f32)], axis=1))
        return jnp.concatenate([z] * 4, axis=1)

    columns = turned(col[...].astype(f32))
    kind = lax.bitwise_and(columns.astype(i32), 7)
    tile = (8, LANES)
    sub = lax.broadcasted_iota(i32, tile, 0)
    count = jnp.zeros(tile, i32)
    match, earlier = [], []
    for k in range(SLOTS):
        here = sub == jnp.broadcast_to(kind[k : k + 1], tile)
        match.append(here)
        earlier.append(count)
        count = count + here.astype(i32)
    left = jnp.zeros((1, LANES), i32)
    start = []
    for n in range(16):
        if n >= 8:
            start.append(left)
        left = jnp.maximum(left + count[n % 8 : n % 8 + 1] - 4, 0)
    start = jnp.concatenate(start, axis=0) + 4 * sub
    place = 4 * sub + lax.shift_right_logical(lax.broadcasted_iota(i32, tile, 1), 5)
    slot = jnp.full(tile, 31, i32)
    for k in range(SLOTS):
        at = jnp.sum(jnp.where(match[k], start + earlier[k], 0), axis=0, keepdims=True)
        slot = jnp.where(place == jnp.broadcast_to(lax.bitwise_and(at, 31), tile), k, slot)
    inner, outer = lax.bitwise_and(slot, 7), lax.shift_right_logical(slot, 3)

    def placed(z):
        got = None
        for g in range(4):
            part = jnp.take_along_axis(
                z[8 * g : 8 * g + 8], inner, axis=0, mode="promise_in_bounds"
            )
            got = part if got is None else jnp.where(outer == g, part, got)
        return got

    parts = [placed(turned(blk[i, j])) for i in range(3) for j in range(3)]
    parts.append(jnp.where(slot == 31, sub.astype(f32), placed(columns)))
    for m in range(10):
        for d in range(PEERS):
            send[d, 8 * m : 8 * m + 8, :] = parts[m]


def spread(parts):
    group = lax.shift_right_logical(lax.broadcasted_iota(i32, parts[0].shape, 1), 5)
    return jnp.where(group == 0, parts[0], jnp.where(group == 1, parts[1], parts[2]))


def coarse_lookup(table, chunk, lane):
    near = [jnp.zeros(chunk.shape, f32) for _ in range(3)]
    for c in range(32):
        here = chunk == c
        for j in range(3):
            row = table[32 * j + c : 32 * j + c + 1, :]
            near[j] = jnp.where(here, picked(row, lane), near[j])
    return near


def coarse_step(table, where, passes, data, own, rhs, dia, gather):
    gather[...] = jnp.zeros(gather.shape, f32)

    def one_pass(t, carry):
        rows = [
            [pltpu.roll(table[32 * j + 8 * v : 32 * j + 8 * v + 8, :], t, axis=0) for v in range(4)]
            for j in range(3)
        ]
        for d in range(PEERS):
            w = where[d]
            code, lane = lax.bitwise_and(w, 31), lax.shift_right_logical(w, 5)
            near = [jnp.zeros((8, LANES), f32) for _ in range(3)]
            for v in range(4):
                here = code == 4 * t + v
                for j in range(3):
                    near[j] = jnp.where(here, picked(rows[j][v], lane), near[j])
            for i in range(3):
                a = data[d, lanes8(3 * i), :] * near[0]
                a = a + data[d, lanes8(3 * i + 1), :] * near[1]
                a = a + data[d, lanes8(3 * i + 2), :] * near[2]
                gather[i, d : d + 1, :] += jnp.sum(a, axis=0, keepdims=True)
        return carry

    lax.fori_loop(0, passes, one_pass, 0)
    parts = []
    for i in range(3):
        s = gather[i]
        s = s + pltpu.roll(s, 64, axis=1)
        parts.append(s + pltpu.roll(s, 32, axis=1))
    return own + damping * (rhs - (dia * own - spread(parts))) / dia


def lanes8(m):
    return slice(8 * m, 8 * m + 8)


def coarse_first_kernel(me_ref, sums, data, far_up, far_down, new, rhs, dia, where, passes,
                        table, gather, left, right):
    me = me_ref[0]
    got = jnp.transpose(sums[:, 0, :])
    rows = got[96:128].astype(i32)
    s = got[0:96]
    split = []
    for _ in range(3):
        t = s.astype(jnp.bfloat16).astype(f32)
        split.append(t)
        s = s - t
    chunk = lax.broadcasted_iota(i32, (32, LANES), 0)
    place = lax.broadcasted_iota(i32, (LANES, LANES), 0)
    low = lax.bitwise_and(rows, 31)
    lane = lane_of_device(lax.shift_right_logical(rows, 5), me)
    for a in range(32):
        here = chunk == jnp.broadcast_to(low[a : a + 1], (32, LANES))
        for t in range(3):
            for i in range(3):
                value = jnp.broadcast_to(split[t][32 * i + a : 32 * i + a + 1], (32, LANES))
                left[96 * t + 32 * i : 96 * t + 32 * i + 32, lanes(LANES * a)] = jnp.where(
                    here, value, 0.0
                ).astype(jnp.bfloat16)
        right[:, lanes(LANES * a)] = jnp.where(
            place == jnp.broadcast_to(lane[a : a + 1], (LANES, LANES)), 1.0, 0.0
        ).astype(jnp.bfloat16)
    both = lax.dot_general(
        left[...], right[...], (((1,), (1,)), ((), ())), preferred_element_type=f32
    )
    crhs = both[0:96] + both[96:192] + both[192:288]
    order = device_of_lane(lax.broadcasted_iota(i32, (96, LANES), 1), me)
    cdia = jnp.take_along_axis(
        jnp.transpose(sums[:, 1, :])[0:96], order, axis=1, mode="promise_in_bounds"
    )
    pad = jnp.zeros((32, LANES), f32)
    first = jnp.concatenate([damping * crhs / cdia, pad], axis=0)
    table[...] = first
    own = jnp.transpose(first)[0:PEERS]
    rhs[...] = jnp.transpose(jnp.concatenate([crhs, pad], axis=0))[0:PEERS]
    dia[...] = jnp.transpose(jnp.concatenate([cdia, pad + 1.0], axis=0))[0:PEERS]
    sub = lax.broadcasted_iota(i32, (8, LANES), 0)
    most = jnp.zeros((8, LANES), i32)
    for d in range(PEERS):
        c = data[d, 72:80, :].astype(i32)
        off = lax.bitwise_and(sub - c, 7)
        most = jnp.maximum(most, off)
        at = lane_of_device(lax.shift_right_logical(c, 5), me)
        code = lax.bitwise_and(lax.shift_right_logical(c, 3), 3) + lax.shift_left(off, 2)
        where[d] = code + lax.shift_left(at, 5)
    passes[0] = jnp.max(most) + 1
    new[...] = coarse_step(
        table, where, passes[0], data, own, rhs[...], dia[...], gather
    )


def gathered(table, pieces, mine):
    row = 0
    for piece in pieces:
        size = piece.shape[0]
        mine[row : row + size, :] = piece[...]
        row += size
    table[...] = jnp.transpose(mine[...])


def coarse_kernel(me_ref, passes, p0, p1, p2, rhs, dia, where, data, new, correction,
                  table, mine, gather):
    gathered(table, (p0, p1, p2), mine)
    got = coarse_step(table, where, passes[0], data, p0[...], rhs[...], dia[...], gather)
    new[...] = got
    mine[0:PEERS, :] = got
    me = me_ref[0]
    at = lane_of_device(me, me)
    row = mine[pl.ds(at, 1), :]
    correction[...] = jnp.concatenate([row[:, 32 * i : 32 * i + 32] for i in range(3)], axis=0)


def post_kernel(base_ref, p0, p1, p2, first_iter, rhs, dia, col, blk, node_row, before, after,
                before2, after2, out, table, mine, one, two):
    base = base_ref[0]
    me = lax.shift_right_logical(base, 10)
    gathered(table, (p0, p1, p2), mine)
    one[...] = first_iter[...]
    one[:, lanes(0, HALO)] = before2[...]
    one[:, lanes(WIDE + ROWS + HALO, HALO)] = after2[...]
    edge = [
        h[P_ROW + t : P_ROW + t + 1, lanes(LANES * q)]
        for h in (before, after) for t in range(2) for q in range(2)
    ]
    edge = jnp.concatenate(edge, axis=0)

    def found(rows):
        rows = rows.astype(i32)
        lane = lane_of_device(lax.shift_right_logical(rows, 5), me)
        return coarse_lookup(table, lax.bitwise_and(rows, 31), lane)

    own, far = found(node_row[...]), found(edge)
    for s in range(16):
        if s < 4:
            row = [f[s : s + 1, :] for f in far]
        elif s < 12:
            row = [f[s - 4 : s - 3, :] for f in own]
        else:
            row = [f[s - 8 : s - 7, :] for f in far]
        one[:, lanes(s * LANES)] = one[:, lanes(s * LANES)] + jnp.concatenate(row, axis=0)
    two[...] = jnp.zeros(two.shape, f32)
    sweep_halo(two, one, rhs, dia, before, base, WIDE - HALO)
    sweep_halo(two, one, rhs, dia, after, base, WIDE + ROWS)

    def first(b):
        at = WIDE + b * LANES
        pull = own_block(one, col, blk, base, b)
        two[:, lanes(at)] = smoothed(one, pull, rhs, dia, at)

    def second(b):
        at = WIDE + b * LANES
        pull = own_block(two, col, blk, base, b)
        out[:, lanes(b * LANES)] = smoothed(two, pull, rhs, dia, at)

    each_block(first)
    each_block(second)


def call(kernel, outs, args, scratch=(), scalars=0, scalar_outs=0):
    vmem = pl.BlockSpec(memory_space=pltpu.VMEM)
    smem = pl.BlockSpec(memory_space=pltpu.SMEM)
    return pl.pallas_call(
        kernel,
        in_specs=[smem] * scalars + [vmem] * (len(args) - scalars),
        out_specs=[vmem] * (len(outs) - scalar_outs) + [smem] * scalar_outs,
        out_shape=[jax.ShapeDtypeStruct(o, t) for o, t in outs],
        scratch_shapes=[
            pltpu.VMEM(*s) if isinstance(s[0], tuple) else pltpu.VMEM(s, f32) for s in scratch
        ],
        compiler_params=pltpu.CompilerParams(vmem_limit_bytes=12 * 2**20),
    )(*args)


def in_group(new):
    swap = [(0, 1), (1, 0)]
    p1 = lax.ppermute(new, "dom_5", swap)
    a = jnp.concatenate([new, p1], axis=0)
    p2 = lax.ppermute(a, "dom_4", swap)
    return new, p1, p2


def shifts(up, down):
    count = lax.axis_size(DOM)
    forward = [(i, i + 1) for i in range(count - 1)]
    backward = [(i + 1, i) for i in range(count - 1)]
    return lax.ppermute(up, DOM, forward), lax.ppermute(down, DOM, backward)


def cycle(right_side, fine_diagonal, fine_columns, fine_blocks, aggregate_of_node,
         coarse_row_of_aggregate, coarse_diagonal, coarse_columns, coarse_blocks):
    rhs, dia = right_side.T, fine_diagonal.T
    col, blk = fine_columns.T, fine_blocks.transpose(2, 3, 1, 0)
    agg = aggregate_of_node.reshape(8, LANES)
    owner = coarse_row_of_aggregate.reshape(1, 32)
    cdia, cblk = coarse_diagonal.T, coarse_blocks.transpose(2, 3, 0, 1)
    me = lax.axis_index(DOM).astype(i32).reshape(1)
    base = me * ROWS
    wide = WIDE + ROWS + WIDE

    dsend, = call(coarse_pack_kernel, [((PEERS, 80, LANES), f32)], [coarse_columns, cblk])
    data = lax.all_to_all(dsend, OTHERS, 0, 0, tiled=True)
    vmem, far = pl.BlockSpec(memory_space=pltpu.VMEM), pl.BlockSpec(memory_space=pltpu.HBM)
    up, down, node_row = pl.pallas_call(
        pack_kernel,
        name="pack",
        in_specs=[far] * 6,
        out_specs=[vmem] * 3,
        out_shape=[jax.ShapeDtypeStruct(o, f32) for o in ((P_ALL, HALO), (P_ALL, HALO), (8, LANES))],
        scratch_shapes=[
            pltpu.VMEM((3, ROWS), f32), pltpu.VMEM((3, ROWS), f32),
            pltpu.VMEM((2, SLOTS, HALO), i32), pltpu.VMEM((2, 3, 3, SLOTS, HALO), f32),
            pltpu.VMEM((8, LANES), i32), pltpu.VMEM((1, 32), i32), pltpu.SemaphoreType.DMA((8,)),
        ],
        compiler_params=pltpu.CompilerParams(vmem_limit_bytes=12 * 2**20),
    )(rhs, dia, col, blk, agg, owner)
    before, after = shifts(up, down)
    send, first_iter, wrhs, wdia, up2, down2 = call(
        pre_kernel,
        [((LANES, 2, LANES), f32), ((3, wide), f32), ((3, wide), f32), ((3, wide), f32),
         ((3, HALO), f32), ((3, HALO), f32)],
        [base, rhs, dia, col, blk, agg, owner, cdia, before, after],
        scratch=[(3, wide), (3, wide), (8, ROWS)], scalars=1,
    )
    before2, after2 = shifts(up2, down2)
    sums = lax.all_to_all(send, DOM, 0, 0, tiled=True)
    peers = ((PEERS, LANES), f32)
    gather = (3, PEERS, LANES)
    square = (LANES, LANES)
    new, crhs, cd, where, passes = call(
        coarse_first_kernel,
        [peers, peers, peers, ((PEERS, 8, LANES), i32), ((1,), i32)],
        [me, sums, data, before2, after2],
        scratch=[square, gather, ((288, 4096), jnp.bfloat16), ((LANES, 4096), jnp.bfloat16)],
        scalars=1, scalar_outs=1,
    )
    for _ in range(CSWEEPS - 2):
        new, mine = call(
            coarse_kernel, [peers, ((3, 32), f32)],
            [me, passes, *in_group(new), crhs, cd, where, data],
            scratch=[square, square, gather], scalars=2,
        )
    solution, = call(
        post_kernel, [((3, ROWS), f32)],
        [base, *in_group(new), first_iter, wrhs, wdia, col, blk, node_row,
         before, after, before2, after2],
        scratch=[square, square, (3, wide), (3, wide)], scalars=1,
    )
    return solution.T, mine.T


def solution(mesh):
    torus = Mesh(mesh.devices.reshape(4, 2, 2, 2, 2, 2), DOM)
    return jax.shard_map(
        cycle,
        mesh=torus,
        in_specs=(
            P(DOM, None),
            P(DOM, None),
            P(DOM, None),
            P(DOM, None, None, None),
            P(DOM),
            P(DOM),
            P(DOM, None),
            P(DOM, None),
            P(DOM, None, None, None),
        ),
        out_specs=(P(DOM, None), P(DOM, None)),
        check_vma=False,
    )
```

```python
import jax
import jax.numpy as jnp
from jax import lax
from jax.experimental import pallas as pl
from jax.experimental.pallas import tpu as pltpu
from jax.sharding import Mesh
from jax.sharding import PartitionSpec as P


DOM = ("dom_0", "dom_1", "dom_2", "dom_3", "dom_4", "dom_5")
OTHERS = ("dom_0", "dom_1", "dom_2", "dom_3")
PEERS = 32
UNROLL = 2
CSWEEPS = 6
damping = 0.7
highest = lax.Precision.HIGHEST

ROWS = 1024
LANES = 128
SLOTS = 27
FULL = 24
HALO = 256
WIDE = 512
BLOCKS = ROWS // LANES
P_COL = 9 * FULL
P_BTAIL = P_COL + FULL
P_CTAIL = P_BTAIL + 27
P_RHS = P_CTAIL + 3
P_DIA = P_RHS + 6
P_ROW = P_DIA + 6
P_ALL = 288
f32 = jnp.float32
i32 = jnp.int32


def lanes(start, size=LANES):
    if isinstance(start, int):
        return slice(start, start + size)
    return pl.ds(pl.multiple_of(start, LANES), size)


def picked(row, where):
    return jnp.take_along_axis(
        jnp.broadcast_to(row, where.shape), where, axis=1, mode="promise_in_bounds"
    )


def pack_kernel(rhs_in, dia_in, col_in, blk_in, agg_in, owner_in, up, down, node_row,
                rhs, dia, col, blk, agg, owner, sem):
    copies = [(rhs_in, rhs), (dia_in, dia), (agg_in, agg), (owner_in, owner)]
    for t, near in enumerate((ROWS - HALO, 0)):
        copies.append((col_in.at[:, lanes(near, HALO)], col.at[t]))
        copies.append((blk_in.at[:, :, :, lanes(near, HALO)], blk.at[t]))
    copies = [pltpu.make_async_copy(a, b, sem.at[n]) for n, (a, b) in enumerate(copies)]
    for c in copies:
        c.start()
    for c in copies:
        c.wait()
    table = jnp.concatenate([owner[...]] * 4, axis=1)
    found = picked(table, agg[...]).astype(f32)
    node_row[...] = found
    for t, (out, wide) in enumerate(((up, ROWS - WIDE), (down, 0))):
        for i in range(3):
            for j in range(3):
                g = 3 * i + j
                out[g * FULL : (g + 1) * FULL, :] = blk[t, i, j, 0:FULL, :]
                out[P_BTAIL + 3 * g : P_BTAIL + 3 * g + 3, :] = blk[t, i, j, FULL:SLOTS, :]
        out[P_COL : P_COL + FULL, :] = col[t, 0:FULL, :].astype(f32)
        out[P_CTAIL : P_CTAIL + 3, :] = col[t, FULL:SLOTS, :].astype(f32)
        for h in range(2):
            out[P_RHS + 3 * h : P_RHS + 3 * h + 3, :] = rhs[:, lanes(wide + HALO * h, HALO)]
            out[P_DIA + 3 * h : P_DIA + 3 * h + 3, :] = dia[:, lanes(wide + HALO * h, HALO)]
            for q in range(2):
                s = wide // LANES + 2 * h + q
                out[P_ROW + h : P_ROW + h + 1, lanes(LANES * q)] = found[s : s + 1, :]
        out[P_ROW + 2 : P_ALL, :] = jnp.zeros((P_ALL - P_ROW - 2, HALO), f32)


def pulled_block(columns, blocks, table, first_chunk):
    total = [None, None, None]
    for part in range(4):
        where = columns(part)
        chunk = lax.shift_right_arithmetic(where, 7)
        lane = lax.bitwise_and(where, 127)
        near = [jnp.zeros(where.shape, f32) for _ in range(3)]
        for c in range(5):
            here = chunk == c
            for j in range(3):
                row = table[j : j + 1, lanes(first_chunk * LANES + c * LANES)]
                near[j] = jnp.where(here, picked(row, lane), near[j])
        for i in range(3):
            s = blocks(i, 0, part) * near[0]
            s = s + blocks(i, 1, part) * near[1]
            s = s + blocks(i, 2, part) * near[2]
            if part < 3:
                total[i] = s if total[i] is None else total[i] + s
            else:
                total[i] = jnp.sum(total[i], axis=0, keepdims=True) + jnp.sum(
                    s, axis=0, keepdims=True
                )
    return total


def local_getters(col, blk, start, b):
    def columns(part):
        lo, hi = 8 * part, min(8 * part + 8, SLOTS)
        return col[lo:hi, lanes(b * LANES)] - start

    def blocks(i, j, part):
        lo, hi = 8 * part, min(8 * part + 8, SLOTS)
        return blk[i, j, lo:hi, lanes(b * LANES)]

    return columns, blocks


def halo_getters(halo, start, b):
    def columns(part):
        if part < 3:
            got = halo[P_COL + 8 * part : P_COL + 8 * part + 8, lanes(b * LANES)]
        else:
            got = halo[P_CTAIL : P_CTAIL + 3, lanes(b * LANES)]
        return got.astype(i32) - start

    def blocks(i, j, part):
        g = 3 * i + j
        if part < 3:
            return halo[g * FULL + 8 * part : g * FULL + 8 * part + 8, lanes(b * LANES)]
        return halo[P_BTAIL + 3 * g : P_BTAIL + 3 * g + 3, lanes(b * LANES)]

    return columns, blocks


def wide_vector(out, local, before, after, row):
    out[:, lanes(WIDE, ROWS)] = local[...]
    for h in range(2):
        out[:, lanes(HALO * h, HALO)] = before[row + 3 * h : row + 3 * h + 3, :]
        out[:, lanes(WIDE + ROWS + HALO * h, HALO)] = after[row + 3 * h : row + 3 * h + 3, :]


def smoothed(table, pulled, rhs, dia, at):
    pull = jnp.concatenate(pulled, axis=0)
    s = table[:, lanes(at)]
    b = rhs[:, lanes(at)]
    d = dia[:, lanes(at)]
    return s + damping * (b - (d * s - pull)) / d


def sweep_halo(out, table, rhs, dia, halo, base, first):
    for b in range(2):
        at = first + LANES * b
        start = base + (at - WIDE) - 2 * LANES
        cols, blks = halo_getters(halo, start, b)
        pull = pulled_block(cols, blks, table, at // LANES - 2)
        out[:, lanes(at)] = smoothed(table, pull, rhs, dia, at)


def each_block(step):
    def some(t, carry):
        for u in range(UNROLL):
            step(t * UNROLL + u)
        return carry

    lax.fori_loop(0, BLOCKS // UNROLL, some, 0)


def own_block(table, col, blk, base, b):
    start = base + b * LANES - 2 * LANES
    cols, blks = local_getters(col, blk, start, b)
    return pulled_block(cols, blks, table, b + WIDE // LANES - 2)


def pre_kernel(base_ref, rhs, dia, col, blk, agg, owner_row, cdia, before, after,
               send, first_iter, keep_rhs, keep_dia, up2, down2, one, two, res):
    base = base_ref[0]
    wide_vector(keep_rhs, rhs, before, after, P_RHS)
    wide_vector(keep_dia, dia, before, after, P_DIA)
    raw = keep_dia[...]
    keep_dia[...] = jnp.where(raw == 0.0, 1.0, raw)
    one[...] = damping * keep_rhs[...] / keep_dia[...]
    two[...] = jnp.zeros(two.shape, f32)
    sweep_halo(two, one, keep_rhs, keep_dia, before, base, WIDE - HALO)
    sweep_halo(two, one, keep_rhs, keep_dia, after, base, WIDE + ROWS)

    def second(b):
        at = WIDE + b * LANES
        pull = own_block(one, col, blk, base, b)
        two[:, lanes(at)] = smoothed(one, pull, keep_rhs, keep_dia, at)

    each_block(second)

    def third(b):
        at = WIDE + b * LANES
        pull = jnp.concatenate(own_block(two, col, blk, base, b), axis=0)
        s, d = two[:, lanes(at)], keep_dia[:, lanes(at)]
        res[0:3, lanes(b * LANES)] = keep_rhs[:, lanes(at)] - (d * s - pull)

    res[...] = jnp.zeros(res.shape, f32)
    each_block(third)
    first_iter[...] = two[...]
    up2[...] = two[:, lanes(WIDE + ROWS - WIDE, HALO)]
    down2[...] = two[:, lanes(WIDE + HALO, HALO)]
    label = lax.broadcasted_iota(i32, (32, LANES), 0)
    sums = None
    for b in range(BLOCKS):
        member = (label == jnp.broadcast_to(agg[b : b + 1, :], (32, LANES))).astype(f32)
        part = lax.dot_general(
            res[:, lanes(b * LANES)], member, (((1,), (1,)), ((), ())),
            precision=highest, preferred_element_type=f32,
        )
        sums = part if sums is None else sums + part
    row = jnp.concatenate(
        [sums[0:1], sums[1:2], sums[2:3], owner_row[...].astype(f32)], axis=1
    )
    send[:, 0, :] = jnp.broadcast_to(row, (LANES, LANES))
    row = jnp.concatenate(
        [cdia[0:1], cdia[1:2], cdia[2:3], jnp.ones((1, 32), f32)], axis=1
    )
    send[:, 1, :] = jnp.broadcast_to(row, (LANES, LANES))


def lane_of_device(p, me):
    p = lax.bitwise_xor(p, lax.bitwise_and(me, 3))
    return lax.shift_left(lax.bitwise_and(p, 3), 5) + lax.shift_right_logical(p, 2)


def device_of_lane(q, me):
    p = lax.shift_left(lax.bitwise_and(q, 31), 2) + lax.shift_right_logical(q, 5)
    return lax.bitwise_xor(p, lax.bitwise_and(me, 3))


def coarse_pack_kernel(col, blk, send):
    def turned(a):
        z = jnp.transpose(jnp.concatenate([a, jnp.zeros((32, 5), f32)], axis=1))
        return jnp.concatenate([z] * 4, axis=1)

    columns = turned(col[...].astype(f32))
    kind = lax.bitwise_and(columns.astype(i32), 7)
    tile = (8, LANES)
    sub = lax.broadcasted_iota(i32, tile, 0)
    count = jnp.zeros(tile, i32)
    match, earlier = [], []
    for k in range(SLOTS):
        here = sub == jnp.broadcast_to(kind[k : k + 1], tile)
        match.append(here)
        earlier.append(count)
        count = count + here.astype(i32)
    left = jnp.zeros((1, LANES), i32)
    start = []
    for n in range(16):
        if n >= 8:
            start.append(left)
        left = jnp.maximum(left + count[n % 8 : n % 8 + 1] - 4, 0)
    start = jnp.concatenate(start, axis=0) + 4 * sub
    place = 4 * sub + lax.shift_right_logical(lax.broadcasted_iota(i32, tile, 1), 5)
    slot = jnp.full(tile, 31, i32)
    for k in range(SLOTS):
        at = jnp.sum(jnp.where(match[k], start + earlier[k], 0), axis=0, keepdims=True)
        slot = jnp.where(place == jnp.broadcast_to(lax.bitwise_and(at, 31), tile), k, slot)
    inner, outer = lax.bitwise_and(slot, 7), lax.shift_right_logical(slot, 3)

    def placed(z):
        got = None
        for g in range(4):
            part = jnp.take_along_axis(
                z[8 * g : 8 * g + 8], inner, axis=0, mode="promise_in_bounds"
            )
            got = part if got is None else jnp.where(outer == g, part, got)
        return got

    parts = [placed(turned(blk[i, j])) for i in range(3) for j in range(3)]
    parts.append(jnp.where(slot == 31, sub.astype(f32), placed(columns)))
    for m in range(10):
        for d in range(PEERS):
            send[d, 8 * m : 8 * m + 8, :] = parts[m]


def spread(parts):
    group = lax.shift_right_logical(lax.broadcasted_iota(i32, parts[0].shape, 1), 5)
    return jnp.where(group == 0, parts[0], jnp.where(group == 1, parts[1], parts[2]))


def coarse_lookup(table, chunk, lane):
    near = [jnp.zeros(chunk.shape, f32) for _ in range(3)]
    for c in range(32):
        here = chunk == c
        for j in range(3):
            row = table[32 * j + c : 32 * j + c + 1, :]
            near[j] = jnp.where(here, picked(row, lane), near[j])
    return near


def coarse_step(table, where, passes, data, own, rhs, dia, gather):
    gather[...] = jnp.zeros(gather.shape, f32)

    def one_pass(t, carry):
        rows = [
            [pltpu.roll(table[32 * j + 8 * v : 32 * j + 8 * v + 8, :], t, axis=0) for v in range(4)]
            for j in range(3)
        ]
        for d in range(PEERS):
            w = where[d]
            code, lane = lax.bitwise_and(w, 31), lax.shift_right_logical(w, 5)
            near = [jnp.zeros((8, LANES), f32) for _ in range(3)]
            for v in range(4):
                here = code == 4 * t + v
                for j in range(3):
                    near[j] = jnp.where(here, picked(rows[j][v], lane), near[j])
            for i in range(3):
                a = data[d, lanes8(3 * i), :] * near[0]
                a = a + data[d, lanes8(3 * i + 1), :] * near[1]
                a = a + data[d, lanes8(3 * i + 2), :] * near[2]
                gather[i, d : d + 1, :] += jnp.sum(a, axis=0, keepdims=True)
        return carry

    lax.fori_loop(0, passes, one_pass, 0)
    parts = []
    for i in range(3):
        s = gather[i]
        s = s + pltpu.roll(s, 64, axis=1)
        parts.append(s + pltpu.roll(s, 32, axis=1))
    return own + damping * (rhs - (dia * own - spread(parts))) / dia


def lanes8(m):
    return slice(8 * m, 8 * m + 8)


def coarse_first_kernel(base_ref, sums, data, far_up, far_down, new, rhs, dia, where, passes,
                        table, gather, left, right):
    me = lax.shift_right_logical(base_ref[0], 10)
    got = jnp.transpose(sums[:, 0, :])
    rows = got[96:128].astype(i32)
    s = got[0:96]
    split = []
    for _ in range(3):
        t = s.astype(jnp.bfloat16).astype(f32)
        split.append(t)
        s = s - t
    chunk = lax.broadcasted_iota(i32, (32, LANES), 0)
    place = lax.broadcasted_iota(i32, (LANES, LANES), 0)
    low = lax.bitwise_and(rows, 31)
    lane = lane_of_device(lax.shift_right_logical(rows, 5), me)
    for a in range(32):
        here = chunk == jnp.broadcast_to(low[a : a + 1], (32, LANES))
        for t in range(3):
            for i in range(3):
                value = jnp.broadcast_to(split[t][32 * i + a : 32 * i + a + 1], (32, LANES))
                left[96 * t + 32 * i : 96 * t + 32 * i + 32, lanes(LANES * a)] = jnp.where(
                    here, value, 0.0
                ).astype(jnp.bfloat16)
        right[:, lanes(LANES * a)] = jnp.where(
            place == jnp.broadcast_to(lane[a : a + 1], (LANES, LANES)), 1.0, 0.0
        ).astype(jnp.bfloat16)
    both = lax.dot_general(
        left[...], right[...], (((1,), (1,)), ((), ())), preferred_element_type=f32
    )
    crhs = both[0:96] + both[96:192] + both[192:288]
    order = device_of_lane(lax.broadcasted_iota(i32, (96, LANES), 1), me)
    cdia = jnp.take_along_axis(
        jnp.transpose(sums[:, 1, :])[0:96], order, axis=1, mode="promise_in_bounds"
    )
    pad = jnp.zeros((32, LANES), f32)
    first = jnp.concatenate([damping * crhs / cdia, pad], axis=0)
    table[...] = first
    own = jnp.transpose(first)[0:PEERS]
    rhs[...] = jnp.transpose(jnp.concatenate([crhs, pad], axis=0))[0:PEERS]
    dia[...] = jnp.transpose(jnp.concatenate([cdia, pad + 1.0], axis=0))[0:PEERS]
    sub = lax.broadcasted_iota(i32, (8, LANES), 0)
    most = jnp.zeros((8, LANES), i32)
    for d in range(PEERS):
        c = data[d, 72:80, :].astype(i32)
        off = lax.bitwise_and(sub - c, 7)
        most = jnp.maximum(most, off)
        at = lane_of_device(lax.shift_right_logical(c, 5), me)
        code = lax.bitwise_and(lax.shift_right_logical(c, 3), 3) + lax.shift_left(off, 2)
        where[d] = code + lax.shift_left(at, 5)
    most = jnp.max(most.astype(f32)).astype(i32) + 1
    passes[...] = jnp.broadcast_to(most, passes.shape)
    new[...] = coarse_step(
        table, where, most, data, own, rhs[...], dia[...], gather
    )


def gathered(table, pieces, mine):
    row = 0
    for piece in pieces:
        size = piece.shape[0]
        mine[row : row + size, :] = piece[...]
        row += size
    table[...] = jnp.transpose(mine[...])


def coarse_kernel(base_ref, passes, p0, p1, p2, rhs, dia, where, data, new, table, mine, gather):
    gathered(table, (p0, p1, p2), mine)
    new[...] = coarse_step(
        table, where, passes[...][0, 0], data, p0[...], rhs[...], dia[...], gather
    )


def post_kernel(base_ref, p0, p1, p2, first_iter, rhs, dia, col, blk, node_row, before, after,
                before2, after2, out, correction, table, mine, one, two):
    base = base_ref[0]
    me = lax.shift_right_logical(base, 10)
    gathered(table, (p0, p1, p2), mine)
    row = mine[pl.ds(lane_of_device(me, me), 1), :]
    correction[...] = jnp.concatenate([row[:, 32 * i : 32 * i + 32] for i in range(3)], axis=0)
    one[...] = first_iter[...]
    one[:, lanes(0, HALO)] = before2[...]
    one[:, lanes(WIDE + ROWS + HALO, HALO)] = after2[...]
    edge = [
        h[P_ROW + t : P_ROW + t + 1, lanes(LANES * q)]
        for h in (before, after) for t in range(2) for q in range(2)
    ]
    edge = jnp.concatenate(edge, axis=0)

    def found(rows):
        rows = rows.astype(i32)
        lane = lane_of_device(lax.shift_right_logical(rows, 5), me)
        return coarse_lookup(table, lax.bitwise_and(rows, 31), lane)

    own, far = found(node_row[...]), found(edge)
    for s in range(16):
        if s < 4:
            row = [f[s : s + 1, :] for f in far]
        elif s < 12:
            row = [f[s - 4 : s - 3, :] for f in own]
        else:
            row = [f[s - 8 : s - 7, :] for f in far]
        one[:, lanes(s * LANES)] = one[:, lanes(s * LANES)] + jnp.concatenate(row, axis=0)
    two[...] = jnp.zeros(two.shape, f32)
    sweep_halo(two, one, rhs, dia, before, base, WIDE - HALO)
    sweep_halo(two, one, rhs, dia, after, base, WIDE + ROWS)

    def first(b):
        at = WIDE + b * LANES
        pull = own_block(one, col, blk, base, b)
        two[:, lanes(at)] = smoothed(one, pull, rhs, dia, at)

    def second(b):
        at = WIDE + b * LANES
        pull = own_block(two, col, blk, base, b)
        out[:, lanes(b * LANES)] = smoothed(two, pull, rhs, dia, at)

    each_block(first)
    each_block(second)


def call(kernel, outs, args, scratch=(), scalars=0, limit=12):
    vmem = pl.BlockSpec(memory_space=pltpu.VMEM)
    smem = pl.BlockSpec(memory_space=pltpu.SMEM)
    return pl.pallas_call(
        kernel,
        in_specs=[smem] * scalars + [vmem] * (len(args) - scalars),
        out_specs=[vmem] * len(outs),
        out_shape=[jax.ShapeDtypeStruct(o, t) for o, t in outs],
        scratch_shapes=[
            pltpu.VMEM(*s) if isinstance(s[0], tuple) else pltpu.VMEM(s, f32) for s in scratch
        ],
        compiler_params=pltpu.CompilerParams(vmem_limit_bytes=limit * 2**20),
    )(*args)


def in_group(new):
    swap = [(0, 1), (1, 0)]
    p1 = lax.ppermute(new, "dom_5", swap)
    a = jnp.concatenate([new, p1], axis=0)
    p2 = lax.ppermute(a, "dom_4", swap)
    return new, p1, p2


def shifts(up, down):
    count = lax.axis_size(DOM)
    forward = [(i, i + 1) for i in range(count - 1)]
    backward = [(i + 1, i) for i in range(count - 1)]
    return lax.ppermute(up, DOM, forward), lax.ppermute(down, DOM, backward)


def cycle(right_side, fine_diagonal, fine_columns, fine_blocks, aggregate_of_node,
         coarse_row_of_aggregate, coarse_diagonal, coarse_columns, coarse_blocks):
    rhs, dia = right_side.T, fine_diagonal.T
    col, blk = fine_columns.T, fine_blocks.transpose(2, 3, 1, 0)
    agg = aggregate_of_node.reshape(8, LANES)
    owner = coarse_row_of_aggregate.reshape(1, 32)
    cdia, cblk = coarse_diagonal.T, coarse_blocks.transpose(2, 3, 0, 1)
    me = lax.axis_index(DOM).astype(i32).reshape(1)
    base = me * ROWS
    wide = WIDE + ROWS + WIDE

    dsend, = call(
        coarse_pack_kernel, [((PEERS, 80, LANES), f32)], [coarse_columns, cblk],
        limit=60,
    )
    data = lax.all_to_all(dsend, OTHERS, 0, 0, tiled=True)
    vmem, far = pl.BlockSpec(memory_space=pltpu.VMEM), pl.BlockSpec(memory_space=pltpu.HBM)
    up, down, node_row = pl.pallas_call(
        pack_kernel,
        name="pack",
        in_specs=[far] * 6,
        out_specs=[vmem] * 3,
        out_shape=[jax.ShapeDtypeStruct(o, f32) for o in ((P_ALL, HALO), (P_ALL, HALO), (8, LANES))],
        scratch_shapes=[
            pltpu.VMEM((3, ROWS), f32), pltpu.VMEM((3, ROWS), f32),
            pltpu.VMEM((2, SLOTS, HALO), i32), pltpu.VMEM((2, 3, 3, SLOTS, HALO), f32),
            pltpu.VMEM((8, LANES), i32), pltpu.VMEM((1, 32), i32), pltpu.SemaphoreType.DMA((8,)),
        ],
        compiler_params=pltpu.CompilerParams(vmem_limit_bytes=12 * 2**20),
    )(rhs, dia, col, blk, agg, owner)
    before, after = shifts(up, down)
    send, first_iter, wrhs, wdia, up2, down2 = call(
        pre_kernel,
        [((LANES, 2, LANES), f32), ((3, wide), f32), ((3, wide), f32), ((3, wide), f32),
         ((3, HALO), f32), ((3, HALO), f32)],
        [base, rhs, dia, col, blk, agg, owner, cdia, before, after],
        scratch=[(3, wide), (3, wide), (8, ROWS)], scalars=1,
    )
    before2, after2 = shifts(up2, down2)
    sums = lax.all_to_all(send, DOM, 0, 0, tiled=True)
    peers = ((PEERS, LANES), f32)
    gather = (3, PEERS, LANES)
    square = (LANES, LANES)
    new, crhs, cd, where, passes = call(
        coarse_first_kernel,
        [peers, peers, peers, ((PEERS, 8, LANES), i32), ((8, LANES), i32)],
        [base, sums, data, before2, after2],
        scratch=[square, gather, ((288, 4096), jnp.bfloat16), ((LANES, 4096), jnp.bfloat16)],
        scalars=1,
    )
    for _ in range(CSWEEPS - 2):
        new, = call(
            coarse_kernel, [peers],
            [base, passes, *in_group(new), crhs, cd, where, data],
            scratch=[square, square, gather], scalars=1,
        )
    solution, mine = call(
        post_kernel, [((3, ROWS), f32), ((3, 32), f32)],
        [base, *in_group(new), first_iter, wrhs, wdia, col, blk, node_row,
         before, after, before2, after2],
        scratch=[square, square, (3, wide), (3, wide)], scalars=1,
    )
    return solution.T, mine.T


def solution(mesh):
    torus = Mesh(mesh.devices.reshape(4, 2, 2, 2, 2, 2), DOM)
    return jax.shard_map(
        cycle,
        mesh=torus,
        in_specs=(
            P(DOM, None),
            P(DOM, None),
            P(DOM, None),
            P(DOM, None, None, None),
            P(DOM),
            P(DOM),
            P(DOM, None),
            P(DOM, None),
            P(DOM, None, None, None),
        ),
        out_specs=(P(DOM, None), P(DOM, None)),
        check_vma=False,
    )
```

```python
import jax
import jax.numpy as jnp
from jax import lax
from jax.experimental import pallas as pl
from jax.experimental.pallas import tpu as pltpu
from jax.sharding import Mesh
from jax.sharding import PartitionSpec as P


DOM = ("dom_0", "dom_1", "dom_2", "dom_3", "dom_4", "dom_5")
OTHERS = ("dom_0", "dom_1", "dom_2", "dom_3")
PEERS = 32
UNROLL = 8
CSWEEPS = 6
damping = 0.7
highest = lax.Precision.HIGHEST

ROWS = 1024
LANES = 128
SLOTS = 27
FULL = 24
HALO = 256
WIDE = 512
BLOCKS = ROWS // LANES
P_COL = 9 * FULL
P_BTAIL = P_COL + FULL
P_CTAIL = P_BTAIL + 27
P_RHS = P_CTAIL + 3
P_DIA = P_RHS + 6
P_ROW = P_DIA + 6
P_ALL = 288
f32 = jnp.float32
i32 = jnp.int32


def lanes(start, size=LANES):
    if isinstance(start, int):
        return slice(start, start + size)
    return pl.ds(pl.multiple_of(start, LANES), size)


def picked(row, where):
    return jnp.take_along_axis(
        jnp.broadcast_to(row, where.shape), where, axis=1, mode="promise_in_bounds"
    )


def pack_kernel(rhs_in, dia_in, col_in, blk_in, agg_in, owner_in, up, down, node_row,
                rhs, dia, col, blk, agg, owner, sem):
    copies = [(rhs_in, rhs), (dia_in, dia), (agg_in, agg), (owner_in, owner)]
    for t, near in enumerate((ROWS - HALO, 0)):
        copies.append((col_in.at[:, lanes(near, HALO)], col.at[t]))
        copies.append((blk_in.at[:, :, :, lanes(near, HALO)], blk.at[t]))
    copies = [pltpu.make_async_copy(a, b, sem.at[n]) for n, (a, b) in enumerate(copies)]
    for c in copies:
        c.start()
    for c in copies:
        c.wait()
    table = jnp.concatenate([owner[...]] * 4, axis=1)
    found = picked(table, agg[...]).astype(f32)
    node_row[...] = found
    for t, (out, wide) in enumerate(((up, ROWS - WIDE), (down, 0))):
        for i in range(3):
            for j in range(3):
                g = 3 * i + j
                out[g * FULL : (g + 1) * FULL, :] = blk[t, i, j, 0:FULL, :]
                out[P_BTAIL + 3 * g : P_BTAIL + 3 * g + 3, :] = blk[t, i, j, FULL:SLOTS, :]
        out[P_COL : P_COL + FULL, :] = col[t, 0:FULL, :].astype(f32)
        out[P_CTAIL : P_CTAIL + 3, :] = col[t, FULL:SLOTS, :].astype(f32)
        for h in range(2):
            out[P_RHS + 3 * h : P_RHS + 3 * h + 3, :] = rhs[:, lanes(wide + HALO * h, HALO)]
            out[P_DIA + 3 * h : P_DIA + 3 * h + 3, :] = dia[:, lanes(wide + HALO * h, HALO)]
            for q in range(2):
                s = wide // LANES + 2 * h + q
                out[P_ROW + h : P_ROW + h + 1, lanes(LANES * q)] = found[s : s + 1, :]
        out[P_ROW + 2 : P_ALL, :] = jnp.zeros((P_ALL - P_ROW - 2, HALO), f32)


def pulled_block(columns, blocks, table, first_chunk):
    total = [None, None, None]
    for part in range(4):
        where = columns(part)
        chunk = lax.shift_right_arithmetic(where, 7)
        lane = lax.bitwise_and(where, 127)
        near = [jnp.zeros(where.shape, f32) for _ in range(3)]
        for c in range(5):
            here = chunk == c
            for j in range(3):
                row = table[j : j + 1, lanes(first_chunk * LANES + c * LANES)]
                near[j] = jnp.where(here, picked(row, lane), near[j])
        for i in range(3):
            s = blocks(i, 0, part) * near[0]
            s = s + blocks(i, 1, part) * near[1]
            s = s + blocks(i, 2, part) * near[2]
            if part < 3:
                total[i] = s if total[i] is None else total[i] + s
            else:
                total[i] = jnp.sum(total[i], axis=0, keepdims=True) + jnp.sum(
                    s, axis=0, keepdims=True
                )
    return total


def local_getters(col, blk, start, b):
    def columns(part):
        lo, hi = 8 * part, min(8 * part + 8, SLOTS)
        return col[lo:hi, lanes(b * LANES)] - start

    def blocks(i, j, part):
        lo, hi = 8 * part, min(8 * part + 8, SLOTS)
        return blk[i, j, lo:hi, lanes(b * LANES)]

    return columns, blocks


def halo_getters(halo, start, b):
    def columns(part):
        if part < 3:
            got = halo[P_COL + 8 * part : P_COL + 8 * part + 8, lanes(b * LANES)]
        else:
            got = halo[P_CTAIL : P_CTAIL + 3, lanes(b * LANES)]
        return got.astype(i32) - start

    def blocks(i, j, part):
        g = 3 * i + j
        if part < 3:
            return halo[g * FULL + 8 * part : g * FULL + 8 * part + 8, lanes(b * LANES)]
        return halo[P_BTAIL + 3 * g : P_BTAIL + 3 * g + 3, lanes(b * LANES)]

    return columns, blocks


def wide_vector(out, local, before, after, row):
    out[:, lanes(WIDE, ROWS)] = local[...]
    for h in range(2):
        out[:, lanes(HALO * h, HALO)] = before[row + 3 * h : row + 3 * h + 3, :]
        out[:, lanes(WIDE + ROWS + HALO * h, HALO)] = after[row + 3 * h : row + 3 * h + 3, :]


def smoothed(table, pulled, rhs, dia, at):
    pull = jnp.concatenate(pulled, axis=0)
    s = table[:, lanes(at)]
    b = rhs[:, lanes(at)]
    d = dia[:, lanes(at)]
    return s + damping * (b - (d * s - pull)) / d


def sweep_halo(out, table, rhs, dia, halo, base, first):
    for b in range(2):
        at = first + LANES * b
        start = base + (at - WIDE) - 2 * LANES
        cols, blks = halo_getters(halo, start, b)
        pull = pulled_block(cols, blks, table, at // LANES - 2)
        out[:, lanes(at)] = smoothed(table, pull, rhs, dia, at)


def each_block(step):
    def some(t, carry):
        for u in range(UNROLL):
            step(t * UNROLL + u)
        return carry

    lax.fori_loop(0, BLOCKS // UNROLL, some, 0)


def own_block(table, col, blk, base, b):
    start = base + b * LANES - 2 * LANES
    cols, blks = local_getters(col, blk, start, b)
    return pulled_block(cols, blks, table, b + WIDE // LANES - 2)


def pre_kernel(base_ref, rhs, dia, col, blk, agg, owner_row, cdia, before, after,
               send, first_iter, keep_rhs, keep_dia, up2, down2, one, two, res):
    base = base_ref[0]
    wide_vector(keep_rhs, rhs, before, after, P_RHS)
    wide_vector(keep_dia, dia, before, after, P_DIA)
    raw = keep_dia[...]
    keep_dia[...] = jnp.where(raw == 0.0, 1.0, raw)
    one[...] = damping * keep_rhs[...] / keep_dia[...]
    two[...] = jnp.zeros(two.shape, f32)
    sweep_halo(two, one, keep_rhs, keep_dia, before, base, WIDE - HALO)
    sweep_halo(two, one, keep_rhs, keep_dia, after, base, WIDE + ROWS)

    def second(b):
        at = WIDE + b * LANES
        pull = own_block(one, col, blk, base, b)
        two[:, lanes(at)] = smoothed(one, pull, keep_rhs, keep_dia, at)

    each_block(second)

    def third(b):
        at = WIDE + b * LANES
        pull = jnp.concatenate(own_block(two, col, blk, base, b), axis=0)
        s, d = two[:, lanes(at)], keep_dia[:, lanes(at)]
        res[0:3, lanes(b * LANES)] = keep_rhs[:, lanes(at)] - (d * s - pull)

    res[...] = jnp.zeros(res.shape, f32)
    each_block(third)
    first_iter[...] = two[...]
    up2[...] = two[:, lanes(WIDE + ROWS - WIDE, HALO)]
    down2[...] = two[:, lanes(WIDE + HALO, HALO)]
    label = lax.broadcasted_iota(i32, (32, LANES), 0)
    sums = None
    for b in range(BLOCKS):
        member = (label == jnp.broadcast_to(agg[b : b + 1, :], (32, LANES))).astype(f32)
        part = lax.dot_general(
            res[:, lanes(b * LANES)], member, (((1,), (1,)), ((), ())),
            precision=highest, preferred_element_type=f32,
        )
        sums = part if sums is None else sums + part
    row = jnp.concatenate(
        [sums[0:1], sums[1:2], sums[2:3], owner_row[...].astype(f32)], axis=1
    )
    send[:, 0, :] = jnp.broadcast_to(row, (LANES, LANES))
    row = jnp.concatenate(
        [cdia[0:1], cdia[1:2], cdia[2:3], jnp.ones((1, 32), f32)], axis=1
    )
    send[:, 1, :] = jnp.broadcast_to(row, (LANES, LANES))


def lane_of_device(p, me):
    p = lax.bitwise_xor(p, lax.bitwise_and(me, 3))
    return lax.shift_left(lax.bitwise_and(p, 3), 5) + lax.shift_right_logical(p, 2)


def device_of_lane(q, me):
    p = lax.shift_left(lax.bitwise_and(q, 31), 2) + lax.shift_right_logical(q, 5)
    return lax.bitwise_xor(p, lax.bitwise_and(me, 3))


def coarse_pack_kernel(col, blk, send):
    def turned(a):
        z = jnp.transpose(jnp.concatenate([a, jnp.zeros((32, 5), f32)], axis=1))
        return jnp.concatenate([z] * 4, axis=1)

    columns = turned(col[...].astype(f32))
    kind = lax.bitwise_and(columns.astype(i32), 7)
    tile = (8, LANES)
    sub = lax.broadcasted_iota(i32, tile, 0)
    count = jnp.zeros(tile, i32)
    match, earlier = [], []
    for k in range(SLOTS):
        here = sub == jnp.broadcast_to(kind[k : k + 1], tile)
        match.append(here)
        earlier.append(count)
        count = count + here.astype(i32)
    left = jnp.zeros((1, LANES), i32)
    start = []
    for n in range(16):
        if n >= 8:
            start.append(left)
        left = jnp.maximum(left + count[n % 8 : n % 8 + 1] - 4, 0)
    start = jnp.concatenate(start, axis=0) + 4 * sub
    place = 4 * sub + lax.shift_right_logical(lax.broadcasted_iota(i32, tile, 1), 5)
    slot = jnp.full(tile, 31, i32)
    for k in range(SLOTS):
        at = jnp.sum(jnp.where(match[k], start + earlier[k], 0), axis=0, keepdims=True)
        slot = jnp.where(place == jnp.broadcast_to(lax.bitwise_and(at, 31), tile), k, slot)
    inner, outer = lax.bitwise_and(slot, 7), lax.shift_right_logical(slot, 3)

    def placed(z):
        got = None
        for g in range(4):
            part = jnp.take_along_axis(
                z[8 * g : 8 * g + 8], inner, axis=0, mode="promise_in_bounds"
            )
            got = part if got is None else jnp.where(outer == g, part, got)
        return got

    parts = [placed(turned(blk[i, j])) for i in range(3) for j in range(3)]
    parts.append(jnp.where(slot == 31, sub.astype(f32), placed(columns)))
    for m in range(10):
        for d in range(PEERS):
            send[d, 8 * m : 8 * m + 8, :] = parts[m]


def spread(parts):
    group = lax.shift_right_logical(lax.broadcasted_iota(i32, parts[0].shape, 1), 5)
    return jnp.where(group == 0, parts[0], jnp.where(group == 1, parts[1], parts[2]))


def coarse_lookup(table, chunk, lane):
    near = [jnp.zeros(chunk.shape, f32) for _ in range(3)]
    for c in range(32):
        here = chunk == c
        for j in range(3):
            row = table[32 * j + c : 32 * j + c + 1, :]
            near[j] = jnp.where(here, picked(row, lane), near[j])
    return near


def coarse_step(table, where, passes, data, own, rhs, dia, gather):
    gather[...] = jnp.zeros(gather.shape, f32)

    def one_pass(t, carry):
        rows = [
            [pltpu.roll(table[32 * j + 8 * v : 32 * j + 8 * v + 8, :], t, axis=0) for v in range(4)]
            for j in range(3)
        ]
        for d in range(PEERS):
            w = where[d]
            code, lane = lax.bitwise_and(w, 31), lax.shift_right_logical(w, 5)
            near = [jnp.zeros((8, LANES), f32) for _ in range(3)]
            for v in range(4):
                here = code == 4 * t + v
                for j in range(3):
                    near[j] = jnp.where(here, picked(rows[j][v], lane), near[j])
            for i in range(3):
                a = data[d, lanes8(3 * i), :] * near[0]
                a = a + data[d, lanes8(3 * i + 1), :] * near[1]
                a = a + data[d, lanes8(3 * i + 2), :] * near[2]
                gather[i, d : d + 1, :] += jnp.sum(a, axis=0, keepdims=True)
        return carry

    lax.fori_loop(0, passes, one_pass, 0)
    parts = []
    for i in range(3):
        s = gather[i]
        s = s + pltpu.roll(s, 64, axis=1)
        parts.append(s + pltpu.roll(s, 32, axis=1))
    return own + damping * (rhs - (dia * own - spread(parts))) / dia


def lanes8(m):
    return slice(8 * m, 8 * m + 8)


def coarse_first_kernel(base_ref, sums, data, far_up, far_down, new, rhs, dia, where, passes,
                        table, gather, left, right):
    me = lax.shift_right_logical(base_ref[0], 10)
    got = jnp.transpose(sums[:, 0, :])
    rows = got[96:128].astype(i32)
    s = got[0:96]
    split = []
    for _ in range(3):
        t = s.astype(jnp.bfloat16).astype(f32)
        split.append(t)
        s = s - t
    chunk = lax.broadcasted_iota(i32, (32, LANES), 0)
    place = lax.broadcasted_iota(i32, (LANES, LANES), 0)
    low = lax.bitwise_and(rows, 31)
    lane = lane_of_device(lax.shift_right_logical(rows, 5), me)
    for a in range(32):
        here = chunk == jnp.broadcast_to(low[a : a + 1], (32, LANES))
        for t in range(3):
            for i in range(3):
                value = jnp.broadcast_to(split[t][32 * i + a : 32 * i + a + 1], (32, LANES))
                left[96 * t + 32 * i : 96 * t + 32 * i + 32, lanes(LANES * a)] = jnp.where(
                    here, value, 0.0
                ).astype(jnp.bfloat16)
        right[:, lanes(LANES * a)] = jnp.where(
            place == jnp.broadcast_to(lane[a : a + 1], (LANES, LANES)), 1.0, 0.0
        ).astype(jnp.bfloat16)
    both = lax.dot_general(
        left[...], right[...], (((1,), (1,)), ((), ())), preferred_element_type=f32
    )
    crhs = both[0:96] + both[96:192] + both[192:288]
    order = device_of_lane(lax.broadcasted_iota(i32, (96, LANES), 1), me)
    cdia = jnp.take_along_axis(
        jnp.transpose(sums[:, 1, :])[0:96], order, axis=1, mode="promise_in_bounds"
    )
    pad = jnp.zeros((32, LANES), f32)
    first = jnp.concatenate([damping * crhs / cdia, pad], axis=0)
    table[...] = first
    own = jnp.transpose(first)[0:PEERS]
    rhs[...] = jnp.transpose(jnp.concatenate([crhs, pad], axis=0))[0:PEERS]
    dia[...] = jnp.transpose(jnp.concatenate([cdia, pad + 1.0], axis=0))[0:PEERS]
    sub = lax.broadcasted_iota(i32, (8, LANES), 0)
    most = jnp.zeros((8, LANES), i32)
    for d in range(PEERS):
        c = data[d, 72:80, :].astype(i32)
        off = lax.bitwise_and(sub - c, 7)
        most = jnp.maximum(most, off)
        at = lane_of_device(lax.shift_right_logical(c, 5), me)
        code = lax.bitwise_and(lax.shift_right_logical(c, 3), 3) + lax.shift_left(off, 2)
        where[d] = code + lax.shift_left(at, 5)
    most = jnp.max(most.astype(f32)).astype(i32) + 1
    passes[...] = jnp.broadcast_to(most, passes.shape)
    new[...] = coarse_step(
        table, where, most, data, own, rhs[...], dia[...], gather
    )


def gathered(table, pieces, mine):
    row = 0
    for piece in pieces:
        size = piece.shape[0]
        mine[row : row + size, :] = piece[...]
        row += size
    table[...] = jnp.transpose(mine[...])


def coarse_kernel(base_ref, passes, p0, p1, p2, p3, rhs, dia, where, data, new, table, mine, gather):
    gathered(table, (p0, p1, p2, p3), mine)
    new[...] = coarse_step(
        table, where, passes[...][0, 0], data, p0[...], rhs[...], dia[...], gather
    )


def post_kernel(base_ref, p0, p1, p2, p3, first_iter, rhs, dia, col, blk, node_row, before, after,
                before2, after2, out, correction, table, mine, one, two):
    base = base_ref[0]
    me = lax.shift_right_logical(base, 10)
    gathered(table, (p0, p1, p2, p3), mine)
    row = mine[pl.ds(lane_of_device(me, me), 1), :]
    correction[...] = jnp.concatenate([row[:, 32 * i : 32 * i + 32] for i in range(3)], axis=0)
    one[...] = first_iter[...]
    one[:, lanes(0, HALO)] = before2[...]
    one[:, lanes(WIDE + ROWS + HALO, HALO)] = after2[...]
    edge = [
        h[P_ROW + t : P_ROW + t + 1, lanes(LANES * q)]
        for h in (before, after) for t in range(2) for q in range(2)
    ]
    edge = jnp.concatenate(edge, axis=0)

    def found(rows):
        rows = rows.astype(i32)
        lane = lane_of_device(lax.shift_right_logical(rows, 5), me)
        return coarse_lookup(table, lax.bitwise_and(rows, 31), lane)

    own, far = found(node_row[...]), found(edge)
    for s in range(16):
        if s < 4:
            row = [f[s : s + 1, :] for f in far]
        elif s < 12:
            row = [f[s - 4 : s - 3, :] for f in own]
        else:
            row = [f[s - 8 : s - 7, :] for f in far]
        one[:, lanes(s * LANES)] = one[:, lanes(s * LANES)] + jnp.concatenate(row, axis=0)
    two[...] = jnp.zeros(two.shape, f32)
    sweep_halo(two, one, rhs, dia, before, base, WIDE - HALO)
    sweep_halo(two, one, rhs, dia, after, base, WIDE + ROWS)

    def first(b):
        at = WIDE + b * LANES
        pull = own_block(one, col, blk, base, b)
        two[:, lanes(at)] = smoothed(one, pull, rhs, dia, at)

    def second(b):
        at = WIDE + b * LANES
        pull = own_block(two, col, blk, base, b)
        out[:, lanes(b * LANES)] = smoothed(two, pull, rhs, dia, at)

    each_block(first)
    each_block(second)


def call(kernel, outs, args, scratch=(), scalars=0, limit=12):
    vmem = pl.BlockSpec(memory_space=pltpu.VMEM)
    smem = pl.BlockSpec(memory_space=pltpu.SMEM)
    return pl.pallas_call(
        kernel,
        in_specs=[smem] * scalars + [vmem] * (len(args) - scalars),
        out_specs=[vmem] * len(outs),
        out_shape=[jax.ShapeDtypeStruct(o, t) for o, t in outs],
        scratch_shapes=[
            pltpu.VMEM(*s) if isinstance(s[0], tuple) else pltpu.VMEM(s, f32) for s in scratch
        ],
        compiler_params=pltpu.CompilerParams(vmem_limit_bytes=limit * 2**20),
    )(*args)


def in_group(new):
    swap = [(0, 1), (1, 0)]
    both = [(i, 3 - i) for i in range(4)]
    p2 = lax.ppermute(new, "dom_4", swap)
    p3 = lax.ppermute(new, ("dom_4", "dom_5"), both)
    p1 = lax.ppermute(new, "dom_5", swap)
    return new, p1, p2, p3


def shifts(up, down):
    count = lax.axis_size(DOM)
    forward = [(i, i + 1) for i in range(count - 1)]
    backward = [(i + 1, i) for i in range(count - 1)]
    return lax.ppermute(up, DOM, forward), lax.ppermute(down, DOM, backward)


def cycle(right_side, fine_diagonal, fine_columns, fine_blocks, aggregate_of_node,
         coarse_row_of_aggregate, coarse_diagonal, coarse_columns, coarse_blocks):
    rhs, dia = right_side.T, fine_diagonal.T
    col, blk = fine_columns.T, fine_blocks.transpose(2, 3, 1, 0)
    agg = aggregate_of_node.reshape(8, LANES)
    owner = coarse_row_of_aggregate.reshape(1, 32)
    cdia, cblk = coarse_diagonal.T, coarse_blocks.transpose(2, 3, 0, 1)
    me = lax.axis_index(DOM).astype(i32).reshape(1)
    base = me * ROWS
    wide = WIDE + ROWS + WIDE

    dsend, = call(
        coarse_pack_kernel, [((PEERS, 80, LANES), f32)], [coarse_columns, cblk],
        limit=60,
    )
    data = lax.all_to_all(dsend, OTHERS, 0, 0, tiled=True)
    vmem, far = pl.BlockSpec(memory_space=pltpu.VMEM), pl.BlockSpec(memory_space=pltpu.HBM)
    up, down, node_row = pl.pallas_call(
        pack_kernel,
        name="pack",
        in_specs=[far] * 6,
        out_specs=[vmem] * 3,
        out_shape=[jax.ShapeDtypeStruct(o, f32) for o in ((P_ALL, HALO), (P_ALL, HALO), (8, LANES))],
        scratch_shapes=[
            pltpu.VMEM((3, ROWS), f32), pltpu.VMEM((3, ROWS), f32),
            pltpu.VMEM((2, SLOTS, HALO), i32), pltpu.VMEM((2, 3, 3, SLOTS, HALO), f32),
            pltpu.VMEM((8, LANES), i32), pltpu.VMEM((1, 32), i32), pltpu.SemaphoreType.DMA((8,)),
        ],
        compiler_params=pltpu.CompilerParams(vmem_limit_bytes=12 * 2**20),
    )(rhs, dia, col, blk, agg, owner)
    before, after = shifts(up, down)
    send, first_iter, wrhs, wdia, up2, down2 = call(
        pre_kernel,
        [((LANES, 2, LANES), f32), ((3, wide), f32), ((3, wide), f32), ((3, wide), f32),
         ((3, HALO), f32), ((3, HALO), f32)],
        [base, rhs, dia, col, blk, agg, owner, cdia, before, after],
        scratch=[(3, wide), (3, wide), (8, ROWS)], scalars=1,
    )
    before2, after2 = shifts(up2, down2)
    sums = lax.all_to_all(send, DOM, 0, 0, tiled=True)
    peers = ((PEERS, LANES), f32)
    gather = (3, PEERS, LANES)
    square = (LANES, LANES)
    new, crhs, cd, where, passes = call(
        coarse_first_kernel,
        [peers, peers, peers, ((PEERS, 8, LANES), i32), ((8, LANES), i32)],
        [base, sums, data, before2, after2],
        scratch=[square, gather, ((288, 4096), jnp.bfloat16), ((LANES, 4096), jnp.bfloat16)],
        scalars=1,
    )
    for _ in range(CSWEEPS - 2):
        new, = call(
            coarse_kernel, [peers],
            [base, passes, *in_group(new), crhs, cd, where, data],
            scratch=[square, square, gather], scalars=1,
        )
    solution, mine = call(
        post_kernel, [((3, ROWS), f32), ((3, 32), f32)],
        [base, *in_group(new), first_iter, wrhs, wdia, col, blk, node_row,
         before, after, before2, after2],
        scratch=[square, square, (3, wide), (3, wide)], scalars=1,
    )
    return solution.T, mine.T


def solution(mesh):
    torus = Mesh(mesh.devices.reshape(4, 2, 2, 2, 2, 2), DOM)
    return jax.shard_map(
        cycle,
        mesh=torus,
        in_specs=(
            P(DOM, None),
            P(DOM, None),
            P(DOM, None),
            P(DOM, None, None, None),
            P(DOM),
            P(DOM),
            P(DOM, None),
            P(DOM, None),
            P(DOM, None, None, None),
        ),
        out_specs=(P(DOM, None), P(DOM, None)),
        check_vma=False,
    )
```

```python
import jax
import jax.numpy as jnp
from jax import lax
from jax.experimental import pallas as pl
from jax.experimental.pallas import tpu as pltpu
from jax.sharding import PartitionSpec as P


DOM = "dom"
PEERS = 32
UNROLL = 8
CSWEEPS = 6
damping = 0.7
highest = lax.Precision.HIGHEST

ROWS = 1024
LANES = 128
SLOTS = 27
FULL = 24
HALO = 256
WIDE = 512
BLOCKS = ROWS // LANES
P_COL = 9 * FULL
P_BTAIL = P_COL + FULL
P_CTAIL = P_BTAIL + 27
P_RHS = P_CTAIL + 3
P_DIA = P_RHS + 6
P_ROW = P_DIA + 6
P_ALL = 288
f32 = jnp.float32
i32 = jnp.int32


def lanes(start, size=LANES):
    if isinstance(start, int):
        return slice(start, start + size)
    return pl.ds(pl.multiple_of(start, LANES), size)


def picked(row, where):
    return jnp.take_along_axis(
        jnp.broadcast_to(row, where.shape), where, axis=1, mode="promise_in_bounds"
    )


def pack_kernel(rhs_in, dia_in, col_in, blk_in, agg_in, owner_in, up, down, node_row,
                rhs, dia, col, blk, agg, owner, sem):
    copies = [(rhs_in, rhs), (dia_in, dia), (agg_in, agg), (owner_in, owner)]
    for t, near in enumerate((ROWS - HALO, 0)):
        copies.append((col_in.at[:, lanes(near, HALO)], col.at[t]))
        copies.append((blk_in.at[:, :, :, lanes(near, HALO)], blk.at[t]))
    copies = [pltpu.make_async_copy(a, b, sem.at[n]) for n, (a, b) in enumerate(copies)]
    for c in copies:
        c.start()
    for c in copies:
        c.wait()
    table = jnp.concatenate([owner[...]] * 4, axis=1)
    found = picked(table, agg[...]).astype(f32)
    node_row[...] = found
    for t, (out, wide) in enumerate(((up, ROWS - WIDE), (down, 0))):
        for i in range(3):
            for j in range(3):
                g = 3 * i + j
                out[g * FULL : (g + 1) * FULL, :] = blk[t, i, j, 0:FULL, :]
                out[P_BTAIL + 3 * g : P_BTAIL + 3 * g + 3, :] = blk[t, i, j, FULL:SLOTS, :]
        out[P_COL : P_COL + FULL, :] = col[t, 0:FULL, :].astype(f32)
        out[P_CTAIL : P_CTAIL + 3, :] = col[t, FULL:SLOTS, :].astype(f32)
        for h in range(2):
            out[P_RHS + 3 * h : P_RHS + 3 * h + 3, :] = rhs[:, lanes(wide + HALO * h, HALO)]
            out[P_DIA + 3 * h : P_DIA + 3 * h + 3, :] = dia[:, lanes(wide + HALO * h, HALO)]
            for q in range(2):
                s = wide // LANES + 2 * h + q
                out[P_ROW + h : P_ROW + h + 1, lanes(LANES * q)] = found[s : s + 1, :]
        out[P_ROW + 2 : P_ALL, :] = jnp.zeros((P_ALL - P_ROW - 2, HALO), f32)


def pulled_block(columns, blocks, table, first_chunk):
    total = [None, None, None]
    for part in range(4):
        where = columns(part)
        chunk = lax.shift_right_arithmetic(where, 7)
        lane = lax.bitwise_and(where, 127)
        near = [jnp.zeros(where.shape, f32) for _ in range(3)]
        for c in range(5):
            here = chunk == c
            for j in range(3):
                row = table[j : j + 1, lanes(first_chunk * LANES + c * LANES)]
                near[j] = jnp.where(here, picked(row, lane), near[j])
        for i in range(3):
            s = blocks(i, 0, part) * near[0]
            s = s + blocks(i, 1, part) * near[1]
            s = s + blocks(i, 2, part) * near[2]
            if part < 3:
                total[i] = s if total[i] is None else total[i] + s
            else:
                total[i] = jnp.sum(total[i], axis=0, keepdims=True) + jnp.sum(
                    s, axis=0, keepdims=True
                )
    return total


def local_getters(col, blk, start, b):
    def columns(part):
        lo, hi = 8 * part, min(8 * part + 8, SLOTS)
        return col[lo:hi, lanes(b * LANES)] - start

    def blocks(i, j, part):
        lo, hi = 8 * part, min(8 * part + 8, SLOTS)
        return blk[i, j, lo:hi, lanes(b * LANES)]

    return columns, blocks


def halo_getters(halo, start, b):
    def columns(part):
        if part < 3:
            got = halo[P_COL + 8 * part : P_COL + 8 * part + 8, lanes(b * LANES)]
        else:
            got = halo[P_CTAIL : P_CTAIL + 3, lanes(b * LANES)]
        return got.astype(i32) - start

    def blocks(i, j, part):
        g = 3 * i + j
        if part < 3:
            return halo[g * FULL + 8 * part : g * FULL + 8 * part + 8, lanes(b * LANES)]
        return halo[P_BTAIL + 3 * g : P_BTAIL + 3 * g + 3, lanes(b * LANES)]

    return columns, blocks


def wide_vector(out, local, before, after, row):
    out[:, lanes(WIDE, ROWS)] = local[...]
    for h in range(2):
        out[:, lanes(HALO * h, HALO)] = before[row + 3 * h : row + 3 * h + 3, :]
        out[:, lanes(WIDE + ROWS + HALO * h, HALO)] = after[row + 3 * h : row + 3 * h + 3, :]


def smoothed(table, pulled, rhs, dia, at):
    pull = jnp.concatenate(pulled, axis=0)
    s = table[:, lanes(at)]
    b = rhs[:, lanes(at)]
    d = dia[:, lanes(at)]
    return s + damping * (b - (d * s - pull)) / d


def sweep_halo(out, table, rhs, dia, halo, base, first):
    for b in range(2):
        at = first + LANES * b
        start = base + (at - WIDE) - 2 * LANES
        cols, blks = halo_getters(halo, start, b)
        pull = pulled_block(cols, blks, table, at // LANES - 2)
        out[:, lanes(at)] = smoothed(table, pull, rhs, dia, at)


def each_block(step):
    def some(t, carry):
        for u in range(UNROLL):
            step(t * UNROLL + u)
        return carry

    lax.fori_loop(0, BLOCKS // UNROLL, some, 0)


def own_block(table, col, blk, base, b):
    start = base + b * LANES - 2 * LANES
    cols, blks = local_getters(col, blk, start, b)
    return pulled_block(cols, blks, table, b + WIDE // LANES - 2)


def pre_kernel(base_ref, rhs, dia, col, blk, agg, owner_row, cdia, before, after,
               send, first_iter, keep_rhs, keep_dia, up2, down2, one, two, res):
    base = base_ref[0]
    wide_vector(keep_rhs, rhs, before, after, P_RHS)
    wide_vector(keep_dia, dia, before, after, P_DIA)
    raw = keep_dia[...]
    keep_dia[...] = jnp.where(raw == 0.0, 1.0, raw)
    one[...] = damping * keep_rhs[...] / keep_dia[...]
    two[...] = jnp.zeros(two.shape, f32)
    sweep_halo(two, one, keep_rhs, keep_dia, before, base, WIDE - HALO)
    sweep_halo(two, one, keep_rhs, keep_dia, after, base, WIDE + ROWS)

    def second(b):
        at = WIDE + b * LANES
        pull = own_block(one, col, blk, base, b)
        two[:, lanes(at)] = smoothed(one, pull, keep_rhs, keep_dia, at)

    each_block(second)

    def third(b):
        at = WIDE + b * LANES
        pull = jnp.concatenate(own_block(two, col, blk, base, b), axis=0)
        s, d = two[:, lanes(at)], keep_dia[:, lanes(at)]
        res[0:3, lanes(b * LANES)] = keep_rhs[:, lanes(at)] - (d * s - pull)

    res[...] = jnp.zeros(res.shape, f32)
    each_block(third)
    first_iter[...] = two[...]
    up2[...] = two[:, lanes(WIDE + ROWS - WIDE, HALO)]
    down2[...] = two[:, lanes(WIDE + HALO, HALO)]
    label = lax.broadcasted_iota(i32, (32, LANES), 0)
    sums = None
    for b in range(BLOCKS):
        member = (label == jnp.broadcast_to(agg[b : b + 1, :], (32, LANES))).astype(f32)
        part = lax.dot_general(
            res[:, lanes(b * LANES)], member, (((1,), (1,)), ((), ())),
            precision=highest, preferred_element_type=f32,
        )
        sums = part if sums is None else sums + part
    row = jnp.concatenate(
        [sums[0:1], sums[1:2], sums[2:3], owner_row[...].astype(f32)], axis=1
    )
    send[:, 0, :] = jnp.broadcast_to(row, (LANES, LANES))
    row = jnp.concatenate(
        [cdia[0:1], cdia[1:2], cdia[2:3], jnp.ones((1, 32), f32)], axis=1
    )
    send[:, 1, :] = jnp.broadcast_to(row, (LANES, LANES))


def parity(p):
    return lax.bitwise_and(
        lax.bitwise_xor(lax.shift_right_logical(p, 1), lax.shift_right_logical(p, 2)), 1
    )


def lane_of_device(p, me):
    side = lax.shift_left(lax.bitwise_xor(parity(p), parity(me)), 6)
    core = lax.shift_left(lax.bitwise_and(lax.bitwise_xor(p, me), 1), 5)
    return side + core + lax.shift_right_logical(p, 2)


def device_of_lane(q, me):
    side = lax.bitwise_xor(lax.shift_right_logical(q, 6), parity(me))
    side = lax.bitwise_xor(side, lax.bitwise_and(q, 1))
    core = lax.bitwise_and(lax.bitwise_xor(lax.shift_right_logical(q, 5), me), 1)
    return lax.shift_left(lax.bitwise_and(q, 31), 2) + lax.shift_left(side, 1) + core


def row_groups():
    return [
        [4 * m + 2 * (side ^ (m & 1)) + core for m in range(PEERS)]
        for side in range(2) for core in range(2)
    ]


def coarse_pack_kernel(col, blk, send):
    def turned(a):
        z = jnp.transpose(jnp.concatenate([a, jnp.zeros((32, 5), f32)], axis=1))
        return jnp.concatenate([z] * 4, axis=1)

    columns = turned(col[...].astype(f32))
    kind = lax.bitwise_and(columns.astype(i32), 7)
    tile = (8, LANES)
    sub = lax.broadcasted_iota(i32, tile, 0)
    count = jnp.zeros(tile, i32)
    match, earlier = [], []
    for k in range(SLOTS):
        here = sub == jnp.broadcast_to(kind[k : k + 1], tile)
        match.append(here)
        earlier.append(count)
        count = count + here.astype(i32)
    left = jnp.zeros((1, LANES), i32)
    start = []
    for n in range(16):
        if n >= 8:
            start.append(left)
        left = jnp.maximum(left + count[n % 8 : n % 8 + 1] - 4, 0)
    start = jnp.concatenate(start, axis=0) + 4 * sub
    place = 4 * sub + lax.shift_right_logical(lax.broadcasted_iota(i32, tile, 1), 5)
    slot = jnp.full(tile, 31, i32)
    for k in range(SLOTS):
        at = jnp.sum(jnp.where(match[k], start + earlier[k], 0), axis=0, keepdims=True)
        slot = jnp.where(place == jnp.broadcast_to(lax.bitwise_and(at, 31), tile), k, slot)
    inner, outer = lax.bitwise_and(slot, 7), lax.shift_right_logical(slot, 3)

    def placed(z):
        got = None
        for g in range(4):
            part = jnp.take_along_axis(
                z[8 * g : 8 * g + 8], inner, axis=0, mode="promise_in_bounds"
            )
            got = part if got is None else jnp.where(outer == g, part, got)
        return got

    parts = [placed(turned(blk[i, j])) for i in range(3) for j in range(3)]
    parts.append(jnp.where(slot == 31, sub.astype(f32), placed(columns)))
    for m in range(10):
        for d in range(PEERS):
            send[d, 8 * m : 8 * m + 8, :] = parts[m]


def spread(parts):
    group = lax.shift_right_logical(lax.broadcasted_iota(i32, parts[0].shape, 1), 5)
    return jnp.where(group == 0, parts[0], jnp.where(group == 1, parts[1], parts[2]))


def coarse_lookup(table, chunk, lane):
    near = [jnp.zeros(chunk.shape, f32) for _ in range(3)]
    for c in range(32):
        here = chunk == c
        for j in range(3):
            row = table[32 * j + c : 32 * j + c + 1, :]
            near[j] = jnp.where(here, picked(row, lane), near[j])
    return near


def coarse_step(table, where, passes, data, own, rhs, dia, gather):
    gather[...] = jnp.zeros(gather.shape, f32)

    def one_pass(t, carry):
        rows = [
            [pltpu.roll(table[32 * j + 8 * v : 32 * j + 8 * v + 8, :], t, axis=0) for v in range(4)]
            for j in range(3)
        ]
        for d in range(PEERS):
            w = where[d]
            code, lane = lax.bitwise_and(w, 31), lax.shift_right_logical(w, 5)
            near = [jnp.zeros((8, LANES), f32) for _ in range(3)]
            for v in range(4):
                here = code == 4 * t + v
                for j in range(3):
                    near[j] = jnp.where(here, picked(rows[j][v], lane), near[j])
            for i in range(3):
                a = data[d, lanes8(3 * i), :] * near[0]
                a = a + data[d, lanes8(3 * i + 1), :] * near[1]
                a = a + data[d, lanes8(3 * i + 2), :] * near[2]
                gather[i, d : d + 1, :] += jnp.sum(a, axis=0, keepdims=True)
        return carry

    lax.fori_loop(0, passes, one_pass, 0)
    parts = []
    for i in range(3):
        s = gather[i]
        s = s + pltpu.roll(s, 64, axis=1)
        parts.append(s + pltpu.roll(s, 32, axis=1))
    return own + damping * (rhs - (dia * own - spread(parts))) / dia


def lanes8(m):
    return slice(8 * m, 8 * m + 8)


def coarse_first_kernel(base_ref, sums, data, far_up, far_down, new, rhs, dia, where, passes,
                        table, gather, left, right):
    me = lax.shift_right_logical(base_ref[0], 10)
    got = jnp.transpose(sums[:, 0, :])
    rows = got[96:128].astype(i32)
    s = got[0:96]
    split = []
    for _ in range(3):
        t = s.astype(jnp.bfloat16).astype(f32)
        split.append(t)
        s = s - t
    chunk = lax.broadcasted_iota(i32, (32, LANES), 0)
    place = lax.broadcasted_iota(i32, (LANES, LANES), 0)
    low = lax.bitwise_and(rows, 31)
    lane = lane_of_device(lax.shift_right_logical(rows, 5), me)
    for a in range(32):
        here = chunk == jnp.broadcast_to(low[a : a + 1], (32, LANES))
        for t in range(3):
            for i in range(3):
                value = jnp.broadcast_to(split[t][32 * i + a : 32 * i + a + 1], (32, LANES))
                left[96 * t + 32 * i : 96 * t + 32 * i + 32, lanes(LANES * a)] = jnp.where(
                    here, value, 0.0
                ).astype(jnp.bfloat16)
        right[:, lanes(LANES * a)] = jnp.where(
            place == jnp.broadcast_to(lane[a : a + 1], (LANES, LANES)), 1.0, 0.0
        ).astype(jnp.bfloat16)
    both = lax.dot_general(
        left[...], right[...], (((1,), (1,)), ((), ())), preferred_element_type=f32
    )
    crhs = both[0:96] + both[96:192] + both[192:288]
    order = device_of_lane(lax.broadcasted_iota(i32, (96, LANES), 1), me)
    cdia = jnp.take_along_axis(
        jnp.transpose(sums[:, 1, :])[0:96], order, axis=1, mode="promise_in_bounds"
    )
    pad = jnp.zeros((32, LANES), f32)
    first = jnp.concatenate([damping * crhs / cdia, pad], axis=0)
    table[...] = first
    own = jnp.transpose(first)[0:PEERS]
    rhs[...] = jnp.transpose(jnp.concatenate([crhs, pad], axis=0))[0:PEERS]
    dia[...] = jnp.transpose(jnp.concatenate([cdia, pad + 1.0], axis=0))[0:PEERS]
    sub = lax.broadcasted_iota(i32, (8, LANES), 0)
    most = jnp.zeros((8, LANES), i32)
    for d in range(PEERS):
        c = data[d, 72:80, :].astype(i32)
        off = lax.bitwise_and(sub - c, 7)
        most = jnp.maximum(most, off)
        at = lane_of_device(lax.shift_right_logical(c, 5), me)
        code = lax.bitwise_and(lax.shift_right_logical(c, 3), 3) + lax.shift_left(off, 2)
        where[d] = code + lax.shift_left(at, 5)
    most = jnp.max(most.astype(f32)).astype(i32) + 1
    passes[...] = jnp.broadcast_to(most, passes.shape)
    new[...] = coarse_step(
        table, where, most, data, own, rhs[...], dia[...], gather
    )


def gathered(table, pieces, mine):
    row = 0
    for piece in pieces:
        size = piece.shape[0]
        mine[row : row + size, :] = piece[...]
        row += size
    table[...] = jnp.transpose(mine[...])


def coarse_kernel(base_ref, passes, p0, p1, p2, p3, rhs, dia, where, data, new, table, mine, gather):
    gathered(table, (p0, p1, p2, p3), mine)
    new[...] = coarse_step(
        table, where, passes[...][0, 0], data, p0[...], rhs[...], dia[...], gather
    )


def post_kernel(base_ref, p0, p1, p2, p3, first_iter, rhs, dia, col, blk, node_row, before, after,
                before2, after2, out, correction, table, mine, one, two):
    base = base_ref[0]
    me = lax.shift_right_logical(base, 10)
    gathered(table, (p0, p1, p2, p3), mine)
    row = mine[pl.ds(lane_of_device(me, me), 1), :]
    correction[...] = jnp.concatenate([row[:, 32 * i : 32 * i + 32] for i in range(3)], axis=0)
    one[...] = first_iter[...]
    one[:, lanes(0, HALO)] = before2[...]
    one[:, lanes(WIDE + ROWS + HALO, HALO)] = after2[...]
    edge = [
        h[P_ROW + t : P_ROW + t + 1, lanes(LANES * q)]
        for h in (before, after) for t in range(2) for q in range(2)
    ]
    edge = jnp.concatenate(edge, axis=0)

    def found(rows):
        rows = rows.astype(i32)
        lane = lane_of_device(lax.shift_right_logical(rows, 5), me)
        return coarse_lookup(table, lax.bitwise_and(rows, 31), lane)

    own, far = found(node_row[...]), found(edge)
    for s in range(16):
        if s < 4:
            row = [f[s : s + 1, :] for f in far]
        elif s < 12:
            row = [f[s - 4 : s - 3, :] for f in own]
        else:
            row = [f[s - 8 : s - 7, :] for f in far]
        one[:, lanes(s * LANES)] = one[:, lanes(s * LANES)] + jnp.concatenate(row, axis=0)
    two[...] = jnp.zeros(two.shape, f32)
    sweep_halo(two, one, rhs, dia, before, base, WIDE - HALO)
    sweep_halo(two, one, rhs, dia, after, base, WIDE + ROWS)

    def first(b):
        at = WIDE + b * LANES
        pull = own_block(one, col, blk, base, b)
        two[:, lanes(at)] = smoothed(one, pull, rhs, dia, at)

    def second(b):
        at = WIDE + b * LANES
        pull = own_block(two, col, blk, base, b)
        out[:, lanes(b * LANES)] = smoothed(two, pull, rhs, dia, at)

    each_block(first)
    each_block(second)


def call(kernel, outs, args, scratch=(), scalars=0, limit=12):
    vmem = pl.BlockSpec(memory_space=pltpu.VMEM)
    smem = pl.BlockSpec(memory_space=pltpu.SMEM)
    return pl.pallas_call(
        kernel,
        in_specs=[smem] * scalars + [vmem] * (len(args) - scalars),
        out_specs=[vmem] * len(outs),
        out_shape=[jax.ShapeDtypeStruct(o, t) for o, t in outs],
        scratch_shapes=[
            pltpu.VMEM(*s) if isinstance(s[0], tuple) else pltpu.VMEM(s, f32) for s in scratch
        ],
        compiler_params=pltpu.CompilerParams(vmem_limit_bytes=limit * 2**20),
    )(*args)


def in_group(new):
    def partner(bits):
        return lax.ppermute(new, DOM, [(i, i ^ bits) for i in range(lax.axis_size(DOM))])

    p2, p3, p1 = partner(2), partner(3), partner(1)
    return new, p1, p2, p3


def shifts(up, down):
    count = lax.axis_size(DOM)
    forward = [(i, i + 1) for i in range(count - 1)]
    backward = [(i + 1, i) for i in range(count - 1)]
    return lax.ppermute(up, DOM, forward), lax.ppermute(down, DOM, backward)


def cycle(right_side, fine_diagonal, fine_columns, fine_blocks, aggregate_of_node,
         coarse_row_of_aggregate, coarse_diagonal, coarse_columns, coarse_blocks):
    rhs, dia = right_side.T, fine_diagonal.T
    col, blk = fine_columns.T, fine_blocks.transpose(2, 3, 1, 0)
    agg = aggregate_of_node.reshape(8, LANES)
    owner = coarse_row_of_aggregate.reshape(1, 32)
    cdia, cblk = coarse_diagonal.T, coarse_blocks.transpose(2, 3, 0, 1)
    me = lax.axis_index(DOM).astype(i32).reshape(1)
    base = me * ROWS
    wide = WIDE + ROWS + WIDE

    dsend, = call(
        coarse_pack_kernel, [((PEERS, 80, LANES), f32)], [coarse_columns, cblk],
        limit=60,
    )
    data = lax.all_to_all(
        dsend, DOM, 0, 0, axis_index_groups=row_groups(), tiled=True
    )
    vmem, far = pl.BlockSpec(memory_space=pltpu.VMEM), pl.BlockSpec(memory_space=pltpu.HBM)
    up, down, node_row = pl.pallas_call(
        pack_kernel,
        name="pack",
        in_specs=[far] * 6,
        out_specs=[vmem] * 3,
        out_shape=[jax.ShapeDtypeStruct(o, f32) for o in ((P_ALL, HALO), (P_ALL, HALO), (8, LANES))],
        scratch_shapes=[
            pltpu.VMEM((3, ROWS), f32), pltpu.VMEM((3, ROWS), f32),
            pltpu.VMEM((2, SLOTS, HALO), i32), pltpu.VMEM((2, 3, 3, SLOTS, HALO), f32),
            pltpu.VMEM((8, LANES), i32), pltpu.VMEM((1, 32), i32), pltpu.SemaphoreType.DMA((8,)),
        ],
        compiler_params=pltpu.CompilerParams(vmem_limit_bytes=12 * 2**20),
    )(rhs, dia, col, blk, agg, owner)
    before, after = shifts(up, down)
    send, first_iter, wrhs, wdia, up2, down2 = call(
        pre_kernel,
        [((LANES, 2, LANES), f32), ((3, wide), f32), ((3, wide), f32), ((3, wide), f32),
         ((3, HALO), f32), ((3, HALO), f32)],
        [base, rhs, dia, col, blk, agg, owner, cdia, before, after],
        scratch=[(3, wide), (3, wide), (8, ROWS)], scalars=1,
    )
    before2, after2 = shifts(up2, down2)
    sums = lax.all_to_all(send, DOM, 0, 0, tiled=True)
    peers = ((PEERS, LANES), f32)
    gather = (3, PEERS, LANES)
    square = (LANES, LANES)
    new, crhs, cd, where, passes = call(
        coarse_first_kernel,
        [peers, peers, peers, ((PEERS, 8, LANES), i32), ((8, LANES), i32)],
        [base, sums, data, before2, after2],
        scratch=[square, gather, ((288, 4096), jnp.bfloat16), ((LANES, 4096), jnp.bfloat16)],
        scalars=1,
    )
    for _ in range(CSWEEPS - 2):
        new, = call(
            coarse_kernel, [peers],
            [base, passes, *in_group(new), crhs, cd, where, data],
            scratch=[square, square, gather], scalars=1,
        )
    solution, mine = call(
        post_kernel, [((3, ROWS), f32), ((3, 32), f32)],
        [base, *in_group(new), first_iter, wrhs, wdia, col, blk, node_row,
         before, after, before2, after2],
        scratch=[square, square, (3, wide), (3, wide)], scalars=1,
    )
    return solution.T, mine.T


def solution(mesh):
    return jax.shard_map(
        cycle,
        mesh=mesh,
        in_specs=(
            P(DOM, None),
            P(DOM, None),
            P(DOM, None),
            P(DOM, None, None, None),
            P(DOM),
            P(DOM),
            P(DOM, None),
            P(DOM, None),
            P(DOM, None, None, None),
        ),
        out_specs=(P(DOM, None), P(DOM, None)),
        check_vma=False,
    )
```

```python
import jax
import jax.numpy as jnp
from jax import lax
from jax.experimental import pallas as pl
from jax.experimental.pallas import tpu as pltpu
from jax.sharding import PartitionSpec as P


DOM = "dom"
PEERS = 32
UNROLL = 8
CSWEEPS = 6
damping = 0.7
highest = lax.Precision.HIGHEST

ROWS = 1024
LANES = 128
SLOTS = 27
FULL = 24
HALO = 256
WIDE = 512
BLOCKS = ROWS // LANES
P_COL = 9 * FULL
P_BTAIL = P_COL + FULL
P_CTAIL = P_BTAIL + 27
P_RHS = P_CTAIL + 3
P_DIA = P_RHS + 6
P_ROW = P_DIA + 6
P_ALL = 288
f32 = jnp.float32
i32 = jnp.int32


def lanes(start, size=LANES):
    if isinstance(start, int):
        return slice(start, start + size)
    return pl.ds(pl.multiple_of(start, LANES), size)


def picked(row, where):
    return jnp.take_along_axis(
        jnp.broadcast_to(row, where.shape), where, axis=1, mode="promise_in_bounds"
    )


def pack_kernel(rhs_in, dia_in, col_in, blk_in, agg_in, owner_in, up, down, node_row,
                rhs, dia, col, blk, agg, owner, sem):
    copies = [(rhs_in, rhs), (dia_in, dia), (agg_in, agg), (owner_in, owner)]
    for t, near in enumerate((ROWS - HALO, 0)):
        copies.append((col_in.at[:, lanes(near, HALO)], col.at[t]))
        copies.append((blk_in.at[:, :, :, lanes(near, HALO)], blk.at[t]))
    copies = [pltpu.make_async_copy(a, b, sem.at[n]) for n, (a, b) in enumerate(copies)]
    for c in copies:
        c.start()
    for c in copies:
        c.wait()
    table = jnp.concatenate([owner[...]] * 4, axis=1)
    found = picked(table, agg[...]).astype(f32)
    node_row[...] = found
    for t, (out, wide) in enumerate(((up, ROWS - WIDE), (down, 0))):
        for i in range(3):
            for j in range(3):
                g = 3 * i + j
                out[g * FULL : (g + 1) * FULL, :] = blk[t, i, j, 0:FULL, :]
                out[P_BTAIL + 3 * g : P_BTAIL + 3 * g + 3, :] = blk[t, i, j, FULL:SLOTS, :]
        out[P_COL : P_COL + FULL, :] = col[t, 0:FULL, :].astype(f32)
        out[P_CTAIL : P_CTAIL + 3, :] = col[t, FULL:SLOTS, :].astype(f32)
        for h in range(2):
            out[P_RHS + 3 * h : P_RHS + 3 * h + 3, :] = rhs[:, lanes(wide + HALO * h, HALO)]
            out[P_DIA + 3 * h : P_DIA + 3 * h + 3, :] = dia[:, lanes(wide + HALO * h, HALO)]
            for q in range(2):
                s = wide // LANES + 2 * h + q
                out[P_ROW + h : P_ROW + h + 1, lanes(LANES * q)] = found[s : s + 1, :]
        out[P_ROW + 2 : P_ALL, :] = jnp.zeros((P_ALL - P_ROW - 2, HALO), f32)


def pulled_block(columns, blocks, table, first_chunk):
    total = [None, None, None]
    for part in range(4):
        where = columns(part)
        chunk = lax.shift_right_arithmetic(where, 7)
        lane = lax.bitwise_and(where, 127)
        near = [jnp.zeros(where.shape, f32) for _ in range(3)]
        for c in range(5):
            here = chunk == c
            for j in range(3):
                row = table[j : j + 1, lanes(first_chunk * LANES + c * LANES)]
                near[j] = jnp.where(here, picked(row, lane), near[j])
        for i in range(3):
            s = blocks(i, 0, part) * near[0]
            s = s + blocks(i, 1, part) * near[1]
            s = s + blocks(i, 2, part) * near[2]
            if part < 3:
                total[i] = s if total[i] is None else total[i] + s
            else:
                total[i] = jnp.sum(total[i], axis=0, keepdims=True) + jnp.sum(
                    s, axis=0, keepdims=True
                )
    return total


def local_getters(col, blk, start, b):
    def columns(part):
        lo, hi = 8 * part, min(8 * part + 8, SLOTS)
        return col[lo:hi, lanes(b * LANES)] - start

    def blocks(i, j, part):
        lo, hi = 8 * part, min(8 * part + 8, SLOTS)
        return blk[i, j, lo:hi, lanes(b * LANES)]

    return columns, blocks


def halo_getters(halo, start, b):
    def columns(part):
        if part < 3:
            got = halo[P_COL + 8 * part : P_COL + 8 * part + 8, lanes(b * LANES)]
        else:
            got = halo[P_CTAIL : P_CTAIL + 3, lanes(b * LANES)]
        return got.astype(i32) - start

    def blocks(i, j, part):
        g = 3 * i + j
        if part < 3:
            return halo[g * FULL + 8 * part : g * FULL + 8 * part + 8, lanes(b * LANES)]
        return halo[P_BTAIL + 3 * g : P_BTAIL + 3 * g + 3, lanes(b * LANES)]

    return columns, blocks


def wide_vector(out, local, before, after, row):
    out[:, lanes(WIDE, ROWS)] = local[...]
    for h in range(2):
        out[:, lanes(HALO * h, HALO)] = before[row + 3 * h : row + 3 * h + 3, :]
        out[:, lanes(WIDE + ROWS + HALO * h, HALO)] = after[row + 3 * h : row + 3 * h + 3, :]


def smoothed(table, pulled, rhs, dia, at):
    pull = jnp.concatenate(pulled, axis=0)
    s = table[:, lanes(at)]
    b = rhs[:, lanes(at)]
    d = dia[:, lanes(at)]
    return s + damping * (b - (d * s - pull)) / d


def sweep_halo(out, table, rhs, dia, halo, base, first):
    for b in range(2):
        at = first + LANES * b
        start = base + (at - WIDE) - 2 * LANES
        cols, blks = halo_getters(halo, start, b)
        pull = pulled_block(cols, blks, table, at // LANES - 2)
        out[:, lanes(at)] = smoothed(table, pull, rhs, dia, at)


def each_block(step):
    def some(t, carry):
        for u in range(UNROLL):
            step(t * UNROLL + u)
        return carry

    lax.fori_loop(0, BLOCKS // UNROLL, some, 0)


def own_block(table, col, blk, base, b):
    start = base + b * LANES - 2 * LANES
    cols, blks = local_getters(col, blk, start, b)
    return pulled_block(cols, blks, table, b + WIDE // LANES - 2)


def pre_kernel(base_ref, rhs, dia, col, blk, agg, owner_row, cdia, before, after,
               send, first_iter, keep_rhs, keep_dia, up2, down2, one, two, res):
    base = base_ref[0]
    wide_vector(keep_rhs, rhs, before, after, P_RHS)
    wide_vector(keep_dia, dia, before, after, P_DIA)
    raw = keep_dia[...]
    keep_dia[...] = jnp.where(raw == 0.0, 1.0, raw)
    one[...] = damping * keep_rhs[...] / keep_dia[...]
    two[...] = jnp.zeros(two.shape, f32)
    sweep_halo(two, one, keep_rhs, keep_dia, before, base, WIDE - HALO)
    sweep_halo(two, one, keep_rhs, keep_dia, after, base, WIDE + ROWS)

    def second(b):
        at = WIDE + b * LANES
        pull = own_block(one, col, blk, base, b)
        two[:, lanes(at)] = smoothed(one, pull, keep_rhs, keep_dia, at)

    each_block(second)

    def third(b):
        at = WIDE + b * LANES
        pull = jnp.concatenate(own_block(two, col, blk, base, b), axis=0)
        s, d = two[:, lanes(at)], keep_dia[:, lanes(at)]
        res[0:3, lanes(b * LANES)] = keep_rhs[:, lanes(at)] - (d * s - pull)

    res[...] = jnp.zeros(res.shape, f32)
    each_block(third)
    first_iter[...] = two[...]
    up2[...] = two[:, lanes(WIDE + ROWS - WIDE, HALO)]
    down2[...] = two[:, lanes(WIDE + HALO, HALO)]
    label = lax.broadcasted_iota(i32, (32, LANES), 0)
    sums = None
    for b in range(BLOCKS):
        member = (label == jnp.broadcast_to(agg[b : b + 1, :], (32, LANES))).astype(f32)
        part = lax.dot_general(
            res[:, lanes(b * LANES)], member, (((1,), (1,)), ((), ())),
            precision=highest, preferred_element_type=f32,
        )
        sums = part if sums is None else sums + part
    row = jnp.concatenate(
        [sums[0:1], sums[1:2], sums[2:3], owner_row[...].astype(f32)], axis=1
    )
    send[0, 0:1, :] = row
    row = jnp.concatenate(
        [cdia[0:1], cdia[1:2], cdia[2:3], jnp.ones((1, 32), f32)], axis=1
    )
    send[0, 1:2, :] = row


def parity(p):
    return lax.bitwise_and(
        lax.bitwise_xor(lax.shift_right_logical(p, 1), lax.shift_right_logical(p, 2)), 1
    )


def lane_of_device(p, me):
    side = lax.shift_left(lax.bitwise_xor(parity(p), parity(me)), 6)
    core = lax.shift_left(lax.bitwise_and(lax.bitwise_xor(p, me), 1), 5)
    return side + core + lax.shift_right_logical(p, 2)


def device_of_lane(q, me):
    side = lax.bitwise_xor(lax.shift_right_logical(q, 6), parity(me))
    side = lax.bitwise_xor(side, lax.bitwise_and(q, 1))
    core = lax.bitwise_and(lax.bitwise_xor(lax.shift_right_logical(q, 5), me), 1)
    return lax.shift_left(lax.bitwise_and(q, 31), 2) + lax.shift_left(side, 1) + core


def row_of_device(p, me):
    p = lax.bitwise_xor(p, me)
    far = lax.shift_left(lax.bitwise_and(lax.shift_right_logical(p, 2), 1), 6)
    yz = lax.shift_left(lax.shift_right_logical(p, 3), 2)
    return far + yz + lax.bitwise_and(p, 3)


def row_groups():
    return [
        [4 * m + 2 * (side ^ (m & 1)) + core for m in range(PEERS)]
        for side in range(2) for core in range(2)
    ]


def coarse_pack_kernel(col, blk, send):
    def turned(a):
        z = jnp.transpose(jnp.concatenate([a, jnp.zeros((32, 5), f32)], axis=1))
        return jnp.concatenate([z] * 4, axis=1)

    columns = turned(col[...].astype(f32))
    kind = lax.bitwise_and(columns.astype(i32), 7)
    tile = (8, LANES)
    sub = lax.broadcasted_iota(i32, tile, 0)
    count = jnp.zeros(tile, i32)
    match, earlier = [], []
    for k in range(SLOTS):
        here = sub == jnp.broadcast_to(kind[k : k + 1], tile)
        match.append(here)
        earlier.append(count)
        count = count + here.astype(i32)
    left = jnp.zeros((1, LANES), i32)
    start = []
    for n in range(16):
        if n >= 8:
            start.append(left)
        left = jnp.maximum(left + count[n % 8 : n % 8 + 1] - 4, 0)
    start = jnp.concatenate(start, axis=0) + 4 * sub
    place = 4 * sub + lax.shift_right_logical(lax.broadcasted_iota(i32, tile, 1), 5)
    slot = jnp.full(tile, 31, i32)
    for k in range(SLOTS):
        at = jnp.sum(jnp.where(match[k], start + earlier[k], 0), axis=0, keepdims=True)
        slot = jnp.where(place == jnp.broadcast_to(lax.bitwise_and(at, 31), tile), k, slot)
    inner, outer = lax.bitwise_and(slot, 7), lax.shift_right_logical(slot, 3)

    def placed(z):
        got = None
        for g in range(4):
            part = jnp.take_along_axis(
                z[8 * g : 8 * g + 8], inner, axis=0, mode="promise_in_bounds"
            )
            got = part if got is None else jnp.where(outer == g, part, got)
        return got

    parts = [placed(turned(blk[i, j])) for i in range(3) for j in range(3)]
    parts.append(jnp.where(slot == 31, sub.astype(f32), placed(columns)))
    for m in range(10):
        for d in range(PEERS):
            send[d, 8 * m : 8 * m + 8, :] = parts[m]


def spread(parts):
    group = lax.shift_right_logical(lax.broadcasted_iota(i32, parts[0].shape, 1), 5)
    return jnp.where(group == 0, parts[0], jnp.where(group == 1, parts[1], parts[2]))


def coarse_lookup(table, chunk, lane):
    near = [jnp.zeros(chunk.shape, f32) for _ in range(3)]
    for c in range(32):
        here = chunk == c
        for j in range(3):
            row = table[32 * j + c : 32 * j + c + 1, :]
            near[j] = jnp.where(here, picked(row, lane), near[j])
    return near


def coarse_step(table, where, passes, data, own, rhs, dia, gather):
    gather[...] = jnp.zeros(gather.shape, f32)

    def one_pass(t, carry):
        rows = [
            [pltpu.roll(table[32 * j + 8 * v : 32 * j + 8 * v + 8, :], t, axis=0) for v in range(4)]
            for j in range(3)
        ]
        for d in range(PEERS):
            w = where[d]
            code, lane = lax.bitwise_and(w, 31), lax.shift_right_logical(w, 5)
            near = [jnp.zeros((8, LANES), f32) for _ in range(3)]
            for v in range(4):
                here = code == 4 * t + v
                for j in range(3):
                    near[j] = jnp.where(here, picked(rows[j][v], lane), near[j])
            for i in range(3):
                a = data[d, lanes8(3 * i), :] * near[0]
                a = a + data[d, lanes8(3 * i + 1), :] * near[1]
                a = a + data[d, lanes8(3 * i + 2), :] * near[2]
                gather[i, d : d + 1, :] += jnp.sum(a, axis=0, keepdims=True)
        return carry

    lax.fori_loop(0, passes, one_pass, 0)
    parts = []
    for i in range(3):
        s = gather[i]
        s = s + pltpu.roll(s, 64, axis=1)
        parts.append(s + pltpu.roll(s, 32, axis=1))
    return own + damping * (rhs - (dia * own - spread(parts))) / dia


def lanes8(m):
    return slice(8 * m, 8 * m + 8)


def coarse_first_kernel(base_ref, sums, data, far_up, far_down, new, rhs, dia, where, passes,
                        table, gather, left, right):
    me = lax.shift_right_logical(base_ref[0], 10)
    got = jnp.transpose(sums[:, 0, :])
    rows = got[96:128].astype(i32)
    s = got[0:96]
    split = []
    for _ in range(3):
        t = s.astype(jnp.bfloat16).astype(f32)
        split.append(t)
        s = s - t
    chunk = lax.broadcasted_iota(i32, (32, LANES), 0)
    place = lax.broadcasted_iota(i32, (LANES, LANES), 0)
    low = lax.bitwise_and(rows, 31)
    lane = lane_of_device(lax.shift_right_logical(rows, 5), me)
    for a in range(32):
        here = chunk == jnp.broadcast_to(low[a : a + 1], (32, LANES))
        for t in range(3):
            for i in range(3):
                value = jnp.broadcast_to(split[t][32 * i + a : 32 * i + a + 1], (32, LANES))
                left[96 * t + 32 * i : 96 * t + 32 * i + 32, lanes(LANES * a)] = jnp.where(
                    here, value, 0.0
                ).astype(jnp.bfloat16)
        right[:, lanes(LANES * a)] = jnp.where(
            place == jnp.broadcast_to(lane[a : a + 1], (LANES, LANES)), 1.0, 0.0
        ).astype(jnp.bfloat16)
    both = lax.dot_general(
        left[...], right[...], (((1,), (1,)), ((), ())), preferred_element_type=f32
    )
    crhs = both[0:96] + both[96:192] + both[192:288]
    order = row_of_device(device_of_lane(lax.broadcasted_iota(i32, (96, LANES), 1), me), me)
    cdia = jnp.take_along_axis(
        jnp.transpose(sums[:, 1, :])[0:96], order, axis=1, mode="promise_in_bounds"
    )
    pad = jnp.zeros((32, LANES), f32)
    first = jnp.concatenate([damping * crhs / cdia, pad], axis=0)
    table[...] = first
    own = jnp.transpose(first)[0:PEERS]
    rhs[...] = jnp.transpose(jnp.concatenate([crhs, pad], axis=0))[0:PEERS]
    dia[...] = jnp.transpose(jnp.concatenate([cdia, pad + 1.0], axis=0))[0:PEERS]
    sub = lax.broadcasted_iota(i32, (8, LANES), 0)
    most = jnp.zeros((8, LANES), i32)
    for d in range(PEERS):
        c = data[d, 72:80, :].astype(i32)
        off = lax.bitwise_and(sub - c, 7)
        most = jnp.maximum(most, off)
        at = lane_of_device(lax.shift_right_logical(c, 5), me)
        code = lax.bitwise_and(lax.shift_right_logical(c, 3), 3) + lax.shift_left(off, 2)
        where[d] = code + lax.shift_left(at, 5)
    most = jnp.max(most.astype(f32)).astype(i32) + 1
    passes[...] = jnp.broadcast_to(most, passes.shape)
    new[...] = coarse_step(
        table, where, most, data, own, rhs[...], dia[...], gather
    )


def gathered(table, pieces, mine):
    row = 0
    for piece in pieces:
        size = piece.shape[0]
        mine[row : row + size, :] = piece[...]
        row += size
    table[...] = jnp.transpose(mine[...])


def coarse_kernel(base_ref, passes, p0, p1, p2, p3, rhs, dia, where, data, new, table, mine, gather):
    gathered(table, (p0, p1, p2, p3), mine)
    new[...] = coarse_step(
        table, where, passes[...][0, 0], data, p0[...], rhs[...], dia[...], gather
    )


def post_kernel(base_ref, p0, p1, p2, p3, first_iter, rhs, dia, col, blk, node_row, before, after,
                before2, after2, out, correction, table, mine, one, two):
    base = base_ref[0]
    me = lax.shift_right_logical(base, 10)
    gathered(table, (p0, p1, p2, p3), mine)
    row = mine[pl.ds(lane_of_device(me, me), 1), :]
    correction[...] = jnp.concatenate([row[:, 32 * i : 32 * i + 32] for i in range(3)], axis=0)
    one[...] = first_iter[...]
    one[:, lanes(0, HALO)] = before2[...]
    one[:, lanes(WIDE + ROWS + HALO, HALO)] = after2[...]
    edge = [
        h[P_ROW + t : P_ROW + t + 1, lanes(LANES * q)]
        for h in (before, after) for t in range(2) for q in range(2)
    ]
    edge = jnp.concatenate(edge, axis=0)

    def found(rows):
        rows = rows.astype(i32)
        lane = lane_of_device(lax.shift_right_logical(rows, 5), me)
        return coarse_lookup(table, lax.bitwise_and(rows, 31), lane)

    own, far = found(node_row[...]), found(edge)
    for s in range(16):
        if s < 4:
            row = [f[s : s + 1, :] for f in far]
        elif s < 12:
            row = [f[s - 4 : s - 3, :] for f in own]
        else:
            row = [f[s - 8 : s - 7, :] for f in far]
        one[:, lanes(s * LANES)] = one[:, lanes(s * LANES)] + jnp.concatenate(row, axis=0)
    two[...] = jnp.zeros(two.shape, f32)
    sweep_halo(two, one, rhs, dia, before, base, WIDE - HALO)
    sweep_halo(two, one, rhs, dia, after, base, WIDE + ROWS)

    def first(b):
        at = WIDE + b * LANES
        pull = own_block(one, col, blk, base, b)
        two[:, lanes(at)] = smoothed(one, pull, rhs, dia, at)

    def second(b):
        at = WIDE + b * LANES
        pull = own_block(two, col, blk, base, b)
        out[:, lanes(b * LANES)] = smoothed(two, pull, rhs, dia, at)

    each_block(first)
    each_block(second)


def call(kernel, outs, args, scratch=(), scalars=0, limit=12):
    vmem = pl.BlockSpec(memory_space=pltpu.VMEM)
    smem = pl.BlockSpec(memory_space=pltpu.SMEM)
    return pl.pallas_call(
        kernel,
        in_specs=[smem] * scalars + [vmem] * (len(args) - scalars),
        out_specs=[vmem] * len(outs),
        out_shape=[jax.ShapeDtypeStruct(o, t) for o, t in outs],
        scratch_shapes=[
            pltpu.VMEM(*s) if isinstance(s[0], tuple) else pltpu.VMEM(s, f32) for s in scratch
        ],
        compiler_params=pltpu.CompilerParams(vmem_limit_bytes=limit * 2**20),
    )(*args)


def partner(value, bits):
    return lax.ppermute(value, DOM, [(i, i ^ bits) for i in range(lax.axis_size(DOM))])


def in_group(new):
    p2, p3, p1 = partner(new, 2), partner(new, 3), partner(new, 1)
    return new, p1, p2, p3


def shifts(up, down):
    count = lax.axis_size(DOM)
    forward = [(i, i + 1) for i in range(count - 1)]
    backward = [(i + 1, i) for i in range(count - 1)]
    return lax.ppermute(up, DOM, forward), lax.ppermute(down, DOM, backward)


def cycle(right_side, fine_diagonal, fine_columns, fine_blocks, aggregate_of_node,
         coarse_row_of_aggregate, coarse_diagonal, coarse_columns, coarse_blocks):
    rhs, dia = right_side.T, fine_diagonal.T
    col, blk = fine_columns.T, fine_blocks.transpose(2, 3, 1, 0)
    agg = aggregate_of_node.reshape(8, LANES)
    owner = coarse_row_of_aggregate.reshape(1, 32)
    cdia, cblk = coarse_diagonal.T, coarse_blocks.transpose(2, 3, 0, 1)
    me = lax.axis_index(DOM).astype(i32).reshape(1)
    base = me * ROWS
    wide = WIDE + ROWS + WIDE

    dsend, = call(
        coarse_pack_kernel, [((PEERS, 80, LANES), f32)], [coarse_columns, cblk],
        limit=60,
    )
    data = lax.all_to_all(
        dsend, DOM, 0, 0, axis_index_groups=row_groups(), tiled=True
    )
    vmem, far = pl.BlockSpec(memory_space=pltpu.VMEM), pl.BlockSpec(memory_space=pltpu.HBM)
    up, down, node_row = pl.pallas_call(
        pack_kernel,
        name="pack",
        in_specs=[far] * 6,
        out_specs=[vmem] * 3,
        out_shape=[jax.ShapeDtypeStruct(o, f32) for o in ((P_ALL, HALO), (P_ALL, HALO), (8, LANES))],
        scratch_shapes=[
            pltpu.VMEM((3, ROWS), f32), pltpu.VMEM((3, ROWS), f32),
            pltpu.VMEM((2, SLOTS, HALO), i32), pltpu.VMEM((2, 3, 3, SLOTS, HALO), f32),
            pltpu.VMEM((8, LANES), i32), pltpu.VMEM((1, 32), i32), pltpu.SemaphoreType.DMA((8,)),
        ],
        compiler_params=pltpu.CompilerParams(vmem_limit_bytes=60 * 2**20),
    )(rhs, dia, col, blk, agg, owner)
    before, after = shifts(up, down)
    send, first_iter, wrhs, wdia, up2, down2 = call(
        pre_kernel,
        [((1, 2, LANES), f32), ((3, wide), f32), ((3, wide), f32), ((3, wide), f32),
         ((3, HALO), f32), ((3, HALO), f32)],
        [base, rhs, dia, col, blk, agg, owner, cdia, before, after],
        scratch=[(3, wide), (3, wide), (8, ROWS)], scalars=1,
    )
    before2, after2 = shifts(up2, down2)
    sums = send
    for bits in ((1, 2, 3), (8, 16, 24), (32, 64, 96), (4,)):
        sums = jnp.concatenate([sums] + [partner(sums, b) for b in bits], axis=0)
    peers = ((PEERS, LANES), f32)
    gather = (3, PEERS, LANES)
    square = (LANES, LANES)
    new, crhs, cd, where, passes = call(
        coarse_first_kernel,
        [peers, peers, peers, ((PEERS, 8, LANES), i32), ((8, LANES), i32)],
        [base, sums, data, before2, after2],
        scratch=[square, gather, ((288, 4096), jnp.bfloat16), ((LANES, 4096), jnp.bfloat16)],
        scalars=1,
    )
    for _ in range(CSWEEPS - 2):
        new, = call(
            coarse_kernel, [peers],
            [base, passes, *in_group(new), crhs, cd, where, data],
            scratch=[square, square, gather], scalars=1,
        )
    solution, mine = call(
        post_kernel, [((3, ROWS), f32), ((3, 32), f32)],
        [base, *in_group(new), first_iter, wrhs, wdia, col, blk, node_row,
         before, after, before2, after2],
        scratch=[square, square, (3, wide), (3, wide)], scalars=1,
    )
    return solution.T, mine.T


def solution(mesh):
    return jax.shard_map(
        cycle,
        mesh=mesh,
        in_specs=(
            P(DOM, None),
            P(DOM, None),
            P(DOM, None),
            P(DOM, None, None, None),
            P(DOM),
            P(DOM),
            P(DOM, None),
            P(DOM, None),
            P(DOM, None, None, None),
        ),
        out_specs=(P(DOM, None), P(DOM, None)),
        check_vma=False,
    )
```

```python
import jax
import jax.numpy as jnp
from jax import lax
from jax.experimental import pallas as pl
from jax.experimental.pallas import tpu as pltpu
from jax.sharding import PartitionSpec as P


DOM = "dom"
PEERS = 32
UNROLL = 8
CSWEEPS = 6
damping = 0.7
highest = lax.Precision.HIGHEST

ROWS = 1024
LANES = 128
SLOTS = 27
FULL = 24
HALO = 256
WIDE = 512
BLOCKS = ROWS // LANES
P_COL = 9 * FULL
P_BTAIL = P_COL + FULL
P_CTAIL = P_BTAIL + 27
P_RHS = P_CTAIL + 3
P_DIA = P_RHS + 6
P_ROW = P_DIA + 6
P_ALL = 288
f32 = jnp.float32
i32 = jnp.int32


def lanes(start, size=LANES):
    if isinstance(start, int):
        return slice(start, start + size)
    return pl.ds(pl.multiple_of(start, LANES), size)


def picked(row, where):
    return jnp.take_along_axis(
        jnp.broadcast_to(row, where.shape), where, axis=1, mode="promise_in_bounds"
    )


def pack_kernel(rhs_in, dia_in, col_in, blk_in, agg_in, owner_in, up, down, node_row,
                rhs, dia, col, blk, agg, owner, sem):
    copies = [(rhs_in, rhs), (dia_in, dia), (agg_in, agg), (owner_in, owner)]
    for t, near in enumerate((ROWS - HALO, 0)):
        copies.append((col_in.at[:, lanes(near, HALO)], col.at[t]))
        copies.append((blk_in.at[:, :, :, lanes(near, HALO)], blk.at[t]))
    copies = [pltpu.make_async_copy(a, b, sem.at[n]) for n, (a, b) in enumerate(copies)]
    for c in copies:
        c.start()
    for c in copies:
        c.wait()
    table = jnp.concatenate([owner[...]] * 4, axis=1)
    found = picked(table, agg[...]).astype(f32)
    node_row[...] = found
    for t, (out, wide) in enumerate(((up, ROWS - WIDE), (down, 0))):
        for i in range(3):
            for j in range(3):
                g = 3 * i + j
                out[g * FULL : (g + 1) * FULL, :] = blk[t, i, j, 0:FULL, :]
                out[P_BTAIL + 3 * g : P_BTAIL + 3 * g + 3, :] = blk[t, i, j, FULL:SLOTS, :]
        out[P_COL : P_COL + FULL, :] = col[t, 0:FULL, :].astype(f32)
        out[P_CTAIL : P_CTAIL + 3, :] = col[t, FULL:SLOTS, :].astype(f32)
        for h in range(2):
            out[P_RHS + 3 * h : P_RHS + 3 * h + 3, :] = rhs[:, lanes(wide + HALO * h, HALO)]
            out[P_DIA + 3 * h : P_DIA + 3 * h + 3, :] = dia[:, lanes(wide + HALO * h, HALO)]
            for q in range(2):
                s = wide // LANES + 2 * h + q
                out[P_ROW + h : P_ROW + h + 1, lanes(LANES * q)] = found[s : s + 1, :]
        out[P_ROW + 2 : P_ALL, :] = jnp.zeros((P_ALL - P_ROW - 2, HALO), f32)


def pulled_block(columns, blocks, table, first_chunk):
    total = [None, None, None]
    for part in range(4):
        where = columns(part)
        chunk = lax.shift_right_arithmetic(where, 7)
        lane = lax.bitwise_and(where, 127)
        near = [jnp.zeros(where.shape, f32) for _ in range(3)]
        for c in range(5):
            here = chunk == c
            for j in range(3):
                row = table[j : j + 1, lanes(first_chunk * LANES + c * LANES)]
                near[j] = jnp.where(here, picked(row, lane), near[j])
        for i in range(3):
            s = blocks(i, 0, part) * near[0]
            s = s + blocks(i, 1, part) * near[1]
            s = s + blocks(i, 2, part) * near[2]
            if part < 3:
                total[i] = s if total[i] is None else total[i] + s
            else:
                total[i] = jnp.sum(total[i], axis=0, keepdims=True) + jnp.sum(
                    s, axis=0, keepdims=True
                )
    return total


def local_getters(col, blk, start, b):
    def columns(part):
        lo, hi = 8 * part, min(8 * part + 8, SLOTS)
        return col[lo:hi, lanes(b * LANES)] - start

    def blocks(i, j, part):
        lo, hi = 8 * part, min(8 * part + 8, SLOTS)
        return blk[i, j, lo:hi, lanes(b * LANES)]

    return columns, blocks


def halo_getters(halo, start, b):
    def columns(part):
        if part < 3:
            got = halo[P_COL + 8 * part : P_COL + 8 * part + 8, lanes(b * LANES)]
        else:
            got = halo[P_CTAIL : P_CTAIL + 3, lanes(b * LANES)]
        return got.astype(i32) - start

    def blocks(i, j, part):
        g = 3 * i + j
        if part < 3:
            return halo[g * FULL + 8 * part : g * FULL + 8 * part + 8, lanes(b * LANES)]
        return halo[P_BTAIL + 3 * g : P_BTAIL + 3 * g + 3, lanes(b * LANES)]

    return columns, blocks


def wide_vector(out, local, before, after, row):
    out[:, lanes(WIDE, ROWS)] = local[...]
    for h in range(2):
        out[:, lanes(HALO * h, HALO)] = before[row + 3 * h : row + 3 * h + 3, :]
        out[:, lanes(WIDE + ROWS + HALO * h, HALO)] = after[row + 3 * h : row + 3 * h + 3, :]


def smoothed(table, pulled, rhs, dia, at):
    pull = jnp.concatenate(pulled, axis=0)
    s = table[:, lanes(at)]
    b = rhs[:, lanes(at)]
    d = dia[:, lanes(at)]
    return s + damping * (b - (d * s - pull)) / d


def sweep_halo(out, table, rhs, dia, halo, base, first):
    for b in range(2):
        at = first + LANES * b
        start = base + (at - WIDE) - 2 * LANES
        cols, blks = halo_getters(halo, start, b)
        pull = pulled_block(cols, blks, table, at // LANES - 2)
        out[:, lanes(at)] = smoothed(table, pull, rhs, dia, at)


def each_block(step):
    def some(t, carry):
        for u in range(UNROLL):
            step(t * UNROLL + u)
        return carry

    lax.fori_loop(0, BLOCKS // UNROLL, some, 0)


def own_block(table, col, blk, base, b):
    start = base + b * LANES - 2 * LANES
    cols, blks = local_getters(col, blk, start, b)
    return pulled_block(cols, blks, table, b + WIDE // LANES - 2)


def pre_kernel(base_ref, rhs, dia, col, blk, agg, owner_row, cdia, before, after,
               send, first_iter, keep_rhs, keep_dia, up2, down2, one, two, res):
    base = base_ref[0]
    wide_vector(keep_rhs, rhs, before, after, P_RHS)
    wide_vector(keep_dia, dia, before, after, P_DIA)
    raw = keep_dia[...]
    keep_dia[...] = jnp.where(raw == 0.0, 1.0, raw)
    one[...] = damping * keep_rhs[...] / keep_dia[...]
    two[...] = jnp.zeros(two.shape, f32)
    sweep_halo(two, one, keep_rhs, keep_dia, before, base, WIDE - HALO)
    sweep_halo(two, one, keep_rhs, keep_dia, after, base, WIDE + ROWS)

    def second(b):
        at = WIDE + b * LANES
        pull = own_block(one, col, blk, base, b)
        two[:, lanes(at)] = smoothed(one, pull, keep_rhs, keep_dia, at)

    each_block(second)

    def third(b):
        at = WIDE + b * LANES
        pull = jnp.concatenate(own_block(two, col, blk, base, b), axis=0)
        s, d = two[:, lanes(at)], keep_dia[:, lanes(at)]
        res[0:3, lanes(b * LANES)] = keep_rhs[:, lanes(at)] - (d * s - pull)

    res[...] = jnp.zeros(res.shape, f32)
    each_block(third)
    first_iter[...] = two[...]
    up2[...] = two[:, lanes(WIDE + ROWS - WIDE, HALO)]
    down2[...] = two[:, lanes(WIDE + HALO, HALO)]
    label = lax.broadcasted_iota(i32, (32, LANES), 0)
    sums = None
    for b in range(BLOCKS):
        member = (label == jnp.broadcast_to(agg[b : b + 1, :], (32, LANES))).astype(f32)
        part = lax.dot_general(
            res[:, lanes(b * LANES)], member, (((1,), (1,)), ((), ())),
            precision=highest, preferred_element_type=f32,
        )
        sums = part if sums is None else sums + part
    row = jnp.concatenate(
        [sums[0:1], sums[1:2], sums[2:3], owner_row[...].astype(f32)], axis=1
    )
    send[0, 0:1, :] = row
    row = jnp.concatenate(
        [cdia[0:1], cdia[1:2], cdia[2:3], jnp.ones((1, 32), f32)], axis=1
    )
    send[0, 1:2, :] = row


def parity(p):
    return lax.bitwise_and(
        lax.bitwise_xor(lax.shift_right_logical(p, 1), lax.shift_right_logical(p, 2)), 1
    )


def lane_of_device(p, me):
    side = lax.shift_left(lax.bitwise_xor(parity(p), parity(me)), 6)
    core = lax.shift_left(lax.bitwise_and(lax.bitwise_xor(p, me), 1), 5)
    return side + core + lax.shift_right_logical(p, 2)


def device_of_lane(q, me):
    side = lax.bitwise_xor(lax.shift_right_logical(q, 6), parity(me))
    side = lax.bitwise_xor(side, lax.bitwise_and(q, 1))
    core = lax.bitwise_and(lax.bitwise_xor(lax.shift_right_logical(q, 5), me), 1)
    return lax.shift_left(lax.bitwise_and(q, 31), 2) + lax.shift_left(side, 1) + core


def row_of_device(p, me):
    p = lax.bitwise_xor(p, me)
    far = lax.shift_left(lax.bitwise_and(lax.shift_right_logical(p, 2), 1), 6)
    yz = lax.shift_left(lax.shift_right_logical(p, 3), 2)
    return far + yz + lax.bitwise_and(p, 3)


def row_groups():
    return [
        [4 * m + 2 * (side ^ (m & 1)) + core for m in range(PEERS)]
        for side in range(2) for core in range(2)
    ]


def coarse_pack_kernel(col, blk, send):
    def turned(a):
        z = jnp.transpose(jnp.concatenate([a, jnp.zeros((32, 5), f32)], axis=1))
        return jnp.concatenate([z] * 4, axis=1)

    columns = turned(col[...].astype(f32))
    kind = lax.bitwise_and(columns.astype(i32), 7)
    tile = (8, LANES)
    sub = lax.broadcasted_iota(i32, tile, 0)
    count = jnp.zeros(tile, i32)
    match, earlier = [], []
    for k in range(SLOTS):
        here = sub == jnp.broadcast_to(kind[k : k + 1], tile)
        match.append(here)
        earlier.append(count)
        count = count + here.astype(i32)
    left = jnp.zeros((1, LANES), i32)
    start = []
    for n in range(16):
        if n >= 8:
            start.append(left)
        left = jnp.maximum(left + count[n % 8 : n % 8 + 1] - 4, 0)
    start = jnp.concatenate(start, axis=0) + 4 * sub
    place = 4 * sub + lax.shift_right_logical(lax.broadcasted_iota(i32, tile, 1), 5)
    slot = jnp.full(tile, 31, i32)
    for k in range(SLOTS):
        at = jnp.sum(jnp.where(match[k], start + earlier[k], 0), axis=0, keepdims=True)
        slot = jnp.where(place == jnp.broadcast_to(lax.bitwise_and(at, 31), tile), k, slot)
    inner, outer = lax.bitwise_and(slot, 7), lax.shift_right_logical(slot, 3)

    def placed(z):
        got = None
        for g in range(4):
            part = jnp.take_along_axis(
                z[8 * g : 8 * g + 8], inner, axis=0, mode="promise_in_bounds"
            )
            got = part if got is None else jnp.where(outer == g, part, got)
        return got

    parts = [placed(turned(blk[i, j])) for i in range(3) for j in range(3)]
    parts.append(jnp.where(slot == 31, sub.astype(f32), placed(columns)))
    for m in range(10):
        for d in range(PEERS):
            send[d, 8 * m : 8 * m + 8, :] = parts[m]


def spread(parts):
    group = lax.shift_right_logical(lax.broadcasted_iota(i32, parts[0].shape, 1), 5)
    return jnp.where(group == 0, parts[0], jnp.where(group == 1, parts[1], parts[2]))


def coarse_lookup(table, chunk, lane):
    near = [jnp.zeros(chunk.shape, f32) for _ in range(3)]
    for c in range(32):
        here = chunk == c
        for j in range(3):
            row = table[32 * j + c : 32 * j + c + 1, :]
            near[j] = jnp.where(here, picked(row, lane), near[j])
    return near


def coarse_step(table, where, passes, data, own, rhs, dia, gather):
    gather[...] = jnp.zeros(gather.shape, f32)

    def one_pass(t, carry):
        rows = [
            [pltpu.roll(table[32 * j + 8 * v : 32 * j + 8 * v + 8, :], t, axis=0) for v in range(4)]
            for j in range(3)
        ]
        for d in range(PEERS):
            w = where[d]
            code, lane = lax.bitwise_and(w, 31), lax.shift_right_logical(w, 5)
            near = [jnp.zeros((8, LANES), f32) for _ in range(3)]
            for v in range(4):
                here = code == 4 * t + v
                for j in range(3):
                    near[j] = jnp.where(here, picked(rows[j][v], lane), near[j])
            for i in range(3):
                a = data[d, lanes8(3 * i), :] * near[0]
                a = a + data[d, lanes8(3 * i + 1), :] * near[1]
                a = a + data[d, lanes8(3 * i + 2), :] * near[2]
                gather[i, d : d + 1, :] += jnp.sum(a, axis=0, keepdims=True)
        return carry

    lax.fori_loop(0, passes, one_pass, 0)
    parts = []
    for i in range(3):
        s = gather[i]
        s = s + pltpu.roll(s, 64, axis=1)
        parts.append(s + pltpu.roll(s, 32, axis=1))
    return own + damping * (rhs - (dia * own - spread(parts))) / dia


def lanes8(m):
    return slice(8 * m, 8 * m + 8)


def coarse_first_kernel(base_ref, sums, data, new, rhs, dia, where, passes,
                        table, gather, left, right):
    me = lax.shift_right_logical(base_ref[0], 10)
    got = jnp.transpose(sums[:, 0, :])
    rows = got[96:128].astype(i32)
    s = got[0:96]
    split = []
    for _ in range(3):
        t = s.astype(jnp.bfloat16).astype(f32)
        split.append(t)
        s = s - t
    chunk = lax.broadcasted_iota(i32, (32, LANES), 0)
    place = lax.broadcasted_iota(i32, (LANES, LANES), 0)
    low = lax.bitwise_and(rows, 31)
    lane = lane_of_device(lax.shift_right_logical(rows, 5), me)
    for a in range(32):
        here = chunk == jnp.broadcast_to(low[a : a + 1], (32, LANES))
        for t in range(3):
            for i in range(3):
                value = jnp.broadcast_to(split[t][32 * i + a : 32 * i + a + 1], (32, LANES))
                left[96 * t + 32 * i : 96 * t + 32 * i + 32, lanes(LANES * a)] = jnp.where(
                    here, value, 0.0
                ).astype(jnp.bfloat16)
        right[:, lanes(LANES * a)] = jnp.where(
            place == jnp.broadcast_to(lane[a : a + 1], (LANES, LANES)), 1.0, 0.0
        ).astype(jnp.bfloat16)
    both = lax.dot_general(
        left[...], right[...], (((1,), (1,)), ((), ())), preferred_element_type=f32
    )
    crhs = both[0:96] + both[96:192] + both[192:288]
    order = row_of_device(device_of_lane(lax.broadcasted_iota(i32, (96, LANES), 1), me), me)
    cdia = jnp.take_along_axis(
        jnp.transpose(sums[:, 1, :])[0:96], order, axis=1, mode="promise_in_bounds"
    )
    pad = jnp.zeros((32, LANES), f32)
    first = jnp.concatenate([damping * crhs / cdia, pad], axis=0)
    table[...] = first
    own = jnp.transpose(first)[0:PEERS]
    rhs[...] = jnp.transpose(jnp.concatenate([crhs, pad], axis=0))[0:PEERS]
    dia[...] = jnp.transpose(jnp.concatenate([cdia, pad + 1.0], axis=0))[0:PEERS]
    sub = lax.broadcasted_iota(i32, (8, LANES), 0)
    most = jnp.zeros((8, LANES), i32)
    for d in range(PEERS):
        c = data[d, 72:80, :].astype(i32)
        off = lax.bitwise_and(sub - c, 7)
        most = jnp.maximum(most, off)
        at = lane_of_device(lax.shift_right_logical(c, 5), me)
        code = lax.bitwise_and(lax.shift_right_logical(c, 3), 3) + lax.shift_left(off, 2)
        where[d] = code + lax.shift_left(at, 5)
    most = jnp.max(most.astype(f32)).astype(i32) + 1
    passes[...] = jnp.broadcast_to(most, passes.shape)
    new[...] = coarse_step(
        table, where, most, data, own, rhs[...], dia[...], gather
    )


def gathered(table, pieces, mine):
    row = 0
    for piece in pieces:
        size = piece.shape[0]
        mine[row : row + size, :] = piece[...]
        row += size
    table[...] = jnp.transpose(mine[...])


def coarse_kernel(base_ref, passes, p0, p1, p2, p3, rhs, dia, where, data, *rest):
    new, table, mine, gather = rest[-4:]
    gathered(table, (p0, p1, p2, p3), mine)
    new[...] = coarse_step(
        table, where, passes[...][0, 0], data, p0[...], rhs[...], dia[...], gather
    )


def post_kernel(base_ref, p0, p1, p2, p3, first_iter, rhs, dia, col, blk, node_row, before, after,
                before2, after2, out, correction, table, mine, one, two):
    base = base_ref[0]
    me = lax.shift_right_logical(base, 10)
    gathered(table, (p0, p1, p2, p3), mine)
    row = mine[pl.ds(lane_of_device(me, me), 1), :]
    correction[...] = jnp.concatenate([row[:, 32 * i : 32 * i + 32] for i in range(3)], axis=0)
    one[...] = first_iter[...]
    one[:, lanes(0, HALO)] = before2[...]
    one[:, lanes(WIDE + ROWS + HALO, HALO)] = after2[...]
    edge = [
        h[P_ROW + t : P_ROW + t + 1, lanes(LANES * q)]
        for h in (before, after) for t in range(2) for q in range(2)
    ]
    edge = jnp.concatenate(edge, axis=0)

    def found(rows):
        rows = rows.astype(i32)
        lane = lane_of_device(lax.shift_right_logical(rows, 5), me)
        return coarse_lookup(table, lax.bitwise_and(rows, 31), lane)

    own, far = found(node_row[...]), found(edge)
    for s in range(16):
        if s < 4:
            row = [f[s : s + 1, :] for f in far]
        elif s < 12:
            row = [f[s - 4 : s - 3, :] for f in own]
        else:
            row = [f[s - 8 : s - 7, :] for f in far]
        one[:, lanes(s * LANES)] = one[:, lanes(s * LANES)] + jnp.concatenate(row, axis=0)
    two[...] = jnp.zeros(two.shape, f32)
    sweep_halo(two, one, rhs, dia, before, base, WIDE - HALO)
    sweep_halo(two, one, rhs, dia, after, base, WIDE + ROWS)

    def first(b):
        at = WIDE + b * LANES
        pull = own_block(one, col, blk, base, b)
        two[:, lanes(at)] = smoothed(one, pull, rhs, dia, at)

    def second(b):
        at = WIDE + b * LANES
        pull = own_block(two, col, blk, base, b)
        out[:, lanes(b * LANES)] = smoothed(two, pull, rhs, dia, at)

    each_block(first)
    each_block(second)


def call(kernel, outs, args, scratch=(), scalars=0, limit=12):
    vmem = pl.BlockSpec(memory_space=pltpu.VMEM)
    smem = pl.BlockSpec(memory_space=pltpu.SMEM)
    return pl.pallas_call(
        kernel,
        in_specs=[smem] * scalars + [vmem] * (len(args) - scalars),
        out_specs=[vmem] * len(outs),
        out_shape=[jax.ShapeDtypeStruct(o, t) for o, t in outs],
        scratch_shapes=[
            pltpu.VMEM(*s) if isinstance(s[0], tuple) else pltpu.VMEM(s, f32) for s in scratch
        ],
        compiler_params=pltpu.CompilerParams(vmem_limit_bytes=limit * 2**20),
    )(*args)


def partner(value, bits):
    return lax.ppermute(value, DOM, [(i, i ^ bits) for i in range(lax.axis_size(DOM))])


def in_group(new):
    p2, p3, p1 = partner(new, 2), partner(new, 3), partner(new, 1)
    return new, p1, p2, p3


def shifts(up, down):
    count = lax.axis_size(DOM)
    forward = [(i, i + 1) for i in range(count - 1)]
    backward = [(i + 1, i) for i in range(count - 1)]
    return lax.ppermute(up, DOM, forward), lax.ppermute(down, DOM, backward)


def cycle(right_side, fine_diagonal, fine_columns, fine_blocks, aggregate_of_node,
         coarse_row_of_aggregate, coarse_diagonal, coarse_columns, coarse_blocks):
    rhs, dia = right_side.T, fine_diagonal.T
    col, blk = fine_columns.T, fine_blocks.transpose(2, 3, 1, 0)
    agg = aggregate_of_node.reshape(8, LANES)
    owner = coarse_row_of_aggregate.reshape(1, 32)
    cdia, cblk = coarse_diagonal.T, coarse_blocks.transpose(2, 3, 0, 1)
    me = lax.axis_index(DOM).astype(i32).reshape(1)
    base = me * ROWS
    wide = WIDE + ROWS + WIDE

    dsend, = call(
        coarse_pack_kernel, [((PEERS, 80, LANES), f32)], [coarse_columns, cblk],
        limit=60,
    )
    data = lax.all_to_all(
        dsend, DOM, 0, 0, axis_index_groups=row_groups(), tiled=True
    )
    vmem, far = pl.BlockSpec(memory_space=pltpu.VMEM), pl.BlockSpec(memory_space=pltpu.HBM)
    up, down, node_row = pl.pallas_call(
        pack_kernel,
        name="pack",
        in_specs=[far] * 6,
        out_specs=[vmem] * 3,
        out_shape=[jax.ShapeDtypeStruct(o, f32) for o in ((P_ALL, HALO), (P_ALL, HALO), (8, LANES))],
        scratch_shapes=[
            pltpu.VMEM((3, ROWS), f32), pltpu.VMEM((3, ROWS), f32),
            pltpu.VMEM((2, SLOTS, HALO), i32), pltpu.VMEM((2, 3, 3, SLOTS, HALO), f32),
            pltpu.VMEM((8, LANES), i32), pltpu.VMEM((1, 32), i32), pltpu.SemaphoreType.DMA((8,)),
        ],
        compiler_params=pltpu.CompilerParams(vmem_limit_bytes=60 * 2**20),
    )(rhs, dia, col, blk, agg, owner)
    before, after = shifts(up, down)
    send, first_iter, wrhs, wdia, up2, down2 = call(
        pre_kernel,
        [((1, 2, LANES), f32), ((3, wide), f32), ((3, wide), f32), ((3, wide), f32),
         ((3, HALO), f32), ((3, HALO), f32)],
        [base, rhs, dia, col, blk, agg, owner, cdia, before, after],
        scratch=[(3, wide), (3, wide), (8, ROWS)], scalars=1,
    )
    before2, after2 = shifts(up2, down2)
    sums = send
    for bits in ((1, 2, 3), (8, 16, 24), (32, 64, 96), (4,)):
        sums = jnp.concatenate([sums] + [partner(sums, b) for b in bits], axis=0)
    peers = ((PEERS, LANES), f32)
    gather = (3, PEERS, LANES)
    square = (LANES, LANES)
    new, crhs, cd, where, passes = call(
        coarse_first_kernel,
        [peers, peers, peers, ((PEERS, 8, LANES), i32), ((8, LANES), i32)],
        [base, sums, data],
        scratch=[square, gather, ((288, 4096), jnp.bfloat16), ((LANES, 4096), jnp.bfloat16)],
        scalars=1,
    )
    awaited = [(), (before2,), (after2,)] + [()] * CSWEEPS
    for sweep in range(CSWEEPS - 2):
        new, = call(
            coarse_kernel, [peers],
            [base, passes, *in_group(new), crhs, cd, where, data, *awaited[sweep]],
            scratch=[square, square, gather], scalars=1,
        )
    solution, mine = call(
        post_kernel, [((3, ROWS), f32), ((3, 32), f32)],
        [base, *in_group(new), first_iter, wrhs, wdia, col, blk, node_row,
         before, after, before2, after2],
        scratch=[square, square, (3, wide), (3, wide)], scalars=1,
    )
    return solution.T, mine.T


def solution(mesh):
    return jax.shard_map(
        cycle,
        mesh=mesh,
        in_specs=(
            P(DOM, None),
            P(DOM, None),
            P(DOM, None),
            P(DOM, None, None, None),
            P(DOM),
            P(DOM),
            P(DOM, None),
            P(DOM, None),
            P(DOM, None, None, None),
        ),
        out_specs=(P(DOM, None), P(DOM, None)),
        check_vma=False,
    )
```

```python
import jax
import jax.numpy as jnp
from jax import lax
from jax.experimental import pallas as pl
from jax.experimental.pallas import tpu as pltpu
from jax.sharding import PartitionSpec as P


DOM = "dom"
PEERS = 64
NEAR = 8
PARTS = PEERS // NEAR
PIECES = 128 // PEERS
UNROLL = 8
CSWEEPS = 6
damping = 0.7
highest = lax.Precision.HIGHEST

ROWS = 1024
LANES = 128
SLOTS = 27
FULL = 24
HALO = 256
WIDE = 512
BLOCKS = ROWS // LANES
P_COL = 9 * FULL
P_BTAIL = P_COL + FULL
P_CTAIL = P_BTAIL + 27
P_RHS = P_CTAIL + 3
P_DIA = P_RHS + 6
P_ROW = P_DIA + 6
P_ALL = 288
f32 = jnp.float32
i32 = jnp.int32


def lanes(start, size=LANES):
    if isinstance(start, int):
        return slice(start, start + size)
    return pl.ds(pl.multiple_of(start, LANES), size)


def picked(row, where):
    return jnp.take_along_axis(
        jnp.broadcast_to(row, where.shape), where, axis=1, mode="promise_in_bounds"
    )


def pack_kernel(rhs_in, dia_in, col_in, blk_in, agg_in, owner_in, up, down, node_row,
                rhs, dia, col, blk, agg, owner, sem):
    copies = [(rhs_in, rhs), (dia_in, dia), (agg_in, agg), (owner_in, owner)]
    for t, near in enumerate((ROWS - HALO, 0)):
        copies.append((col_in.at[:, lanes(near, HALO)], col.at[t]))
        copies.append((blk_in.at[:, :, :, lanes(near, HALO)], blk.at[t]))
    copies = [pltpu.make_async_copy(a, b, sem.at[n]) for n, (a, b) in enumerate(copies)]
    for c in copies:
        c.start()
    for c in copies:
        c.wait()
    table = jnp.concatenate([owner[...]] * 4, axis=1)
    found = picked(table, agg[...]).astype(f32)
    node_row[...] = found
    for t, (out, wide) in enumerate(((up, ROWS - WIDE), (down, 0))):
        for i in range(3):
            for j in range(3):
                g = 3 * i + j
                out[g * FULL : (g + 1) * FULL, :] = blk[t, i, j, 0:FULL, :]
                out[P_BTAIL + 3 * g : P_BTAIL + 3 * g + 3, :] = blk[t, i, j, FULL:SLOTS, :]
        out[P_COL : P_COL + FULL, :] = col[t, 0:FULL, :].astype(f32)
        out[P_CTAIL : P_CTAIL + 3, :] = col[t, FULL:SLOTS, :].astype(f32)
        for h in range(2):
            out[P_RHS + 3 * h : P_RHS + 3 * h + 3, :] = rhs[:, lanes(wide + HALO * h, HALO)]
            out[P_DIA + 3 * h : P_DIA + 3 * h + 3, :] = dia[:, lanes(wide + HALO * h, HALO)]
            for q in range(2):
                s = wide // LANES + 2 * h + q
                out[P_ROW + h : P_ROW + h + 1, lanes(LANES * q)] = found[s : s + 1, :]
        out[P_ROW + 2 : P_ALL, :] = jnp.zeros((P_ALL - P_ROW - 2, HALO), f32)


def pulled_block(columns, blocks, table, first_chunk):
    total = [None, None, None]
    for part in range(4):
        where = columns(part)
        chunk = lax.shift_right_arithmetic(where, 7)
        lane = lax.bitwise_and(where, 127)
        near = [jnp.zeros(where.shape, f32) for _ in range(3)]
        for c in range(5):
            here = chunk == c
            for j in range(3):
                row = table[j : j + 1, lanes(first_chunk * LANES + c * LANES)]
                near[j] = jnp.where(here, picked(row, lane), near[j])
        for i in range(3):
            s = blocks(i, 0, part) * near[0]
            s = s + blocks(i, 1, part) * near[1]
            s = s + blocks(i, 2, part) * near[2]
            if part < 3:
                total[i] = s if total[i] is None else total[i] + s
            else:
                total[i] = jnp.sum(total[i], axis=0, keepdims=True) + jnp.sum(
                    s, axis=0, keepdims=True
                )
    return total


def local_getters(col, blk, start, b):
    def columns(part):
        lo, hi = 8 * part, min(8 * part + 8, SLOTS)
        return col[lo:hi, lanes(b * LANES)] - start

    def blocks(i, j, part):
        lo, hi = 8 * part, min(8 * part + 8, SLOTS)
        return blk[i, j, lo:hi, lanes(b * LANES)]

    return columns, blocks


def halo_getters(halo, start, b):
    def columns(part):
        if part < 3:
            got = halo[P_COL + 8 * part : P_COL + 8 * part + 8, lanes(b * LANES)]
        else:
            got = halo[P_CTAIL : P_CTAIL + 3, lanes(b * LANES)]
        return got.astype(i32) - start

    def blocks(i, j, part):
        g = 3 * i + j
        if part < 3:
            return halo[g * FULL + 8 * part : g * FULL + 8 * part + 8, lanes(b * LANES)]
        return halo[P_BTAIL + 3 * g : P_BTAIL + 3 * g + 3, lanes(b * LANES)]

    return columns, blocks


def wide_vector(out, local, before, after, row):
    out[:, lanes(WIDE, ROWS)] = local[...]
    for h in range(2):
        out[:, lanes(HALO * h, HALO)] = before[row + 3 * h : row + 3 * h + 3, :]
        out[:, lanes(WIDE + ROWS + HALO * h, HALO)] = after[row + 3 * h : row + 3 * h + 3, :]


def smoothed(table, pulled, rhs, dia, at):
    pull = jnp.concatenate(pulled, axis=0)
    s = table[:, lanes(at)]
    b = rhs[:, lanes(at)]
    d = dia[:, lanes(at)]
    return s + damping * (b - (d * s - pull)) / d


def sweep_halo(out, table, rhs, dia, halo, base, first):
    for b in range(2):
        at = first + LANES * b
        start = base + (at - WIDE) - 2 * LANES
        cols, blks = halo_getters(halo, start, b)
        pull = pulled_block(cols, blks, table, at // LANES - 2)
        out[:, lanes(at)] = smoothed(table, pull, rhs, dia, at)


def each_block(step):
    def some(t, carry):
        for u in range(UNROLL):
            step(t * UNROLL + u)
        return carry

    lax.fori_loop(0, BLOCKS // UNROLL, some, 0)


def own_block(table, col, blk, base, b):
    start = base + b * LANES - 2 * LANES
    cols, blks = local_getters(col, blk, start, b)
    return pulled_block(cols, blks, table, b + WIDE // LANES - 2)


def pre_kernel(base_ref, rhs, dia, col, blk, agg, owner_row, cdia, before, after,
               send, first_iter, keep_rhs, keep_dia, up2, down2, one, two, res):
    base = base_ref[0]
    wide_vector(keep_rhs, rhs, before, after, P_RHS)
    wide_vector(keep_dia, dia, before, after, P_DIA)
    raw = keep_dia[...]
    keep_dia[...] = jnp.where(raw == 0.0, 1.0, raw)
    one[...] = damping * keep_rhs[...] / keep_dia[...]
    two[...] = jnp.zeros(two.shape, f32)
    sweep_halo(two, one, keep_rhs, keep_dia, before, base, WIDE - HALO)
    sweep_halo(two, one, keep_rhs, keep_dia, after, base, WIDE + ROWS)

    def second(b):
        at = WIDE + b * LANES
        pull = own_block(one, col, blk, base, b)
        two[:, lanes(at)] = smoothed(one, pull, keep_rhs, keep_dia, at)

    each_block(second)

    def third(b):
        at = WIDE + b * LANES
        pull = jnp.concatenate(own_block(two, col, blk, base, b), axis=0)
        s, d = two[:, lanes(at)], keep_dia[:, lanes(at)]
        res[0:3, lanes(b * LANES)] = keep_rhs[:, lanes(at)] - (d * s - pull)

    res[...] = jnp.zeros(res.shape, f32)
    each_block(third)
    first_iter[...] = two[...]
    up2[...] = two[:, lanes(WIDE + ROWS - WIDE, HALO)]
    down2[...] = two[:, lanes(WIDE + HALO, HALO)]
    label = lax.broadcasted_iota(i32, (32, LANES), 0)
    sums = None
    for b in range(BLOCKS):
        member = (label == jnp.broadcast_to(agg[b : b + 1, :], (32, LANES))).astype(f32)
        part = lax.dot_general(
            res[:, lanes(b * LANES)], member, (((1,), (1,)), ((), ())),
            precision=highest, preferred_element_type=f32,
        )
        sums = part if sums is None else sums + part
    row = jnp.concatenate(
        [sums[0:1], sums[1:2], sums[2:3], owner_row[...].astype(f32)], axis=1
    )
    send[:, 0, :] = jnp.broadcast_to(row, (LANES, LANES))
    row = jnp.concatenate(
        [cdia[0:1], cdia[1:2], cdia[2:3], jnp.ones((1, 32), f32)], axis=1
    )
    send[:, 1, :] = jnp.broadcast_to(row, (LANES, LANES))


def bit_of(p, at):
    return lax.bitwise_and(lax.shift_right_logical(p, at), 1)


def bit_parity(p, at):
    return lax.bitwise_xor(bit_of(p, at), bit_of(p, at + 1))


def lane_of_device(p, me):
    off = lax.bitwise_xor(p, me)
    rest = 4 * bit_of(p, 6) + 2 * bit_of(p, 4) + bit_of(p, 2)
    return (
        64 * bit_of(off, 0) + 32 * bit_parity(off, 1) + 16 * bit_parity(off, 5) + 8 * bit_parity(off, 3)
        + rest
    )


def device_of_lane(q, me):
    def last(relative, at, first):
        return lax.bitwise_xor(lax.bitwise_xor(relative, bit_parity(me, at)), first)

    x, z, y = bit_of(q, 0), bit_of(q, 1), bit_of(q, 2)
    p = 64 * y + 32 * last(bit_of(q, 4), 5, y) + 16 * z + 8 * last(bit_of(q, 3), 3, z)
    core = lax.bitwise_xor(bit_of(q, 6), bit_of(me, 0))
    return p + 4 * x + 2 * last(bit_of(q, 5), 1, x) + core


def row_groups():
    def member(kind, m):
        y, z, x = m >> 2, m >> 1 & 1, m & 1
        py, pz, px, core = kind >> 3, kind >> 2 & 1, kind >> 1 & 1, kind & 1
        return 64 * y + 32 * (y ^ py) + 16 * z + 8 * (z ^ pz) + 4 * x + 2 * (x ^ px) + core

    return [[member(kind, m) for m in range(NEAR)] for kind in range(16)]


def coarse_pack_kernel(col, blk, send):
    def turned(a):
        z = jnp.transpose(jnp.concatenate([a, jnp.zeros((32, 5), f32)], axis=1))
        return jnp.concatenate([z] * 4, axis=1)

    columns = turned(col[...].astype(f32))
    kind = lax.bitwise_and(columns.astype(i32), 7)
    tile = (8, LANES)
    sub = lax.broadcasted_iota(i32, tile, 0)
    count = jnp.zeros(tile, i32)
    match, earlier = [], []
    for k in range(SLOTS):
        here = sub == jnp.broadcast_to(kind[k : k + 1], tile)
        match.append(here)
        earlier.append(count)
        count = count + here.astype(i32)
    left = jnp.zeros((1, LANES), i32)
    start = []
    for n in range(16):
        if n >= 8:
            start.append(left)
        left = jnp.maximum(left + count[n % 8 : n % 8 + 1] - 4, 0)
    start = jnp.concatenate(start, axis=0) + 4 * sub
    place = 4 * sub + lax.shift_right_logical(lax.broadcasted_iota(i32, tile, 1), 5)
    slot = jnp.full(tile, 31, i32)
    for k in range(SLOTS):
        at = jnp.sum(jnp.where(match[k], start + earlier[k], 0), axis=0, keepdims=True)
        slot = jnp.where(place == jnp.broadcast_to(lax.bitwise_and(at, 31), tile), k, slot)
    inner, outer = lax.bitwise_and(slot, 7), lax.shift_right_logical(slot, 3)

    def placed(z):
        got = None
        for g in range(4):
            part = jnp.take_along_axis(
                z[8 * g : 8 * g + 8], inner, axis=0, mode="promise_in_bounds"
            )
            got = part if got is None else jnp.where(outer == g, part, got)
        return got

    parts = [placed(turned(blk[i, j])) for i in range(3) for j in range(3)]
    parts.append(jnp.where(slot == 31, sub.astype(f32), placed(columns)))
    for m in range(10):
        for d in range(NEAR):
            send[d, 8 * m : 8 * m + 8, :] = parts[m]


def spread(parts):
    group = lax.shift_right_logical(lax.broadcasted_iota(i32, parts[0].shape, 1), 5)
    return jnp.where(group == 0, parts[0], jnp.where(group == 1, parts[1], parts[2]))


def coarse_lookup(table, chunk, lane):
    near = [jnp.zeros(chunk.shape, f32) for _ in range(3)]
    for c in range(32):
        here = chunk == c
        for j in range(3):
            row = table[32 * j + c : 32 * j + c + 1, :]
            near[j] = jnp.where(here, picked(row, lane), near[j])
    return near


def coarse_step(table, where, passes, data, own, rhs, dia, gather):
    gather[...] = jnp.zeros(gather.shape, f32)

    def one_pass(t, carry):
        rows = [
            [pltpu.roll(table[32 * j + 8 * v : 32 * j + 8 * v + 8, :], t, axis=0) for v in range(4)]
            for j in range(3)
        ]
        for d in range(PEERS):
            w = where[d]
            code, lane = lax.bitwise_and(w, 31), lax.shift_right_logical(w, 5)
            near = [jnp.zeros((8, LANES), f32) for _ in range(3)]
            for v in range(4):
                here = code == 4 * t + v
                for j in range(3):
                    near[j] = jnp.where(here, picked(rows[j][v], lane), near[j])
            for i in range(3):
                a = data[d // NEAR][d % NEAR, lanes8(3 * i), :] * near[0]
                a = a + data[d // NEAR][d % NEAR, lanes8(3 * i + 1), :] * near[1]
                a = a + data[d // NEAR][d % NEAR, lanes8(3 * i + 2), :] * near[2]
                gather[i, d : d + 1, :] += jnp.sum(a, axis=0, keepdims=True)
        return carry

    lax.fori_loop(0, passes, one_pass, 0)
    parts = []
    for i in range(3):
        s = gather[i]
        s = s + pltpu.roll(s, 64, axis=1)
        parts.append(s + pltpu.roll(s, 32, axis=1))
    return own + damping * (rhs - (dia * own - spread(parts))) / dia


def lanes8(m):
    return slice(8 * m, 8 * m + 8)


def coarse_first_kernel(base_ref, sums, *rest):
    data = rest[:PARTS]
    new, rhs, dia, where, passes, table, gather, left, right = rest[PARTS + 2 :]
    me = lax.shift_right_logical(base_ref[0], 10)
    got = jnp.transpose(sums[:, 0, :])
    rows = got[96:128].astype(i32)
    s = got[0:96]
    split = []
    for _ in range(3):
        t = s.astype(jnp.bfloat16).astype(f32)
        split.append(t)
        s = s - t
    chunk = lax.broadcasted_iota(i32, (32, LANES), 0)
    place = lax.broadcasted_iota(i32, (LANES, LANES), 0)
    low = lax.bitwise_and(rows, 31)
    lane = lane_of_device(lax.shift_right_logical(rows, 5), me)
    for a in range(32):
        here = chunk == jnp.broadcast_to(low[a : a + 1], (32, LANES))
        for t in range(3):
            for i in range(3):
                value = jnp.broadcast_to(split[t][32 * i + a : 32 * i + a + 1], (32, LANES))
                left[96 * t + 32 * i : 96 * t + 32 * i + 32, lanes(LANES * a)] = jnp.where(
                    here, value, 0.0
                ).astype(jnp.bfloat16)
        right[:, lanes(LANES * a)] = jnp.where(
            place == jnp.broadcast_to(lane[a : a + 1], (LANES, LANES)), 1.0, 0.0
        ).astype(jnp.bfloat16)
    both = lax.dot_general(
        left[...], right[...], (((1,), (1,)), ((), ())), preferred_element_type=f32
    )
    crhs = both[0:96] + both[96:192] + both[192:288]
    order = device_of_lane(lax.broadcasted_iota(i32, (96, LANES), 1), me)
    cdia = jnp.take_along_axis(
        jnp.transpose(sums[:, 1, :])[0:96], order, axis=1, mode="promise_in_bounds"
    )
    pad = jnp.zeros((32, LANES), f32)
    first = jnp.concatenate([damping * crhs / cdia, pad], axis=0)
    table[...] = first
    own = jnp.transpose(first)[0:PEERS]
    rhs[...] = jnp.transpose(jnp.concatenate([crhs, pad], axis=0))[0:PEERS]
    dia[...] = jnp.transpose(jnp.concatenate([cdia, pad + 1.0], axis=0))[0:PEERS]
    sub = lax.broadcasted_iota(i32, (8, LANES), 0)
    most = jnp.zeros((8, LANES), i32)
    for d in range(PEERS):
        c = data[d // NEAR][d % NEAR, 72:80, :].astype(i32)
        off = lax.bitwise_and(sub - c, 7)
        most = jnp.maximum(most, off)
        at = lane_of_device(lax.shift_right_logical(c, 5), me)
        code = lax.bitwise_and(lax.shift_right_logical(c, 3), 3) + lax.shift_left(off, 2)
        where[d] = code + lax.shift_left(at, 5)
    most = jnp.max(most.astype(f32)).astype(i32) + 1
    passes[...] = jnp.broadcast_to(most, passes.shape)
    new[...] = coarse_step(
        table, where, most, data, own, rhs[...], dia[...], gather
    )


def gathered(table, pieces, mine):
    row = 0
    for piece in pieces:
        size = piece.shape[0]
        mine[row : row + size, :] = piece[...]
        row += size
    table[...] = jnp.transpose(mine[...])


def coarse_kernel(base_ref, passes, *rest):
    pieces, (rhs, dia, where) = rest[:PIECES], rest[PIECES : PIECES + 3]
    data = rest[PIECES + 3 : PIECES + 3 + PARTS]
    new, table, mine, gather = rest[PIECES + 3 + PARTS :]
    gathered(table, pieces, mine)
    new[...] = coarse_step(
        table, where, passes[...][0, 0], data, pieces[0][...], rhs[...], dia[...], gather
    )


def post_kernel(base_ref, *rest):
    pieces = rest[:PIECES]
    (first_iter, rhs, dia, col, blk, node_row, before, after, before2, after2,
     out, correction, table, mine, one, two) = rest[PIECES:]
    base = base_ref[0]
    me = lax.shift_right_logical(base, 10)
    gathered(table, pieces, mine)
    row = mine[pl.ds(lane_of_device(me, me), 1), :]
    correction[...] = jnp.concatenate([row[:, 32 * i : 32 * i + 32] for i in range(3)], axis=0)
    one[...] = first_iter[...]
    one[:, lanes(0, HALO)] = before2[...]
    one[:, lanes(WIDE + ROWS + HALO, HALO)] = after2[...]
    edge = [
        h[P_ROW + t : P_ROW + t + 1, lanes(LANES * q)]
        for h in (before, after) for t in range(2) for q in range(2)
    ]
    edge = jnp.concatenate(edge, axis=0)

    def found(rows):
        rows = rows.astype(i32)
        lane = lane_of_device(lax.shift_right_logical(rows, 5), me)
        return coarse_lookup(table, lax.bitwise_and(rows, 31), lane)

    own, far = found(node_row[...]), found(edge)
    for s in range(16):
        if s < 4:
            row = [f[s : s + 1, :] for f in far]
        elif s < 12:
            row = [f[s - 4 : s - 3, :] for f in own]
        else:
            row = [f[s - 8 : s - 7, :] for f in far]
        one[:, lanes(s * LANES)] = one[:, lanes(s * LANES)] + jnp.concatenate(row, axis=0)
    two[...] = jnp.zeros(two.shape, f32)
    sweep_halo(two, one, rhs, dia, before, base, WIDE - HALO)
    sweep_halo(two, one, rhs, dia, after, base, WIDE + ROWS)

    def first(b):
        at = WIDE + b * LANES
        pull = own_block(one, col, blk, base, b)
        two[:, lanes(at)] = smoothed(one, pull, rhs, dia, at)

    def second(b):
        at = WIDE + b * LANES
        pull = own_block(two, col, blk, base, b)
        out[:, lanes(b * LANES)] = smoothed(two, pull, rhs, dia, at)

    each_block(first)
    each_block(second)


def call(kernel, outs, args, scratch=(), scalars=0, limit=12):
    vmem = pl.BlockSpec(memory_space=pltpu.VMEM)
    smem = pl.BlockSpec(memory_space=pltpu.SMEM)
    return pl.pallas_call(
        kernel,
        in_specs=[smem] * scalars + [vmem] * (len(args) - scalars),
        out_specs=[vmem] * len(outs),
        out_shape=[jax.ShapeDtypeStruct(o, t) for o, t in outs],
        scratch_shapes=[
            pltpu.VMEM(*s) if isinstance(s[0], tuple) else pltpu.VMEM(s, f32) for s in scratch
        ],
        compiler_params=pltpu.CompilerParams(vmem_limit_bytes=limit * 2**20),
    )(*args)


def partner(value, bits):
    return lax.ppermute(value, DOM, [(i, i ^ bits) for i in range(lax.axis_size(DOM))])


def in_group(new):
    return new, partner(new, 1)


def shifts(up, down):
    count = lax.axis_size(DOM)
    forward = [(i, i + 1) for i in range(count - 1)]
    backward = [(i + 1, i) for i in range(count - 1)]
    return lax.ppermute(up, DOM, forward), lax.ppermute(down, DOM, backward)


def cycle(right_side, fine_diagonal, fine_columns, fine_blocks, aggregate_of_node,
         coarse_row_of_aggregate, coarse_diagonal, coarse_columns, coarse_blocks):
    rhs, dia = right_side.T, fine_diagonal.T
    col, blk = fine_columns.T, fine_blocks.transpose(2, 3, 1, 0)
    agg = aggregate_of_node.reshape(8, LANES)
    owner = coarse_row_of_aggregate.reshape(1, 32)
    cdia, cblk = coarse_diagonal.T, coarse_blocks.transpose(2, 3, 0, 1)
    me = lax.axis_index(DOM).astype(i32).reshape(1)
    base = me * ROWS
    wide = WIDE + ROWS + WIDE

    dsend, = call(
        coarse_pack_kernel, [((NEAR, 80, LANES), f32)], [coarse_columns, cblk],
        limit=60,
    )
    data = lax.all_to_all(
        dsend, DOM, 0, 0, axis_index_groups=row_groups(), tiled=True
    )
    along_x, along_y, along_z = partner(data, 2), partner(data, 32), partner(data, 8)
    along_xy, along_yz, along_xz = partner(along_x, 32), partner(along_y, 8), partner(along_z, 2)
    along_all = partner(along_yz, 2)
    data = (data, along_z, along_y, along_yz, along_x, along_xz, along_xy, along_all)
    vmem, far = pl.BlockSpec(memory_space=pltpu.VMEM), pl.BlockSpec(memory_space=pltpu.HBM)
    up, down, node_row = pl.pallas_call(
        pack_kernel,
        name="pack",
        in_specs=[far] * 6,
        out_specs=[vmem] * 3,
        out_shape=[jax.ShapeDtypeStruct(o, f32) for o in ((P_ALL, HALO), (P_ALL, HALO), (8, LANES))],
        scratch_shapes=[
            pltpu.VMEM((3, ROWS), f32), pltpu.VMEM((3, ROWS), f32),
            pltpu.VMEM((2, SLOTS, HALO), i32), pltpu.VMEM((2, 3, 3, SLOTS, HALO), f32),
            pltpu.VMEM((8, LANES), i32), pltpu.VMEM((1, 32), i32), pltpu.SemaphoreType.DMA((8,)),
        ],
        compiler_params=pltpu.CompilerParams(vmem_limit_bytes=60 * 2**20),
    )(rhs, dia, col, blk, agg, owner)
    before, after = shifts(up, down)
    send, first_iter, wrhs, wdia, up2, down2 = call(
        pre_kernel,
        [((LANES, 2, LANES), f32), ((3, wide), f32), ((3, wide), f32), ((3, wide), f32),
         ((3, HALO), f32), ((3, HALO), f32)],
        [base, rhs, dia, col, blk, agg, owner, cdia, before, after],
        scratch=[(3, wide), (3, wide), (8, ROWS)], scalars=1,
    )
    before2, after2 = shifts(up2, down2)
    sums = lax.all_to_all(send, DOM, 0, 0, tiled=True)
    peers = ((PEERS, LANES), f32)
    gather = (3, PEERS, LANES)
    square = (LANES, LANES)
    new, crhs, cd, where, passes = call(
        coarse_first_kernel,
        [peers, peers, peers, ((PEERS, 8, LANES), i32), ((8, LANES), i32)],
        [base, sums, *data, before2, after2],
        scratch=[square, gather, ((288, 4096), jnp.bfloat16), ((LANES, 4096), jnp.bfloat16)],
        scalars=1,
    )
    for _ in range(CSWEEPS - 2):
        new, = call(
            coarse_kernel, [peers],
            [base, passes, *in_group(new), crhs, cd, where, *data],
            scratch=[square, square, gather], scalars=1,
        )
    solution, mine = call(
        post_kernel, [((3, ROWS), f32), ((3, 32), f32)],
        [base, *in_group(new), first_iter, wrhs, wdia, col, blk, node_row,
         before, after, before2, after2],
        scratch=[square, square, (3, wide), (3, wide)], scalars=1,
    )
    return solution.T, mine.T


def solution(mesh):
    return jax.shard_map(
        cycle,
        mesh=mesh,
        in_specs=(
            P(DOM, None),
            P(DOM, None),
            P(DOM, None),
            P(DOM, None, None, None),
            P(DOM),
            P(DOM),
            P(DOM, None),
            P(DOM, None),
            P(DOM, None, None, None),
        ),
        out_specs=(P(DOM, None), P(DOM, None)),
        check_vma=False,
    )
```

```python
import jax
import jax.numpy as jnp
from jax import lax
from jax.experimental import pallas as pl
from jax.experimental.pallas import tpu as pltpu
from jax.sharding import PartitionSpec as P


DOM = "dom"
PEERS = 32
NEAR = 16
UNROLL = 8
CSWEEPS = 6
damping = 0.7
highest = lax.Precision.HIGHEST

ROWS = 1024
LANES = 128
SLOTS = 27
FULL = 24
HALO = 256
WIDE = 512
BLOCKS = ROWS // LANES
P_COL = 9 * FULL
P_BTAIL = P_COL + FULL
P_CTAIL = P_BTAIL + 27
P_RHS = P_CTAIL + 3
P_DIA = P_RHS + 6
P_ROW = P_DIA + 6
P_ALL = 288
f32 = jnp.float32
i32 = jnp.int32


def lanes(start, size=LANES):
    if isinstance(start, int):
        return slice(start, start + size)
    return pl.ds(pl.multiple_of(start, LANES), size)


def picked(row, where):
    return jnp.take_along_axis(
        jnp.broadcast_to(row, where.shape), where, axis=1, mode="promise_in_bounds"
    )


def pack_kernel(rhs_in, dia_in, col_in, blk_in, agg_in, owner_in, up, down, node_row,
                rhs, dia, col, blk, agg, owner, sem):
    copies = [(rhs_in, rhs), (dia_in, dia), (agg_in, agg), (owner_in, owner)]
    for t, near in enumerate((ROWS - HALO, 0)):
        copies.append((col_in.at[:, lanes(near, HALO)], col.at[t]))
        copies.append((blk_in.at[:, :, :, lanes(near, HALO)], blk.at[t]))
    copies = [pltpu.make_async_copy(a, b, sem.at[n]) for n, (a, b) in enumerate(copies)]
    for c in copies:
        c.start()
    for c in copies:
        c.wait()
    table = jnp.concatenate([owner[...]] * 4, axis=1)
    found = picked(table, agg[...]).astype(f32)
    node_row[...] = found
    for t, (out, wide) in enumerate(((up, ROWS - WIDE), (down, 0))):
        for i in range(3):
            for j in range(3):
                g = 3 * i + j
                out[g * FULL : (g + 1) * FULL, :] = blk[t, i, j, 0:FULL, :]
                out[P_BTAIL + 3 * g : P_BTAIL + 3 * g + 3, :] = blk[t, i, j, FULL:SLOTS, :]
        out[P_COL : P_COL + FULL, :] = col[t, 0:FULL, :].astype(f32)
        out[P_CTAIL : P_CTAIL + 3, :] = col[t, FULL:SLOTS, :].astype(f32)
        for h in range(2):
            out[P_RHS + 3 * h : P_RHS + 3 * h + 3, :] = rhs[:, lanes(wide + HALO * h, HALO)]
            out[P_DIA + 3 * h : P_DIA + 3 * h + 3, :] = dia[:, lanes(wide + HALO * h, HALO)]
            for q in range(2):
                s = wide // LANES + 2 * h + q
                out[P_ROW + h : P_ROW + h + 1, lanes(LANES * q)] = found[s : s + 1, :]
        out[P_ROW + 2 : P_ALL, :] = jnp.zeros((P_ALL - P_ROW - 2, HALO), f32)


def pulled_block(columns, blocks, table, first_chunk):
    total = [None, None, None]
    for part in range(4):
        where = columns(part)
        chunk = lax.shift_right_arithmetic(where, 7)
        lane = lax.bitwise_and(where, 127)
        near = [jnp.zeros(where.shape, f32) for _ in range(3)]
        for c in range(5):
            here = chunk == c
            for j in range(3):
                row = table[j : j + 1, lanes(first_chunk * LANES + c * LANES)]
                near[j] = jnp.where(here, picked(row, lane), near[j])
        for i in range(3):
            s = blocks(i, 0, part) * near[0]
            s = s + blocks(i, 1, part) * near[1]
            s = s + blocks(i, 2, part) * near[2]
            if part < 3:
                total[i] = s if total[i] is None else total[i] + s
            else:
                total[i] = jnp.sum(total[i], axis=0, keepdims=True) + jnp.sum(
                    s, axis=0, keepdims=True
                )
    return total


def local_getters(col, blk, start, b):
    def columns(part):
        lo, hi = 8 * part, min(8 * part + 8, SLOTS)
        return col[lo:hi, lanes(b * LANES)] - start

    def blocks(i, j, part):
        lo, hi = 8 * part, min(8 * part + 8, SLOTS)
        return blk[i, j, lo:hi, lanes(b * LANES)]

    return columns, blocks


def halo_getters(halo, start, b):
    def columns(part):
        if part < 3:
            got = halo[P_COL + 8 * part : P_COL + 8 * part + 8, lanes(b * LANES)]
        else:
            got = halo[P_CTAIL : P_CTAIL + 3, lanes(b * LANES)]
        return got.astype(i32) - start

    def blocks(i, j, part):
        g = 3 * i + j
        if part < 3:
            return halo[g * FULL + 8 * part : g * FULL + 8 * part + 8, lanes(b * LANES)]
        return halo[P_BTAIL + 3 * g : P_BTAIL + 3 * g + 3, lanes(b * LANES)]

    return columns, blocks


def wide_vector(out, local, before, after, row):
    out[:, lanes(WIDE, ROWS)] = local[...]
    for h in range(2):
        out[:, lanes(HALO * h, HALO)] = before[row + 3 * h : row + 3 * h + 3, :]
        out[:, lanes(WIDE + ROWS + HALO * h, HALO)] = after[row + 3 * h : row + 3 * h + 3, :]


def smoothed(table, pulled, rhs, dia, at):
    pull = jnp.concatenate(pulled, axis=0)
    s = table[:, lanes(at)]
    b = rhs[:, lanes(at)]
    d = dia[:, lanes(at)]
    return s + damping * (b - (d * s - pull)) / d


def sweep_halo(out, table, rhs, dia, halo, base, first):
    for b in range(2):
        at = first + LANES * b
        start = base + (at - WIDE) - 2 * LANES
        cols, blks = halo_getters(halo, start, b)
        pull = pulled_block(cols, blks, table, at // LANES - 2)
        out[:, lanes(at)] = smoothed(table, pull, rhs, dia, at)


def each_block(step):
    def some(t, carry):
        for u in range(UNROLL):
            step(t * UNROLL + u)
        return carry

    lax.fori_loop(0, BLOCKS // UNROLL, some, 0)


def own_block(table, col, blk, base, b):
    start = base + b * LANES - 2 * LANES
    cols, blks = local_getters(col, blk, start, b)
    return pulled_block(cols, blks, table, b + WIDE // LANES - 2)


def pre_kernel(base_ref, rhs, dia, col, blk, agg, owner_row, cdia, before, after,
               send, first_iter, keep_rhs, keep_dia, up2, down2, one, two, res):
    base = base_ref[0]
    wide_vector(keep_rhs, rhs, before, after, P_RHS)
    wide_vector(keep_dia, dia, before, after, P_DIA)
    raw = keep_dia[...]
    keep_dia[...] = jnp.where(raw == 0.0, 1.0, raw)
    one[...] = damping * keep_rhs[...] / keep_dia[...]
    two[...] = jnp.zeros(two.shape, f32)
    sweep_halo(two, one, keep_rhs, keep_dia, before, base, WIDE - HALO)
    sweep_halo(two, one, keep_rhs, keep_dia, after, base, WIDE + ROWS)

    def second(b):
        at = WIDE + b * LANES
        pull = own_block(one, col, blk, base, b)
        two[:, lanes(at)] = smoothed(one, pull, keep_rhs, keep_dia, at)

    each_block(second)

    def third(b):
        at = WIDE + b * LANES
        pull = jnp.concatenate(own_block(two, col, blk, base, b), axis=0)
        s, d = two[:, lanes(at)], keep_dia[:, lanes(at)]
        res[0:3, lanes(b * LANES)] = keep_rhs[:, lanes(at)] - (d * s - pull)

    res[...] = jnp.zeros(res.shape, f32)
    each_block(third)
    first_iter[...] = two[...]
    up2[...] = two[:, lanes(WIDE + ROWS - WIDE, HALO)]
    down2[...] = two[:, lanes(WIDE + HALO, HALO)]
    label = lax.broadcasted_iota(i32, (32, LANES), 0)
    sums = None
    for b in range(BLOCKS):
        member = (label == jnp.broadcast_to(agg[b : b + 1, :], (32, LANES))).astype(f32)
        part = lax.dot_general(
            res[:, lanes(b * LANES)], member, (((1,), (1,)), ((), ())),
            precision=highest, preferred_element_type=f32,
        )
        sums = part if sums is None else sums + part
    row = jnp.concatenate(
        [sums[0:1], sums[1:2], sums[2:3], owner_row[...].astype(f32)], axis=1
    )
    send[:, 0, :] = jnp.broadcast_to(row, (LANES, LANES))
    row = jnp.concatenate(
        [cdia[0:1], cdia[1:2], cdia[2:3], jnp.ones((1, 32), f32)], axis=1
    )
    send[:, 1, :] = jnp.broadcast_to(row, (LANES, LANES))


def bit_of(p, at):
    return lax.bitwise_and(lax.shift_right_logical(p, at), 1)


def parity(p):
    return lax.bitwise_xor(bit_of(p, 1), bit_of(p, 2))


def lane_of_device(p, me):
    side = lax.shift_left(lax.bitwise_xor(parity(p), parity(me)), 6)
    off = lax.bitwise_xor(p, me)
    core, near = lax.shift_left(bit_of(off, 0), 5), lax.shift_left(bit_of(off, 3), 4)
    rest = lax.shift_left(lax.shift_right_logical(p, 4), 1) + bit_of(p, 2)
    return side + core + near + rest


def device_of_lane(q, me):
    side = lax.bitwise_xor(lax.bitwise_xor(bit_of(q, 6), parity(me)), bit_of(q, 0))
    core = lax.bitwise_xor(bit_of(q, 5), bit_of(me, 0))
    near = lax.bitwise_xor(bit_of(q, 4), bit_of(me, 3))
    yz = lax.shift_left(lax.bitwise_and(lax.shift_right_logical(q, 1), 7), 4)
    return yz + 8 * near + 4 * bit_of(q, 0) + 2 * side + core


def row_groups():
    return [
        [16 * (m >> 1) + 8 * near + 4 * (m & 1) + 2 * (side ^ (m & 1)) + core for m in range(NEAR)]
        for near in range(2) for side in range(2) for core in range(2)
    ]


def coarse_pack_kernel(col, blk, send):
    def turned(a):
        z = jnp.transpose(jnp.concatenate([a, jnp.zeros((32, 5), f32)], axis=1))
        return jnp.concatenate([z] * 4, axis=1)

    columns = turned(col[...].astype(f32))
    kind = lax.bitwise_and(columns.astype(i32), 7)
    tile = (8, LANES)
    sub = lax.broadcasted_iota(i32, tile, 0)
    count = jnp.zeros(tile, i32)
    match, earlier = [], []
    for k in range(SLOTS):
        here = sub == jnp.broadcast_to(kind[k : k + 1], tile)
        match.append(here)
        earlier.append(count)
        count = count + here.astype(i32)
    left = jnp.zeros((1, LANES), i32)
    start = []
    for n in range(16):
        if n >= 8:
            start.append(left)
        left = jnp.maximum(left + count[n % 8 : n % 8 + 1] - 4, 0)
    start = jnp.concatenate(start, axis=0) + 4 * sub
    place = 4 * sub + lax.shift_right_logical(lax.broadcasted_iota(i32, tile, 1), 5)
    slot = jnp.full(tile, 31, i32)
    for k in range(SLOTS):
        at = jnp.sum(jnp.where(match[k], start + earlier[k], 0), axis=0, keepdims=True)
        slot = jnp.where(place == jnp.broadcast_to(lax.bitwise_and(at, 31), tile), k, slot)
    inner, outer = lax.bitwise_and(slot, 7), lax.shift_right_logical(slot, 3)

    def placed(z):
        got = None
        for g in range(4):
            part = jnp.take_along_axis(
                z[8 * g : 8 * g + 8], inner, axis=0, mode="promise_in_bounds"
            )
            got = part if got is None else jnp.where(outer == g, part, got)
        return got

    parts = [placed(turned(blk[i, j])) for i in range(3) for j in range(3)]
    parts.append(jnp.where(slot == 31, sub.astype(f32), placed(columns)))
    for m in range(10):
        for d in range(NEAR):
            send[d, 8 * m : 8 * m + 8, :] = parts[m]


def spread(parts):
    group = lax.shift_right_logical(lax.broadcasted_iota(i32, parts[0].shape, 1), 5)
    return jnp.where(group == 0, parts[0], jnp.where(group == 1, parts[1], parts[2]))


def coarse_lookup(table, chunk, lane):
    near = [jnp.zeros(chunk.shape, f32) for _ in range(3)]
    for c in range(32):
        here = chunk == c
        for j in range(3):
            row = table[32 * j + c : 32 * j + c + 1, :]
            near[j] = jnp.where(here, picked(row, lane), near[j])
    return near


def coarse_step(table, where, passes, data, own, rhs, dia, gather):
    gather[...] = jnp.zeros(gather.shape, f32)

    def one_pass(t, carry):
        rows = [
            [pltpu.roll(table[32 * j + 8 * v : 32 * j + 8 * v + 8, :], t, axis=0) for v in range(4)]
            for j in range(3)
        ]
        for d in range(PEERS):
            w = where[d]
            code, lane = lax.bitwise_and(w, 31), lax.shift_right_logical(w, 5)
            near = [jnp.zeros((8, LANES), f32) for _ in range(3)]
            for v in range(4):
                here = code == 4 * t + v
                for j in range(3):
                    near[j] = jnp.where(here, picked(rows[j][v], lane), near[j])
            for i in range(3):
                a = data[d // NEAR][d % NEAR, lanes8(3 * i), :] * near[0]
                a = a + data[d // NEAR][d % NEAR, lanes8(3 * i + 1), :] * near[1]
                a = a + data[d // NEAR][d % NEAR, lanes8(3 * i + 2), :] * near[2]
                gather[i, d : d + 1, :] += jnp.sum(a, axis=0, keepdims=True)
        return carry

    lax.fori_loop(0, passes, one_pass, 0)
    parts = []
    for i in range(3):
        s = gather[i]
        s = s + pltpu.roll(s, 64, axis=1)
        parts.append(s + pltpu.roll(s, 32, axis=1))
    return own + damping * (rhs - (dia * own - spread(parts))) / dia


def lanes8(m):
    return slice(8 * m, 8 * m + 8)


def coarse_first_kernel(base_ref, sums, data0, data1, far_up, far_down, new, rhs, dia, where, passes,
                        table, gather, left, right):
    me = lax.shift_right_logical(base_ref[0], 10)
    got = jnp.transpose(sums[:, 0, :])
    rows = got[96:128].astype(i32)
    s = got[0:96]
    split = []
    for _ in range(3):
        t = s.astype(jnp.bfloat16).astype(f32)
        split.append(t)
        s = s - t
    chunk = lax.broadcasted_iota(i32, (32, LANES), 0)
    place = lax.broadcasted_iota(i32, (LANES, LANES), 0)
    low = lax.bitwise_and(rows, 31)
    lane = lane_of_device(lax.shift_right_logical(rows, 5), me)
    for a in range(32):
        here = chunk == jnp.broadcast_to(low[a : a + 1], (32, LANES))
        for t in range(3):
            for i in range(3):
                value = jnp.broadcast_to(split[t][32 * i + a : 32 * i + a + 1], (32, LANES))
                left[96 * t + 32 * i : 96 * t + 32 * i + 32, lanes(LANES * a)] = jnp.where(
                    here, value, 0.0
                ).astype(jnp.bfloat16)
        right[:, lanes(LANES * a)] = jnp.where(
            place == jnp.broadcast_to(lane[a : a + 1], (LANES, LANES)), 1.0, 0.0
        ).astype(jnp.bfloat16)
    both = lax.dot_general(
        left[...], right[...], (((1,), (1,)), ((), ())), preferred_element_type=f32
    )
    crhs = both[0:96] + both[96:192] + both[192:288]
    order = device_of_lane(lax.broadcasted_iota(i32, (96, LANES), 1), me)
    cdia = jnp.take_along_axis(
        jnp.transpose(sums[:, 1, :])[0:96], order, axis=1, mode="promise_in_bounds"
    )
    pad = jnp.zeros((32, LANES), f32)
    first = jnp.concatenate([damping * crhs / cdia, pad], axis=0)
    table[...] = first
    own = jnp.transpose(first)[0:PEERS]
    rhs[...] = jnp.transpose(jnp.concatenate([crhs, pad], axis=0))[0:PEERS]
    dia[...] = jnp.transpose(jnp.concatenate([cdia, pad + 1.0], axis=0))[0:PEERS]
    sub = lax.broadcasted_iota(i32, (8, LANES), 0)
    most = jnp.zeros((8, LANES), i32)
    for d in range(PEERS):
        c = (data0, data1)[d // NEAR][d % NEAR, 72:80, :].astype(i32)
        off = lax.bitwise_and(sub - c, 7)
        most = jnp.maximum(most, off)
        at = lane_of_device(lax.shift_right_logical(c, 5), me)
        code = lax.bitwise_and(lax.shift_right_logical(c, 3), 3) + lax.shift_left(off, 2)
        where[d] = code + lax.shift_left(at, 5)
    most = jnp.max(most.astype(f32)).astype(i32) + 1
    passes[...] = jnp.broadcast_to(most, passes.shape)
    new[...] = coarse_step(
        table, where, most, (data0, data1), own, rhs[...], dia[...], gather
    )


def gathered(table, pieces, mine):
    row = 0
    for piece in pieces:
        size = piece.shape[0]
        mine[row : row + size, :] = piece[...]
        row += size
    table[...] = jnp.transpose(mine[...])


def coarse_kernel(base_ref, passes, p0, p1, p2, p3, rhs, dia, where, data0, data1, new, table, mine, gather):
    gathered(table, (p0, p1, p2, p3), mine)
    new[...] = coarse_step(
        table, where, passes[...][0, 0], (data0, data1), p0[...], rhs[...], dia[...], gather
    )


def post_kernel(base_ref, p0, p1, p2, p3, first_iter, rhs, dia, col, blk, node_row, before, after,
                before2, after2, out, correction, table, mine, one, two):
    base = base_ref[0]
    me = lax.shift_right_logical(base, 10)
    gathered(table, (p0, p1, p2, p3), mine)
    row = mine[pl.ds(lane_of_device(me, me), 1), :]
    correction[...] = jnp.concatenate([row[:, 32 * i : 32 * i + 32] for i in range(3)], axis=0)
    one[...] = first_iter[...]
    one[:, lanes(0, HALO)] = before2[...]
    one[:, lanes(WIDE + ROWS + HALO, HALO)] = after2[...]
    edge = [
        h[P_ROW + t : P_ROW + t + 1, lanes(LANES * q)]
        for h in (before, after) for t in range(2) for q in range(2)
    ]
    edge = jnp.concatenate(edge, axis=0)

    def found(rows):
        rows = rows.astype(i32)
        lane = lane_of_device(lax.shift_right_logical(rows, 5), me)
        return coarse_lookup(table, lax.bitwise_and(rows, 31), lane)

    own, far = found(node_row[...]), found(edge)
    for s in range(16):
        if s < 4:
            row = [f[s : s + 1, :] for f in far]
        elif s < 12:
            row = [f[s - 4 : s - 3, :] for f in own]
        else:
            row = [f[s - 8 : s - 7, :] for f in far]
        one[:, lanes(s * LANES)] = one[:, lanes(s * LANES)] + jnp.concatenate(row, axis=0)
    two[...] = jnp.zeros(two.shape, f32)
    sweep_halo(two, one, rhs, dia, before, base, WIDE - HALO)
    sweep_halo(two, one, rhs, dia, after, base, WIDE + ROWS)

    def first(b):
        at = WIDE + b * LANES
        pull = own_block(one, col, blk, base, b)
        two[:, lanes(at)] = smoothed(one, pull, rhs, dia, at)

    def second(b):
        at = WIDE + b * LANES
        pull = own_block(two, col, blk, base, b)
        out[:, lanes(b * LANES)] = smoothed(two, pull, rhs, dia, at)

    each_block(first)
    each_block(second)


def call(kernel, outs, args, scratch=(), scalars=0, limit=12):
    vmem = pl.BlockSpec(memory_space=pltpu.VMEM)
    smem = pl.BlockSpec(memory_space=pltpu.SMEM)
    return pl.pallas_call(
        kernel,
        in_specs=[smem] * scalars + [vmem] * (len(args) - scalars),
        out_specs=[vmem] * len(outs),
        out_shape=[jax.ShapeDtypeStruct(o, t) for o, t in outs],
        scratch_shapes=[
            pltpu.VMEM(*s) if isinstance(s[0], tuple) else pltpu.VMEM(s, f32) for s in scratch
        ],
        compiler_params=pltpu.CompilerParams(vmem_limit_bytes=limit * 2**20),
    )(*args)


def partner(value, bits):
    return lax.ppermute(value, DOM, [(i, i ^ bits) for i in range(lax.axis_size(DOM))])


def in_group(new):
    p2, p3, p1 = partner(new, 2), partner(new, 3), partner(new, 1)
    return new, p1, p2, p3


def shifts(up, down):
    count = lax.axis_size(DOM)
    forward = [(i, i + 1) for i in range(count - 1)]
    backward = [(i + 1, i) for i in range(count - 1)]
    return lax.ppermute(up, DOM, forward), lax.ppermute(down, DOM, backward)


def cycle(right_side, fine_diagonal, fine_columns, fine_blocks, aggregate_of_node,
         coarse_row_of_aggregate, coarse_diagonal, coarse_columns, coarse_blocks):
    rhs, dia = right_side.T, fine_diagonal.T
    col, blk = fine_columns.T, fine_blocks.transpose(2, 3, 1, 0)
    agg = aggregate_of_node.reshape(8, LANES)
    owner = coarse_row_of_aggregate.reshape(1, 32)
    cdia, cblk = coarse_diagonal.T, coarse_blocks.transpose(2, 3, 0, 1)
    me = lax.axis_index(DOM).astype(i32).reshape(1)
    base = me * ROWS
    wide = WIDE + ROWS + WIDE

    dsend, = call(
        coarse_pack_kernel, [((NEAR, 80, LANES), f32)], [coarse_columns, cblk],
        limit=60,
    )
    data = lax.all_to_all(
        dsend, DOM, 0, 0, axis_index_groups=row_groups(), tiled=True
    )
    far_data = partner(data, 8)
    vmem, far = pl.BlockSpec(memory_space=pltpu.VMEM), pl.BlockSpec(memory_space=pltpu.HBM)
    up, down, node_row = pl.pallas_call(
        pack_kernel,
        name="pack",
        in_specs=[far] * 6,
        out_specs=[vmem] * 3,
        out_shape=[jax.ShapeDtypeStruct(o, f32) for o in ((P_ALL, HALO), (P_ALL, HALO), (8, LANES))],
        scratch_shapes=[
            pltpu.VMEM((3, ROWS), f32), pltpu.VMEM((3, ROWS), f32),
            pltpu.VMEM((2, SLOTS, HALO), i32), pltpu.VMEM((2, 3, 3, SLOTS, HALO), f32),
            pltpu.VMEM((8, LANES), i32), pltpu.VMEM((1, 32), i32), pltpu.SemaphoreType.DMA((8,)),
        ],
        compiler_params=pltpu.CompilerParams(vmem_limit_bytes=60 * 2**20),
    )(rhs, dia, col, blk, agg, owner)
    before, after = shifts(up, down)
    send, first_iter, wrhs, wdia, up2, down2 = call(
        pre_kernel,
        [((LANES, 2, LANES), f32), ((3, wide), f32), ((3, wide), f32), ((3, wide), f32),
         ((3, HALO), f32), ((3, HALO), f32)],
        [base, rhs, dia, col, blk, agg, owner, cdia, before, after],
        scratch=[(3, wide), (3, wide), (8, ROWS)], scalars=1,
    )
    before2, after2 = shifts(up2, down2)
    sums = lax.all_to_all(send, DOM, 0, 0, tiled=True)
    peers = ((PEERS, LANES), f32)
    gather = (3, PEERS, LANES)
    square = (LANES, LANES)
    new, crhs, cd, where, passes = call(
        coarse_first_kernel,
        [peers, peers, peers, ((PEERS, 8, LANES), i32), ((8, LANES), i32)],
        [base, sums, data, far_data, before2, after2],
        scratch=[square, gather, ((288, 4096), jnp.bfloat16), ((LANES, 4096), jnp.bfloat16)],
        scalars=1,
    )
    for _ in range(CSWEEPS - 2):
        new, = call(
            coarse_kernel, [peers],
            [base, passes, *in_group(new), crhs, cd, where, data, far_data],
            scratch=[square, square, gather], scalars=1,
        )
    solution, mine = call(
        post_kernel, [((3, ROWS), f32), ((3, 32), f32)],
        [base, *in_group(new), first_iter, wrhs, wdia, col, blk, node_row,
         before, after, before2, after2],
        scratch=[square, square, (3, wide), (3, wide)], scalars=1,
    )
    return solution.T, mine.T


def solution(mesh):
    return jax.shard_map(
        cycle,
        mesh=mesh,
        in_specs=(
            P(DOM, None),
            P(DOM, None),
            P(DOM, None),
            P(DOM, None, None, None),
            P(DOM),
            P(DOM),
            P(DOM, None),
            P(DOM, None),
            P(DOM, None, None, None),
        ),
        out_specs=(P(DOM, None), P(DOM, None)),
        check_vma=False,
    )
```

```python
import jax
import jax.numpy as jnp
from jax import lax
from jax.experimental import pallas as pl
from jax.experimental.pallas import tpu as pltpu
from jax.sharding import PartitionSpec as P


DOM = "dom"
PEERS = 32
NEAR = 8
PARTS = PEERS // NEAR
PIECES = 128 // PEERS
UNROLL = 8
CSWEEPS = 6
damping = 0.7
highest = lax.Precision.HIGHEST

ROWS = 1024
LANES = 128
SLOTS = 27
FULL = 24
HALO = 256
WIDE = 512
BLOCKS = ROWS // LANES
P_COL = 9 * FULL
P_BTAIL = P_COL + FULL
P_CTAIL = P_BTAIL + 27
P_RHS = P_CTAIL + 3
P_DIA = P_RHS + 6
P_ROW = P_DIA + 6
P_ALL = 288
f32 = jnp.float32
i32 = jnp.int32


def lanes(start, size=LANES):
    if isinstance(start, int):
        return slice(start, start + size)
    return pl.ds(pl.multiple_of(start, LANES), size)


def picked(row, where):
    return jnp.take_along_axis(
        jnp.broadcast_to(row, where.shape), where, axis=1, mode="promise_in_bounds"
    )


def pack_kernel(rhs_in, dia_in, col_in, blk_in, agg_in, owner_in, up, down, node_row,
                rhs, dia, col, blk, agg, owner, sem):
    copies = [(rhs_in, rhs), (dia_in, dia), (agg_in, agg), (owner_in, owner)]
    for t, near in enumerate((ROWS - HALO, 0)):
        copies.append((col_in.at[:, lanes(near, HALO)], col.at[t]))
        copies.append((blk_in.at[:, :, :, lanes(near, HALO)], blk.at[t]))
    copies = [pltpu.make_async_copy(a, b, sem.at[n]) for n, (a, b) in enumerate(copies)]
    for c in copies:
        c.start()
    for c in copies:
        c.wait()
    table = jnp.concatenate([owner[...]] * 4, axis=1)
    found = picked(table, agg[...]).astype(f32)
    node_row[...] = found
    for t, (out, wide) in enumerate(((up, ROWS - WIDE), (down, 0))):
        for i in range(3):
            for j in range(3):
                g = 3 * i + j
                out[g * FULL : (g + 1) * FULL, :] = blk[t, i, j, 0:FULL, :]
                out[P_BTAIL + 3 * g : P_BTAIL + 3 * g + 3, :] = blk[t, i, j, FULL:SLOTS, :]
        out[P_COL : P_COL + FULL, :] = col[t, 0:FULL, :].astype(f32)
        out[P_CTAIL : P_CTAIL + 3, :] = col[t, FULL:SLOTS, :].astype(f32)
        for h in range(2):
            out[P_RHS + 3 * h : P_RHS + 3 * h + 3, :] = rhs[:, lanes(wide + HALO * h, HALO)]
            out[P_DIA + 3 * h : P_DIA + 3 * h + 3, :] = dia[:, lanes(wide + HALO * h, HALO)]
            for q in range(2):
                s = wide // LANES + 2 * h + q
                out[P_ROW + h : P_ROW + h + 1, lanes(LANES * q)] = found[s : s + 1, :]
        out[P_ROW + 2 : P_ALL, :] = jnp.zeros((P_ALL - P_ROW - 2, HALO), f32)


def pulled_block(columns, blocks, table, first_chunk):
    total = [None, None, None]
    for part in range(4):
        where = columns(part)
        chunk = lax.shift_right_arithmetic(where, 7)
        lane = lax.bitwise_and(where, 127)
        near = [jnp.zeros(where.shape, f32) for _ in range(3)]
        for c in range(5):
            here = chunk == c
            for j in range(3):
                row = table[j : j + 1, lanes(first_chunk * LANES + c * LANES)]
                near[j] = jnp.where(here, picked(row, lane), near[j])
        for i in range(3):
            s = blocks(i, 0, part) * near[0]
            s = s + blocks(i, 1, part) * near[1]
            s = s + blocks(i, 2, part) * near[2]
            if part < 3:
                total[i] = s if total[i] is None else total[i] + s
            else:
                total[i] = jnp.sum(total[i], axis=0, keepdims=True) + jnp.sum(
                    s, axis=0, keepdims=True
                )
    return total


def local_getters(col, blk, start, b):
    def columns(part):
        lo, hi = 8 * part, min(8 * part + 8, SLOTS)
        return col[lo:hi, lanes(b * LANES)] - start

    def blocks(i, j, part):
        lo, hi = 8 * part, min(8 * part + 8, SLOTS)
        return blk[i, j, lo:hi, lanes(b * LANES)]

    return columns, blocks


def halo_getters(halo, start, b):
    def columns(part):
        if part < 3:
            got = halo[P_COL + 8 * part : P_COL + 8 * part + 8, lanes(b * LANES)]
        else:
            got = halo[P_CTAIL : P_CTAIL + 3, lanes(b * LANES)]
        return got.astype(i32) - start

    def blocks(i, j, part):
        g = 3 * i + j
        if part < 3:
            return halo[g * FULL + 8 * part : g * FULL + 8 * part + 8, lanes(b * LANES)]
        return halo[P_BTAIL + 3 * g : P_BTAIL + 3 * g + 3, lanes(b * LANES)]

    return columns, blocks


def wide_vector(out, local, before, after, row):
    out[:, lanes(WIDE, ROWS)] = local[...]
    for h in range(2):
        out[:, lanes(HALO * h, HALO)] = before[row + 3 * h : row + 3 * h + 3, :]
        out[:, lanes(WIDE + ROWS + HALO * h, HALO)] = after[row + 3 * h : row + 3 * h + 3, :]


def smoothed(table, pulled, rhs, dia, at):
    pull = jnp.concatenate(pulled, axis=0)
    s = table[:, lanes(at)]
    b = rhs[:, lanes(at)]
    d = dia[:, lanes(at)]
    return s + damping * (b - (d * s - pull)) / d


def sweep_halo(out, table, rhs, dia, halo, base, first):
    for b in range(2):
        at = first + LANES * b
        start = base + (at - WIDE) - 2 * LANES
        cols, blks = halo_getters(halo, start, b)
        pull = pulled_block(cols, blks, table, at // LANES - 2)
        out[:, lanes(at)] = smoothed(table, pull, rhs, dia, at)


def each_block(step):
    def some(t, carry):
        for u in range(UNROLL):
            step(t * UNROLL + u)
        return carry

    lax.fori_loop(0, BLOCKS // UNROLL, some, 0)


def own_block(table, col, blk, base, b):
    start = base + b * LANES - 2 * LANES
    cols, blks = local_getters(col, blk, start, b)
    return pulled_block(cols, blks, table, b + WIDE // LANES - 2)


def pre_kernel(base_ref, rhs, dia, col, blk, agg, owner_row, cdia, before, after,
               send, first_iter, keep_rhs, keep_dia, up2, down2, one, two, res):
    base = base_ref[0]
    wide_vector(keep_rhs, rhs, before, after, P_RHS)
    wide_vector(keep_dia, dia, before, after, P_DIA)
    raw = keep_dia[...]
    keep_dia[...] = jnp.where(raw == 0.0, 1.0, raw)
    one[...] = damping * keep_rhs[...] / keep_dia[...]
    two[...] = jnp.zeros(two.shape, f32)
    sweep_halo(two, one, keep_rhs, keep_dia, before, base, WIDE - HALO)
    sweep_halo(two, one, keep_rhs, keep_dia, after, base, WIDE + ROWS)

    def second(b):
        at = WIDE + b * LANES
        pull = own_block(one, col, blk, base, b)
        two[:, lanes(at)] = smoothed(one, pull, keep_rhs, keep_dia, at)

    each_block(second)

    def third(b):
        at = WIDE + b * LANES
        pull = jnp.concatenate(own_block(two, col, blk, base, b), axis=0)
        s, d = two[:, lanes(at)], keep_dia[:, lanes(at)]
        res[0:3, lanes(b * LANES)] = keep_rhs[:, lanes(at)] - (d * s - pull)

    res[...] = jnp.zeros(res.shape, f32)
    each_block(third)
    first_iter[...] = two[...]
    up2[...] = two[:, lanes(WIDE + ROWS - WIDE, HALO)]
    down2[...] = two[:, lanes(WIDE + HALO, HALO)]
    label = lax.broadcasted_iota(i32, (32, LANES), 0)
    sums = None
    for b in range(BLOCKS):
        member = (label == jnp.broadcast_to(agg[b : b + 1, :], (32, LANES))).astype(f32)
        part = lax.dot_general(
            res[:, lanes(b * LANES)], member, (((1,), (1,)), ((), ())),
            precision=highest, preferred_element_type=f32,
        )
        sums = part if sums is None else sums + part
    row = jnp.concatenate(
        [sums[0:1], sums[1:2], sums[2:3], owner_row[...].astype(f32)], axis=1
    )
    send[:, 0, :] = jnp.broadcast_to(row, (LANES, LANES))
    row = jnp.concatenate(
        [cdia[0:1], cdia[1:2], cdia[2:3], jnp.ones((1, 32), f32)], axis=1
    )
    send[:, 1, :] = jnp.broadcast_to(row, (LANES, LANES))


def bit_of(p, at):
    return lax.bitwise_and(lax.shift_right_logical(p, at), 1)


def bit_parity(p, at):
    return lax.bitwise_xor(bit_of(p, at), bit_of(p, at + 1))


def lane_of_device(p, me):
    off = lax.bitwise_xor(p, me)
    rest = 4 * bit_of(p, 6) + 2 * bit_of(p, 4) + bit_of(p, 2)
    return (
        64 * bit_parity(off, 1) + 32 * bit_of(off, 0) + 16 * bit_parity(off, 5) + 8 * bit_parity(off, 3)
        + rest
    )


def device_of_lane(q, me):
    def last(relative, at, first):
        return lax.bitwise_xor(lax.bitwise_xor(relative, bit_parity(me, at)), first)

    x, z, y = bit_of(q, 0), bit_of(q, 1), bit_of(q, 2)
    p = 64 * y + 32 * last(bit_of(q, 4), 5, y) + 16 * z + 8 * last(bit_of(q, 3), 3, z)
    core = lax.bitwise_xor(bit_of(q, 5), bit_of(me, 0))
    return p + 4 * x + 2 * last(bit_of(q, 6), 1, x) + core


def row_groups():
    def member(kind, m):
        y, z, x = m >> 2, m >> 1 & 1, m & 1
        py, pz, px, core = kind >> 3, kind >> 2 & 1, kind >> 1 & 1, kind & 1
        return 64 * y + 32 * (y ^ py) + 16 * z + 8 * (z ^ pz) + 4 * x + 2 * (x ^ px) + core

    return [[member(kind, m) for m in range(NEAR)] for kind in range(16)]


def coarse_pack_kernel(col, blk, send):
    def turned(a):
        z = jnp.transpose(jnp.concatenate([a, jnp.zeros((32, 5), f32)], axis=1))
        return jnp.concatenate([z] * 4, axis=1)

    columns = turned(col[...].astype(f32))
    kind = lax.bitwise_and(columns.astype(i32), 7)
    tile = (8, LANES)
    sub = lax.broadcasted_iota(i32, tile, 0)
    count = jnp.zeros(tile, i32)
    match, earlier = [], []
    for k in range(SLOTS):
        here = sub == jnp.broadcast_to(kind[k : k + 1], tile)
        match.append(here)
        earlier.append(count)
        count = count + here.astype(i32)
    left = jnp.zeros((1, LANES), i32)
    start = []
    for n in range(16):
        if n >= 8:
            start.append(left)
        left = jnp.maximum(left + count[n % 8 : n % 8 + 1] - 4, 0)
    start = jnp.concatenate(start, axis=0) + 4 * sub
    place = 4 * sub + lax.shift_right_logical(lax.broadcasted_iota(i32, tile, 1), 5)
    slot = jnp.full(tile, 31, i32)
    for k in range(SLOTS):
        at = jnp.sum(jnp.where(match[k], start + earlier[k], 0), axis=0, keepdims=True)
        slot = jnp.where(place == jnp.broadcast_to(lax.bitwise_and(at, 31), tile), k, slot)
    inner, outer = lax.bitwise_and(slot, 7), lax.shift_right_logical(slot, 3)

    def placed(z):
        got = None
        for g in range(4):
            part = jnp.take_along_axis(
                z[8 * g : 8 * g + 8], inner, axis=0, mode="promise_in_bounds"
            )
            got = part if got is None else jnp.where(outer == g, part, got)
        return got

    parts = [placed(turned(blk[i, j])) for i in range(3) for j in range(3)]
    parts.append(jnp.where(slot == 31, sub.astype(f32), placed(columns)))
    for m in range(10):
        for d in range(NEAR):
            send[d, 8 * m : 8 * m + 8, :] = parts[m]


def spread(parts):
    group = lax.shift_right_logical(lax.broadcasted_iota(i32, parts[0].shape, 1), 5)
    return jnp.where(group == 0, parts[0], jnp.where(group == 1, parts[1], parts[2]))


def coarse_lookup(table, chunk, lane):
    near = [jnp.zeros(chunk.shape, f32) for _ in range(3)]
    for c in range(32):
        here = chunk == c
        for j in range(3):
            row = table[32 * j + c : 32 * j + c + 1, :]
            near[j] = jnp.where(here, picked(row, lane), near[j])
    return near


def coarse_step(table, where, passes, data, own, rhs, dia, gather):
    gather[...] = jnp.zeros(gather.shape, f32)

    def one_pass(t, carry):
        rows = [
            [pltpu.roll(table[32 * j + 8 * v : 32 * j + 8 * v + 8, :], t, axis=0) for v in range(4)]
            for j in range(3)
        ]
        for d in range(PEERS):
            w = where[d]
            code, lane = lax.bitwise_and(w, 31), lax.shift_right_logical(w, 5)
            near = [jnp.zeros((8, LANES), f32) for _ in range(3)]
            for v in range(4):
                here = code == 4 * t + v
                for j in range(3):
                    near[j] = jnp.where(here, picked(rows[j][v], lane), near[j])
            for i in range(3):
                a = data[d // NEAR][d % NEAR, lanes8(3 * i), :] * near[0]
                a = a + data[d // NEAR][d % NEAR, lanes8(3 * i + 1), :] * near[1]
                a = a + data[d // NEAR][d % NEAR, lanes8(3 * i + 2), :] * near[2]
                gather[i, d : d + 1, :] += jnp.sum(a, axis=0, keepdims=True)
        return carry

    lax.fori_loop(0, passes, one_pass, 0)
    parts = []
    for i in range(3):
        s = gather[i]
        s = s + pltpu.roll(s, 64, axis=1)
        parts.append(s + pltpu.roll(s, 32, axis=1))
    return own + damping * (rhs - (dia * own - spread(parts))) / dia


def lanes8(m):
    return slice(8 * m, 8 * m + 8)


def coarse_first_kernel(base_ref, sums, *rest):
    data = rest[:PARTS]
    new, rhs, dia, where, passes, table, gather, left, right = rest[PARTS + 2 :]
    me = lax.shift_right_logical(base_ref[0], 10)
    got = jnp.transpose(sums[:, 0, :])
    rows = got[96:128].astype(i32)
    s = got[0:96]
    split = []
    for _ in range(3):
        t = s.astype(jnp.bfloat16).astype(f32)
        split.append(t)
        s = s - t
    chunk = lax.broadcasted_iota(i32, (32, LANES), 0)
    place = lax.broadcasted_iota(i32, (LANES, LANES), 0)
    low = lax.bitwise_and(rows, 31)
    lane = lane_of_device(lax.shift_right_logical(rows, 5), me)
    for a in range(32):
        here = chunk == jnp.broadcast_to(low[a : a + 1], (32, LANES))
        for t in range(3):
            for i in range(3):
                value = jnp.broadcast_to(split[t][32 * i + a : 32 * i + a + 1], (32, LANES))
                left[96 * t + 32 * i : 96 * t + 32 * i + 32, lanes(LANES * a)] = jnp.where(
                    here, value, 0.0
                ).astype(jnp.bfloat16)
        right[:, lanes(LANES * a)] = jnp.where(
            place == jnp.broadcast_to(lane[a : a + 1], (LANES, LANES)), 1.0, 0.0
        ).astype(jnp.bfloat16)
    both = lax.dot_general(
        left[...], right[...], (((1,), (1,)), ((), ())), preferred_element_type=f32
    )
    crhs = both[0:96] + both[96:192] + both[192:288]
    order = device_of_lane(lax.broadcasted_iota(i32, (96, LANES), 1), me)
    cdia = jnp.take_along_axis(
        jnp.transpose(sums[:, 1, :])[0:96], order, axis=1, mode="promise_in_bounds"
    )
    pad = jnp.zeros((32, LANES), f32)
    first = jnp.concatenate([damping * crhs / cdia, pad], axis=0)
    table[...] = first
    own = jnp.transpose(first)[0:PEERS]
    rhs[...] = jnp.transpose(jnp.concatenate([crhs, pad], axis=0))[0:PEERS]
    dia[...] = jnp.transpose(jnp.concatenate([cdia, pad + 1.0], axis=0))[0:PEERS]
    sub = lax.broadcasted_iota(i32, (8, LANES), 0)
    most = jnp.zeros((8, LANES), i32)
    for d in range(PEERS):
        c = data[d // NEAR][d % NEAR, 72:80, :].astype(i32)
        off = lax.bitwise_and(sub - c, 7)
        most = jnp.maximum(most, off)
        at = lane_of_device(lax.shift_right_logical(c, 5), me)
        code = lax.bitwise_and(lax.shift_right_logical(c, 3), 3) + lax.shift_left(off, 2)
        where[d] = code + lax.shift_left(at, 5)
    most = jnp.max(most.astype(f32)).astype(i32) + 1
    passes[...] = jnp.broadcast_to(most, passes.shape)
    new[...] = coarse_step(
        table, where, most, data, own, rhs[...], dia[...], gather
    )


def gathered(table, pieces, mine):
    row = 0
    for piece in pieces:
        size = piece.shape[0]
        mine[row : row + size, :] = piece[...]
        row += size
    table[...] = jnp.transpose(mine[...])


def coarse_kernel(base_ref, passes, *rest):
    pieces, (rhs, dia, where) = rest[:PIECES], rest[PIECES : PIECES + 3]
    data = rest[PIECES + 3 : PIECES + 3 + PARTS]
    new, table, mine, gather = rest[PIECES + 3 + PARTS :]
    gathered(table, pieces, mine)
    new[...] = coarse_step(
        table, where, passes[...][0, 0], data, pieces[0][...], rhs[...], dia[...], gather
    )


def post_kernel(base_ref, *rest):
    pieces = rest[:PIECES]
    (first_iter, rhs, dia, col, blk, node_row, before, after, before2, after2,
     out, correction, table, mine, one, two) = rest[PIECES:]
    base = base_ref[0]
    me = lax.shift_right_logical(base, 10)
    gathered(table, pieces, mine)
    row = mine[pl.ds(lane_of_device(me, me), 1), :]
    correction[...] = jnp.concatenate([row[:, 32 * i : 32 * i + 32] for i in range(3)], axis=0)
    one[...] = first_iter[...]
    one[:, lanes(0, HALO)] = before2[...]
    one[:, lanes(WIDE + ROWS + HALO, HALO)] = after2[...]
    edge = [
        h[P_ROW + t : P_ROW + t + 1, lanes(LANES * q)]
        for h in (before, after) for t in range(2) for q in range(2)
    ]
    edge = jnp.concatenate(edge, axis=0)

    def found(rows):
        rows = rows.astype(i32)
        lane = lane_of_device(lax.shift_right_logical(rows, 5), me)
        return coarse_lookup(table, lax.bitwise_and(rows, 31), lane)

    own, far = found(node_row[...]), found(edge)
    for s in range(16):
        if s < 4:
            row = [f[s : s + 1, :] for f in far]
        elif s < 12:
            row = [f[s - 4 : s - 3, :] for f in own]
        else:
            row = [f[s - 8 : s - 7, :] for f in far]
        one[:, lanes(s * LANES)] = one[:, lanes(s * LANES)] + jnp.concatenate(row, axis=0)
    two[...] = jnp.zeros(two.shape, f32)
    sweep_halo(two, one, rhs, dia, before, base, WIDE - HALO)
    sweep_halo(two, one, rhs, dia, after, base, WIDE + ROWS)

    def first(b):
        at = WIDE + b * LANES
        pull = own_block(one, col, blk, base, b)
        two[:, lanes(at)] = smoothed(one, pull, rhs, dia, at)

    def second(b):
        at = WIDE + b * LANES
        pull = own_block(two, col, blk, base, b)
        out[:, lanes(b * LANES)] = smoothed(two, pull, rhs, dia, at)

    each_block(first)
    each_block(second)


def call(kernel, outs, args, scratch=(), scalars=0, limit=12):
    vmem = pl.BlockSpec(memory_space=pltpu.VMEM)
    smem = pl.BlockSpec(memory_space=pltpu.SMEM)
    return pl.pallas_call(
        kernel,
        in_specs=[smem] * scalars + [vmem] * (len(args) - scalars),
        out_specs=[vmem] * len(outs),
        out_shape=[jax.ShapeDtypeStruct(o, t) for o, t in outs],
        scratch_shapes=[
            pltpu.VMEM(*s) if isinstance(s[0], tuple) else pltpu.VMEM(s, f32) for s in scratch
        ],
        compiler_params=pltpu.CompilerParams(vmem_limit_bytes=limit * 2**20),
    )(*args)


def partner(value, bits):
    return lax.ppermute(value, DOM, [(i, i ^ bits) for i in range(lax.axis_size(DOM))])


def in_group(new):
    p2, p3, p1 = partner(new, 2), partner(new, 3), partner(new, 1)
    return new, p1, p2, p3


def shifts(up, down):
    count = lax.axis_size(DOM)
    forward = [(i, i + 1) for i in range(count - 1)]
    backward = [(i + 1, i) for i in range(count - 1)]
    return lax.ppermute(up, DOM, forward), lax.ppermute(down, DOM, backward)


def cycle(right_side, fine_diagonal, fine_columns, fine_blocks, aggregate_of_node,
         coarse_row_of_aggregate, coarse_diagonal, coarse_columns, coarse_blocks):
    rhs, dia = right_side.T, fine_diagonal.T
    col, blk = fine_columns.T, fine_blocks.transpose(2, 3, 1, 0)
    agg = aggregate_of_node.reshape(8, LANES)
    owner = coarse_row_of_aggregate.reshape(1, 32)
    cdia, cblk = coarse_diagonal.T, coarse_blocks.transpose(2, 3, 0, 1)
    me = lax.axis_index(DOM).astype(i32).reshape(1)
    base = me * ROWS
    wide = WIDE + ROWS + WIDE

    dsend, = call(
        coarse_pack_kernel, [((NEAR, 80, LANES), f32)], [coarse_columns, cblk],
        limit=60,
    )
    data = lax.all_to_all(
        dsend, DOM, 0, 0, axis_index_groups=row_groups(), tiled=True
    )
    along_z, along_y = partner(data, 8), partner(data, 32)
    data = (data, along_z, along_y, partner(along_z, 32))
    vmem, far = pl.BlockSpec(memory_space=pltpu.VMEM), pl.BlockSpec(memory_space=pltpu.HBM)
    up, down, node_row = pl.pallas_call(
        pack_kernel,
        name="pack",
        in_specs=[far] * 6,
        out_specs=[vmem] * 3,
        out_shape=[jax.ShapeDtypeStruct(o, f32) for o in ((P_ALL, HALO), (P_ALL, HALO), (8, LANES))],
        scratch_shapes=[
            pltpu.VMEM((3, ROWS), f32), pltpu.VMEM((3, ROWS), f32),
            pltpu.VMEM((2, SLOTS, HALO), i32), pltpu.VMEM((2, 3, 3, SLOTS, HALO), f32),
            pltpu.VMEM((8, LANES), i32), pltpu.VMEM((1, 32), i32), pltpu.SemaphoreType.DMA((8,)),
        ],
        compiler_params=pltpu.CompilerParams(vmem_limit_bytes=60 * 2**20),
    )(rhs, dia, col, blk, agg, owner)
    before, after = shifts(up, down)
    send, first_iter, wrhs, wdia, up2, down2 = call(
        pre_kernel,
        [((LANES, 2, LANES), f32), ((3, wide), f32), ((3, wide), f32), ((3, wide), f32),
         ((3, HALO), f32), ((3, HALO), f32)],
        [base, rhs, dia, col, blk, agg, owner, cdia, before, after],
        scratch=[(3, wide), (3, wide), (8, ROWS)], scalars=1,
    )
    before2, after2 = shifts(up2, down2)
    sums = lax.all_to_all(send, DOM, 0, 0, tiled=True)
    peers = ((PEERS, LANES), f32)
    gather = (3, PEERS, LANES)
    square = (LANES, LANES)
    new, crhs, cd, where, passes = call(
        coarse_first_kernel,
        [peers, peers, peers, ((PEERS, 8, LANES), i32), ((8, LANES), i32)],
        [base, sums, *data, before2, after2],
        scratch=[square, gather, ((288, 4096), jnp.bfloat16), ((LANES, 4096), jnp.bfloat16)],
        scalars=1,
    )
    for _ in range(CSWEEPS - 2):
        new, = call(
            coarse_kernel, [peers],
            [base, passes, *in_group(new), crhs, cd, where, *data],
            scratch=[square, square, gather], scalars=1,
        )
    solution, mine = call(
        post_kernel, [((3, ROWS), f32), ((3, 32), f32)],
        [base, *in_group(new), first_iter, wrhs, wdia, col, blk, node_row,
         before, after, before2, after2],
        scratch=[square, square, (3, wide), (3, wide)], scalars=1,
    )
    return solution.T, mine.T


def solution(mesh):
    return jax.shard_map(
        cycle,
        mesh=mesh,
        in_specs=(
            P(DOM, None),
            P(DOM, None),
            P(DOM, None),
            P(DOM, None, None, None),
            P(DOM),
            P(DOM),
            P(DOM, None),
            P(DOM, None),
            P(DOM, None, None, None),
        ),
        out_specs=(P(DOM, None), P(DOM, None)),
        check_vma=False,
    )
```

```python
import jax
import jax.numpy as jnp
from jax import lax
from jax.experimental import pallas as pl
from jax.experimental.pallas import tpu as pltpu
from jax.sharding import PartitionSpec as P


DOM = "dom"
PEERS = 32
NEAR = 8
PARTS = PEERS // NEAR
PIECES = 128 // PEERS
UNROLL = 8
CSWEEPS = 6
damping = 0.7
highest = lax.Precision.HIGHEST

ROWS = 1024
LANES = 128
SLOTS = 27
FULL = 24
HALO = 256
WIDE = 512
BLOCKS = ROWS // LANES
P_COL = 9 * FULL
P_BTAIL = P_COL + FULL
P_CTAIL = P_BTAIL + 27
P_RHS = P_CTAIL + 3
P_DIA = P_RHS + 6
P_ROW = P_DIA + 6
P_ALL = 288
f32 = jnp.float32
i32 = jnp.int32


def lanes(start, size=LANES):
    if isinstance(start, int):
        return slice(start, start + size)
    return pl.ds(pl.multiple_of(start, LANES), size)


def picked(row, where):
    return jnp.take_along_axis(
        jnp.broadcast_to(row, where.shape), where, axis=1, mode="promise_in_bounds"
    )


def pack_kernel(rhs_in, dia_in, col_in, blk_in, agg_in, owner_in, ccol_in, cblk_in,
                up, down, node_row, send, rhs, dia, col, blk, agg, owner, ccol, cblk, sem):
    copies = [(ccol_in, ccol), (cblk_in, cblk)]
    copies += [(rhs_in, rhs), (dia_in, dia), (agg_in, agg), (owner_in, owner)]
    for t, near in enumerate((ROWS - HALO, 0)):
        copies.append((col_in.at[:, lanes(near, HALO)], col.at[t]))
        copies.append((blk_in.at[:, :, :, lanes(near, HALO)], blk.at[t]))
    copies = [pltpu.make_async_copy(a, b, sem.at[n]) for n, (a, b) in enumerate(copies)]
    for c in copies:
        c.start()
    for c in copies[:2]:
        c.wait()
    pack_coarse(ccol, cblk, send)
    for c in copies[2:]:
        c.wait()
    table = jnp.concatenate([owner[...]] * 4, axis=1)
    found = picked(table, agg[...]).astype(f32)
    node_row[...] = found
    for t, (out, wide) in enumerate(((up, ROWS - WIDE), (down, 0))):
        for i in range(3):
            for j in range(3):
                g = 3 * i + j
                out[g * FULL : (g + 1) * FULL, :] = blk[t, i, j, 0:FULL, :]
                out[P_BTAIL + 3 * g : P_BTAIL + 3 * g + 3, :] = blk[t, i, j, FULL:SLOTS, :]
        out[P_COL : P_COL + FULL, :] = col[t, 0:FULL, :].astype(f32)
        out[P_CTAIL : P_CTAIL + 3, :] = col[t, FULL:SLOTS, :].astype(f32)
        for h in range(2):
            out[P_RHS + 3 * h : P_RHS + 3 * h + 3, :] = rhs[:, lanes(wide + HALO * h, HALO)]
            out[P_DIA + 3 * h : P_DIA + 3 * h + 3, :] = dia[:, lanes(wide + HALO * h, HALO)]
            for q in range(2):
                s = wide // LANES + 2 * h + q
                out[P_ROW + h : P_ROW + h + 1, lanes(LANES * q)] = found[s : s + 1, :]
        out[P_ROW + 2 : P_ALL, :] = jnp.zeros((P_ALL - P_ROW - 2, HALO), f32)


def pulled_block(columns, blocks, table, first_chunk):
    total = [None, None, None]
    for part in range(4):
        where = columns(part)
        chunk = lax.shift_right_arithmetic(where, 7)
        lane = lax.bitwise_and(where, 127)
        near = [jnp.zeros(where.shape, f32) for _ in range(3)]
        for c in range(5):
            here = chunk == c
            for j in range(3):
                row = table[j : j + 1, lanes(first_chunk * LANES + c * LANES)]
                near[j] = jnp.where(here, picked(row, lane), near[j])
        for i in range(3):
            s = blocks(i, 0, part) * near[0]
            s = s + blocks(i, 1, part) * near[1]
            s = s + blocks(i, 2, part) * near[2]
            if part < 3:
                total[i] = s if total[i] is None else total[i] + s
            else:
                total[i] = jnp.sum(total[i], axis=0, keepdims=True) + jnp.sum(
                    s, axis=0, keepdims=True
                )
    return total


def local_getters(col, blk, start, b):
    def columns(part):
        lo, hi = 8 * part, min(8 * part + 8, SLOTS)
        return col[lo:hi, lanes(b * LANES)] - start

    def blocks(i, j, part):
        lo, hi = 8 * part, min(8 * part + 8, SLOTS)
        return blk[i, j, lo:hi, lanes(b * LANES)]

    return columns, blocks


def halo_getters(halo, start, b):
    def columns(part):
        if part < 3:
            got = halo[P_COL + 8 * part : P_COL + 8 * part + 8, lanes(b * LANES)]
        else:
            got = halo[P_CTAIL : P_CTAIL + 3, lanes(b * LANES)]
        return got.astype(i32) - start

    def blocks(i, j, part):
        g = 3 * i + j
        if part < 3:
            return halo[g * FULL + 8 * part : g * FULL + 8 * part + 8, lanes(b * LANES)]
        return halo[P_BTAIL + 3 * g : P_BTAIL + 3 * g + 3, lanes(b * LANES)]

    return columns, blocks


def wide_vector(out, local, before, after, row):
    out[:, lanes(WIDE, ROWS)] = local[...]
    for h in range(2):
        out[:, lanes(HALO * h, HALO)] = before[row + 3 * h : row + 3 * h + 3, :]
        out[:, lanes(WIDE + ROWS + HALO * h, HALO)] = after[row + 3 * h : row + 3 * h + 3, :]


def smoothed(table, pulled, rhs, dia, at):
    pull = jnp.concatenate(pulled, axis=0)
    s = table[:, lanes(at)]
    b = rhs[:, lanes(at)]
    d = dia[:, lanes(at)]
    return s + damping * (b - (d * s - pull)) / d


def sweep_halo(out, table, rhs, dia, halo, base, first):
    for b in range(2):
        at = first + LANES * b
        start = base + (at - WIDE) - 2 * LANES
        cols, blks = halo_getters(halo, start, b)
        pull = pulled_block(cols, blks, table, at // LANES - 2)
        out[:, lanes(at)] = smoothed(table, pull, rhs, dia, at)


def each_block(step):
    def some(t, carry):
        for u in range(UNROLL):
            step(t * UNROLL + u)
        return carry

    lax.fori_loop(0, BLOCKS // UNROLL, some, 0)


def own_block(table, col, blk, base, b):
    start = base + b * LANES - 2 * LANES
    cols, blks = local_getters(col, blk, start, b)
    return pulled_block(cols, blks, table, b + WIDE // LANES - 2)


def pre_kernel(base_ref, rhs, dia, col, blk, agg, owner_row, cdia, before, after,
               send, first_iter, keep_rhs, keep_dia, up2, down2, one, two, res):
    base = base_ref[0]
    wide_vector(keep_rhs, rhs, before, after, P_RHS)
    wide_vector(keep_dia, dia, before, after, P_DIA)
    raw = keep_dia[...]
    keep_dia[...] = jnp.where(raw == 0.0, 1.0, raw)
    one[...] = damping * keep_rhs[...] / keep_dia[...]
    two[...] = jnp.zeros(two.shape, f32)
    sweep_halo(two, one, keep_rhs, keep_dia, before, base, WIDE - HALO)
    sweep_halo(two, one, keep_rhs, keep_dia, after, base, WIDE + ROWS)

    def second(b):
        at = WIDE + b * LANES
        pull = own_block(one, col, blk, base, b)
        two[:, lanes(at)] = smoothed(one, pull, keep_rhs, keep_dia, at)

    each_block(second)

    def third(b):
        at = WIDE + b * LANES
        pull = jnp.concatenate(own_block(two, col, blk, base, b), axis=0)
        s, d = two[:, lanes(at)], keep_dia[:, lanes(at)]
        res[0:3, lanes(b * LANES)] = keep_rhs[:, lanes(at)] - (d * s - pull)

    res[...] = jnp.zeros(res.shape, f32)
    each_block(third)
    first_iter[...] = two[...]
    up2[...] = two[:, lanes(WIDE + ROWS - WIDE, HALO)]
    down2[...] = two[:, lanes(WIDE + HALO, HALO)]
    label = lax.broadcasted_iota(i32, (32, LANES), 0)
    sums = None
    for b in range(BLOCKS):
        member = (label == jnp.broadcast_to(agg[b : b + 1, :], (32, LANES))).astype(f32)
        part = lax.dot_general(
            res[:, lanes(b * LANES)], member, (((1,), (1,)), ((), ())),
            precision=highest, preferred_element_type=f32,
        )
        sums = part if sums is None else sums + part
    row = jnp.concatenate(
        [sums[0:1], sums[1:2], sums[2:3], owner_row[...].astype(f32)], axis=1
    )
    send[:, 0, :] = jnp.broadcast_to(row, (LANES, LANES))
    row = jnp.concatenate(
        [cdia[0:1], cdia[1:2], cdia[2:3], jnp.ones((1, 32), f32)], axis=1
    )
    send[:, 1, :] = jnp.broadcast_to(row, (LANES, LANES))


def bit_of(p, at):
    return lax.bitwise_and(lax.shift_right_logical(p, at), 1)


def bit_parity(p, at):
    return lax.bitwise_xor(bit_of(p, at), bit_of(p, at + 1))


def lane_of_device(p, me):
    off = lax.bitwise_xor(p, me)
    rest = 4 * bit_of(p, 6) + 2 * bit_of(p, 4) + bit_of(p, 2)
    return (
        64 * bit_parity(off, 1) + 32 * bit_of(off, 0) + 16 * bit_parity(off, 5) + 8 * bit_parity(off, 3)
        + rest
    )


def device_of_lane(q, me):
    def last(relative, at, first):
        return lax.bitwise_xor(lax.bitwise_xor(relative, bit_parity(me, at)), first)

    x, z, y = bit_of(q, 0), bit_of(q, 1), bit_of(q, 2)
    p = 64 * y + 32 * last(bit_of(q, 4), 5, y) + 16 * z + 8 * last(bit_of(q, 3), 3, z)
    core = lax.bitwise_xor(bit_of(q, 5), bit_of(me, 0))
    return p + 4 * x + 2 * last(bit_of(q, 6), 1, x) + core


def row_groups():
    def member(kind, m):
        y, z, x = m >> 2, m >> 1 & 1, m & 1
        py, pz, px, core = kind >> 3, kind >> 2 & 1, kind >> 1 & 1, kind & 1
        return 64 * y + 32 * (y ^ py) + 16 * z + 8 * (z ^ pz) + 4 * x + 2 * (x ^ px) + core

    return [[member(kind, m) for m in range(NEAR)] for kind in range(16)]


def pack_coarse(col, blk, send):
    def turned(a):
        z = jnp.transpose(jnp.concatenate([a, jnp.zeros((32, 5), f32)], axis=1))
        return jnp.concatenate([z] * 4, axis=1)

    columns = turned(col[...].astype(f32))
    kind = lax.bitwise_and(columns.astype(i32), 7)
    tile = (8, LANES)
    sub = lax.broadcasted_iota(i32, tile, 0)
    count = jnp.zeros(tile, i32)
    match, earlier = [], []
    for k in range(SLOTS):
        here = sub == jnp.broadcast_to(kind[k : k + 1], tile)
        match.append(here)
        earlier.append(count)
        count = count + here.astype(i32)
    left = jnp.zeros((1, LANES), i32)
    start = []
    for n in range(16):
        if n >= 8:
            start.append(left)
        left = jnp.maximum(left + count[n % 8 : n % 8 + 1] - 4, 0)
    start = jnp.concatenate(start, axis=0) + 4 * sub
    place = 4 * sub + lax.shift_right_logical(lax.broadcasted_iota(i32, tile, 1), 5)
    slot = jnp.full(tile, 31, i32)
    for k in range(SLOTS):
        at = jnp.sum(jnp.where(match[k], start + earlier[k], 0), axis=0, keepdims=True)
        slot = jnp.where(place == jnp.broadcast_to(lax.bitwise_and(at, 31), tile), k, slot)
    inner, outer = lax.bitwise_and(slot, 7), lax.shift_right_logical(slot, 3)

    def placed(z):
        got = None
        for g in range(4):
            part = jnp.take_along_axis(
                z[8 * g : 8 * g + 8], inner, axis=0, mode="promise_in_bounds"
            )
            got = part if got is None else jnp.where(outer == g, part, got)
        return got

    parts = [placed(turned(blk[i, j])) for i in range(3) for j in range(3)]
    parts.append(jnp.where(slot == 31, sub.astype(f32), placed(columns)))
    for m in range(10):
        for d in range(NEAR):
            send[d, 8 * m : 8 * m + 8, :] = parts[m]


def spread(parts):
    group = lax.shift_right_logical(lax.broadcasted_iota(i32, parts[0].shape, 1), 5)
    return jnp.where(group == 0, parts[0], jnp.where(group == 1, parts[1], parts[2]))


def coarse_lookup(table, chunk, lane):
    near = [jnp.zeros(chunk.shape, f32) for _ in range(3)]
    for c in range(32):
        here = chunk == c
        for j in range(3):
            row = table[32 * j + c : 32 * j + c + 1, :]
            near[j] = jnp.where(here, picked(row, lane), near[j])
    return near


def coarse_step(table, where, passes, data, own, rhs, dia, gather):
    gather[...] = jnp.zeros(gather.shape, f32)

    def one_pass(t, carry):
        rows = [
            [pltpu.roll(table[32 * j + 8 * v : 32 * j + 8 * v + 8, :], t, axis=0) for v in range(4)]
            for j in range(3)
        ]
        for d in range(PEERS):
            w = where[d]
            code, lane = lax.bitwise_and(w, 31), lax.shift_right_logical(w, 5)
            near = [jnp.zeros((8, LANES), f32) for _ in range(3)]
            for v in range(4):
                here = code == 4 * t + v
                for j in range(3):
                    near[j] = jnp.where(here, picked(rows[j][v], lane), near[j])
            for i in range(3):
                a = data[d // NEAR][d % NEAR, lanes8(3 * i), :] * near[0]
                a = a + data[d // NEAR][d % NEAR, lanes8(3 * i + 1), :] * near[1]
                a = a + data[d // NEAR][d % NEAR, lanes8(3 * i + 2), :] * near[2]
                gather[i, d : d + 1, :] += jnp.sum(a, axis=0, keepdims=True)
        return carry

    lax.fori_loop(0, passes, one_pass, 0)
    parts = []
    for i in range(3):
        s = gather[i]
        s = s + pltpu.roll(s, 64, axis=1)
        parts.append(s + pltpu.roll(s, 32, axis=1))
    return own + damping * (rhs - (dia * own - spread(parts))) / dia


def lanes8(m):
    return slice(8 * m, 8 * m + 8)


def coarse_first_kernel(base_ref, sums, *rest):
    data = rest[:PARTS]
    new, rhs, dia, where, passes, table, gather, left, right = rest[PARTS:]
    me = lax.shift_right_logical(base_ref[0], 10)
    got = jnp.transpose(sums[:, 0, :])
    rows = got[96:128].astype(i32)
    s = got[0:96]
    split = []
    for _ in range(3):
        t = s.astype(jnp.bfloat16).astype(f32)
        split.append(t)
        s = s - t
    chunk = lax.broadcasted_iota(i32, (32, LANES), 0)
    place = lax.broadcasted_iota(i32, (LANES, LANES), 0)
    low = lax.bitwise_and(rows, 31)
    lane = lane_of_device(lax.shift_right_logical(rows, 5), me)
    for a in range(32):
        here = chunk == jnp.broadcast_to(low[a : a + 1], (32, LANES))
        for t in range(3):
            for i in range(3):
                value = jnp.broadcast_to(split[t][32 * i + a : 32 * i + a + 1], (32, LANES))
                left[96 * t + 32 * i : 96 * t + 32 * i + 32, lanes(LANES * a)] = jnp.where(
                    here, value, 0.0
                ).astype(jnp.bfloat16)
        right[:, lanes(LANES * a)] = jnp.where(
            place == jnp.broadcast_to(lane[a : a + 1], (LANES, LANES)), 1.0, 0.0
        ).astype(jnp.bfloat16)
    both = lax.dot_general(
        left[...], right[...], (((1,), (1,)), ((), ())), preferred_element_type=f32
    )
    crhs = both[0:96] + both[96:192] + both[192:288]
    order = device_of_lane(lax.broadcasted_iota(i32, (96, LANES), 1), me)
    cdia = jnp.take_along_axis(
        jnp.transpose(sums[:, 1, :])[0:96], order, axis=1, mode="promise_in_bounds"
    )
    pad = jnp.zeros((32, LANES), f32)
    first = jnp.concatenate([damping * crhs / cdia, pad], axis=0)
    table[...] = first
    own = jnp.transpose(first)[0:PEERS]
    rhs[...] = jnp.transpose(jnp.concatenate([crhs, pad], axis=0))[0:PEERS]
    dia[...] = jnp.transpose(jnp.concatenate([cdia, pad + 1.0], axis=0))[0:PEERS]
    sub = lax.broadcasted_iota(i32, (8, LANES), 0)
    most = jnp.zeros((8, LANES), i32)
    for d in range(PEERS):
        c = data[d // NEAR][d % NEAR, 72:80, :].astype(i32)
        off = lax.bitwise_and(sub - c, 7)
        most = jnp.maximum(most, off)
        at = lane_of_device(lax.shift_right_logical(c, 5), me)
        code = lax.bitwise_and(lax.shift_right_logical(c, 3), 3) + lax.shift_left(off, 2)
        where[d] = code + lax.shift_left(at, 5)
    most = jnp.max(most.astype(f32)).astype(i32) + 1
    passes[...] = jnp.broadcast_to(most, passes.shape)
    new[...] = coarse_step(
        table, where, most, data, own, rhs[...], dia[...], gather
    )


def gathered(table, pieces, mine):
    row = 0
    for piece in pieces:
        size = piece.shape[0]
        mine[row : row + size, :] = piece[...]
        row += size
    table[...] = jnp.transpose(mine[...])


def coarse_kernel(base_ref, passes, *rest):
    pieces, (rhs, dia, where) = rest[:PIECES], rest[PIECES : PIECES + 3]
    data = rest[PIECES + 3 : PIECES + 3 + PARTS]
    new, table, mine, gather = rest[PIECES + 3 + PARTS :]
    gathered(table, pieces, mine)
    new[...] = coarse_step(
        table, where, passes[...][0, 0], data, pieces[0][...], rhs[...], dia[...], gather
    )


def post_kernel(base_ref, *rest):
    pieces = rest[:PIECES]
    (first_iter, rhs, dia, col, blk, node_row, before, after, before2, after2,
     out, correction, table, mine, one, two) = rest[PIECES:]
    base = base_ref[0]
    me = lax.shift_right_logical(base, 10)
    gathered(table, pieces, mine)
    row = mine[pl.ds(lane_of_device(me, me), 1), :]
    correction[...] = jnp.concatenate([row[:, 32 * i : 32 * i + 32] for i in range(3)], axis=0)
    one[...] = first_iter[...]
    one[:, lanes(0, HALO)] = before2[...]
    one[:, lanes(WIDE + ROWS + HALO, HALO)] = after2[...]
    edge = [
        h[P_ROW + t : P_ROW + t + 1, lanes(LANES * q)]
        for h in (before, after) for t in range(2) for q in range(2)
    ]
    edge = jnp.concatenate(edge, axis=0)

    def found(rows):
        rows = rows.astype(i32)
        lane = lane_of_device(lax.shift_right_logical(rows, 5), me)
        return coarse_lookup(table, lax.bitwise_and(rows, 31), lane)

    own, far = found(node_row[...]), found(edge)
    for s in range(16):
        if s < 4:
            row = [f[s : s + 1, :] for f in far]
        elif s < 12:
            row = [f[s - 4 : s - 3, :] for f in own]
        else:
            row = [f[s - 8 : s - 7, :] for f in far]
        one[:, lanes(s * LANES)] = one[:, lanes(s * LANES)] + jnp.concatenate(row, axis=0)
    two[...] = jnp.zeros(two.shape, f32)
    sweep_halo(two, one, rhs, dia, before, base, WIDE - HALO)
    sweep_halo(two, one, rhs, dia, after, base, WIDE + ROWS)

    def first(b):
        at = WIDE + b * LANES
        pull = own_block(one, col, blk, base, b)
        two[:, lanes(at)] = smoothed(one, pull, rhs, dia, at)

    def second(b):
        at = WIDE + b * LANES
        pull = own_block(two, col, blk, base, b)
        out[:, lanes(b * LANES)] = smoothed(two, pull, rhs, dia, at)

    each_block(first)
    each_block(second)


def call(kernel, outs, args, scratch=(), scalars=0, limit=12):
    vmem = pl.BlockSpec(memory_space=pltpu.VMEM)
    smem = pl.BlockSpec(memory_space=pltpu.SMEM)
    return pl.pallas_call(
        kernel,
        in_specs=[smem] * scalars + [vmem] * (len(args) - scalars),
        out_specs=[vmem] * len(outs),
        out_shape=[jax.ShapeDtypeStruct(o, t) for o, t in outs],
        scratch_shapes=[
            pltpu.VMEM(*s) if isinstance(s[0], tuple) else pltpu.VMEM(s, f32) for s in scratch
        ],
        compiler_params=pltpu.CompilerParams(vmem_limit_bytes=limit * 2**20),
    )(*args)


def partner(value, bits):
    return lax.ppermute(value, DOM, [(i, i ^ bits) for i in range(lax.axis_size(DOM))])


def in_group(new):
    p2, p3, p1 = partner(new, 2), partner(new, 3), partner(new, 1)
    return new, p1, p2, p3


def shifts(up, down):
    count = lax.axis_size(DOM)
    forward = [(i, i + 1) for i in range(count - 1)]
    backward = [(i + 1, i) for i in range(count - 1)]
    return lax.ppermute(up, DOM, forward), lax.ppermute(down, DOM, backward)


def cycle(right_side, fine_diagonal, fine_columns, fine_blocks, aggregate_of_node,
         coarse_row_of_aggregate, coarse_diagonal, coarse_columns, coarse_blocks):
    rhs, dia = right_side.T, fine_diagonal.T
    col, blk = fine_columns.T, fine_blocks.transpose(2, 3, 1, 0)
    agg = aggregate_of_node.reshape(8, LANES)
    owner = coarse_row_of_aggregate.reshape(1, 32)
    cdia, cblk = coarse_diagonal.T, coarse_blocks.transpose(2, 3, 0, 1)
    me = lax.axis_index(DOM).astype(i32).reshape(1)
    base = me * ROWS
    wide = WIDE + ROWS + WIDE

    vmem, far = pl.BlockSpec(memory_space=pltpu.VMEM), pl.BlockSpec(memory_space=pltpu.HBM)
    up, down, node_row, dsend = pl.pallas_call(
        pack_kernel,
        name="pack",
        in_specs=[far] * 8,
        out_specs=[vmem] * 4,
        out_shape=[jax.ShapeDtypeStruct(o, f32)
            for o in ((P_ALL, HALO), (P_ALL, HALO), (8, LANES), (NEAR, 80, LANES))],
        scratch_shapes=[
            pltpu.VMEM((3, ROWS), f32), pltpu.VMEM((3, ROWS), f32),
            pltpu.VMEM((2, SLOTS, HALO), i32), pltpu.VMEM((2, 3, 3, SLOTS, HALO), f32),
            pltpu.VMEM((8, LANES), i32), pltpu.VMEM((1, 32), i32),
            pltpu.VMEM((32, SLOTS), i32), pltpu.VMEM((3, 3, 32, SLOTS), f32),
            pltpu.SemaphoreType.DMA((10,)),
        ],
        compiler_params=pltpu.CompilerParams(vmem_limit_bytes=60 * 2**20),
    )(rhs, dia, col, blk, agg, owner, coarse_columns, cblk)
    data = lax.all_to_all(
        dsend, DOM, 0, 0, axis_index_groups=row_groups(), tiled=True
    )
    along_z, along_y = partner(data, 8), partner(data, 32)
    data = (data, along_z, along_y, partner(along_z, 32))
    before, after = shifts(up, down)
    send, first_iter, wrhs, wdia, up2, down2 = call(
        pre_kernel,
        [((LANES, 2, LANES), f32), ((3, wide), f32), ((3, wide), f32), ((3, wide), f32),
         ((3, HALO), f32), ((3, HALO), f32)],
        [base, rhs, dia, col, blk, agg, owner, cdia, before, after],
        scratch=[(3, wide), (3, wide), (8, ROWS)], scalars=1, limit=4,
    )
    before2, after2 = shifts(up2, down2)
    sums = lax.all_to_all(send, DOM, 0, 0, tiled=True)
    peers = ((PEERS, LANES), f32)
    gather = (3, PEERS, LANES)
    square = (LANES, LANES)
    new, crhs, cd, where, passes = call(
        coarse_first_kernel,
        [peers, peers, peers, ((PEERS, 8, LANES), i32), ((8, LANES), i32)],
        [base, sums, *data],
        scratch=[square, gather, ((288, 4096), jnp.bfloat16), ((LANES, 4096), jnp.bfloat16)],
        scalars=1,
    )
    for _ in range(CSWEEPS - 2):
        new, = call(
            coarse_kernel, [peers],
            [base, passes, *in_group(new), crhs, cd, where, *data],
            scratch=[square, square, gather], scalars=1,
        )
    solution, mine = call(
        post_kernel, [((3, ROWS), f32), ((3, 32), f32)],
        [base, *in_group(new), first_iter, wrhs, wdia, col, blk, node_row,
         before, after, before2, after2],
        scratch=[square, square, (3, wide), (3, wide)], scalars=1,
    )
    return solution.T, mine.T


def solution(mesh):
    return jax.shard_map(
        cycle,
        mesh=mesh,
        in_specs=(
            P(DOM, None),
            P(DOM, None),
            P(DOM, None),
            P(DOM, None, None, None),
            P(DOM),
            P(DOM),
            P(DOM, None),
            P(DOM, None),
            P(DOM, None, None, None),
        ),
        out_specs=(P(DOM, None), P(DOM, None)),
        check_vma=False,
    )
```

```python
import jax
import jax.numpy as jnp
from jax import lax
from jax.experimental import pallas as pl
from jax.experimental.pallas import tpu as pltpu
from jax.sharding import PartitionSpec as P


DOM = "dom"
PEERS = 32
NEAR = 8
PARTS = 5
PIECES = 128 // PEERS
UNROLL = 8
CSWEEPS = 6
damping = 0.7
highest = lax.Precision.HIGHEST

ROWS = 1024
LANES = 128
SLOTS = 27
FULL = 24
HALO = 256
WIDE = 512
BLOCKS = ROWS // LANES
P_COL = 9 * FULL
P_BTAIL = P_COL + FULL
P_CTAIL = P_BTAIL + 27
P_RHS = P_CTAIL + 3
P_DIA = P_RHS + 6
P_ROW = P_DIA + 6
P_ALL = 288
f32 = jnp.float32
i32 = jnp.int32


def lanes(start, size=LANES):
    if isinstance(start, int):
        return slice(start, start + size)
    return pl.ds(pl.multiple_of(start, LANES), size)


def picked(row, where):
    return jnp.take_along_axis(
        jnp.broadcast_to(row, where.shape), where, axis=1, mode="promise_in_bounds"
    )


def pack_kernel(rhs_in, dia_in, col_in, blk_in, agg_in, owner_in, ccol_in, cblk_in,
                up, down, node_row, send, rhs, dia, col, blk, agg, owner, ccol, cblk, sem):
    copies = [(ccol_in, ccol), (cblk_in, cblk)]
    copies += [(rhs_in, rhs), (dia_in, dia), (agg_in, agg), (owner_in, owner)]
    for t, near in enumerate((ROWS - HALO, 0)):
        copies.append((col_in.at[:, lanes(near, HALO)], col.at[t]))
        copies.append((blk_in.at[:, :, :, lanes(near, HALO)], blk.at[t]))
    copies = [pltpu.make_async_copy(a, b, sem.at[n]) for n, (a, b) in enumerate(copies)]
    for c in copies:
        c.start()
    for c in copies[:2]:
        c.wait()
    pack_coarse(ccol, cblk, send)
    for c in copies[2:]:
        c.wait()
    table = jnp.concatenate([owner[...]] * 4, axis=1)
    found = picked(table, agg[...]).astype(f32)
    node_row[...] = found
    for t, (out, wide) in enumerate(((up, ROWS - WIDE), (down, 0))):
        for i in range(3):
            for j in range(3):
                g = 3 * i + j
                out[g * FULL : (g + 1) * FULL, :] = blk[t, i, j, 0:FULL, :]
                out[P_BTAIL + 3 * g : P_BTAIL + 3 * g + 3, :] = blk[t, i, j, FULL:SLOTS, :]
        out[P_COL : P_COL + FULL, :] = col[t, 0:FULL, :].astype(f32)
        out[P_CTAIL : P_CTAIL + 3, :] = col[t, FULL:SLOTS, :].astype(f32)
        for h in range(2):
            out[P_RHS + 3 * h : P_RHS + 3 * h + 3, :] = rhs[:, lanes(wide + HALO * h, HALO)]
            out[P_DIA + 3 * h : P_DIA + 3 * h + 3, :] = dia[:, lanes(wide + HALO * h, HALO)]
            for q in range(2):
                s = wide // LANES + 2 * h + q
                out[P_ROW + h : P_ROW + h + 1, lanes(LANES * q)] = found[s : s + 1, :]
        out[P_ROW + 2 : P_ALL, :] = jnp.zeros((P_ALL - P_ROW - 2, HALO), f32)


def pulled_block(columns, blocks, table, first_chunk):
    total = [None, None, None]
    for part in range(4):
        where = columns(part)
        chunk = lax.shift_right_arithmetic(where, 7)
        lane = lax.bitwise_and(where, 127)
        near = [jnp.zeros(where.shape, f32) for _ in range(3)]
        for c in range(5):
            here = chunk == c
            for j in range(3):
                row = table[j : j + 1, lanes(first_chunk * LANES + c * LANES)]
                near[j] = jnp.where(here, picked(row, lane), near[j])
        for i in range(3):
            s = blocks(i, 0, part) * near[0]
            s = s + blocks(i, 1, part) * near[1]
            s = s + blocks(i, 2, part) * near[2]
            if part < 3:
                total[i] = s if total[i] is None else total[i] + s
            else:
                total[i] = jnp.sum(total[i], axis=0, keepdims=True) + jnp.sum(
                    s, axis=0, keepdims=True
                )
    return total


def local_getters(col, blk, start, b):
    def columns(part):
        lo, hi = 8 * part, min(8 * part + 8, SLOTS)
        return col[lo:hi, lanes(b * LANES)] - start

    def blocks(i, j, part):
        lo, hi = 8 * part, min(8 * part + 8, SLOTS)
        return blk[i, j, lo:hi, lanes(b * LANES)]

    return columns, blocks


def halo_getters(halo, start, b):
    def columns(part):
        if part < 3:
            got = halo[P_COL + 8 * part : P_COL + 8 * part + 8, lanes(b * LANES)]
        else:
            got = halo[P_CTAIL : P_CTAIL + 3, lanes(b * LANES)]
        return got.astype(i32) - start

    def blocks(i, j, part):
        g = 3 * i + j
        if part < 3:
            return halo[g * FULL + 8 * part : g * FULL + 8 * part + 8, lanes(b * LANES)]
        return halo[P_BTAIL + 3 * g : P_BTAIL + 3 * g + 3, lanes(b * LANES)]

    return columns, blocks


def wide_vector(out, local, before, after, row):
    out[:, lanes(WIDE, ROWS)] = local[...]
    for h in range(2):
        out[:, lanes(HALO * h, HALO)] = before[row + 3 * h : row + 3 * h + 3, :]
        out[:, lanes(WIDE + ROWS + HALO * h, HALO)] = after[row + 3 * h : row + 3 * h + 3, :]


def smoothed(table, pulled, rhs, dia, at):
    pull = jnp.concatenate(pulled, axis=0)
    s = table[:, lanes(at)]
    b = rhs[:, lanes(at)]
    d = dia[:, lanes(at)]
    return s + damping * (b - (d * s - pull)) / d


def sweep_halo(out, table, rhs, dia, halo, base, first):
    for b in range(2):
        at = first + LANES * b
        start = base + (at - WIDE) - 2 * LANES
        cols, blks = halo_getters(halo, start, b)
        pull = pulled_block(cols, blks, table, at // LANES - 2)
        out[:, lanes(at)] = smoothed(table, pull, rhs, dia, at)


def each_block(step):
    def some(t, carry):
        for u in range(UNROLL):
            step(t * UNROLL + u)
        return carry

    lax.fori_loop(0, BLOCKS // UNROLL, some, 0)


def own_block(table, col, blk, base, b):
    start = base + b * LANES - 2 * LANES
    cols, blks = local_getters(col, blk, start, b)
    return pulled_block(cols, blks, table, b + WIDE // LANES - 2)


def pre_kernel(base_ref, rhs, dia, col, blk, agg, owner_row, cdia, before, after,
               send, first_iter, keep_rhs, keep_dia, up2, down2, one, two, res):
    base = base_ref[0]
    wide_vector(keep_rhs, rhs, before, after, P_RHS)
    wide_vector(keep_dia, dia, before, after, P_DIA)
    raw = keep_dia[...]
    keep_dia[...] = jnp.where(raw == 0.0, 1.0, raw)
    one[...] = damping * keep_rhs[...] / keep_dia[...]
    two[...] = jnp.zeros(two.shape, f32)
    sweep_halo(two, one, keep_rhs, keep_dia, before, base, WIDE - HALO)
    sweep_halo(two, one, keep_rhs, keep_dia, after, base, WIDE + ROWS)

    def second(b):
        at = WIDE + b * LANES
        pull = own_block(one, col, blk, base, b)
        two[:, lanes(at)] = smoothed(one, pull, keep_rhs, keep_dia, at)

    each_block(second)

    def third(b):
        at = WIDE + b * LANES
        pull = jnp.concatenate(own_block(two, col, blk, base, b), axis=0)
        s, d = two[:, lanes(at)], keep_dia[:, lanes(at)]
        res[0:3, lanes(b * LANES)] = keep_rhs[:, lanes(at)] - (d * s - pull)

    res[...] = jnp.zeros(res.shape, f32)
    each_block(third)
    first_iter[...] = two[...]
    up2[...] = two[:, lanes(WIDE + ROWS - WIDE, HALO)]
    down2[...] = two[:, lanes(WIDE + HALO, HALO)]
    label = lax.broadcasted_iota(i32, (32, LANES), 0)
    sums = None
    for b in range(BLOCKS):
        member = (label == jnp.broadcast_to(agg[b : b + 1, :], (32, LANES))).astype(f32)
        part = lax.dot_general(
            res[:, lanes(b * LANES)], member, (((1,), (1,)), ((), ())),
            precision=highest, preferred_element_type=f32,
        )
        sums = part if sums is None else sums + part
    row = jnp.concatenate(
        [sums[0:1], sums[1:2], sums[2:3], owner_row[...].astype(f32)], axis=1
    )
    send[:, 0, :] = jnp.broadcast_to(row, (LANES, LANES))
    row = jnp.concatenate(
        [cdia[0:1], cdia[1:2], cdia[2:3], jnp.ones((1, 32), f32)], axis=1
    )
    send[:, 1, :] = jnp.broadcast_to(row, (LANES, LANES))


def bit_of(p, at):
    return lax.bitwise_and(lax.shift_right_logical(p, at), 1)


def bit_parity(p, at):
    return lax.bitwise_xor(bit_of(p, at), bit_of(p, at + 1))


def lane_of_device(p, me):
    off = lax.bitwise_xor(p, me)
    rest = 4 * bit_of(p, 6) + 2 * bit_of(p, 4) + bit_of(p, 2)
    return (
        64 * bit_parity(off, 1) + 32 * bit_of(off, 0) + 16 * bit_parity(off, 5) + 8 * bit_parity(off, 3)
        + rest
    )


def device_of_lane(q, me):
    def last(relative, at, first):
        return lax.bitwise_xor(lax.bitwise_xor(relative, bit_parity(me, at)), first)

    x, z, y = bit_of(q, 0), bit_of(q, 1), bit_of(q, 2)
    p = 64 * y + 32 * last(bit_of(q, 4), 5, y) + 16 * z + 8 * last(bit_of(q, 3), 3, z)
    core = lax.bitwise_xor(bit_of(q, 5), bit_of(me, 0))
    return p + 4 * x + 2 * last(bit_of(q, 6), 1, x) + core


def row_groups():
    def member(kind, m):
        y, z, x = m >> 2, m >> 1 & 1, m & 1
        py, pz, px, core = kind >> 3, kind >> 2 & 1, kind >> 1 & 1, kind & 1
        return 64 * y + 32 * (y ^ py) + 16 * z + 8 * (z ^ pz) + 4 * x + 2 * (x ^ px) + core

    return [[member(kind, m) for m in range(NEAR)] for kind in range(16)]


def pack_coarse(col, blk, send):
    def turned(a):
        z = jnp.transpose(jnp.concatenate([a, jnp.zeros((32, 5), f32)], axis=1))
        return jnp.concatenate([z] * 4, axis=1)

    columns = turned(col[...].astype(f32))
    kind = lax.bitwise_and(columns.astype(i32), 7)
    tile = (8, LANES)
    sub = lax.broadcasted_iota(i32, tile, 0)
    count = jnp.zeros(tile, i32)
    match, earlier = [], []
    for k in range(SLOTS):
        here = sub == jnp.broadcast_to(kind[k : k + 1], tile)
        match.append(here)
        earlier.append(count)
        count = count + here.astype(i32)
    left = jnp.zeros((1, LANES), i32)
    start = []
    for n in range(16):
        if n >= 8:
            start.append(left)
        left = jnp.maximum(left + count[n % 8 : n % 8 + 1] - 4, 0)
    start = jnp.concatenate(start, axis=0) + 4 * sub
    place = 4 * sub + lax.shift_right_logical(lax.broadcasted_iota(i32, tile, 1), 5)
    slot = jnp.full(tile, 31, i32)
    for k in range(SLOTS):
        at = jnp.sum(jnp.where(match[k], start + earlier[k], 0), axis=0, keepdims=True)
        slot = jnp.where(place == jnp.broadcast_to(lax.bitwise_and(at, 31), tile), k, slot)
    inner, outer = lax.bitwise_and(slot, 7), lax.shift_right_logical(slot, 3)

    def placed(z):
        got = None
        for g in range(4):
            part = jnp.take_along_axis(
                z[8 * g : 8 * g + 8], inner, axis=0, mode="promise_in_bounds"
            )
            got = part if got is None else jnp.where(outer == g, part, got)
        return got

    parts = [placed(turned(blk[i, j])) for i in range(3) for j in range(3)]
    parts.append(jnp.where(slot == 31, sub.astype(f32), placed(columns)))
    for m in range(10):
        for d in range(NEAR):
            send[d, 8 * m : 8 * m + 8, :] = parts[m]


def spread(parts):
    group = lax.shift_right_logical(lax.broadcasted_iota(i32, parts[0].shape, 1), 5)
    return jnp.where(group == 0, parts[0], jnp.where(group == 1, parts[1], parts[2]))


def coarse_lookup(table, chunk, lane):
    near = [jnp.zeros(chunk.shape, f32) for _ in range(3)]
    for c in range(32):
        here = chunk == c
        for j in range(3):
            row = table[32 * j + c : 32 * j + c + 1, :]
            near[j] = jnp.where(here, picked(row, lane), near[j])
    return near


def coarse_step(table, where, passes, data, own, rhs, dia, gather):
    gather[...] = jnp.zeros(gather.shape, f32)

    def one_pass(t, carry):
        rows = [
            [pltpu.roll(table[32 * j + 8 * v : 32 * j + 8 * v + 8, :], t, axis=0) for v in range(4)]
            for j in range(3)
        ]
        for d in range(PEERS):
            w = where[d]
            code, lane = lax.bitwise_and(w, 31), lax.shift_right_logical(w, 5)
            near = [jnp.zeros((8, LANES), f32) for _ in range(3)]
            for v in range(4):
                here = code == 4 * t + v
                for j in range(3):
                    near[j] = jnp.where(here, picked(rows[j][v], lane), near[j])
            for i in range(3):
                a = rows_of(data, d)[lanes8(3 * i), :] * near[0]
                a = a + rows_of(data, d)[lanes8(3 * i + 1), :] * near[1]
                a = a + rows_of(data, d)[lanes8(3 * i + 2), :] * near[2]
                gather[i, d : d + 1, :] += jnp.sum(a, axis=0, keepdims=True)
        return carry

    lax.fori_loop(0, passes, one_pass, 0)
    parts = []
    for i in range(3):
        s = gather[i]
        s = s + pltpu.roll(s, 64, axis=1)
        parts.append(s + pltpu.roll(s, 32, axis=1))
    return own + damping * (rhs - (dia * own - spread(parts))) / dia


def rows_of(data, d):
    part, at = (d // NEAR, d % NEAR) if d < 24 else (3 + (d - 24) // 4, d % 4)
    return data[part].at[at]


def lanes8(m):
    return slice(8 * m, 8 * m + 8)


def coarse_first_kernel(base_ref, sums, *rest):
    data = rest[:PARTS]
    new, rhs, dia, where, passes, table, gather, left, right = rest[PARTS:]
    me = lax.shift_right_logical(base_ref[0], 10)
    got = jnp.transpose(sums[:, 0, :])
    rows = got[96:128].astype(i32)
    s = got[0:96]
    split = []
    for _ in range(3):
        t = s.astype(jnp.bfloat16).astype(f32)
        split.append(t)
        s = s - t
    chunk = lax.broadcasted_iota(i32, (32, LANES), 0)
    place = lax.broadcasted_iota(i32, (LANES, LANES), 0)
    low = lax.bitwise_and(rows, 31)
    lane = lane_of_device(lax.shift_right_logical(rows, 5), me)
    for a in range(32):
        here = chunk == jnp.broadcast_to(low[a : a + 1], (32, LANES))
        for t in range(3):
            for i in range(3):
                value = jnp.broadcast_to(split[t][32 * i + a : 32 * i + a + 1], (32, LANES))
                left[96 * t + 32 * i : 96 * t + 32 * i + 32, lanes(LANES * a)] = jnp.where(
                    here, value, 0.0
                ).astype(jnp.bfloat16)
        right[:, lanes(LANES * a)] = jnp.where(
            place == jnp.broadcast_to(lane[a : a + 1], (LANES, LANES)), 1.0, 0.0
        ).astype(jnp.bfloat16)
    both = lax.dot_general(
        left[...], right[...], (((1,), (1,)), ((), ())), preferred_element_type=f32
    )
    crhs = both[0:96] + both[96:192] + both[192:288]
    order = device_of_lane(lax.broadcasted_iota(i32, (96, LANES), 1), me)
    cdia = jnp.take_along_axis(
        jnp.transpose(sums[:, 1, :])[0:96], order, axis=1, mode="promise_in_bounds"
    )
    pad = jnp.zeros((32, LANES), f32)
    first = jnp.concatenate([damping * crhs / cdia, pad], axis=0)
    table[...] = first
    own = jnp.transpose(first)[0:PEERS]
    rhs[...] = jnp.transpose(jnp.concatenate([crhs, pad], axis=0))[0:PEERS]
    dia[...] = jnp.transpose(jnp.concatenate([cdia, pad + 1.0], axis=0))[0:PEERS]
    sub = lax.broadcasted_iota(i32, (8, LANES), 0)
    most = jnp.zeros((8, LANES), i32)
    for d in range(PEERS):
        c = rows_of(data, d)[72:80, :].astype(i32)
        off = lax.bitwise_and(sub - c, 7)
        most = jnp.maximum(most, off)
        at = lane_of_device(lax.shift_right_logical(c, 5), me)
        code = lax.bitwise_and(lax.shift_right_logical(c, 3), 3) + lax.shift_left(off, 2)
        where[d] = code + lax.shift_left(at, 5)
    most = jnp.max(most.astype(f32)).astype(i32) + 1
    passes[...] = jnp.broadcast_to(most, passes.shape)
    new[...] = coarse_step(
        table, where, most, data, own, rhs[...], dia[...], gather
    )


def gathered(table, pieces, mine):
    row = 0
    for piece in pieces:
        size = piece.shape[0]
        mine[row : row + size, :] = piece[...]
        row += size
    table[...] = jnp.transpose(mine[...])


def coarse_kernel(base_ref, passes, *rest):
    pieces, (rhs, dia, where) = rest[:PIECES], rest[PIECES : PIECES + 3]
    data = rest[PIECES + 3 : PIECES + 3 + PARTS]
    new, table, mine, gather = rest[PIECES + 3 + PARTS :]
    gathered(table, pieces, mine)
    new[...] = coarse_step(
        table, where, passes[...][0, 0], data, pieces[0][...], rhs[...], dia[...], gather
    )


def post_kernel(base_ref, *rest):
    pieces = rest[:PIECES]
    (first_iter, rhs, dia, col, blk, node_row, before, after, before2, after2,
     out, correction, table, mine, one, two) = rest[PIECES:]
    base = base_ref[0]
    me = lax.shift_right_logical(base, 10)
    gathered(table, pieces, mine)
    row = mine[pl.ds(lane_of_device(me, me), 1), :]
    correction[...] = jnp.concatenate([row[:, 32 * i : 32 * i + 32] for i in range(3)], axis=0)
    one[...] = first_iter[...]
    one[:, lanes(0, HALO)] = before2[...]
    one[:, lanes(WIDE + ROWS + HALO, HALO)] = after2[...]
    edge = [
        h[P_ROW + t : P_ROW + t + 1, lanes(LANES * q)]
        for h in (before, after) for t in range(2) for q in range(2)
    ]
    edge = jnp.concatenate(edge, axis=0)

    def found(rows):
        rows = rows.astype(i32)
        lane = lane_of_device(lax.shift_right_logical(rows, 5), me)
        return coarse_lookup(table, lax.bitwise_and(rows, 31), lane)

    own, far = found(node_row[...]), found(edge)
    for s in range(16):
        if s < 4:
            row = [f[s : s + 1, :] for f in far]
        elif s < 12:
            row = [f[s - 4 : s - 3, :] for f in own]
        else:
            row = [f[s - 8 : s - 7, :] for f in far]
        one[:, lanes(s * LANES)] = one[:, lanes(s * LANES)] + jnp.concatenate(row, axis=0)
    two[...] = jnp.zeros(two.shape, f32)
    sweep_halo(two, one, rhs, dia, before, base, WIDE - HALO)
    sweep_halo(two, one, rhs, dia, after, base, WIDE + ROWS)

    def first(b):
        at = WIDE + b * LANES
        pull = own_block(one, col, blk, base, b)
        two[:, lanes(at)] = smoothed(one, pull, rhs, dia, at)

    def second(b):
        at = WIDE + b * LANES
        pull = own_block(two, col, blk, base, b)
        out[:, lanes(b * LANES)] = smoothed(two, pull, rhs, dia, at)

    each_block(first)
    each_block(second)


def call(kernel, outs, args, scratch=(), scalars=0, limit=12):
    vmem = pl.BlockSpec(memory_space=pltpu.VMEM)
    smem = pl.BlockSpec(memory_space=pltpu.SMEM)
    return pl.pallas_call(
        kernel,
        in_specs=[smem] * scalars + [vmem] * (len(args) - scalars),
        out_specs=[vmem] * len(outs),
        out_shape=[jax.ShapeDtypeStruct(o, t) for o, t in outs],
        scratch_shapes=[
            pltpu.VMEM(*s) if isinstance(s[0], tuple) else pltpu.VMEM(s, f32) for s in scratch
        ],
        compiler_params=pltpu.CompilerParams(vmem_limit_bytes=limit * 2**20),
    )(*args)


def partner(value, bits):
    return lax.ppermute(value, DOM, [(i, i ^ bits) for i in range(lax.axis_size(DOM))])


def in_group(new):
    p2, p3, p1 = partner(new, 2), partner(new, 3), partner(new, 1)
    return new, p1, p2, p3


def shifts(up, down):
    count = lax.axis_size(DOM)
    forward = [(i, i + 1) for i in range(count - 1)]
    backward = [(i + 1, i) for i in range(count - 1)]
    return lax.ppermute(up, DOM, forward), lax.ppermute(down, DOM, backward)


def cycle(right_side, fine_diagonal, fine_columns, fine_blocks, aggregate_of_node,
         coarse_row_of_aggregate, coarse_diagonal, coarse_columns, coarse_blocks):
    rhs, dia = right_side.T, fine_diagonal.T
    col, blk = fine_columns.T, fine_blocks.transpose(2, 3, 1, 0)
    agg = aggregate_of_node.reshape(8, LANES)
    owner = coarse_row_of_aggregate.reshape(1, 32)
    cdia, cblk = coarse_diagonal.T, coarse_blocks.transpose(2, 3, 0, 1)
    me = lax.axis_index(DOM).astype(i32).reshape(1)
    base = me * ROWS
    wide = WIDE + ROWS + WIDE

    vmem, far = pl.BlockSpec(memory_space=pltpu.VMEM), pl.BlockSpec(memory_space=pltpu.HBM)
    up, down, node_row, dsend = pl.pallas_call(
        pack_kernel,
        name="pack",
        in_specs=[far] * 8,
        out_specs=[vmem] * 4,
        out_shape=[jax.ShapeDtypeStruct(o, f32)
            for o in ((P_ALL, HALO), (P_ALL, HALO), (8, LANES), (NEAR, 80, LANES))],
        scratch_shapes=[
            pltpu.VMEM((3, ROWS), f32), pltpu.VMEM((3, ROWS), f32),
            pltpu.VMEM((2, SLOTS, HALO), i32), pltpu.VMEM((2, 3, 3, SLOTS, HALO), f32),
            pltpu.VMEM((8, LANES), i32), pltpu.VMEM((1, 32), i32),
            pltpu.VMEM((32, SLOTS), i32), pltpu.VMEM((3, 3, 32, SLOTS), f32),
            pltpu.SemaphoreType.DMA((10,)),
        ],
        compiler_params=pltpu.CompilerParams(vmem_limit_bytes=60 * 2**20),
    )(rhs, dia, col, blk, agg, owner, coarse_columns, cblk)
    data = lax.all_to_all(
        dsend, DOM, 0, 0, axis_index_groups=row_groups(), tiled=True
    )
    along_z, along_y = partner(data, 8), partner(data, 32)
    far_y, far_z = partner(along_z[:4], 32), partner(along_y[4:], 8)
    data = (data, along_z, along_y, far_y, far_z)
    before, after = shifts(up, down)
    send, first_iter, wrhs, wdia, up2, down2 = call(
        pre_kernel,
        [((LANES, 2, LANES), f32), ((3, wide), f32), ((3, wide), f32), ((3, wide), f32),
         ((3, HALO), f32), ((3, HALO), f32)],
        [base, rhs, dia, col, blk, agg, owner, cdia, before, after],
        scratch=[(3, wide), (3, wide), (8, ROWS)], scalars=1, limit=4,
    )
    before2, after2 = shifts(up2, down2)
    sums = lax.all_to_all(send, DOM, 0, 0, tiled=True)
    peers = ((PEERS, LANES), f32)
    gather = (3, PEERS, LANES)
    square = (LANES, LANES)
    new, crhs, cd, where, passes = call(
        coarse_first_kernel,
        [peers, peers, peers, ((PEERS, 8, LANES), i32), ((8, LANES), i32)],
        [base, sums, *data],
        scratch=[square, gather, ((288, 4096), jnp.bfloat16), ((LANES, 4096), jnp.bfloat16)],
        scalars=1,
    )
    for _ in range(CSWEEPS - 2):
        new, = call(
            coarse_kernel, [peers],
            [base, passes, *in_group(new), crhs, cd, where, *data],
            scratch=[square, square, gather], scalars=1,
        )
    solution, mine = call(
        post_kernel, [((3, ROWS), f32), ((3, 32), f32)],
        [base, *in_group(new), first_iter, wrhs, wdia, col, blk, node_row,
         before, after, before2, after2],
        scratch=[square, square, (3, wide), (3, wide)], scalars=1,
    )
    return solution.T, mine.T


def solution(mesh):
    return jax.shard_map(
        cycle,
        mesh=mesh,
        in_specs=(
            P(DOM, None),
            P(DOM, None),
            P(DOM, None),
            P(DOM, None, None, None),
            P(DOM),
            P(DOM),
            P(DOM, None),
            P(DOM, None),
            P(DOM, None, None, None),
        ),
        out_specs=(P(DOM, None), P(DOM, None)),
        check_vma=False,
    )
```

```python
import jax
import jax.numpy as jnp
from jax import lax
from jax.experimental import pallas as pl
from jax.experimental.pallas import tpu as pltpu
from jax.sharding import PartitionSpec as P


DOM = "dom"
PEERS = 32
NEAR = 8
PARTS = PEERS // NEAR
PIECES = 128 // PEERS
UNROLL = 8
CSWEEPS = 6
damping = 0.7
highest = lax.Precision.HIGHEST

ROWS = 1024
LANES = 128
SLOTS = 27
FULL = 24
HALO = 256
WIDE = 512
BLOCKS = ROWS // LANES
P_COL = 9 * FULL
P_BTAIL = P_COL + FULL
P_CTAIL = P_BTAIL + 27
P_RHS = P_CTAIL + 3
P_DIA = P_RHS + 6
P_ROW = P_DIA + 6
P_ALL = 288
f32 = jnp.float32
i32 = jnp.int32


def lanes(start, size=LANES):
    if isinstance(start, int):
        return slice(start, start + size)
    return pl.ds(pl.multiple_of(start, LANES), size)


def picked(row, where):
    return jnp.take_along_axis(
        jnp.broadcast_to(row, where.shape), where, axis=1, mode="promise_in_bounds"
    )


def pack_kernel(rhs_in, dia_in, col_in, blk_in, agg_in, owner_in, ccol_in, cblk_in,
                up, down, node_row, send, rhs, dia, col, blk, agg, owner, ccol, cblk, sem):
    copies = [(ccol_in, ccol), (cblk_in, cblk)]
    copies += [(rhs_in, rhs), (dia_in, dia), (agg_in, agg), (owner_in, owner)]
    for t, near in enumerate((ROWS - HALO, 0)):
        copies.append((col_in.at[:, lanes(near, HALO)], col.at[t]))
        copies.append((blk_in.at[:, :, :, lanes(near, HALO)], blk.at[t]))
    copies = [pltpu.make_async_copy(a, b, sem.at[n]) for n, (a, b) in enumerate(copies)]
    for c in copies:
        c.start()
    for c in copies[:2]:
        c.wait()
    pack_coarse(ccol, cblk, send)
    for c in copies[2:]:
        c.wait()
    table = jnp.concatenate([owner[...]] * 4, axis=1)
    found = picked(table, agg[...]).astype(f32)
    node_row[...] = found
    for t, (out, wide) in enumerate(((up, ROWS - WIDE), (down, 0))):
        for i in range(3):
            for j in range(3):
                g = 3 * i + j
                out[g * FULL : (g + 1) * FULL, :] = blk[t, i, j, 0:FULL, :]
                out[P_BTAIL + 3 * g : P_BTAIL + 3 * g + 3, :] = blk[t, i, j, FULL:SLOTS, :]
        out[P_COL : P_COL + FULL, :] = col[t, 0:FULL, :].astype(f32)
        out[P_CTAIL : P_CTAIL + 3, :] = col[t, FULL:SLOTS, :].astype(f32)
        for h in range(2):
            out[P_RHS + 3 * h : P_RHS + 3 * h + 3, :] = rhs[:, lanes(wide + HALO * h, HALO)]
            out[P_DIA + 3 * h : P_DIA + 3 * h + 3, :] = dia[:, lanes(wide + HALO * h, HALO)]
            for q in range(2):
                s = wide // LANES + 2 * h + q
                out[P_ROW + h : P_ROW + h + 1, lanes(LANES * q)] = found[s : s + 1, :]
        out[P_ROW + 2 : P_ALL, :] = jnp.zeros((P_ALL - P_ROW - 2, HALO), f32)


def pulled_block(columns, blocks, table, first_chunk):
    total = [None, None, None]
    for part in range(4):
        where = columns(part)
        chunk = lax.shift_right_arithmetic(where, 7)
        lane = lax.bitwise_and(where, 127)
        near = [jnp.zeros(where.shape, f32) for _ in range(3)]
        for c in range(5):
            here = chunk == c
            for j in range(3):
                row = table[j : j + 1, lanes(first_chunk * LANES + c * LANES)]
                near[j] = jnp.where(here, picked(row, lane), near[j])
        for i in range(3):
            s = blocks(i, 0, part) * near[0]
            s = s + blocks(i, 1, part) * near[1]
            s = s + blocks(i, 2, part) * near[2]
            if part < 3:
                total[i] = s if total[i] is None else total[i] + s
            else:
                total[i] = jnp.sum(total[i], axis=0, keepdims=True) + jnp.sum(
                    s, axis=0, keepdims=True
                )
    return total


def local_getters(col, blk, start, b):
    def columns(part):
        lo, hi = 8 * part, min(8 * part + 8, SLOTS)
        return col[lo:hi, lanes(b * LANES)] - start

    def blocks(i, j, part):
        lo, hi = 8 * part, min(8 * part + 8, SLOTS)
        return blk[i, j, lo:hi, lanes(b * LANES)]

    return columns, blocks


def halo_getters(halo, start, b):
    def columns(part):
        if part < 3:
            got = halo[P_COL + 8 * part : P_COL + 8 * part + 8, lanes(b * LANES)]
        else:
            got = halo[P_CTAIL : P_CTAIL + 3, lanes(b * LANES)]
        return got.astype(i32) - start

    def blocks(i, j, part):
        g = 3 * i + j
        if part < 3:
            return halo[g * FULL + 8 * part : g * FULL + 8 * part + 8, lanes(b * LANES)]
        return halo[P_BTAIL + 3 * g : P_BTAIL + 3 * g + 3, lanes(b * LANES)]

    return columns, blocks


def wide_vector(out, local, before, after, row):
    out[:, lanes(WIDE, ROWS)] = local[...]
    for h in range(2):
        out[:, lanes(HALO * h, HALO)] = before[row + 3 * h : row + 3 * h + 3, :]
        out[:, lanes(WIDE + ROWS + HALO * h, HALO)] = after[row + 3 * h : row + 3 * h + 3, :]


def smoothed(table, pulled, rhs, dia, at):
    pull = jnp.concatenate(pulled, axis=0)
    s = table[:, lanes(at)]
    b = rhs[:, lanes(at)]
    d = dia[:, lanes(at)]
    return s + damping * (b - (d * s - pull)) / d


def sweep_halo(out, table, rhs, dia, halo, base, first):
    for b in range(2):
        at = first + LANES * b
        start = base + (at - WIDE) - 2 * LANES
        cols, blks = halo_getters(halo, start, b)
        pull = pulled_block(cols, blks, table, at // LANES - 2)
        out[:, lanes(at)] = smoothed(table, pull, rhs, dia, at)


def each_block(step):
    def some(t, carry):
        for u in range(UNROLL):
            step(t * UNROLL + u)
        return carry

    lax.fori_loop(0, BLOCKS // UNROLL, some, 0)


def own_block(table, col, blk, base, b):
    start = base + b * LANES - 2 * LANES
    cols, blks = local_getters(col, blk, start, b)
    return pulled_block(cols, blks, table, b + WIDE // LANES - 2)


def pre_kernel(base_ref, rhs, dia, col, blk, agg, owner_row, cdia, before, after,
               send, first_iter, keep_rhs, keep_dia, up2, down2, one, two, res):
    base = base_ref[0]
    wide_vector(keep_rhs, rhs, before, after, P_RHS)
    wide_vector(keep_dia, dia, before, after, P_DIA)
    raw = keep_dia[...]
    keep_dia[...] = jnp.where(raw == 0.0, 1.0, raw)
    one[...] = damping * keep_rhs[...] / keep_dia[...]
    two[...] = jnp.zeros(two.shape, f32)
    sweep_halo(two, one, keep_rhs, keep_dia, before, base, WIDE - HALO)
    sweep_halo(two, one, keep_rhs, keep_dia, after, base, WIDE + ROWS)

    def second(b):
        at = WIDE + b * LANES
        pull = own_block(one, col, blk, base, b)
        two[:, lanes(at)] = smoothed(one, pull, keep_rhs, keep_dia, at)

    each_block(second)

    def third(b):
        at = WIDE + b * LANES
        pull = jnp.concatenate(own_block(two, col, blk, base, b), axis=0)
        s, d = two[:, lanes(at)], keep_dia[:, lanes(at)]
        res[0:3, lanes(b * LANES)] = keep_rhs[:, lanes(at)] - (d * s - pull)

    res[...] = jnp.zeros(res.shape, f32)
    each_block(third)
    first_iter[...] = two[...]
    up2[...] = two[:, lanes(WIDE + ROWS - WIDE, HALO)]
    down2[...] = two[:, lanes(WIDE + HALO, HALO)]
    label = lax.broadcasted_iota(i32, (32, LANES), 0)
    sums = None
    for b in range(BLOCKS):
        member = (label == jnp.broadcast_to(agg[b : b + 1, :], (32, LANES))).astype(f32)
        part = lax.dot_general(
            res[:, lanes(b * LANES)], member, (((1,), (1,)), ((), ())),
            precision=highest, preferred_element_type=f32,
        )
        sums = part if sums is None else sums + part
    row = jnp.concatenate(
        [sums[0:1], sums[1:2], sums[2:3], owner_row[...].astype(f32)], axis=1
    )
    send[:, 0, :] = jnp.broadcast_to(row, (LANES, LANES))
    row = jnp.concatenate(
        [cdia[0:1], cdia[1:2], cdia[2:3], jnp.ones((1, 32), f32)], axis=1
    )
    send[:, 1, :] = jnp.broadcast_to(row, (LANES, LANES))


def bit_of(p, at):
    return lax.bitwise_and(lax.shift_right_logical(p, at), 1)


def bit_parity(p, at):
    return lax.bitwise_xor(bit_of(p, at), bit_of(p, at + 1))


def lane_of_device(p, me):
    off = lax.bitwise_xor(p, me)
    rest = 4 * bit_of(p, 6) + 2 * bit_of(p, 4) + bit_of(p, 2)
    return (
        64 * bit_parity(off, 1) + 32 * bit_of(off, 0) + 16 * bit_parity(off, 5) + 8 * bit_parity(off, 3)
        + rest
    )


def device_of_lane(q, me):
    def last(relative, at, first):
        return lax.bitwise_xor(lax.bitwise_xor(relative, bit_parity(me, at)), first)

    x, z, y = bit_of(q, 0), bit_of(q, 1), bit_of(q, 2)
    p = 64 * y + 32 * last(bit_of(q, 4), 5, y) + 16 * z + 8 * last(bit_of(q, 3), 3, z)
    core = lax.bitwise_xor(bit_of(q, 5), bit_of(me, 0))
    return p + 4 * x + 2 * last(bit_of(q, 6), 1, x) + core


def row_groups():
    def member(kind, m):
        y, z, x = m >> 2, m >> 1 & 1, m & 1
        py, pz, px, core = kind >> 3, kind >> 2 & 1, kind >> 1 & 1, kind & 1
        return 64 * y + 32 * (y ^ py) + 16 * z + 8 * (z ^ pz) + 4 * x + 2 * (x ^ px) + core

    return [[member(kind, m) for m in range(NEAR)] for kind in range(16)]


def pack_coarse(col, blk, send):
    def turned(a):
        z = jnp.transpose(jnp.concatenate([a, jnp.zeros((32, 5), f32)], axis=1))
        return jnp.concatenate([z] * 4, axis=1)

    columns = turned(col[...].astype(f32))
    kind = lax.bitwise_and(columns.astype(i32), 7)
    tile = (8, LANES)
    sub = lax.broadcasted_iota(i32, tile, 0)
    count = jnp.zeros(tile, i32)
    match, earlier = [], []
    for k in range(SLOTS):
        here = sub == jnp.broadcast_to(kind[k : k + 1], tile)
        match.append(here)
        earlier.append(count)
        count = count + here.astype(i32)
    left = jnp.zeros((1, LANES), i32)
    start = []
    for n in range(16):
        if n >= 8:
            start.append(left)
        left = jnp.maximum(left + count[n % 8 : n % 8 + 1] - 4, 0)
    start = jnp.concatenate(start, axis=0) + 4 * sub
    place = 4 * sub + lax.shift_right_logical(lax.broadcasted_iota(i32, tile, 1), 5)
    slot = jnp.full(tile, 31, i32)
    for k in range(SLOTS):
        at = jnp.sum(jnp.where(match[k], start + earlier[k], 0), axis=0, keepdims=True)
        slot = jnp.where(place == jnp.broadcast_to(lax.bitwise_and(at, 31), tile), k, slot)
    inner, outer = lax.bitwise_and(slot, 7), lax.shift_right_logical(slot, 3)

    def placed(z):
        got = None
        for g in range(4):
            part = jnp.take_along_axis(
                z[8 * g : 8 * g + 8], inner, axis=0, mode="promise_in_bounds"
            )
            got = part if got is None else jnp.where(outer == g, part, got)
        return got

    parts = [placed(turned(blk[i, j])) for i in range(3) for j in range(3)]
    parts.append(jnp.where(slot == 31, sub.astype(f32), placed(columns)))
    for m in range(10):
        for d in range(NEAR):
            send[d, 8 * m : 8 * m + 8, :] = parts[m]


def spread(parts):
    group = lax.shift_right_logical(lax.broadcasted_iota(i32, parts[0].shape, 1), 5)
    return jnp.where(group == 0, parts[0], jnp.where(group == 1, parts[1], parts[2]))


def coarse_lookup(table, chunk, lane):
    near = [jnp.zeros(chunk.shape, f32) for _ in range(3)]
    for c in range(32):
        here = chunk == c
        for j in range(3):
            row = table[32 * j + c : 32 * j + c + 1, :]
            near[j] = jnp.where(here, picked(row, lane), near[j])
    return near


def coarse_step(table, where, passes, data, own, rhs, dia, gather):
    gather[...] = jnp.zeros(gather.shape, f32)

    def one_pass(t, carry):
        rows = [
            [pltpu.roll(table[32 * j + 8 * v : 32 * j + 8 * v + 8, :], t, axis=0) for v in range(4)]
            for j in range(3)
        ]
        for d in range(PEERS):
            w = where[d]
            code, lane = lax.bitwise_and(w, 31), lax.shift_right_logical(w, 5)
            near = [jnp.zeros((8, LANES), f32) for _ in range(3)]
            for v in range(4):
                here = code == 4 * t + v
                for j in range(3):
                    near[j] = jnp.where(here, picked(rows[j][v], lane), near[j])
            for i in range(3):
                a = data[d // NEAR][d % NEAR, lanes8(3 * i), :] * near[0]
                a = a + data[d // NEAR][d % NEAR, lanes8(3 * i + 1), :] * near[1]
                a = a + data[d // NEAR][d % NEAR, lanes8(3 * i + 2), :] * near[2]
                gather[i, d : d + 1, :] += jnp.sum(a, axis=0, keepdims=True)
        return carry

    lax.fori_loop(0, passes, one_pass, 0)
    parts = []
    for i in range(3):
        s = gather[i]
        s = s + pltpu.roll(s, 64, axis=1)
        parts.append(s + pltpu.roll(s, 32, axis=1))
    return own + damping * (rhs - (dia * own - spread(parts))) / dia


def lanes8(m):
    return slice(8 * m, 8 * m + 8)


def coarse_first_kernel(base_ref, sums, *rest):
    data = rest[:PARTS]
    new, rhs, dia, where, passes, table, gather, left, right = rest[PARTS:]
    me = lax.shift_right_logical(base_ref[0], 10)
    got = jnp.transpose(sums[:, 0, :])
    rows = got[96:128].astype(i32)
    s = got[0:96]
    split = []
    for _ in range(3):
        t = s.astype(jnp.bfloat16).astype(f32)
        split.append(t)
        s = s - t
    chunk = lax.broadcasted_iota(i32, (32, LANES), 0)
    place = lax.broadcasted_iota(i32, (LANES, LANES), 0)
    low = lax.bitwise_and(rows, 31)
    lane = lane_of_device(lax.shift_right_logical(rows, 5), me)
    for a in range(32):
        here = chunk == jnp.broadcast_to(low[a : a + 1], (32, LANES))
        for t in range(3):
            for i in range(3):
                value = jnp.broadcast_to(split[t][32 * i + a : 32 * i + a + 1], (32, LANES))
                left[96 * t + 32 * i : 96 * t + 32 * i + 32, lanes(LANES * a)] = jnp.where(
                    here, value, 0.0
                ).astype(jnp.bfloat16)
        right[:, lanes(LANES * a)] = jnp.where(
            place == jnp.broadcast_to(lane[a : a + 1], (LANES, LANES)), 1.0, 0.0
        ).astype(jnp.bfloat16)
    both = lax.dot_general(
        left[...], right[...], (((1,), (1,)), ((), ())), preferred_element_type=f32
    )
    crhs = both[0:96] + both[96:192] + both[192:288]
    order = device_of_lane(lax.broadcasted_iota(i32, (96, LANES), 1), me)
    cdia = jnp.take_along_axis(
        jnp.transpose(sums[:, 1, :])[0:96], order, axis=1, mode="promise_in_bounds"
    )
    pad = jnp.zeros((32, LANES), f32)
    first = jnp.concatenate([damping * crhs / cdia, pad], axis=0)
    table[...] = first
    own = jnp.transpose(first)[0:PEERS]
    rhs[...] = jnp.transpose(jnp.concatenate([crhs, pad], axis=0))[0:PEERS]
    dia[...] = jnp.transpose(jnp.concatenate([cdia, pad + 1.0], axis=0))[0:PEERS]
    sub = lax.broadcasted_iota(i32, (8, LANES), 0)
    most = jnp.zeros((8, LANES), i32)
    for d in range(PEERS):
        c = data[d // NEAR][d % NEAR, 72:80, :].astype(i32)
        off = lax.bitwise_and(sub - c, 7)
        most = jnp.maximum(most, off)
        at = lane_of_device(lax.shift_right_logical(c, 5), me)
        code = lax.bitwise_and(lax.shift_right_logical(c, 3), 3) + lax.shift_left(off, 2)
        where[d] = code + lax.shift_left(at, 5)
    most = jnp.max(most.astype(f32)).astype(i32) + 1
    passes[...] = jnp.broadcast_to(most, passes.shape)
    new[...] = coarse_step(
        table, where, most, data, own, rhs[...], dia[...], gather
    )


def gathered(table, pieces, mine):
    row = 0
    for piece in pieces:
        size = piece.shape[0]
        mine[row : row + size, :] = piece[...]
        row += size
    table[...] = jnp.transpose(mine[...])


def coarse_kernel(base_ref, passes, *rest):
    pieces, (rhs, dia, where) = rest[:PIECES], rest[PIECES : PIECES + 3]
    data = rest[PIECES + 3 : PIECES + 3 + PARTS]
    new, table, mine, gather = rest[PIECES + 3 + PARTS :]
    gathered(table, pieces, mine)
    new[...] = coarse_step(
        table, where, passes[...][0, 0], data, pieces[0][...], rhs[...], dia[...], gather
    )


def post_kernel(base_ref, *rest):
    pieces = rest[:PIECES]
    (first_iter, rhs, dia, col, blk, node_row, before, after, before2, after2,
     out, correction, table, mine, one, two) = rest[PIECES:]
    base = base_ref[0]
    me = lax.shift_right_logical(base, 10)
    gathered(table, pieces, mine)
    row = mine[pl.ds(lane_of_device(me, me), 1), :]
    correction[...] = jnp.concatenate([row[:, 32 * i : 32 * i + 32] for i in range(3)], axis=0)
    one[...] = first_iter[...]
    one[:, lanes(0, HALO)] = before2[...]
    one[:, lanes(WIDE + ROWS + HALO, HALO)] = after2[...]
    edge = [
        h[P_ROW + t : P_ROW + t + 1, lanes(LANES * q)]
        for h in (before, after) for t in range(2) for q in range(2)
    ]
    edge = jnp.concatenate(edge, axis=0)

    def found(rows):
        rows = rows.astype(i32)
        lane = lane_of_device(lax.shift_right_logical(rows, 5), me)
        return coarse_lookup(table, lax.bitwise_and(rows, 31), lane)

    own, far = found(node_row[...]), found(edge)
    for s in range(16):
        if s < 4:
            row = [f[s : s + 1, :] for f in far]
        elif s < 12:
            row = [f[s - 4 : s - 3, :] for f in own]
        else:
            row = [f[s - 8 : s - 7, :] for f in far]
        one[:, lanes(s * LANES)] = one[:, lanes(s * LANES)] + jnp.concatenate(row, axis=0)
    two[...] = jnp.zeros(two.shape, f32)
    sweep_halo(two, one, rhs, dia, before, base, WIDE - HALO)
    sweep_halo(two, one, rhs, dia, after, base, WIDE + ROWS)

    def first(b):
        at = WIDE + b * LANES
        pull = own_block(one, col, blk, base, b)
        two[:, lanes(at)] = smoothed(one, pull, rhs, dia, at)

    def second(b):
        at = WIDE + b * LANES
        pull = own_block(two, col, blk, base, b)
        out[:, lanes(b * LANES)] = smoothed(two, pull, rhs, dia, at)

    each_block(first)
    each_block(second)


def call(kernel, outs, args, scratch=(), scalars=0, limit=12):
    vmem = pl.BlockSpec(memory_space=pltpu.VMEM)
    smem = pl.BlockSpec(memory_space=pltpu.SMEM)
    return pl.pallas_call(
        kernel,
        in_specs=[smem] * scalars + [vmem] * (len(args) - scalars),
        out_specs=[vmem] * len(outs),
        out_shape=[jax.ShapeDtypeStruct(o, t) for o, t in outs],
        scratch_shapes=[
            pltpu.VMEM(*s) if isinstance(s[0], tuple) else pltpu.VMEM(s, f32) for s in scratch
        ],
        compiler_params=pltpu.CompilerParams(vmem_limit_bytes=limit * 2**20),
    )(*args)


def partner(value, bits):
    return lax.ppermute(value, DOM, [(i, i ^ bits) for i in range(lax.axis_size(DOM))])


def in_group(new):
    p2, p3, p1 = partner(new, 2), partner(new, 3), partner(new, 1)
    return new, p1, p2, p3


def shifts(up, down):
    count = lax.axis_size(DOM)
    forward = [(i, i + 1) for i in range(count - 1)]
    backward = [(i + 1, i) for i in range(count - 1)]
    return lax.ppermute(up, DOM, forward), lax.ppermute(down, DOM, backward)


def cycle(right_side, fine_diagonal, fine_columns, fine_blocks, aggregate_of_node,
         coarse_row_of_aggregate, coarse_diagonal, coarse_columns, coarse_blocks):
    rhs, dia = right_side.T, fine_diagonal.T
    col, blk = fine_columns.T, fine_blocks.transpose(2, 3, 1, 0)
    agg = aggregate_of_node.reshape(8, LANES)
    owner = coarse_row_of_aggregate.reshape(1, 32)
    cdia, cblk = coarse_diagonal.T, coarse_blocks.transpose(2, 3, 0, 1)
    me = lax.axis_index(DOM).astype(i32).reshape(1)
    base = me * ROWS
    wide = WIDE + ROWS + WIDE

    vmem, far = pl.BlockSpec(memory_space=pltpu.VMEM), pl.BlockSpec(memory_space=pltpu.HBM)
    up, down, node_row, dsend = pl.pallas_call(
        pack_kernel,
        name="pack",
        in_specs=[far] * 8,
        out_specs=[vmem] * 4,
        out_shape=[jax.ShapeDtypeStruct(o, f32)
            for o in ((P_ALL, HALO), (P_ALL, HALO), (8, LANES), (NEAR, 80, LANES))],
        scratch_shapes=[
            pltpu.VMEM((3, ROWS), f32), pltpu.VMEM((3, ROWS), f32),
            pltpu.VMEM((2, SLOTS, HALO), i32), pltpu.VMEM((2, 3, 3, SLOTS, HALO), f32),
            pltpu.VMEM((8, LANES), i32), pltpu.VMEM((1, 32), i32),
            pltpu.VMEM((32, SLOTS), i32), pltpu.VMEM((3, 3, 32, SLOTS), f32),
            pltpu.SemaphoreType.DMA((10,)),
        ],
        compiler_params=pltpu.CompilerParams(vmem_limit_bytes=60 * 2**20),
    )(rhs, dia, col, blk, agg, owner, coarse_columns, cblk)
    data = lax.all_to_all(
        dsend, DOM, 0, 0, axis_index_groups=row_groups(), tiled=True
    )
    data = (data, partner(data, 8), partner(data, 32), partner(data, 40))
    vmem, far = pl.BlockSpec(memory_space=pltpu.VMEM), pl.BlockSpec(memory_space=pltpu.HBM)
    up, down, node_row, dsend = pl.pallas_call(
        pack_kernel,
        name="pack",
        in_specs=[far] * 8,
        out_specs=[vmem] * 4,
        out_shape=[jax.ShapeDtypeStruct(o, f32)
            for o in ((P_ALL, HALO), (P_ALL, HALO), (8, LANES), (NEAR, 80, LANES))],
        scratch_shapes=[
            pltpu.VMEM((3, ROWS), f32), pltpu.VMEM((3, ROWS), f32),
            pltpu.VMEM((2, SLOTS, HALO), i32), pltpu.VMEM((2, 3, 3, SLOTS, HALO), f32),
            pltpu.VMEM((8, LANES), i32), pltpu.VMEM((1, 32), i32),
            pltpu.VMEM((32, SLOTS), i32), pltpu.VMEM((3, 3, 32, SLOTS), f32),
            pltpu.SemaphoreType.DMA((10,)),
        ],
        compiler_params=pltpu.CompilerParams(vmem_limit_bytes=60 * 2**20),
    )(rhs, dia, col, blk, agg, owner, coarse_columns, cblk)
    data = lax.all_to_all(
        dsend, DOM, 0, 0, axis_index_groups=row_groups(), tiled=True
    )
    along_z, along_y = partner(data, 8), partner(data, 32)
    data = (data, along_z, along_y, partner(along_z, 32))
    before, after = shifts(up, down)
    send, first_iter, wrhs, wdia, up2, down2 = call(
        pre_kernel,
        [((LANES, 2, LANES), f32), ((3, wide), f32), ((3, wide), f32), ((3, wide), f32),
         ((3, HALO), f32), ((3, HALO), f32)],
        [base, rhs, dia, col, blk, agg, owner, cdia, before, after],
        scratch=[(3, wide), (3, wide), (8, ROWS)], scalars=1, limit=4,
    )
    before2, after2 = shifts(up2, down2)
    sums = lax.all_to_all(send, DOM, 0, 0, tiled=True)
    peers = ((PEERS, LANES), f32)
    gather = (3, PEERS, LANES)
    square = (LANES, LANES)
    new, crhs, cd, where, passes = call(
        coarse_first_kernel,
        [peers, peers, peers, ((PEERS, 8, LANES), i32), ((8, LANES), i32)],
        [base, sums, *data],
        scratch=[square, gather, ((288, 4096), jnp.bfloat16), ((LANES, 4096), jnp.bfloat16)],
        scalars=1,
    )
    for _ in range(CSWEEPS - 2):
        new, = call(
            coarse_kernel, [peers],
            [base, passes, *in_group(new), crhs, cd, where, *data],
            scratch=[square, square, gather], scalars=1,
        )
    solution, mine = call(
        post_kernel, [((3, ROWS), f32), ((3, 32), f32)],
        [base, *in_group(new), first_iter, wrhs, wdia, col, blk, node_row,
         before, after, before2, after2],
        scratch=[square, square, (3, wide), (3, wide)], scalars=1,
    )
    return solution.T, mine.T


def solution(mesh):
    return jax.shard_map(
        cycle,
        mesh=mesh,
        in_specs=(
            P(DOM, None),
            P(DOM, None),
            P(DOM, None),
            P(DOM, None, None, None),
            P(DOM),
            P(DOM),
            P(DOM, None),
            P(DOM, None),
            P(DOM, None, None, None),
        ),
        out_specs=(P(DOM, None), P(DOM, None)),
        check_vma=False,
    )
```

```python
import jax
import jax.numpy as jnp
from jax import lax
from jax.experimental import pallas as pl
from jax.experimental.pallas import tpu as pltpu
from jax.sharding import PartitionSpec as P


DOM = "dom"
PEERS = 32
NEAR = 8
PARTS = PEERS // NEAR
PIECES = 128 // PEERS
UNROLL = 8
CSWEEPS = 6
damping = 0.7
highest = lax.Precision.HIGHEST

ROWS = 1024
LANES = 128
SLOTS = 27
FULL = 24
HALO = 256
WIDE = 512
BLOCKS = ROWS // LANES
P_COL = 9 * FULL
P_BTAIL = P_COL + FULL
P_CTAIL = P_BTAIL + 27
P_RHS = P_CTAIL + 3
P_DIA = P_RHS + 6
P_ROW = P_DIA + 6
P_ALL = 288
f32 = jnp.float32
i32 = jnp.int32


def lanes(start, size=LANES):
    if isinstance(start, int):
        return slice(start, start + size)
    return pl.ds(pl.multiple_of(start, LANES), size)


def picked(row, where):
    return jnp.take_along_axis(
        jnp.broadcast_to(row, where.shape), where, axis=1, mode="promise_in_bounds"
    )


def pack_kernel(rhs_in, dia_in, col_in, blk_in, agg_in, owner_in, ccol_in, cblk_in,
                up, down, node_row, send, rhs, dia, col, blk, agg, owner, ccol, cblk, sem):
    copies = [(ccol_in, ccol), (cblk_in, cblk)]
    copies += [(rhs_in, rhs), (dia_in, dia), (agg_in, agg), (owner_in, owner)]
    for t, near in enumerate((ROWS - HALO, 0)):
        copies.append((col_in.at[:, lanes(near, HALO)], col.at[t]))
        copies.append((blk_in.at[:, :, :, lanes(near, HALO)], blk.at[t]))
    copies = [pltpu.make_async_copy(a, b, sem.at[n]) for n, (a, b) in enumerate(copies)]
    for c in copies:
        c.start()
    for c in copies[:2]:
        c.wait()
    pack_coarse(ccol, cblk, send)
    for c in copies[2:]:
        c.wait()
    table = jnp.concatenate([owner[...]] * 4, axis=1)
    found = picked(table, agg[...]).astype(f32)
    node_row[...] = found
    for t, (out, wide) in enumerate(((up, ROWS - WIDE), (down, 0))):
        for i in range(3):
            for j in range(3):
                g = 3 * i + j
                out[g * FULL : (g + 1) * FULL, :] = blk[t, i, j, 0:FULL, :]
                out[P_BTAIL + 3 * g : P_BTAIL + 3 * g + 3, :] = blk[t, i, j, FULL:SLOTS, :]
        out[P_COL : P_COL + FULL, :] = col[t, 0:FULL, :].astype(f32)
        out[P_CTAIL : P_CTAIL + 3, :] = col[t, FULL:SLOTS, :].astype(f32)
        for h in range(2):
            out[P_RHS + 3 * h : P_RHS + 3 * h + 3, :] = rhs[:, lanes(wide + HALO * h, HALO)]
            out[P_DIA + 3 * h : P_DIA + 3 * h + 3, :] = dia[:, lanes(wide + HALO * h, HALO)]
            for q in range(2):
                s = wide // LANES + 2 * h + q
                out[P_ROW + h : P_ROW + h + 1, lanes(LANES * q)] = found[s : s + 1, :]
        out[P_ROW + 2 : P_ALL, :] = jnp.zeros((P_ALL - P_ROW - 2, HALO), f32)


def pulled_block(columns, blocks, table, first_chunk):
    total = [None, None, None]
    for part in range(4):
        where = columns(part)
        chunk = lax.shift_right_arithmetic(where, 7)
        lane = lax.bitwise_and(where, 127)
        near = [jnp.zeros(where.shape, f32) for _ in range(3)]
        for c in range(5):
            here = chunk == c
            for j in range(3):
                row = table[j : j + 1, lanes(first_chunk * LANES + c * LANES)]
                near[j] = jnp.where(here, picked(row, lane), near[j])
        for i in range(3):
            s = blocks(i, 0, part) * near[0]
            s = s + blocks(i, 1, part) * near[1]
            s = s + blocks(i, 2, part) * near[2]
            if part < 3:
                total[i] = s if total[i] is None else total[i] + s
            else:
                total[i] = jnp.sum(total[i], axis=0, keepdims=True) + jnp.sum(
                    s, axis=0, keepdims=True
                )
    return total


def local_getters(col, blk, start, b):
    def columns(part):
        lo, hi = 8 * part, min(8 * part + 8, SLOTS)
        return col[lo:hi, lanes(b * LANES)] - start

    def blocks(i, j, part):
        lo, hi = 8 * part, min(8 * part + 8, SLOTS)
        return blk[i, j, lo:hi, lanes(b * LANES)]

    return columns, blocks


def halo_getters(halo, start, b):
    def columns(part):
        if part < 3:
            got = halo[P_COL + 8 * part : P_COL + 8 * part + 8, lanes(b * LANES)]
        else:
            got = halo[P_CTAIL : P_CTAIL + 3, lanes(b * LANES)]
        return got.astype(i32) - start

    def blocks(i, j, part):
        g = 3 * i + j
        if part < 3:
            return halo[g * FULL + 8 * part : g * FULL + 8 * part + 8, lanes(b * LANES)]
        return halo[P_BTAIL + 3 * g : P_BTAIL + 3 * g + 3, lanes(b * LANES)]

    return columns, blocks


def wide_vector(out, local, before, after, row):
    out[:, lanes(WIDE, ROWS)] = local[...]
    for h in range(2):
        out[:, lanes(HALO * h, HALO)] = before[row + 3 * h : row + 3 * h + 3, :]
        out[:, lanes(WIDE + ROWS + HALO * h, HALO)] = after[row + 3 * h : row + 3 * h + 3, :]


def smoothed(table, pulled, rhs, dia, at):
    pull = jnp.concatenate(pulled, axis=0)
    s = table[:, lanes(at)]
    b = rhs[:, lanes(at)]
    d = dia[:, lanes(at)]
    return s + damping * (b - (d * s - pull)) / d


def sweep_halo(out, table, rhs, dia, halo, base, first):
    for b in range(2):
        at = first + LANES * b
        start = base + (at - WIDE) - 2 * LANES
        cols, blks = halo_getters(halo, start, b)
        pull = pulled_block(cols, blks, table, at // LANES - 2)
        out[:, lanes(at)] = smoothed(table, pull, rhs, dia, at)


def each_block(step):
    def some(t, carry):
        for u in range(UNROLL):
            step(t * UNROLL + u)
        return carry

    lax.fori_loop(0, BLOCKS // UNROLL, some, 0)


def own_block(table, col, blk, base, b):
    start = base + b * LANES - 2 * LANES
    cols, blks = local_getters(col, blk, start, b)
    return pulled_block(cols, blks, table, b + WIDE // LANES - 2)


def pre_kernel(base_ref, rhs, dia, col, blk, agg, owner_row, cdia, before, after,
               send, first_iter, keep_rhs, keep_dia, up2, down2, one, two, res):
    base = base_ref[0]
    wide_vector(keep_rhs, rhs, before, after, P_RHS)
    wide_vector(keep_dia, dia, before, after, P_DIA)
    raw = keep_dia[...]
    keep_dia[...] = jnp.where(raw == 0.0, 1.0, raw)
    one[...] = damping * keep_rhs[...] / keep_dia[...]
    two[...] = jnp.zeros(two.shape, f32)
    sweep_halo(two, one, keep_rhs, keep_dia, before, base, WIDE - HALO)
    sweep_halo(two, one, keep_rhs, keep_dia, after, base, WIDE + ROWS)

    def second(b):
        at = WIDE + b * LANES
        pull = own_block(one, col, blk, base, b)
        two[:, lanes(at)] = smoothed(one, pull, keep_rhs, keep_dia, at)

    each_block(second)

    def third(b):
        at = WIDE + b * LANES
        pull = jnp.concatenate(own_block(two, col, blk, base, b), axis=0)
        s, d = two[:, lanes(at)], keep_dia[:, lanes(at)]
        res[0:3, lanes(b * LANES)] = keep_rhs[:, lanes(at)] - (d * s - pull)

    res[...] = jnp.zeros(res.shape, f32)
    each_block(third)
    first_iter[...] = two[...]
    up2[...] = two[:, lanes(WIDE + ROWS - WIDE, HALO)]
    down2[...] = two[:, lanes(WIDE + HALO, HALO)]
    label = lax.broadcasted_iota(i32, (32, LANES), 0)
    sums = None
    for b in range(BLOCKS):
        member = (label == jnp.broadcast_to(agg[b : b + 1, :], (32, LANES))).astype(f32)
        part = lax.dot_general(
            res[:, lanes(b * LANES)], member, (((1,), (1,)), ((), ())),
            precision=highest, preferred_element_type=f32,
        )
        sums = part if sums is None else sums + part
    row = jnp.concatenate(
        [sums[0:1], sums[1:2], sums[2:3], owner_row[...].astype(f32)], axis=1
    )
    send[:, 0, :] = jnp.broadcast_to(row, (LANES, LANES))
    row = jnp.concatenate(
        [cdia[0:1], cdia[1:2], cdia[2:3], jnp.ones((1, 32), f32)], axis=1
    )
    send[:, 1, :] = jnp.broadcast_to(row, (LANES, LANES))


def bit_of(p, at):
    return lax.bitwise_and(lax.shift_right_logical(p, at), 1)


def bit_parity(p, at):
    return lax.bitwise_xor(bit_of(p, at), bit_of(p, at + 1))


def lane_of_device(p, me):
    off = lax.bitwise_xor(p, me)
    rest = 4 * bit_of(p, 6) + 2 * bit_of(p, 4) + bit_of(p, 2)
    return (
        64 * bit_parity(off, 1) + 32 * bit_of(off, 0) + 16 * bit_parity(off, 5) + 8 * bit_parity(off, 3)
        + rest
    )


def device_of_lane(q, me):
    def last(relative, at, first):
        return lax.bitwise_xor(lax.bitwise_xor(relative, bit_parity(me, at)), first)

    x, z, y = bit_of(q, 0), bit_of(q, 1), bit_of(q, 2)
    p = 64 * y + 32 * last(bit_of(q, 4), 5, y) + 16 * z + 8 * last(bit_of(q, 3), 3, z)
    core = lax.bitwise_xor(bit_of(q, 5), bit_of(me, 0))
    return p + 4 * x + 2 * last(bit_of(q, 6), 1, x) + core


def row_groups():
    def member(kind, m):
        y, z, x = m >> 2, m >> 1 & 1, m & 1
        py, pz, px, core = kind >> 3, kind >> 2 & 1, kind >> 1 & 1, kind & 1
        return 64 * y + 32 * (y ^ py) + 16 * z + 8 * (z ^ pz) + 4 * x + 2 * (x ^ px) + core

    return [[member(kind, m) for m in range(NEAR)] for kind in range(16)]


def pack_coarse(col, blk, send):
    def turned(a):
        z = jnp.transpose(jnp.concatenate([a, jnp.zeros((32, 5), f32)], axis=1))
        return jnp.concatenate([z] * 4, axis=1)

    columns = turned(col[...].astype(f32))
    kind = lax.bitwise_and(columns.astype(i32), 7)
    tile = (8, LANES)
    sub = lax.broadcasted_iota(i32, tile, 0)
    count = jnp.zeros(tile, i32)
    match, earlier = [], []
    for k in range(SLOTS):
        here = sub == jnp.broadcast_to(kind[k : k + 1], tile)
        match.append(here)
        earlier.append(count)
        count = count + here.astype(i32)
    left = jnp.zeros((1, LANES), i32)
    start = []
    for n in range(16):
        if n >= 8:
            start.append(left)
        left = jnp.maximum(left + count[n % 8 : n % 8 + 1] - 4, 0)
    start = jnp.concatenate(start, axis=0) + 4 * sub
    place = 4 * sub + lax.shift_right_logical(lax.broadcasted_iota(i32, tile, 1), 5)
    slot = jnp.full(tile, 31, i32)
    for k in range(SLOTS):
        at = jnp.sum(jnp.where(match[k], start + earlier[k], 0), axis=0, keepdims=True)
        slot = jnp.where(place == jnp.broadcast_to(lax.bitwise_and(at, 31), tile), k, slot)
    inner, outer = lax.bitwise_and(slot, 7), lax.shift_right_logical(slot, 3)

    def placed(z):
        got = None
        for g in range(4):
            part = jnp.take_along_axis(
                z[8 * g : 8 * g + 8], inner, axis=0, mode="promise_in_bounds"
            )
            got = part if got is None else jnp.where(outer == g, part, got)
        return got

    parts = [placed(turned(blk[i, j])) for i in range(3) for j in range(3)]
    parts.append(jnp.where(slot == 31, sub.astype(f32), placed(columns)))
    for m in range(10):
        for d in range(NEAR):
            send[d, 8 * m : 8 * m + 8, :] = parts[m]


def spread(parts):
    group = lax.shift_right_logical(lax.broadcasted_iota(i32, parts[0].shape, 1), 5)
    return jnp.where(group == 0, parts[0], jnp.where(group == 1, parts[1], parts[2]))


def coarse_lookup(table, chunk, lane):
    near = [jnp.zeros(chunk.shape, f32) for _ in range(3)]
    for c in range(32):
        here = chunk == c
        for j in range(3):
            row = table[32 * j + c : 32 * j + c + 1, :]
            near[j] = jnp.where(here, picked(row, lane), near[j])
    return near


def coarse_step(table, where, passes, data, own, rhs, dia, gather):
    gather[...] = jnp.zeros(gather.shape, f32)

    def one_pass(t, carry):
        rows = [
            [pltpu.roll(table[32 * j + 8 * v : 32 * j + 8 * v + 8, :], t, axis=0) for v in range(4)]
            for j in range(3)
        ]
        for d in range(PEERS):
            w = where[d]
            code, lane = lax.bitwise_and(w, 31), lax.shift_right_logical(w, 5)
            near = [jnp.zeros((8, LANES), f32) for _ in range(3)]
            for v in range(4):
                here = code == 4 * t + v
                for j in range(3):
                    near[j] = jnp.where(here, picked(rows[j][v], lane), near[j])
            for i in range(3):
                a = data[d // NEAR][d % NEAR, lanes8(3 * i), :] * near[0]
                a = a + data[d // NEAR][d % NEAR, lanes8(3 * i + 1), :] * near[1]
                a = a + data[d // NEAR][d % NEAR, lanes8(3 * i + 2), :] * near[2]
                gather[i, d] += a
        return carry

    lax.fori_loop(0, passes, one_pass, 0)
    parts = []
    for i in range(3):
        s = jnp.sum(gather[i], axis=1)
        s = s + pltpu.roll(s, 64, axis=1)
        parts.append(s + pltpu.roll(s, 32, axis=1))
    return own + damping * (rhs - (dia * own - spread(parts))) / dia


def lanes8(m):
    return slice(8 * m, 8 * m + 8)


def coarse_first_kernel(base_ref, sums, *rest):
    data = rest[:PARTS]
    new, rhs, dia, where, passes, table, gather, left, right = rest[PARTS:]
    me = lax.shift_right_logical(base_ref[0], 10)
    got = jnp.transpose(sums[:, 0, :])
    rows = got[96:128].astype(i32)
    s = got[0:96]
    split = []
    for _ in range(3):
        t = s.astype(jnp.bfloat16).astype(f32)
        split.append(t)
        s = s - t
    chunk = lax.broadcasted_iota(i32, (32, LANES), 0)
    place = lax.broadcasted_iota(i32, (LANES, LANES), 0)
    low = lax.bitwise_and(rows, 31)
    lane = lane_of_device(lax.shift_right_logical(rows, 5), me)
    for a in range(32):
        here = chunk == jnp.broadcast_to(low[a : a + 1], (32, LANES))
        for t in range(3):
            for i in range(3):
                value = jnp.broadcast_to(split[t][32 * i + a : 32 * i + a + 1], (32, LANES))
                left[96 * t + 32 * i : 96 * t + 32 * i + 32, lanes(LANES * a)] = jnp.where(
                    here, value, 0.0
                ).astype(jnp.bfloat16)
        right[:, lanes(LANES * a)] = jnp.where(
            place == jnp.broadcast_to(lane[a : a + 1], (LANES, LANES)), 1.0, 0.0
        ).astype(jnp.bfloat16)
    both = lax.dot_general(
        left[...], right[...], (((1,), (1,)), ((), ())), preferred_element_type=f32
    )
    crhs = both[0:96] + both[96:192] + both[192:288]
    order = device_of_lane(lax.broadcasted_iota(i32, (96, LANES), 1), me)
    cdia = jnp.take_along_axis(
        jnp.transpose(sums[:, 1, :])[0:96], order, axis=1, mode="promise_in_bounds"
    )
    pad = jnp.zeros((32, LANES), f32)
    first = jnp.concatenate([damping * crhs / cdia, pad], axis=0)
    table[...] = first
    own = jnp.transpose(first)[0:PEERS]
    rhs[...] = jnp.transpose(jnp.concatenate([crhs, pad], axis=0))[0:PEERS]
    dia[...] = jnp.transpose(jnp.concatenate([cdia, pad + 1.0], axis=0))[0:PEERS]
    sub = lax.broadcasted_iota(i32, (8, LANES), 0)
    most = jnp.zeros((8, LANES), i32)
    for d in range(PEERS):
        c = data[d // NEAR][d % NEAR, 72:80, :].astype(i32)
        off = lax.bitwise_and(sub - c, 7)
        most = jnp.maximum(most, off)
        at = lane_of_device(lax.shift_right_logical(c, 5), me)
        code = lax.bitwise_and(lax.shift_right_logical(c, 3), 3) + lax.shift_left(off, 2)
        where[d] = code + lax.shift_left(at, 5)
    most = jnp.max(most.astype(f32)).astype(i32) + 1
    passes[...] = jnp.broadcast_to(most, passes.shape)
    new[...] = coarse_step(
        table, where, most, data, own, rhs[...], dia[...], gather
    )


def gathered(table, pieces, mine):
    row = 0
    for piece in pieces:
        size = piece.shape[0]
        mine[row : row + size, :] = piece[...]
        row += size
    table[...] = jnp.transpose(mine[...])


def coarse_kernel(base_ref, passes, *rest):
    pieces, (rhs, dia, where) = rest[:PIECES], rest[PIECES : PIECES + 3]
    data = rest[PIECES + 3 : PIECES + 3 + PARTS]
    new, table, mine, gather = rest[PIECES + 3 + PARTS :]
    gathered(table, pieces, mine)
    new[...] = coarse_step(
        table, where, passes[...][0, 0], data, pieces[0][...], rhs[...], dia[...], gather
    )


def post_kernel(base_ref, *rest):
    pieces = rest[:PIECES]
    (first_iter, rhs, dia, col, blk, node_row, before, after, before2, after2,
     out, correction, table, mine, one, two) = rest[PIECES:]
    base = base_ref[0]
    me = lax.shift_right_logical(base, 10)
    gathered(table, pieces, mine)
    row = mine[pl.ds(lane_of_device(me, me), 1), :]
    correction[...] = jnp.concatenate([row[:, 32 * i : 32 * i + 32] for i in range(3)], axis=0)
    one[...] = first_iter[...]
    one[:, lanes(0, HALO)] = before2[...]
    one[:, lanes(WIDE + ROWS + HALO, HALO)] = after2[...]
    edge = [
        h[P_ROW + t : P_ROW + t + 1, lanes(LANES * q)]
        for h in (before, after) for t in range(2) for q in range(2)
    ]
    edge = jnp.concatenate(edge, axis=0)

    def found(rows):
        rows = rows.astype(i32)
        lane = lane_of_device(lax.shift_right_logical(rows, 5), me)
        return coarse_lookup(table, lax.bitwise_and(rows, 31), lane)

    own, far = found(node_row[...]), found(edge)
    for s in range(16):
        if s < 4:
            row = [f[s : s + 1, :] for f in far]
        elif s < 12:
            row = [f[s - 4 : s - 3, :] for f in own]
        else:
            row = [f[s - 8 : s - 7, :] for f in far]
        one[:, lanes(s * LANES)] = one[:, lanes(s * LANES)] + jnp.concatenate(row, axis=0)
    two[...] = jnp.zeros(two.shape, f32)
    sweep_halo(two, one, rhs, dia, before, base, WIDE - HALO)
    sweep_halo(two, one, rhs, dia, after, base, WIDE + ROWS)

    def first(b):
        at = WIDE + b * LANES
        pull = own_block(one, col, blk, base, b)
        two[:, lanes(at)] = smoothed(one, pull, rhs, dia, at)

    def second(b):
        at = WIDE + b * LANES
        pull = own_block(two, col, blk, base, b)
        out[:, lanes(b * LANES)] = smoothed(two, pull, rhs, dia, at)

    each_block(first)
    each_block(second)


def call(kernel, outs, args, scratch=(), scalars=0, limit=12):
    vmem = pl.BlockSpec(memory_space=pltpu.VMEM)
    smem = pl.BlockSpec(memory_space=pltpu.SMEM)
    return pl.pallas_call(
        kernel,
        in_specs=[smem] * scalars + [vmem] * (len(args) - scalars),
        out_specs=[vmem] * len(outs),
        out_shape=[jax.ShapeDtypeStruct(o, t) for o, t in outs],
        scratch_shapes=[
            pltpu.VMEM(*s) if isinstance(s[0], tuple) else pltpu.VMEM(s, f32) for s in scratch
        ],
        compiler_params=pltpu.CompilerParams(vmem_limit_bytes=limit * 2**20),
    )(*args)


def partner(value, bits):
    return lax.ppermute(value, DOM, [(i, i ^ bits) for i in range(lax.axis_size(DOM))])


def in_group(new):
    p2, p3, p1 = partner(new, 2), partner(new, 3), partner(new, 1)
    return new, p1, p2, p3


def shifts(up, down):
    count = lax.axis_size(DOM)
    forward = [(i, i + 1) for i in range(count - 1)]
    backward = [(i + 1, i) for i in range(count - 1)]
    return lax.ppermute(up, DOM, forward), lax.ppermute(down, DOM, backward)


def cycle(right_side, fine_diagonal, fine_columns, fine_blocks, aggregate_of_node,
         coarse_row_of_aggregate, coarse_diagonal, coarse_columns, coarse_blocks):
    rhs, dia = right_side.T, fine_diagonal.T
    col, blk = fine_columns.T, fine_blocks.transpose(2, 3, 1, 0)
    agg = aggregate_of_node.reshape(8, LANES)
    owner = coarse_row_of_aggregate.reshape(1, 32)
    cdia, cblk = coarse_diagonal.T, coarse_blocks.transpose(2, 3, 0, 1)
    me = lax.axis_index(DOM).astype(i32).reshape(1)
    base = me * ROWS
    wide = WIDE + ROWS + WIDE

    vmem, far = pl.BlockSpec(memory_space=pltpu.VMEM), pl.BlockSpec(memory_space=pltpu.HBM)
    up, down, node_row, dsend = pl.pallas_call(
        pack_kernel,
        name="pack",
        in_specs=[far] * 8,
        out_specs=[vmem] * 4,
        out_shape=[jax.ShapeDtypeStruct(o, f32)
            for o in ((P_ALL, HALO), (P_ALL, HALO), (8, LANES), (NEAR, 80, LANES))],
        scratch_shapes=[
            pltpu.VMEM((3, ROWS), f32), pltpu.VMEM((3, ROWS), f32),
            pltpu.VMEM((2, SLOTS, HALO), i32), pltpu.VMEM((2, 3, 3, SLOTS, HALO), f32),
            pltpu.VMEM((8, LANES), i32), pltpu.VMEM((1, 32), i32),
            pltpu.VMEM((32, SLOTS), i32), pltpu.VMEM((3, 3, 32, SLOTS), f32),
            pltpu.SemaphoreType.DMA((10,)),
        ],
        compiler_params=pltpu.CompilerParams(vmem_limit_bytes=60 * 2**20),
    )(rhs, dia, col, blk, agg, owner, coarse_columns, cblk)
    data = lax.all_to_all(
        dsend, DOM, 0, 0, axis_index_groups=row_groups(), tiled=True
    )
    along_z, along_y = partner(data, 8), partner(data, 32)
    data = (data, along_z, along_y, partner(along_z, 32))
    before, after = shifts(up, down)
    send, first_iter, wrhs, wdia, up2, down2 = call(
        pre_kernel,
        [((LANES, 2, LANES), f32), ((3, wide), f32), ((3, wide), f32), ((3, wide), f32),
         ((3, HALO), f32), ((3, HALO), f32)],
        [base, rhs, dia, col, blk, agg, owner, cdia, before, after],
        scratch=[(3, wide), (3, wide), (8, ROWS)], scalars=1, limit=4,
    )
    before2, after2 = shifts(up2, down2)
    sums = lax.all_to_all(send, DOM, 0, 0, tiled=True)
    peers = ((PEERS, LANES), f32)
    gather = (3, PEERS, 8, LANES)
    square = (LANES, LANES)
    new, crhs, cd, where, passes = call(
        coarse_first_kernel,
        [peers, peers, peers, ((PEERS, 8, LANES), i32), ((8, LANES), i32)],
        [base, sums, *data],
        scratch=[square, gather, ((288, 4096), jnp.bfloat16), ((LANES, 4096), jnp.bfloat16)],
        scalars=1,
    )
    for _ in range(CSWEEPS - 2):
        new, = call(
            coarse_kernel, [peers],
            [base, passes, *in_group(new), crhs, cd, where, *data],
            scratch=[square, square, gather], scalars=1,
        )
    solution, mine = call(
        post_kernel, [((3, ROWS), f32), ((3, 32), f32)],
        [base, *in_group(new), first_iter, wrhs, wdia, col, blk, node_row,
         before, after, before2, after2],
        scratch=[square, square, (3, wide), (3, wide)], scalars=1,
    )
    return solution.T, mine.T


def solution(mesh):
    return jax.shard_map(
        cycle,
        mesh=mesh,
        in_specs=(
            P(DOM, None),
            P(DOM, None),
            P(DOM, None),
            P(DOM, None, None, None),
            P(DOM),
            P(DOM),
            P(DOM, None),
            P(DOM, None),
            P(DOM, None, None, None),
        ),
        out_specs=(P(DOM, None), P(DOM, None)),
        check_vma=False,
    )
```
